8 devices in a mesh: data: 1 (over z), inner: 2 (over y), stage: 4 (over x, core).
Axes of the slice: x: 2, y: 2, z: 1, core: 2. Of those that a mesh axis runs over, the one named last changes fastest.
Arguments:
- x_tokens: bfloat16 [16, 32, 2048], P(('data', 'stage', 'inner'))
- g_cotan: bfloat16 [16, 32, 2048], P(('data', 'stage', 'inner'))
- w_up: bfloat16 [1, 4, 2048, 8192], P(None, ('data', 'stage'), None, 'inner')
- w_down: bfloat16 [1, 4, 8192, 2048], P(None, ('data', 'stage'), 'inner')
Outputs:
- output 1: bfloat16 [16, 32, 2048], P(('data', 'stage', 'inner'))
- output 2: bfloat16 [16, 32, 2048], P(('data', 'stage', 'inner'))
- output 3: float32 [1, 4, 2048, 8192], P(None, ('data', 'stage'), None, 'inner')
- output 4: float32 [1, 4, 8192, 2048], P(None, ('data', 'stage'), 'inner')
All inputs are finite; a program needn't handle non-finite values.
Results may differ from the reference program's by a relative error of at most 0.0124555.
Values are sent between devices in bfloat16 or wider.
A program may use at most 1 GiB of HBM per device.

```python
import jax
import jax.numpy as jnp
from jax import lax

D_MODEL = 2048
D_FF = 8192
MB_TOKENS = 32
MB_PER_DEV = 2
VIRT_STAGES = 1
CHUNK_LAYERS = 1
NUM_STAGES = 4
INNER_SIZE = 2

NUM_MICRO = MB_PER_DEV * NUM_STAGES * INNER_SIZE
STAGE_LAYERS = NUM_STAGES * CHUNK_LAYERS
NUM_LAYERS = VIRT_STAGES * STAGE_LAYERS


def setup_inputs(seed: int = 0, part: int = 0) -> dict:
    base_key = jax.random.fold_in(jax.random.key(seed), part)
    key_list = jax.random.split(base_key, 4)
    tok_shape = (NUM_MICRO, MB_TOKENS, D_MODEL)
    x_tokens = jax.random.normal(key_list[0], tok_shape, jnp.float32)
    g_cotan = jax.random.normal(key_list[1], tok_shape, jnp.float32)
    up_scale = D_MODEL ** -0.5
    down_scale = 1.5 * (D_FF * NUM_LAYERS) ** -0.5
    w_up = jax.random.normal(key_list[2], (VIRT_STAGES, STAGE_LAYERS, D_MODEL, D_FF), jnp.float32) * up_scale
    w_down = jax.random.normal(key_list[3], (VIRT_STAGES, STAGE_LAYERS, D_FF, D_MODEL), jnp.float32) * down_scale
    return {'x_tokens': x_tokens.astype(jnp.bfloat16), 'g_cotan': g_cotan.astype(jnp.bfloat16), 'w_up': w_up.astype(jnp.bfloat16), 'w_down': w_down.astype(jnp.bfloat16)}


def gelu_pair(pre_act):
    normal_cdf = 0.5 * (1.0 + lax.erf(pre_act * 0.7071067811865476))
    normal_pdf = jnp.exp(-0.5 * pre_act * pre_act) * 0.3989422804014327
    return pre_act * normal_cdf, normal_cdf + pre_act * normal_pdf


def reference(x_tokens, g_cotan, w_up, w_down):
    up_layers = w_up.reshape(NUM_LAYERS, D_MODEL, D_FF)
    down_layers = w_down.reshape(NUM_LAYERS, D_FF, D_MODEL)

    def fwd_layer(h_act, weights):
        w_one, w_two = weights
        pre_act = jnp.dot(h_act, w_one, preferred_element_type=jnp.float32)
        act_val = gelu_pair(pre_act)[0].astype(jnp.bfloat16)
        branch = jnp.dot(act_val, w_two, preferred_element_type=jnp.float32)
        h_next = (h_act.astype(jnp.float32) + branch).astype(jnp.bfloat16)
        return h_next, h_act

    def bwd_layer(g_act, layer_items):
        h_in, w_one, w_two = layer_items
        pre_act = jnp.dot(h_in, w_one, preferred_element_type=jnp.float32)
        gelu_val, gelu_grad = gelu_pair(pre_act)
        act_val = gelu_val.astype(jnp.bfloat16)
        d_act = jnp.dot(g_act, w_two.T, preferred_element_type=jnp.float32)
        d_pre = (d_act * gelu_grad).astype(jnp.bfloat16)
        grad_one = jnp.dot(h_in.T, d_pre, preferred_element_type=jnp.float32)
        grad_two = jnp.dot(act_val.T, g_act, preferred_element_type=jnp.float32)
        back_term = jnp.dot(d_pre, w_one.T, preferred_element_type=jnp.float32)
        g_prev = (g_act.astype(jnp.float32) + back_term).astype(jnp.bfloat16)
        return g_prev, (grad_one, grad_two)

    def one_micro(acc_state, micro_items):
        x_micro, g_micro = micro_items
        y_micro, layer_ins = lax.scan(fwd_layer, x_micro, (up_layers, down_layers))
        dx_micro, grad_pair = lax.scan(bwd_layer, g_micro, (layer_ins, up_layers, down_layers), reverse=True)
        new_state = (acc_state[0] + grad_pair[0], acc_state[1] + grad_pair[1])
        return new_state, (y_micro, dx_micro)

    init_state = (jnp.zeros(up_layers.shape, jnp.float32), jnp.zeros(down_layers.shape, jnp.float32))
    final_state, micro_outs = lax.scan(one_micro, init_state, (x_tokens, g_cotan))
    dw_up = final_state[0].reshape(w_up.shape)
    dw_down = final_state[1].reshape(w_down.shape)
    return (micro_outs[0], micro_outs[1], dw_up, dw_down)
```

```python
import jax
import jax.numpy as jnp
from jax import lax
from jax.sharding import PartitionSpec as P

F32 = jnp.float32
BF16 = jnp.bfloat16


def gelu_pair(pre_act):
    normal_cdf = 0.5 * (1.0 + lax.erf(pre_act * 0.7071067811865476))
    normal_pdf = jnp.exp(-0.5 * pre_act * pre_act) * 0.3989422804014327
    return pre_act * normal_cdf, normal_cdf + pre_act * normal_pdf


def solution(mesh):
    n_stage = mesh.shape['stage']
    tok_spec = P(('data', 'stage', 'inner'))
    up_spec = P(None, ('data', 'stage'), None, 'inner')
    down_spec = P(None, ('data', 'stage'), 'inner', None)
    fwd_perm = [(i, i + 1) for i in range(n_stage - 1)]
    bwd_perm = [(i, i - 1) for i in range(1, n_stage)]

    def device_step(x_loc, g_loc, w_up, w_down):
        w_one = w_up[0, 0]
        w_two = w_down[0, 0]
        stage = lax.axis_index('stage')
        inner = lax.axis_index('inner')
        d_model = x_loc.shape[2]
        x_all = lax.all_gather(x_loc, ('stage', 'inner'), axis=0, tiled=True)
        g_all = lax.all_gather(g_loc, ('stage', 'inner'), axis=0, tiled=True)
        n_micro, tok = x_all.shape[:2]
        rows = 2 * tok
        n_chunk = n_micro // 2
        x_all = x_all.reshape(n_chunk, rows, d_model)
        g_all = g_all.reshape(n_chunk, rows, d_model)
        first = stage == 0
        last = stage == n_stage - 1
        ticks = n_chunk + n_stage - 1

        recv = jnp.zeros((rows, d_model), BF16)
        h_ticks, a_ticks, d_ticks, y_ticks = [], [], [], []
        for t in range(ticks):
            h_in = jnp.where(first, x_all[min(t, n_chunk - 1)], recv)
            z = jnp.dot(h_in, w_one, preferred_element_type=F32)
            act, slope = gelu_pair(z)
            act = act.astype(BF16)
            part = jnp.dot(act, w_two, preferred_element_type=F32)
            h_out = (h_in.astype(F32) + lax.psum(part, 'inner')).astype(BF16)
            h_ticks.append(h_in)
            a_ticks.append(act)
            d_ticks.append(slope)
            y_ticks.append(h_out)
            if t < ticks - 1:
                recv = lax.ppermute(h_out, 'stage', fwd_perm)
        h_all = jnp.stack(h_ticks)
        a_all = jnp.stack(a_ticks)
        s_all = jnp.stack(d_ticks)

        recv = jnp.zeros((rows, d_model), BF16)
        g_ticks, dz_ticks, hb_ticks, ab_ticks, dx_ticks = [], [], [], [], []
        for t in range(ticks):
            chunk = t - (n_stage - 1 - stage)
            valid = (chunk >= 0) & (chunk < n_chunk)
            slot = jnp.clip(chunk, 0, n_chunk - 1) + stage
            g_in = jnp.where(last, g_all[min(t, n_chunk - 1)], recv)
            g_in = jnp.where(valid, g_in, jnp.zeros_like(g_in))
            h_in = lax.dynamic_index_in_dim(h_all, slot, 0, keepdims=False)
            act = lax.dynamic_index_in_dim(a_all, slot, 0, keepdims=False)
            slope = lax.dynamic_index_in_dim(s_all, slot, 0, keepdims=False)
            err = lax.dot_general(g_in, w_two, (((1,), (1,)), ((), ())), preferred_element_type=F32)
            dz = (err * slope).astype(BF16)
            part = lax.dot_general(dz, w_one, (((1,), (1,)), ((), ())), preferred_element_type=F32)
            g_out = (g_in.astype(F32) + lax.psum(part, 'inner')).astype(BF16)
            g_ticks.append(g_in)
            dz_ticks.append(dz)
            hb_ticks.append(h_in)
            ab_ticks.append(act)
            dx_ticks.append(g_out)
            if t < ticks - 1:
                recv = lax.ppermute(g_out, 'stage', bwd_perm)
        cat = lambda items: jnp.concatenate(items, axis=0)
        contract = (((0,), (0,)), ((), ()))
        dw_up = lax.dot_general(cat(hb_ticks), cat(dz_ticks), contract, preferred_element_type=F32)
        dw_down = lax.dot_general(cat(ab_ticks), cat(g_ticks), contract, preferred_element_type=F32)

        def scatter(items, owner):
            src = jnp.stack(items[n_stage - 1:]).reshape(n_micro, tok, d_model)
            src = jnp.where(owner, src, jnp.zeros_like(src))
            mine = lax.psum_scatter(src, 'stage', scatter_dimension=0, tiled=True)
            return lax.dynamic_slice_in_dim(mine, inner * x_loc.shape[0], x_loc.shape[0], 0)

        return scatter(y_ticks, last), scatter(dx_ticks, first), dw_up[None, None], dw_down[None, None]

    return jax.shard_map(device_step, mesh=mesh, in_specs=(tok_spec, tok_spec, up_spec, down_spec), out_specs=(tok_spec, tok_spec, up_spec, down_spec), check_vma=False)
```

```python
import functools

import jax
import jax.numpy as jnp
from jax import lax
from jax.experimental import pallas as pl
from jax.experimental.pallas import tpu as pltpu
from jax.sharding import PartitionSpec as P

F32 = jnp.float32
BF16 = jnp.bfloat16
MESH = pl.DeviceIdType.MESH

STAGES = 4
INNER = 2
CHUNKS = 8
BLK = 512
TILE = 256


def gelu_pair(pre_act):
    normal_cdf = 0.5 * (1.0 + lax.erf(pre_act * 0.7071067811865476))
    normal_pdf = jnp.exp(-0.5 * pre_act * pre_act) * 0.3989422804014327
    return pre_act * normal_cdf, normal_cdf + pre_act * normal_pdf


def wait_bytes(ref, sem):
    pltpu.make_async_copy(ref, ref, sem).wait()


def pipeline_kernel(x_ref, g_ref, w1_ref, w2_ref,
                    y_out, dx_out, h_out, g_out, a_out, d_out,
                    wa, wb, hbuf, gbuf, abuf, dbuf, sbuf, pbuf, precv, qrecv, hsend, gsend, ybuf, xbuf,
                    h_sem, g_sem, p_sem, q_sem, blk_send, hs_send, gs_send, home_send, y_sem, x_sem, in_send, w_sem, out_sem):
    stage = lax.axis_index('stage')
    side = lax.axis_index('inner')
    other = 1 - side
    rows = hbuf.shape[2]
    d_model = hbuf.shape[3]
    d_ff = abuf.shape[2]
    tok = 2 * rows
    n_blk = d_model // BLK

    def peer(s, i):
        return {'stage': s, 'inner': i}

    def cols(j):
        return pl.ds(pl.multiple_of(j * BLK, BLK), BLK)

    load_a = pltpu.make_async_copy(w1_ref, wa, w_sem.at[0])
    load_b = pltpu.make_async_copy(w2_ref, wb, w_sem.at[1])
    load_a.start()
    load_b.start()

    barrier = pltpu.get_barrier_semaphore()
    for s in range(STAGES):
        for i in range(INNER):
            @pl.when(jnp.logical_or(stage != s, side != i))
            def _():
                pl.semaphore_signal(barrier, inc=1, device_id=peer(s, i), device_id_type=MESH)
    pl.semaphore_wait(barrier, STAGES * INNER - 1)

    def chunk_of(k):
        return lax.rem(2 * stage + k + CHUNKS - 1, CHUNKS)

    def home_of(c):
        return lax.rem((c + 1) // 2, STAGES)

    def slot_of(c):
        return lax.rem(c + 1, 2)

    def hand_in(src, dst, sem, target, lane):
        for k in range(2):
            c = chunk_of(k)

            @pl.when(stage == target)
            def _():
                pltpu.make_async_copy(src.at[k], dst.at[c, side], sem.at[c, side]).start()

            @pl.when(stage != target)
            def _():
                pltpu.make_async_remote_copy(src.at[k], dst.at[c, side], in_send.at[lane, k, 0], sem.at[c, side],
                                             device_id=peer(target, side), device_id_type=MESH).start()
            pltpu.make_async_remote_copy(src.at[k], dst.at[c, side], in_send.at[lane, k, 1], sem.at[c, side],
                                         device_id=peer(target, other), device_id_type=MESH).start()

    hand_in(x_ref, hbuf, h_sem, 0, 0)
    hand_in(g_ref, gbuf, g_sem, STAGES - 1, 1)

    def up_product(src, c, mode):
        def body(n, carry):
            lhs = src[c].reshape(tok, d_model)
            z = jnp.dot(lhs, wa[:, cols(n)], preferred_element_type=F32)
            if mode == 'back':
                dbuf[c, :, cols(n)] = (z * sbuf[c, :, cols(n)]).astype(BF16)
            else:
                act, slope = gelu_pair(z)
                abuf[c, :, cols(n)] = act.astype(BF16)
                if mode == 'both':
                    dbuf[c, :, cols(n)] = (sbuf[c, :, cols(n)] * slope).astype(BF16)
                else:
                    sbuf[c, :, cols(n)] = slope
            return carry
        lax.fori_loop(0, d_ff // BLK, body, 0, unroll=2)

    def down_product(src, c, slot, reuse, recv, recv_sem):
        def body(j, carry):
            out = pltpu.make_async_remote_copy(pbuf.at[slot, j, other], recv.at[c, j], blk_send.at[slot, j], recv_sem.at[c, j],
                                               device_id=peer(stage, other), device_id_type=MESH)

            @pl.when(reuse)
            def _():
                out.wait_send()
            part = jnp.dot(src[c], wb[:, cols(j)], preferred_element_type=F32)
            pbuf[slot, j] = part.reshape(2, rows, BLK)
            out.start()
            return carry
        lax.fori_loop(0, n_blk, body, 0)

    def drain(slot, recv, recv_sem):
        for j in range(n_blk):
            pltpu.make_async_remote_copy(pbuf.at[slot, j, other], recv.at[0, j], blk_send.at[slot, j], recv_sem.at[0, j],
                                         device_id=peer(stage, other), device_id_type=MESH).wait_send()

    def hand_on(c, slot, recv, recv_sem, res, send, dst, dst_sem, send_sem, target):
        for j in range(n_blk):
            sl = pl.ds(j * BLK, BLK)
            wait_bytes(recv.at[c, j], recv_sem.at[c, j])
            total = res[c, side, :, sl].astype(F32) + (pbuf[slot, j, side] + recv[c, j])
            send[c, :, sl] = total.astype(BF16)
            if target is not None:
                for i in (side, other):
                    pltpu.make_async_remote_copy(send.at[c, :, sl], dst.at[c, side, :, sl], send_sem, dst_sem.at[c, side],
                                                 device_id=peer(target, i), device_id_type=MESH).start()

    def hand_home(c, send, dst, dst_sem, here):
        @pl.when(home_of(c) != here)
        def _():
            pltpu.make_async_remote_copy(send.at[c], dst.at[slot_of(c)], home_send.at[c], dst_sem.at[slot_of(c)],
                                         device_id=peer(home_of(c), side), device_id_type=MESH).start()

    def hand_home_done(send, dst, dst_sem, here):
        for c in range(CHUNKS):
            if (c + 1) // 2 % STAGES != here:
                pltpu.make_async_remote_copy(send.at[c], dst.at[(c + 1) % 2], home_send.at[c], dst_sem.at[(c + 1) % 2],
                                             device_id=peer((c + 1) // 2 % STAGES, side), device_id_type=MESH).wait_send()

    def keep(ref, out, c, lane):
        pltpu.make_async_copy(ref.at[c], out.at[c], out_sem.at[lane]).start()

    def swap_weights():
        n_i = d_model // TILE

        def body(t, carry):
            i = pl.multiple_of(lax.rem(t, n_i) * TILE, TILE)
            j = pl.multiple_of(lax.div(t, n_i) * TILE, TILE)
            up = wa[pl.ds(i, TILE), pl.ds(j, TILE)]
            down = wb[pl.ds(j, TILE), pl.ds(i, TILE)]
            wa[pl.ds(i, TILE), pl.ds(j, TILE)] = down.T
            wb[pl.ds(j, TILE), pl.ds(i, TILE)] = up.T
            return carry
        lax.fori_loop(0, n_i * (d_ff // TILE), body, 0)

    def transpose_up():
        n_i = d_model // TILE

        def body(t, carry):
            i = pl.multiple_of(lax.rem(t, n_i) * TILE, TILE)
            j = pl.multiple_of(lax.div(t, n_i) * TILE, TILE)
            wb[pl.ds(j, TILE), pl.ds(i, TILE)] = wa[pl.ds(i, TILE), pl.ds(j, TILE)].T
            return carry
        lax.fori_loop(0, n_i * (d_ff // TILE), body, 0)

    @pl.when(stage < STAGES - 1)
    def _():
        load_a.wait()

        def fwd(c, carry):
            for i in range(INNER):
                wait_bytes(hbuf.at[c, i], h_sem.at[c, i])
            keep(hbuf, h_out, c, 0)
            up_product(hbuf, c, 'fwd')

            @pl.when(c == 0)
            def _():
                load_b.wait()

            @pl.when(jnp.logical_and(stage == 0, c > 0))
            def _():
                hand_on(c - 1, lax.rem(c + 1, 2), precv, p_sem, hbuf, hsend, hbuf, h_sem, hs_send.at[0], stage + 1)
            keep(abuf, a_out, c, 2)
            down_product(abuf, c, lax.rem(c, 2), c >= 2, precv, p_sem)

            @pl.when(jnp.logical_or(stage != 0, c == CHUNKS - 1))
            def _():
                hand_on(c, lax.rem(c, 2), precv, p_sem, hbuf, hsend, hbuf, h_sem, hs_send.at[0], stage + 1)
            return carry
        lax.fori_loop(0, CHUNKS, fwd, 0)
        swap_weights()

        def bwd(c, carry):
            for i in range(INNER):
                wait_bytes(gbuf.at[c, i], g_sem.at[c, i])
            keep(gbuf, g_out, c, 1)
            up_product(gbuf, c, 'back')

            def pass_back(q):
                @pl.when(stage > 0)
                def _():
                    hand_on(q, lax.rem(q, 2), qrecv, q_sem, gbuf, gsend, gbuf, g_sem, gs_send.at[0], stage - 1)

                @pl.when(stage == 0)
                def _():
                    hand_on(q, lax.rem(q, 2), qrecv, q_sem, gbuf, gsend, None, None, None, None)
                    hand_home(q, gsend, xbuf, x_sem, 0)

            @pl.when(c > 0)
            def _():
                pass_back(c - 1)
            keep(dbuf, d_out, c, 3)
            down_product(dbuf, c, lax.rem(c, 2), c >= 0, qrecv, q_sem)

            @pl.when(c == CHUNKS - 1)
            def _():
                pass_back(c)
            return carry
        lax.fori_loop(0, CHUNKS, bwd, 0)
        for slot in range(2):
            drain(slot, qrecv, q_sem)
        wait_bytes(hbuf, hs_send.at[0])

        @pl.when(stage > 0)
        def _():
            wait_bytes(gbuf, gs_send.at[0])

        @pl.when(stage == 0)
        def _():
            hand_home_done(gsend, xbuf, x_sem, 0)

    @pl.when(stage == STAGES - 1)
    def _():
        load_b.wait()

        half = CHUNKS // 2
        for q in range(2):
            for c in range(half * q, half * q + half):
                for i in range(INNER):
                    wait_bytes(gbuf.at[c, i], g_sem.at[c, i])
                keep(gbuf, g_out, c, 1)

            def err(n, carry):
                lhs = gbuf[half * q:half * q + half].reshape(half * tok, d_model)
                e = lax.dot_general(lhs, wb[cols(n), :], (((1,), (1,)), ((), ())), preferred_element_type=F32)
                sbuf[half * q:half * q + half, :, cols(n)] = e.reshape(half, tok, BLK)
                return carry
            lax.fori_loop(0, d_ff // BLK, err, 0)
        load_a.wait()
        transpose_up()

        def main(c, carry):
            for i in range(INNER):
                wait_bytes(hbuf.at[c, i], h_sem.at[c, i])
            keep(hbuf, h_out, c, 0)
            up_product(hbuf, c, 'both')
            keep(abuf, a_out, c, 2)
            keep(dbuf, d_out, c, 3)
            down_product(dbuf, c, lax.rem(c, 2), c >= 2, qrecv, q_sem)
            hand_on(c, lax.rem(c, 2), qrecv, q_sem, gbuf, gsend, gbuf, g_sem, gs_send.at[0], stage - 1)
            return carry
        lax.fori_loop(0, CHUNKS, main, 0)
        load_b.start()
        load_b.wait()

        def outputs(c, carry):
            down_product(abuf, c, lax.rem(c, 2), c >= 0, precv, p_sem)

            def pass_home(q):
                hand_on(q, lax.rem(q, 2), precv, p_sem, hbuf, hsend, None, None, None, None)
                hand_home(q, hsend, ybuf, y_sem, STAGES - 1)

            @pl.when(c > 0)
            def _():
                pass_home(c - 1)

            @pl.when(c == CHUNKS - 1)
            def _():
                pass_home(c)
            return carry
        lax.fori_loop(0, CHUNKS, outputs, 0)
        for slot in range(2):
            drain(slot, precv, p_sem)
        wait_bytes(gbuf, gs_send.at[0])
        hand_home_done(hsend, ybuf, y_sem, STAGES - 1)

    def come_home(here, send, recv, recv_sem, out, lane):
        for k in range(2):
            @pl.when(stage == here)
            def _():
                pltpu.make_async_copy(send.at[chunk_of(k)], out.at[k], out_sem.at[lane]).start()

            @pl.when(stage != here)
            def _():
                wait_bytes(recv.at[k], recv_sem.at[k])
                pltpu.make_async_copy(recv.at[k], out.at[k], out_sem.at[lane]).start()
    come_home(STAGES - 1, hsend, ybuf, y_sem, y_out, 4)
    come_home(0, gsend, xbuf, x_sem, dx_out, 5)

    for lane, (src, target) in enumerate(((x_ref, 0), (g_ref, STAGES - 1))):
        for k in range(2):
            @pl.when(stage != target)
            def _():
                wait_bytes(src.at[k], in_send.at[lane, k, 0])
            wait_bytes(src.at[k], in_send.at[lane, k, 1])
    for lane, (ref, out) in enumerate(((hbuf, h_out), (gbuf, g_out), (abuf, a_out), (dbuf, d_out), (ybuf, y_out), (xbuf, dx_out))):
        pltpu.make_async_copy(ref, out, out_sem.at[lane]).wait()


def run_pipeline(x_loc, g_loc, w_one, w_two):
    rows, d_model = x_loc.shape[1:]
    d_ff = w_one.shape[1]
    n_blk = d_model // BLK
    tok = 2 * rows
    hbm = pl.BlockSpec(memory_space=pl.ANY)
    out = lambda shape: jax.ShapeDtypeStruct(shape, BF16)
    dma = pltpu.SemaphoreType.DMA
    return pl.pallas_call(
        pipeline_kernel,
        name='pipeline',
        out_shape=(out(x_loc.shape), out(x_loc.shape), out((CHUNKS, 2, rows, d_model)), out((CHUNKS, 2, rows, d_model)),
                   out((CHUNKS, tok, d_ff)), out((CHUNKS, tok, d_ff))),
        in_specs=[hbm] * 4,
        out_specs=(hbm,) * 6,
        scratch_shapes=[
            pltpu.VMEM((d_model, d_ff), BF16),
            pltpu.VMEM((d_ff, d_model), BF16),
            pltpu.VMEM((CHUNKS, 2, rows, d_model), BF16),
            pltpu.VMEM((CHUNKS, 2, rows, d_model), BF16),
            pltpu.VMEM((CHUNKS, tok, d_ff), BF16),
            pltpu.VMEM((CHUNKS, tok, d_ff), BF16),
            pltpu.VMEM((CHUNKS, tok, d_ff), F32),
            pltpu.VMEM((2, n_blk, 2, rows, BLK), F32),
            pltpu.VMEM((CHUNKS, n_blk, rows, BLK), F32),
            pltpu.VMEM((CHUNKS, n_blk, rows, BLK), F32),
            pltpu.VMEM((CHUNKS, rows, d_model), BF16),
            pltpu.VMEM((CHUNKS, rows, d_model), BF16),
            pltpu.VMEM((2, rows, d_model), BF16),
            pltpu.VMEM((2, rows, d_model), BF16),
            dma((CHUNKS, 2)), dma((CHUNKS, 2)), dma((CHUNKS, n_blk)), dma((CHUNKS, n_blk)), dma((2, n_blk)),
            dma((1,)), dma((1,)), dma((CHUNKS,)), dma((2,)), dma((2,)), dma((2, 2, 2)), dma((2,)), dma((6,)),
        ],
        compiler_params=pltpu.CompilerParams(collective_id=0, has_side_effects=True, vmem_limit_bytes=67043328),
    )(x_loc, g_loc, w_one, w_two)


def weight_grad_kernel(h_ref, d_ref, a_ref, g_ref, up_ref, down_ref, *, n_up):
    contract = (((0,), (0,)), ((), ()))

    @pl.when(pl.program_id(0) < n_up)
    def _():
        up_ref[...] = lax.dot_general(h_ref[...], d_ref[...], contract, preferred_element_type=F32)

    @pl.when(pl.program_id(0) >= n_up)
    def _():
        down_ref[...] = lax.dot_general(a_ref[...], g_ref[...], contract, preferred_element_type=F32)


def weight_grads(h, d, a, g):
    tokens, d_model = h.shape
    d_ff = d.shape[1]
    up_rows, down_rows = 256, 512
    n_up, n_down = d_model // up_rows, d_ff // down_rows
    up_idx = lambda i: jnp.minimum(i, n_up - 1)
    down_idx = lambda i: jnp.maximum(i - n_up, 0)
    return pl.pallas_call(
        functools.partial(weight_grad_kernel, n_up=n_up),
        name='weight_grads',
        grid=(n_up + n_down,),
        out_shape=(jax.ShapeDtypeStruct((d_model, d_ff), F32), jax.ShapeDtypeStruct((d_ff, d_model), F32)),
        in_specs=[pl.BlockSpec((tokens, up_rows), lambda i: (0, up_idx(i))),
                  pl.BlockSpec((tokens, d_ff), lambda i: (0, 0)),
                  pl.BlockSpec((tokens, down_rows), lambda i: (0, down_idx(i))),
                  pl.BlockSpec((tokens, d_model), lambda i: (0, 0))],
        out_specs=(pl.BlockSpec((up_rows, d_ff), lambda i: (up_idx(i), 0)),
                   pl.BlockSpec((down_rows, d_model), lambda i: (down_idx(i), 0))),
        compiler_params=pltpu.CompilerParams(vmem_limit_bytes=60 * 1024 * 1024),
    )(h, d, a, g)


def solution(mesh):
    tok_spec = P(('data', 'stage', 'inner'))
    up_spec = P(None, ('data', 'stage'), None, 'inner')
    down_spec = P(None, ('data', 'stage'), 'inner', None)

    def device_step(x_loc, g_loc, w_up, w_down):
        y, dx, h, g, a, d = run_pipeline(x_loc, g_loc, w_up[0, 0], w_down[0, 0])
        flat = lambda v: v.reshape(-1, v.shape[-1])
        dw_up, dw_down = weight_grads(flat(h), flat(d), flat(a), flat(g))
        return y, dx, dw_up[None, None], dw_down[None, None]

    return jax.shard_map(device_step, mesh=mesh, in_specs=(tok_spec, tok_spec, up_spec, down_spec), out_specs=(tok_spec, tok_spec, up_spec, down_spec), check_vma=False)
```

```python
import functools

import jax
import jax.numpy as jnp
from jax import lax
from jax.experimental import pallas as pl
from jax.experimental.pallas import tpu as pltpu
from jax.sharding import PartitionSpec as P

F32 = jnp.float32
BF16 = jnp.bfloat16
MESH = pl.DeviceIdType.MESH

STAGES = 4
INNER = 2
UNITS = 8
SLOTS = 4
BLK = 512
TILE = 256
FWD, BWD = 0, 1
NT = (((1,), (1,)), ((), ()))

F1, F2, FR, B1, B2, BR, T1, T2, SW, PR, YL, WA, WB, XS = range(1, 15)
PLAN = (
    ((WA, 0, 1), (F1, 0, 1), (WB, 0, 1), (F2, 0, 1), (F1, 1, 2), (FR, 0, 1), (F2, 1, 1), (F2, 2, 1),
     (FR, 1, 1), (F1, 3, 1), (F1, 4, 2), (FR, 2, 1), (F2, 3, 1), (F1, 6, 2), (F2, 4, 1), (FR, 3, 2),
     (F2, 5, 2), (FR, 5, 2), (F2, 7, 1), (SW, 0, 1), (FR, 7, 1), (B1, 0, 2), (B2, 0, 1), (B2, 1, 1),
     (BR, 0, 1), (B1, 2, 2), (B2, 2, 2), (B1, 4, 2), (BR, 1, 3), (B2, 4, 2), (B1, 6, 2), (B2, 6, 2),
     (BR, 4, 4)),
    ((WA, 0, 1), (WB, 0, 1), (F1, 0, 1), (F2, 0, 1), (FR, 0, 1), (F1, 1, 1), (F2, 1, 1), (F1, 2, 1),
     (FR, 1, 1), (F2, 2, 1), (FR, 2, 1), (F1, 3, 2), (F2, 3, 1), (F2, 4, 1), (FR, 3, 1), (F1, 5, 2),
     (F2, 5, 1), (FR, 4, 2), (F2, 6, 1), (F1, 7, 1), (F2, 7, 1), (FR, 6, 2), (SW, 0, 1), (B1, 0, 2),
     (B2, 0, 1), (B2, 1, 1), (BR, 0, 2), (B1, 2, 2), (B2, 2, 2), (BR, 2, 2), (B1, 4, 2), (B2, 4, 1),
     (B2, 5, 1), (B1, 6, 2), (BR, 4, 1), (B2, 6, 1), (BR, 5, 1), (B2, 7, 1), (BR, 6, 2)),
    ((WA, 0, 1), (XS, 0, 1), (WB, 0, 1), (F1, 0, 1), (F2, 0, 1), (FR, 0, 1), (F1, 1, 1), (F2, 1, 1),
     (F1, 2, 1), (FR, 1, 1), (F2, 2, 1), (FR, 2, 1), (F1, 3, 1), (F2, 3, 1), (F1, 4, 2), (F2, 4, 1),
     (F2, 5, 1), (FR, 3, 2), (T1, 0, 2), (FR, 5, 1), (T2, 0, 2), (F1, 6, 2), (F2, 6, 2), (BR, 0, 2),
     (T1, 2, 2), (FR, 6, 2), (T2, 2, 2), (BR, 2, 2), (T1, 4, 2), (T2, 4, 2), (T1, 6, 2), (BR, 4, 2),
     (T2, 6, 2), (BR, 6, 2)),
    ((WB, 0, 1), (XS, 0, 1), (PR, 0, 1), (F1, 0, 1), (B2, 0, 1), (F1, 1, 1), (BR, 0, 1), (B2, 1, 1),
     (BR, 1, 1), (F1, 2, 1), (B2, 2, 1), (BR, 2, 1), (F1, 3, 1), (F1, 4, 1), (B2, 3, 1), (F1, 5, 1),
     (BR, 3, 1), (B2, 4, 2), (F1, 6, 2), (BR, 4, 2), (B2, 6, 2), (BR, 6, 2), (YL, 0, 1), (F2, 0, 2),
     (FR, 0, 1), (F2, 2, 1), (FR, 1, 2), (F2, 3, 1), (F2, 4, 1), (FR, 3, 2), (F2, 5, 2), (FR, 5, 1),
     (F2, 7, 1), (FR, 6, 2)),
)


PACK = 1024


def plan_words():
    rows = [[op + 16 * unit + 128 * (count - 1) for op, unit, count in row] for row in PLAN]
    steps = -(-max(len(row) for row in rows) // 3) * 3
    rows = [row + [0] * (steps - len(row)) for row in rows]
    return steps, [[row[t] + PACK * row[t + 1] + PACK * PACK * row[t + 2] for t in range(0, steps, 3)] for row in rows]


def gelu_pair(pre_act):
    normal_cdf = 0.5 * (1.0 + lax.erf(pre_act * 0.7071067811865476))
    normal_pdf = jnp.exp(-0.5 * pre_act * pre_act) * 0.3989422804014327
    return pre_act * normal_cdf, normal_cdf + pre_act * normal_pdf


def wait_bytes(ref, sem):
    pltpu.make_async_copy(ref, ref, sem).wait()


def pipeline_kernel(x_ref, g_ref, w1_ref, w2_ref,
                    y_out, dx_out, h_out, g_out, a_out, d_out,
                    wa, wb, flow, act, slope, part, recv, send, home,
                    flow_sem, recv_sem, part_send, flow_send, home_send, home_sem, in_send, w_sem, out_sem):
    stage = lax.axis_index('stage')
    side = lax.axis_index('inner')
    other = 1 - side
    rows, d_model = flow.shape[3:]
    tok, d_ff = act.shape[2:]
    n_blk = d_model // BLK

    def peer(s, i):
        return {'stage': s, 'inner': i}

    load_a = pltpu.make_async_copy(w1_ref, wa, w_sem.at[0])
    load_b = pltpu.make_async_copy(w2_ref, wb, w_sem.at[1])

    @pl.when(stage < STAGES - 1)
    def _():
        load_a.start()
    load_b.start()

    @pl.when(stage == STAGES - 1)
    def _():
        load_a.start()

    barrier = pltpu.get_barrier_semaphore()
    for s in range(STAGES):
        for i in range(INNER):
            @pl.when(jnp.logical_or(stage != s, side != i))
            def _():
                pl.semaphore_signal(barrier, inc=1, device_id=peer(s, i), device_id_type=MESH)
    pl.semaphore_wait(barrier, STAGES * INNER - 1)

    def unit_of(k):
        return lax.rem(2 * stage + k + UNITS - 1, UNITS)

    def home_of(u):
        return lax.rem((u + 1) // 2, STAGES)

    def slot_of(u):
        return lax.rem(u + 1, 2)

    def hand_in(kind, src, target, k, lane):
        u = unit_of(k)
        if lane == 0:
            @pl.when(stage == target)
            def _():
                pltpu.make_async_copy(src.at[k], flow.at[kind, u, side], flow_sem.at[kind, u, side]).start()

            @pl.when(stage != target)
            def _():
                pltpu.make_async_remote_copy(src.at[k], flow.at[kind, u, side], in_send.at[kind, k, 0], flow_sem.at[kind, u, side],
                                             device_id=peer(target, side), device_id_type=MESH).start()
        else:
            pltpu.make_async_remote_copy(src.at[k], flow.at[kind, u, side], in_send.at[kind, k, 1], flow_sem.at[kind, u, side],
                                         device_id=peer(target, other), device_id_type=MESH).start()

    for k in (1, 0):
        hand_in(FWD, x_ref, 0, k, 0)

        @pl.when(stage < 2)
        def _():
            hand_in(FWD, x_ref, 0, k, 1)
    for k in (1, 0):
        for lane in range(2):
            hand_in(BWD, g_ref, STAGES - 1, k, lane)

    steps, plan = plan_words()
    words = [jnp.where(stage == 0, a, jnp.where(stage == 1, b, jnp.where(stage == 2, c, d))) for a, b, c, d in zip(*plan)]

    def keep(ref, out, u, lane):
        pltpu.make_async_copy(ref, out.at[u], out_sem.at[lane]).start()

    def blocks(width, group, fn):
        def body(t, carry):
            fn([pl.ds(pl.multiple_of((t * group + k) * BLK, BLK), BLK) for k in range(group)])
            return carry
        lax.fori_loop(0, width // BLK // group, body, 0)

    def arrived(kind, u, count):
        for i in range(count):
            for half in range(INNER):
                wait_bytes(flow.at[kind, u + i, half], flow_sem.at[kind, u + i, half])

    def up_product(u, count):
        arrived(FWD, u, count)
        units = pl.ds(u, count)

        def fn(slices):
            lhs = flow[FWD, units].reshape(count * tok, d_model)
            for sl in slices:
                z = jnp.dot(lhs, wa[:, sl], preferred_element_type=F32).reshape(count, tok, BLK)
                value, grad = gelu_pair(z)
                act[FWD, units, :, sl] = value.astype(BF16)
                act[BWD, units, :, sl] = (slope[units, :, sl] * grad).astype(BF16)
                slope[units, :, sl] = grad
        blocks(d_ff, 4, fn)
        for i in range(count):
            keep(flow.at[FWD, u + i], h_out, u + i, 0)
            keep(act.at[FWD, u + i], a_out, u + i, 2)

            @pl.when(stage == STAGES - 1)
            def _():
                keep(act.at[BWD, u + i], d_out, u + i, 3)

    def back_product(u, count, swapped):
        arrived(BWD, u, count)
        units = pl.ds(u, count)

        def fn(slices):
            lhs = flow[BWD, units].reshape(count * tok, d_model)
            for sl in slices:
                if swapped:
                    e = jnp.dot(lhs, wa[:, sl], preferred_element_type=F32)
                else:
                    e = lax.dot_general(lhs, wb[sl, :], NT, preferred_element_type=F32)
                act[BWD, units, :, sl] = (e.reshape(count, tok, BLK) * slope[units, :, sl]).astype(BF16)
        blocks(d_ff, 4, fn)
        for i in range(count):
            keep(flow.at[BWD, u + i], g_out, u + i, 1)
            keep(act.at[BWD, u + i], d_out, u + i, 3)

    def part_copy(kind, u, j):
        slot = lax.rem(u, SLOTS)
        return pltpu.make_async_remote_copy(part.at[kind, slot, j, other], recv.at[kind, u, j], part_send.at[kind, slot, j],
                                            recv_sem.at[kind, u, j], device_id=peer(stage, other), device_id_type=MESH)

    def down_product(kind, u, count, straight):
        for i in range(count):
            @pl.when(u + i >= SLOTS)
            def _():
                for j in range(n_blk):
                    part_copy(kind, u + i - SLOTS, j).wait_send()

        def body(t, carry):
            lhs = act[kind, pl.ds(u, count)].reshape(count * tok, d_ff)
            for k in range(2):
                j = t * 2 + k
                sl = pl.ds(pl.multiple_of(j * BLK, BLK), BLK)
                if straight:
                    p = jnp.dot(lhs, wb[:, sl], preferred_element_type=F32)
                else:
                    p = lax.dot_general(lhs, wa[sl, :], NT, preferred_element_type=F32)
                p = p.reshape(count, INNER, rows, BLK)
                for i in range(count):
                    part[kind, lax.rem(u + i, SLOTS), j] = p[i]
            for k in range(2):
                for i in range(count):
                    part_copy(kind, u + i, t * 2 + k).start()
            return carry
        lax.fori_loop(0, n_blk // 2, body, 0)

    def hand_on(kind, first, count):
        target = stage + 1 if kind == FWD else stage - 1
        inside = stage < STAGES - 1 if kind == FWD else stage > 0
        out = STAGES - 1 if kind == FWD else 0

        def body(i, carry):
            u = first + i
            slot = lax.rem(u, SLOTS)
            for j in range(n_blk):
                sl = pl.ds(j * BLK, BLK)
                wait_bytes(recv.at[kind, u, j], recv_sem.at[kind, u, j])
                total = flow[kind, u, side, :, sl].astype(F32) + (part[kind, slot, j, side] + recv[kind, u, j])
                send[kind, u, :, sl] = total.astype(BF16)

                @pl.when(inside)
                def _():
                    for half in (side, other):
                        pltpu.make_async_remote_copy(send.at[kind, u, :, sl], flow.at[kind, u, side, :, sl], flow_send.at[kind],
                                                     flow_sem.at[kind, u, side], device_id=peer(target, half), device_id_type=MESH).start()

            @pl.when(jnp.logical_and(jnp.logical_not(inside), home_of(u) != out))
            def _():
                pltpu.make_async_remote_copy(send.at[kind, u], home.at[kind, slot_of(u)], home_send.at[kind, u],
                                             home_sem.at[kind, slot_of(u)], device_id=peer(home_of(u), side), device_id_type=MESH).start()
            return carry
        lax.fori_loop(0, count, body, 0)

    def swap_weights():
        n_i = d_model // TILE

        def body(t, carry):
            i = pl.multiple_of(lax.rem(t, n_i) * TILE, TILE)
            j = pl.multiple_of(lax.div(t, n_i) * TILE, TILE)
            up = wa[pl.ds(i, TILE), pl.ds(j, TILE)]
            down = wb[pl.ds(j, TILE), pl.ds(i, TILE)]
            wa[pl.ds(i, TILE), pl.ds(j, TILE)] = down.T
            wb[pl.ds(j, TILE), pl.ds(i, TILE)] = up.T
            return carry
        lax.fori_loop(0, n_i * (d_ff // TILE), body, 0)

    def prepare_last():
        half = UNITS // 2

        def quarter(q, carry):
            for i in range(half):
                arrived(BWD, q * half + i, 1)
                keep(flow.at[BWD, q * half + i], g_out, q * half + i, 1)
            units = pl.ds(q * half, half)

            def fn(slices):
                lhs = flow[BWD, units].reshape(half * tok, d_model)
                for sl in slices:
                    e = lax.dot_general(lhs, wb[sl, :], NT, preferred_element_type=F32)
                    slope[units, :, sl] = e.reshape(half, tok, BLK)
            blocks(d_ff, 1, fn)
            return carry
        lax.fori_loop(0, 2, quarter, 0)
        load_a.wait()
        n_i = d_model // TILE

        def body(t, carry):
            i = pl.multiple_of(lax.rem(t, n_i) * TILE, TILE)
            j = pl.multiple_of(lax.div(t, n_i) * TILE, TILE)
            wb[pl.ds(j, TILE), pl.ds(i, TILE)] = wa[pl.ds(i, TILE), pl.ds(j, TILE)].T
            return carry
        lax.fori_loop(0, n_i * (d_ff // TILE), body, 0)

    def step(t, carry):
        group, place = lax.div(t, 3), lax.rem(t, 3)
        word = words[0]
        for i, w in enumerate(words[1:], 1):
            word = jnp.where(group == i, w, word)
        code = lax.rem(lax.div(word, jnp.where(place == 0, 1, jnp.where(place == 1, PACK, PACK * PACK))), PACK)
        op = lax.rem(code, 16)
        u = lax.rem(lax.div(code, 16), UNITS)
        count = lax.div(code, 128) + 1

        def on(*want):
            hit = op == want[0]
            if len(want) > 1:
                hit = jnp.logical_and(hit, count == want[1])
            return pl.when(hit)

        for n in (1, 2):
            @on(F1, n)
            def _():
                up_product(u, n)

        for n in (1, 2):
            @pl.when(jnp.logical_and(jnp.logical_or(op == F2, op == B2), count == n))
            def _():
                down_product(jnp.where(op == F2, FWD, BWD), u, n, True)

        @on(FR)
        def _():
            hand_on(FWD, u, count)

        @on(BR)
        def _():
            hand_on(BWD, u, count)

        @on(B1)
        def _():
            back_product(u, 2, True)

        @on(T1)
        def _():
            back_product(u, 2, False)

        @on(T2)
        def _():
            down_product(BWD, u, 2, False)

        @on(SW)
        def _():
            swap_weights()

        @on(PR)
        def _():
            prepare_last()

        @on(YL)
        def _():
            load_b.start()
            load_b.wait()

        @on(WA)
        def _():
            load_a.wait()

        @on(WB)
        def _():
            load_b.wait()

        @on(XS)
        def _():
            for k in (1, 0):
                hand_in(FWD, x_ref, 0, k, 1)
        return carry
    lax.fori_loop(0, steps, step, 0)

    for kind, here, out in ((FWD, STAGES - 1, y_out), (BWD, 0, dx_out)):
        for k in range(2):
            @pl.when(stage == here)
            def _():
                pltpu.make_async_copy(send.at[kind, unit_of(k)], out.at[k], out_sem.at[4 + kind]).start()

            @pl.when(stage != here)
            def _():
                wait_bytes(home.at[kind, k], home_sem.at[kind, k])
                pltpu.make_async_copy(home.at[kind, k], out.at[k], out_sem.at[4 + kind]).start()

    for kind in (FWD, BWD):
        for u in range(UNITS - SLOTS, UNITS):
            for j in range(n_blk):
                @pl.when(stage < STAGES)
                def _():
                    part_copy(kind, u, j).wait_send()
    for kind, target, src in ((FWD, 0, x_ref), (BWD, STAGES - 1, g_ref)):
        last = STAGES - 1 - target
        for k in range(2):
            @pl.when(stage != target)
            def _():
                wait_bytes(src.at[k], in_send.at[kind, k, 0])
            wait_bytes(src.at[k], in_send.at[kind, k, 1])

        @pl.when(stage != last)
        def _():
            wait_bytes(flow.at[kind], flow_send.at[kind])

        @pl.when(stage == last)
        def _():
            for u in range(UNITS):
                if (u + 1) // 2 % STAGES != last:
                    wait_bytes(send.at[kind, u], home_send.at[kind, u])
    for lane, (ref, out) in enumerate(((flow.at[FWD], h_out), (flow.at[BWD], g_out), (act.at[FWD], a_out), (act.at[BWD], d_out),
                                       (home.at[FWD], y_out), (home.at[BWD], dx_out))):
        pltpu.make_async_copy(ref, out, out_sem.at[lane]).wait()


def run_pipeline(x_loc, g_loc, w_one, w_two):
    rows, d_model = x_loc.shape[1:]
    d_ff = w_one.shape[1]
    n_blk = d_model // BLK
    tok = INNER * rows
    hbm = pl.BlockSpec(memory_space=pl.ANY)
    out = lambda *shape: jax.ShapeDtypeStruct(shape, BF16)
    dma = lambda *shape: pltpu.SemaphoreType.DMA(shape)
    return pl.pallas_call(
        pipeline_kernel,
        name='pipeline',
        out_shape=(out(*x_loc.shape), out(*x_loc.shape), out(UNITS, INNER, rows, d_model), out(UNITS, INNER, rows, d_model),
                   out(UNITS, tok, d_ff), out(UNITS, tok, d_ff)),
        in_specs=[hbm] * 4,
        out_specs=(hbm,) * 6,
        scratch_shapes=[
            pltpu.VMEM((d_model, d_ff), BF16),
            pltpu.VMEM((d_ff, d_model), BF16),
            pltpu.VMEM((2, UNITS, INNER, rows, d_model), BF16),
            pltpu.VMEM((2, UNITS, tok, d_ff), BF16),
            pltpu.VMEM((UNITS, tok, d_ff), F32),
            pltpu.VMEM((2, SLOTS, n_blk, INNER, rows, BLK), F32),
            pltpu.VMEM((2, UNITS, n_blk, rows, BLK), F32),
            pltpu.VMEM((2, UNITS, rows, d_model), BF16),
            pltpu.VMEM((2, 2, rows, d_model), BF16),
            dma(2, UNITS, INNER), dma(2, UNITS, n_blk), dma(2, SLOTS, n_blk), dma(2), dma(2, UNITS), dma(2, 2), dma(2, 2, 2), dma(2), dma(6),
        ],
        compiler_params=pltpu.CompilerParams(collective_id=0, has_side_effects=True, vmem_limit_bytes=67043328),
    )(x_loc, g_loc, w_one, w_two)


def weight_grad_kernel(h_ref, d_ref, a_ref, g_ref, y_ref, x_ref, up_ref, down_ref, y_out, x_out, *, n_up):
    contract = (((0,), (0,)), ((), ()))

    @pl.when(pl.program_id(0) == 0)
    def _():
        y_out[...] = y_ref[...]
        x_out[...] = x_ref[...]

    @pl.when(pl.program_id(0) < n_up)
    def _():
        up_ref[...] = lax.dot_general(h_ref[...], d_ref[...], contract, preferred_element_type=F32)

    @pl.when(pl.program_id(0) >= n_up)
    def _():
        down_ref[...] = lax.dot_general(a_ref[...], g_ref[...], contract, preferred_element_type=F32)


def weight_grads(h, d, a, g, y, dx):
    tokens, d_model = h.shape
    d_ff = d.shape[1]
    up_rows, down_rows = 256, 512
    n_up, n_down = d_model // up_rows, d_ff // down_rows
    up_idx = lambda i: jnp.minimum(i, n_up - 1)
    down_idx = lambda i: jnp.maximum(i - n_up, 0)
    whole = pl.BlockSpec(y.shape, lambda i: (0, 0, 0))
    return pl.pallas_call(
        functools.partial(weight_grad_kernel, n_up=n_up),
        name='weight_grads',
        grid=(n_up + n_down,),
        out_shape=(jax.ShapeDtypeStruct((d_model, d_ff), F32), jax.ShapeDtypeStruct((d_ff, d_model), F32),
                   jax.ShapeDtypeStruct(y.shape, BF16), jax.ShapeDtypeStruct(y.shape, BF16)),
        in_specs=[pl.BlockSpec((tokens, up_rows), lambda i: (0, up_idx(i))),
                  pl.BlockSpec((tokens, d_ff), lambda i: (0, 0)),
                  pl.BlockSpec((tokens, down_rows), lambda i: (0, down_idx(i))),
                  pl.BlockSpec((tokens, d_model), lambda i: (0, 0)), whole, whole],
        out_specs=(pl.BlockSpec((up_rows, d_ff), lambda i: (up_idx(i), 0)),
                   pl.BlockSpec((down_rows, d_model), lambda i: (down_idx(i), 0)), whole, whole),
        compiler_params=pltpu.CompilerParams(vmem_limit_bytes=60 * 1024 * 1024),
    )(h, d, a, g, y, dx)


def solution(mesh):
    tok_spec = P(('data', 'stage', 'inner'))
    up_spec = P(None, ('data', 'stage'), None, 'inner')
    down_spec = P(None, ('data', 'stage'), 'inner', None)

    def device_step(x_loc, g_loc, w_up, w_down):
        y, dx, h, g, a, d = run_pipeline(x_loc, g_loc, w_up[0, 0], w_down[0, 0])
        flat = lambda v: v.reshape(-1, v.shape[-1])
        dw_up, dw_down, y, dx = weight_grads(flat(h), flat(d), flat(a), flat(g), y, dx)
        return y, dx, dw_up[None, None], dw_down[None, None]

    return jax.shard_map(device_step, mesh=mesh, in_specs=(tok_spec, tok_spec, up_spec, down_spec), out_specs=(tok_spec, tok_spec, up_spec, down_spec), check_vma=False)
```

```python
import functools

import jax
import jax.numpy as jnp
from jax import lax
from jax.experimental import pallas as pl
from jax.experimental.pallas import tpu as pltpu
from jax.sharding import PartitionSpec as P

F32 = jnp.float32
BF16 = jnp.bfloat16
MESH = pl.DeviceIdType.MESH

STAGES = 4
INNER = 2
UNITS = 8
SLOTS = 4
BLK = 512
TILE = 256
FWD, BWD = 0, 1
NT = (((1,), (1,)), ((), ()))

F1, F2, FR, B1, B2, BR, T1, T2, SW, PR, YL, WA, WB, XS = range(1, 15)
PLAN = (
    ((WA, 0, 1), (F1, 0, 1), (WB, 0, 1), (XS, 0, 1), (F1, 1, 2), (F2, 0, 1), (F2, 1, 1), (FR, 0, 1),
     (F2, 2, 1), (FR, 1, 1), (F1, 3, 2), (FR, 2, 1), (F2, 3, 1), (FR, 3, 1), (F1, 5, 1), (F2, 4, 2),
     (F1, 6, 2), (FR, 4, 2), (F2, 6, 1), (F2, 7, 1), (FR, 6, 2), (SW, 0, 1), (B1, 0, 2), (B2, 0, 1),
     (B2, 1, 1), (BR, 0, 1), (B1, 2, 2), (B2, 2, 2), (BR, 1, 3), (B1, 4, 2), (B2, 4, 2), (B1, 6, 2),
     (B2, 6, 2), (BR, 4, 4)),
    ((WA, 0, 1), (WB, 0, 1), (F1, 0, 1), (F2, 0, 1), (F1, 1, 2), (F2, 1, 2), (FR, 0, 3), (F1, 3, 1),
     (F2, 3, 1), (FR, 3, 1), (F1, 4, 2), (F2, 4, 1), (F2, 5, 1), (F1, 6, 2), (FR, 4, 2), (F2, 6, 1),
     (F2, 7, 1), (FR, 6, 2), (SW, 0, 1), (B1, 0, 2), (B2, 0, 2), (BR, 0, 2), (B1, 2, 2), (B2, 2, 1),
     (B2, 3, 1), (BR, 2, 2), (B1, 4, 1), (B2, 4, 1), (B1, 5, 1), (B2, 5, 1), (B1, 6, 1), (B1, 7, 1),
     (BR, 4, 1), (B2, 6, 1), (BR, 5, 1), (B2, 7, 1), (BR, 6, 2)),
    ((WA, 0, 1), (WB, 0, 1), (XS, 0, 1), (F1, 0, 1), (F2, 0, 1), (F1, 1, 2), (FR, 0, 1), (F2, 1, 1),
     (F2, 2, 1), (FR, 1, 1), (F1, 3, 1), (FR, 2, 1), (F2, 3, 1), (FR, 3, 1), (F1, 4, 2), (F2, 4, 2),
     (F1, 6, 2), (F2, 6, 1), (T1, 0, 2), (FR, 4, 2), (T2, 0, 2), (F2, 7, 1), (BR, 0, 2), (FR, 6, 2),
     (T1, 2, 2), (T2, 2, 2), (T1, 4, 2), (BR, 2, 2), (T2, 4, 2), (T1, 6, 2), (BR, 4, 1), (T2, 6, 2),
     (BR, 5, 3)),
    ((WB, 0, 1), (XS, 0, 1), (PR, 0, 1), (F1, 0, 1), (B2, 0, 1), (F1, 1, 1), (BR, 0, 1), (B2, 1, 1),
     (BR, 1, 1), (F1, 2, 1), (B2, 2, 1), (F1, 3, 1), (B2, 3, 1), (F1, 4, 2), (BR, 2, 2), (B2, 4, 1),
     (B2, 5, 1), (BR, 4, 2), (F1, 6, 2), (B2, 6, 1), (B2, 7, 1), (BR, 6, 2), (YL, 0, 1), (F2, 0, 1),
     (F2, 1, 1), (FR, 0, 2), (F2, 2, 2), (FR, 2, 2), (F2, 4, 2), (FR, 4, 2), (F2, 6, 2), (FR, 6, 2)),
)


PACK = 1024
UP_GROUP = 8
DOWN_GROUP = 2


def plan_words():
    rows = [[op + 16 * unit + 128 * (count - 1) for op, unit, count in row] for row in PLAN]
    steps = -(-max(len(row) for row in rows) // 3) * 3
    rows = [row + [0] * (steps - len(row)) for row in rows]
    return steps, [[row[t] + PACK * row[t + 1] + PACK * PACK * row[t + 2] for t in range(0, steps, 3)] for row in rows]


def gelu_pair(pre_act):
    normal_cdf = 0.5 * (1.0 + lax.erf(pre_act * 0.7071067811865476))
    normal_pdf = jnp.exp(-0.5 * pre_act * pre_act) * 0.3989422804014327
    return pre_act * normal_cdf, normal_cdf + pre_act * normal_pdf


def wait_bytes(ref, sem):
    pltpu.make_async_copy(ref, ref, sem).wait()


def pipeline_kernel(x_ref, g_ref, w1_ref, w2_ref,
                    y_out, dx_out, h_out, g_out, a_out, d_out,
                    wa, wb, flow, act, slope, part, recv, send, home,
                    flow_sem, recv_sem, part_send, flow_send, home_send, home_sem, in_send, w_sem, out_sem):
    stage = lax.axis_index('stage')
    side = lax.axis_index('inner')
    other = 1 - side
    rows, d_model = flow.shape[3:]
    tok, d_ff = act.shape[2:]
    n_blk = d_model // BLK

    def peer(s, i):
        return {'stage': s, 'inner': i}

    load_a = pltpu.make_async_copy(w1_ref, wa, w_sem.at[0])
    load_b = pltpu.make_async_copy(w2_ref, wb, w_sem.at[1])

    @pl.when(stage < STAGES - 1)
    def _():
        load_a.start()
    load_b.start()

    @pl.when(stage == STAGES - 1)
    def _():
        load_a.start()

    barrier = pltpu.get_barrier_semaphore()
    for s in range(STAGES):
        for i in range(INNER):
            @pl.when(jnp.logical_or(stage != s, side != i))
            def _():
                pl.semaphore_signal(barrier, inc=1, device_id=peer(s, i), device_id_type=MESH)
    pl.semaphore_wait(barrier, STAGES * INNER - 1)

    def unit_of(k):
        return lax.rem(2 * stage + k + UNITS - 1, UNITS)

    def home_of(u):
        return lax.rem((u + 1) // 2, STAGES)

    def slot_of(u):
        return lax.rem(u + 1, 2)

    def hand_in(kind, src, target, k, lane):
        u = unit_of(k)
        if lane == 0:
            @pl.when(stage == target)
            def _():
                pltpu.make_async_copy(src.at[k], flow.at[kind, u, side], flow_sem.at[kind, u, side]).start()

            @pl.when(stage != target)
            def _():
                pltpu.make_async_remote_copy(src.at[k], flow.at[kind, u, side], in_send.at[kind, k, 0], flow_sem.at[kind, u, side],
                                             device_id=peer(target, side), device_id_type=MESH).start()
        else:
            pltpu.make_async_remote_copy(src.at[k], flow.at[kind, u, side], in_send.at[kind, k, 1], flow_sem.at[kind, u, side],
                                         device_id=peer(target, other), device_id_type=MESH).start()

    for k in range(2):
        hand_in(FWD, x_ref, 0, k, 0)

        @pl.when(jnp.logical_or(stage == 1, jnp.logical_and(stage == 0, k == 1)))
        def _():
            hand_in(FWD, x_ref, 0, k, 1)
    for k in range(2):
        for lane in range(2):
            hand_in(BWD, g_ref, STAGES - 1, k, lane)

    steps, plan = plan_words()
    words = [jnp.where(stage == 0, a, jnp.where(stage == 1, b, jnp.where(stage == 2, c, d))) for a, b, c, d in zip(*plan)]

    def keep(ref, out, u, lane):
        pltpu.make_async_copy(ref, out.at[u], out_sem.at[lane]).start()

    def blocks(width, group, fn):
        def body(t, carry):
            fn([pl.ds(pl.multiple_of((t * group + k) * BLK, BLK), BLK) for k in range(group)])
            return carry
        lax.fori_loop(0, width // BLK // group, body, 0)

    def arrived(kind, u):
        for half in range(INNER):
            wait_bytes(flow.at[kind, u, half], flow_sem.at[kind, u, half])

    def both_arrived(kind, u, v):
        arrived(kind, u)

        @pl.when(v != u)
        def _():
            arrived(kind, v)

    def pair(ref, kind, u, v):
        width = ref.shape[-1]
        return jnp.concatenate([ref[kind, u].reshape(tok, width), ref[kind, v].reshape(tok, width)], axis=0)

    def kept(u, v, fn):
        fn(u)

        @pl.when(v != u)
        def _():
            fn(v)

    def up_product(u, v):
        both_arrived(FWD, u, v)

        def fn(slices):
            lhs = pair(flow, FWD, u, v)
            for sl in slices:
                z = jnp.dot(lhs, wa[:, sl], preferred_element_type=F32)
                value, grad = gelu_pair(z)
                value = value.astype(BF16)
                first, second = slope[u, :, sl], slope[v, :, sl]
                act[BWD, u, :, sl] = (first * grad[:tok]).astype(BF16)
                act[BWD, v, :, sl] = (second * grad[tok:]).astype(BF16)
                slope[u, :, sl] = grad[:tok]
                slope[v, :, sl] = grad[tok:]
                act[FWD, u, :, sl] = value[:tok]
                act[FWD, v, :, sl] = value[tok:]
        blocks(d_ff, UP_GROUP, fn)

        def out(w):
            keep(flow.at[FWD, w], h_out, w, 0)
            keep(act.at[FWD, w], a_out, w, 2)

            @pl.when(stage == STAGES - 1)
            def _():
                keep(act.at[BWD, w], d_out, w, 3)
        kept(u, v, out)

    def back_product(u, v, swapped):
        both_arrived(BWD, u, v)

        def fn(slices):
            lhs = pair(flow, BWD, u, v)
            for sl in slices:
                if swapped:
                    e = jnp.dot(lhs, wa[:, sl], preferred_element_type=F32)
                else:
                    e = lax.dot_general(lhs, wb[sl, :], NT, preferred_element_type=F32)
                act[BWD, u, :, sl] = (e[:tok] * slope[u, :, sl]).astype(BF16)
                act[BWD, v, :, sl] = (e[tok:] * slope[v, :, sl]).astype(BF16)
        blocks(d_ff, UP_GROUP, fn)

        def out(w):
            keep(flow.at[BWD, w], g_out, w, 1)
            keep(act.at[BWD, w], d_out, w, 3)
        kept(u, v, out)

    def part_copy(kind, u, j):
        slot = lax.rem(u, SLOTS)
        return pltpu.make_async_remote_copy(part.at[kind, slot, j, other], recv.at[kind, u, j], part_send.at[kind, slot, j],
                                            recv_sem.at[kind, u, j], device_id=peer(stage, other), device_id_type=MESH)

    def down_product(kind, u, v, straight):
        def free(w):
            @pl.when(w >= SLOTS)
            def _():
                for j in range(n_blk):
                    part_copy(kind, w - SLOTS, j).wait_send()
        kept(u, v, free)

        def body(t, carry):
            lhs = pair(act, kind, u, v)
            for k in range(DOWN_GROUP):
                j = t * DOWN_GROUP + k
                sl = pl.ds(pl.multiple_of(j * BLK, BLK), BLK)
                if straight:
                    p = jnp.dot(lhs, wb[:, sl], preferred_element_type=F32)
                else:
                    p = lax.dot_general(lhs, wa[sl, :], NT, preferred_element_type=F32)
                p = p.reshape(2, INNER, rows, BLK)
                part[kind, lax.rem(u, SLOTS), j] = p[0]
                part[kind, lax.rem(v, SLOTS), j] = p[1]

            def go(w):
                for k in range(DOWN_GROUP):
                    part_copy(kind, w, t * DOWN_GROUP + k).start()
            kept(u, v, go)
            return carry
        lax.fori_loop(0, n_blk // DOWN_GROUP, body, 0)

    def hand_on(kind, first, count):
        target = stage + 1 if kind == FWD else stage - 1
        inside = stage < STAGES - 1 if kind == FWD else stage > 0
        out = STAGES - 1 if kind == FWD else 0

        def body(i, carry):
            u = first + i
            slot = lax.rem(u, SLOTS)
            for j in range(n_blk):
                sl = pl.ds(j * BLK, BLK)
                wait_bytes(recv.at[kind, u, j], recv_sem.at[kind, u, j])
                total = flow[kind, u, side, :, sl].astype(F32) + (part[kind, slot, j, side] + recv[kind, u, j])
                send[kind, u, :, sl] = total.astype(BF16)

                @pl.when(inside)
                def _():
                    for half in (side, other):
                        pltpu.make_async_remote_copy(send.at[kind, u, :, sl], flow.at[kind, u, side, :, sl], flow_send.at[kind],
                                                     flow_sem.at[kind, u, side], device_id=peer(target, half), device_id_type=MESH).start()

            @pl.when(jnp.logical_and(jnp.logical_not(inside), home_of(u) != out))
            def _():
                pltpu.make_async_remote_copy(send.at[kind, u], home.at[kind, slot_of(u)], home_send.at[kind, u],
                                             home_sem.at[kind, slot_of(u)], device_id=peer(home_of(u), side), device_id_type=MESH).start()
            return carry
        lax.fori_loop(0, count, body, 0)

    def swap_weights():
        n_i = d_model // TILE

        def body(t, carry):
            i = pl.multiple_of(lax.rem(t, n_i) * TILE, TILE)
            j = pl.multiple_of(lax.div(t, n_i) * TILE, TILE)
            up = wa[pl.ds(i, TILE), pl.ds(j, TILE)]
            down = wb[pl.ds(j, TILE), pl.ds(i, TILE)]
            wa[pl.ds(i, TILE), pl.ds(j, TILE)] = down.T
            wb[pl.ds(j, TILE), pl.ds(i, TILE)] = up.T
            return carry
        lax.fori_loop(0, n_i * (d_ff // TILE), body, 0)

    def prepare_last():
        half = UNITS // 2

        def quarter(q, carry):
            for i in range(half):
                arrived(BWD, q * half + i)
                keep(flow.at[BWD, q * half + i], g_out, q * half + i, 1)
            units = pl.ds(q * half, half)

            def fn(slices):
                lhs = flow[BWD, units].reshape(half * tok, d_model)
                for sl in slices:
                    e = lax.dot_general(lhs, wb[sl, :], NT, preferred_element_type=F32)
                    slope[units, :, sl] = e.reshape(half, tok, BLK)
            blocks(d_ff, 1, fn)
            return carry
        lax.fori_loop(0, 2, quarter, 0)
        load_a.wait()
        n_i = d_model // TILE

        def body(t, carry):
            i = pl.multiple_of(lax.rem(t, n_i) * TILE, TILE)
            j = pl.multiple_of(lax.div(t, n_i) * TILE, TILE)
            wb[pl.ds(j, TILE), pl.ds(i, TILE)] = wa[pl.ds(i, TILE), pl.ds(j, TILE)].T
            return carry
        lax.fori_loop(0, n_i * (d_ff // TILE), body, 0)

    def step(t, carry):
        group, place = lax.div(t, 3), lax.rem(t, 3)
        word = words[0]
        for i, w in enumerate(words[1:], 1):
            word = jnp.where(group == i, w, word)
        code = lax.rem(lax.div(word, jnp.where(place == 0, 1, jnp.where(place == 1, PACK, PACK * PACK))), PACK)
        op = lax.rem(code, 16)
        u = lax.rem(lax.div(code, 16), UNITS)
        count = lax.div(code, 128) + 1

        def on(want):
            return pl.when(op == want)

        v = jnp.minimum(u + count - 1, UNITS - 1)

        @on(F1)
        def _():
            up_product(u, v)

        @pl.when(jnp.logical_or(op == F2, op == B2))
        def _():
            down_product(jnp.where(op == F2, FWD, BWD), u, v, True)

        @on(FR)
        def _():
            hand_on(FWD, u, count)

        @on(BR)
        def _():
            hand_on(BWD, u, count)

        @on(B1)
        def _():
            back_product(u, v, True)

        @on(T1)
        def _():
            back_product(u, v, False)

        @on(T2)
        def _():
            down_product(BWD, u, v, False)

        @on(SW)
        def _():
            swap_weights()

        @on(PR)
        def _():
            prepare_last()

        @on(YL)
        def _():
            load_b.start()
            load_b.wait()

        @on(WA)
        def _():
            load_a.wait()

        @on(WB)
        def _():
            load_b.wait()

        @on(XS)
        def _():
            for k in range(2):
                @pl.when(jnp.logical_or(stage > 1, k == 0))
                def _():
                    hand_in(FWD, x_ref, 0, k, 1)
        return carry
    lax.fori_loop(0, steps, step, 0)

    for kind, here, out in ((FWD, STAGES - 1, y_out), (BWD, 0, dx_out)):
        for k in range(2):
            @pl.when(stage == here)
            def _():
                pltpu.make_async_copy(send.at[kind, unit_of(k)], out.at[k], out_sem.at[4 + kind]).start()

            @pl.when(stage != here)
            def _():
                wait_bytes(home.at[kind, k], home_sem.at[kind, k])
                pltpu.make_async_copy(home.at[kind, k], out.at[k], out_sem.at[4 + kind]).start()

    for kind in (FWD, BWD):
        for u in range(UNITS - SLOTS, UNITS):
            for j in range(n_blk):
                part_copy(kind, u, j).wait_send()
    for kind, target, src in ((FWD, 0, x_ref), (BWD, STAGES - 1, g_ref)):
        last = STAGES - 1 - target
        for k in range(2):
            @pl.when(stage != target)
            def _():
                wait_bytes(src.at[k], in_send.at[kind, k, 0])
            wait_bytes(src.at[k], in_send.at[kind, k, 1])

        @pl.when(stage != last)
        def _():
            wait_bytes(flow.at[kind], flow_send.at[kind])

        @pl.when(stage == last)
        def _():
            for u in range(UNITS):
                if (u + 1) // 2 % STAGES != last:
                    wait_bytes(send.at[kind, u], home_send.at[kind, u])
    for lane, (ref, out) in enumerate(((flow.at[FWD], h_out), (flow.at[BWD], g_out), (act.at[FWD], a_out), (act.at[BWD], d_out),
                                       (home.at[FWD], y_out), (home.at[BWD], dx_out))):
        pltpu.make_async_copy(ref, out, out_sem.at[lane]).wait()


def run_pipeline(x_loc, g_loc, w_one, w_two):
    rows, d_model = x_loc.shape[1:]
    d_ff = w_one.shape[1]
    n_blk = d_model // BLK
    tok = INNER * rows
    hbm = pl.BlockSpec(memory_space=pl.ANY)
    out = lambda *shape: jax.ShapeDtypeStruct(shape, BF16)
    dma = lambda *shape: pltpu.SemaphoreType.DMA(shape)
    return pl.pallas_call(
        pipeline_kernel,
        name='pipeline',
        out_shape=(out(*x_loc.shape), out(*x_loc.shape), out(UNITS, INNER, rows, d_model), out(UNITS, INNER, rows, d_model),
                   out(UNITS, tok, d_ff), out(UNITS, tok, d_ff)),
        in_specs=[hbm] * 4,
        out_specs=(hbm,) * 6,
        scratch_shapes=[
            pltpu.VMEM((d_model, d_ff), BF16),
            pltpu.VMEM((d_ff, d_model), BF16),
            pltpu.VMEM((2, UNITS, INNER, rows, d_model), BF16),
            pltpu.VMEM((2, UNITS, tok, d_ff), BF16),
            pltpu.VMEM((UNITS, tok, d_ff), F32),
            pltpu.VMEM((2, SLOTS, n_blk, INNER, rows, BLK), F32),
            pltpu.VMEM((2, UNITS, n_blk, rows, BLK), F32),
            pltpu.VMEM((2, UNITS, rows, d_model), BF16),
            pltpu.VMEM((2, 2, rows, d_model), BF16),
            dma(2, UNITS, INNER), dma(2, UNITS, n_blk), dma(2, SLOTS, n_blk), dma(2), dma(2, UNITS), dma(2, 2), dma(2, 2, 2), dma(2), dma(6),
        ],
        compiler_params=pltpu.CompilerParams(collective_id=0, has_side_effects=True, vmem_limit_bytes=67043328),
    )(x_loc, g_loc, w_one, w_two)


GRAD_ROWS, GRAD_COLS = 1024, 2048


def weight_grad_kernel(h_ref, d_ref, a_ref, g_ref, y_ref, x_ref, up_ref, down_ref, y_out, x_out,
                       h, d, a, g, home, stage, in_sem, home_sem, out_sem):
    tokens, d_model = h.shape
    d_ff = d.shape[1]
    n_down, n_up = d_ff // GRAD_ROWS, d_model // GRAD_ROWS
    n_col = d_ff // GRAD_COLS

    loads = [(g_ref, g)] + [(a_ref.at[:, pl.ds(t * GRAD_ROWS, GRAD_ROWS)], a.at[:, pl.ds(t * GRAD_ROWS, GRAD_ROWS)]) for t in range(n_down)] + [(h_ref, h), (d_ref, d)]
    loads = [pltpu.make_async_copy(src, dst, in_sem.at[t]) for t, (src, dst) in enumerate(loads)]
    homes = [pltpu.make_async_copy(src, home.at[t], home_sem.at[t]) for t, src in enumerate((y_ref, x_ref))]
    for copy in loads + homes:
        copy.start()
    loads[0].wait()

    def block(t, src, first, other, second, out, pieces=1):
        slot = lax.rem(t, 2)
        size = GRAD_ROWS // pieces
        for p in range(pieces):
            rows = pl.ds(pl.multiple_of(first + p * size, size), size)
            cols = pl.ds(pl.multiple_of(second, GRAD_COLS), GRAD_COLS)
            stage[slot, pl.ds(p * size, size)] = lax.dot_general(src[:, rows], other[:, cols], (((0,), (0,)), ((), ())), preferred_element_type=F32)
            pltpu.make_async_copy(stage.at[slot, pl.ds(p * size, size)], out.at[rows, cols], out_sem.at[slot]).start()

    def freed(slot):
        pltpu.make_async_copy(stage.at[slot], stage.at[slot], out_sem.at[slot]).wait()

    def down(t, carry):
        pltpu.make_async_copy(a_ref.at[:, pl.ds(0, GRAD_ROWS)], a.at[:, pl.ds(0, GRAD_ROWS)], in_sem.at[1 + t]).wait()

        @pl.when(t >= 2)
        def _():
            freed(lax.rem(t, 2))
        block(t, a, t * GRAD_ROWS, g, 0, down_ref)
        return carry
    lax.fori_loop(0, n_down, down, 0)
    loads[1 + n_down].wait()
    loads[2 + n_down].wait()
    for copy, (src, dst) in zip(homes, ((home.at[0], y_out), (home.at[1], x_out))):
        copy.wait()
    backs = [pltpu.make_async_copy(home.at[t], dst, home_sem.at[t]) for t, dst in enumerate((y_out, x_out))]
    for copy in backs:
        copy.start()

    def up(t, carry):
        freed(lax.rem(t, 2))
        block(t, h, lax.div(t, n_col) * GRAD_ROWS, d, lax.rem(t, n_col) * GRAD_COLS, up_ref)
        return carry
    n_blocks = n_up * n_col
    lax.fori_loop(0, n_blocks - 1, up, 0)
    freed((n_blocks - 1) % 2)
    block(n_blocks - 1, h, (n_up - 1) * GRAD_ROWS, d, (n_col - 1) * GRAD_COLS, up_ref, 4)
    for slot in range(2):
        freed(slot)
    for copy in backs:
        copy.wait()


def weight_grads(h, d, a, g, y, dx):
    tokens, d_model = h.shape
    d_ff = d.shape[1]
    n_in = 3 + d_ff // GRAD_ROWS
    hbm = pl.BlockSpec(memory_space=pl.ANY)
    dma = lambda *shape: pltpu.SemaphoreType.DMA(shape)
    like = lambda v: pltpu.VMEM(v.shape, v.dtype)
    return pl.pallas_call(
        weight_grad_kernel,
        name='weight_grads',
        out_shape=(jax.ShapeDtypeStruct((d_model, d_ff), F32), jax.ShapeDtypeStruct((d_ff, d_model), F32),
                   jax.ShapeDtypeStruct(y.shape, BF16), jax.ShapeDtypeStruct(y.shape, BF16)),
        in_specs=[hbm] * 6,
        out_specs=(hbm,) * 4,
        scratch_shapes=[like(h), like(d), like(a), like(g), pltpu.VMEM((2,) + y.shape, BF16), pltpu.VMEM((2, GRAD_ROWS, GRAD_COLS), F32),
                        dma(n_in), dma(2), dma(2)],
        compiler_params=pltpu.CompilerParams(vmem_limit_bytes=60 * 1024 * 1024),
    )(h, d, a, g, y, dx)


def solution(mesh):
    tok_spec = P(('data', 'stage', 'inner'))
    up_spec = P(None, ('data', 'stage'), None, 'inner')
    down_spec = P(None, ('data', 'stage'), 'inner', None)

    def device_step(x_loc, g_loc, w_up, w_down):
        y, dx, h, g, a, d = run_pipeline(x_loc, g_loc, w_up[0, 0], w_down[0, 0])
        flat = lambda v: v.reshape(-1, v.shape[-1])
        dw_up, dw_down, y, dx = weight_grads(flat(h), flat(d), flat(a), flat(g), y, dx)
        return y, dx, dw_up[None, None], dw_down[None, None]

    return jax.shard_map(device_step, mesh=mesh, in_specs=(tok_spec, tok_spec, up_spec, down_spec), out_specs=(tok_spec, tok_spec, up_spec, down_spec), check_vma=False)
```

```python
import functools

import jax
import jax.numpy as jnp
from jax import lax
from jax.experimental import pallas as pl
from jax.experimental.pallas import tpu as pltpu
from jax.sharding import PartitionSpec as P

F32 = jnp.float32
BF16 = jnp.bfloat16
MESH = pl.DeviceIdType.MESH

STAGES = 4
INNER = 2
UNITS = 8
SLOTS = 4
BLK = 512
TILE = 256
FWD, BWD = 0, 1
NT = (((1,), (1,)), ((), ()))

F1, F2, FR, B1, B2, BR, T1, T2, SW, PR, YL, WA, WB, XS, M1 = range(1, 16)
PLAN = (
    ((WA, 0, 1), (F1, 0, 1), (WB, 0, 1), (XS, 0, 1), (F1, 1, 2), (F2, 0, 1), (F2, 1, 1), (FR, 0, 1),
     (F2, 2, 1), (FR, 1, 1), (F1, 3, 2), (FR, 2, 1), (F2, 3, 1), (FR, 3, 1), (F1, 5, 1), (F2, 4, 2),
     (F1, 6, 2), (FR, 4, 2), (F2, 6, 1), (F2, 7, 1), (FR, 6, 2), (SW, 0, 1), (B1, 0, 2), (B2, 0, 1),
     (B2, 1, 1), (BR, 0, 1), (B1, 2, 2), (B2, 2, 2), (BR, 1, 3), (B1, 4, 2), (B2, 4, 2), (B1, 6, 2),
     (B2, 6, 2), (BR, 4, 4)),
    ((WA, 0, 1), (WB, 0, 1), (F1, 0, 1), (F2, 0, 1), (F1, 1, 2), (F2, 1, 2), (FR, 0, 3), (F1, 3, 1),
     (F2, 3, 1), (FR, 3, 1), (F1, 4, 2), (F2, 4, 1), (F2, 5, 1), (F1, 6, 2), (FR, 4, 2), (F2, 6, 1),
     (F2, 7, 1), (FR, 6, 2), (SW, 0, 1), (B1, 0, 2), (B2, 0, 2), (BR, 0, 2), (B1, 2, 2), (B2, 2, 1),
     (B2, 3, 1), (BR, 2, 2), (B1, 4, 1), (B2, 4, 1), (B1, 5, 1), (B2, 5, 1), (B1, 6, 1), (B1, 7, 1),
     (BR, 4, 1), (B2, 6, 1), (BR, 5, 1), (B2, 7, 1), (BR, 6, 2)),
    ((WA, 0, 1), (WB, 0, 1), (XS, 0, 1), (F1, 0, 1), (F2, 0, 1), (F1, 1, 2), (FR, 0, 1), (F2, 1, 1),
     (F2, 2, 1), (FR, 1, 1), (F1, 3, 1), (FR, 2, 1), (F2, 3, 1), (FR, 3, 1), (F1, 4, 2), (F2, 4, 2),
     (F1, 6, 2), (F2, 6, 1), (T1, 0, 2), (FR, 4, 2), (T2, 0, 2), (F2, 7, 1), (BR, 0, 2), (FR, 6, 2),
     (T1, 2, 2), (T2, 2, 2), (T1, 4, 2), (BR, 2, 2), (T2, 4, 2), (T1, 6, 2), (BR, 4, 1), (T2, 6, 2),
     (BR, 5, 3)),
    ((WB, 0, 1), (XS, 0, 1), (PR, 0, 1), (M1, 0, 1), (B2, 0, 1), (M1, 1, 1), (BR, 0, 1), (B2, 1, 1),
     (BR, 1, 1), (M1, 2, 1), (B2, 2, 1), (M1, 3, 1), (B2, 3, 1), (M1, 4, 2), (BR, 2, 2), (B2, 4, 1),
     (B2, 5, 1), (BR, 4, 2), (M1, 6, 2), (B2, 6, 1), (B2, 7, 1), (BR, 6, 2), (YL, 0, 1), (F2, 0, 1),
     (F2, 1, 1), (FR, 0, 2), (F2, 2, 2), (FR, 2, 2), (F2, 4, 2), (FR, 4, 2), (F2, 6, 2), (FR, 6, 2)),
)


PACK = 1024
UP_GROUP = 8
TURN = 6
TURN_GROUP = 4
DOWN_GROUP = 2


def plan_words():
    rows = [[op + 16 * unit + 128 * (count - 1) for op, unit, count in row] for row in PLAN]
    steps = -(-max(len(row) for row in rows) // 3) * 3
    rows = [row + [0] * (steps - len(row)) for row in rows]
    return steps, [[row[t] + PACK * row[t + 1] + PACK * PACK * row[t + 2] for t in range(0, steps, 3)] for row in rows]


def gelu_pair(pre_act):
    root = pre_act * 0.7071067811865476
    normal_cdf = 0.5 * (1.0 + lax.erf(root))
    normal_pdf = jnp.exp2(root * root * -1.4426950408889634) * 0.3989422804014327
    return pre_act * normal_cdf, normal_cdf + pre_act * normal_pdf


def wait_bytes(ref, sem):
    pltpu.make_async_copy(ref, ref, sem).wait()


def pipeline_kernel(x_ref, g_ref, w1_ref, w2_ref,
                    y_out, dx_out, h_out, g_out, a_out, d_out,
                    wa, wb, flow, act, slope, part, recv, send, home,
                    flow_sem, recv_sem, part_send, flow_send, home_send, home_sem, in_send, w_sem, out_sem):
    stage = lax.axis_index('stage')
    side = lax.axis_index('inner')
    other = 1 - side
    rows, d_model = flow.shape[3:]
    tok, d_ff = act.shape[2:]
    n_blk = d_model // BLK

    def peer(s, i):
        return {'stage': s, 'inner': i}

    load_a = pltpu.make_async_copy(w1_ref, wa, w_sem.at[0])
    load_b = pltpu.make_async_copy(w2_ref, wb, w_sem.at[1])

    @pl.when(stage < STAGES - 1)
    def _():
        load_a.start()
    load_b.start()

    @pl.when(stage == STAGES - 1)
    def _():
        load_a.start()

    barrier = pltpu.get_barrier_semaphore()
    for s in range(STAGES):
        for i in range(INNER):
            @pl.when(jnp.logical_or(stage != s, side != i))
            def _():
                pl.semaphore_signal(barrier, inc=1, device_id=peer(s, i), device_id_type=MESH)
    pl.semaphore_wait(barrier, STAGES * INNER - 1)

    def unit_of(k):
        return lax.rem(2 * stage + k + UNITS - 1, UNITS)

    def home_of(u):
        return lax.rem((u + 1) // 2, STAGES)

    def slot_of(u):
        return lax.rem(u + 1, 2)

    def hand_in(kind, src, target, k, lane):
        u = unit_of(k)
        if lane == 0:
            @pl.when(stage == target)
            def _():
                pltpu.make_async_copy(src.at[k], flow.at[kind, u, side], flow_sem.at[kind, u, side]).start()

            @pl.when(stage != target)
            def _():
                pltpu.make_async_remote_copy(src.at[k], flow.at[kind, u, side], in_send.at[kind, k, 0], flow_sem.at[kind, u, side],
                                             device_id=peer(target, side), device_id_type=MESH).start()
        else:
            pltpu.make_async_remote_copy(src.at[k], flow.at[kind, u, side], in_send.at[kind, k, 1], flow_sem.at[kind, u, side],
                                         device_id=peer(target, other), device_id_type=MESH).start()

    for k in range(2):
        hand_in(FWD, x_ref, 0, k, 0)

        @pl.when(jnp.logical_or(stage == 1, jnp.logical_and(stage == 0, k == 1)))
        def _():
            hand_in(FWD, x_ref, 0, k, 1)
    for k in range(2):
        for lane in range(2):
            hand_in(BWD, g_ref, STAGES - 1, k, lane)

    steps, plan = plan_words()
    words = [jnp.where(stage == 0, a, jnp.where(stage == 1, b, jnp.where(stage == 2, c, d))) for a, b, c, d in zip(*plan)]

    def keep(ref, out, u, lane):
        pltpu.make_async_copy(ref, out.at[u], out_sem.at[lane]).start()

    def blocks(width, group, fn):
        def body(t, carry):
            fn([pl.ds(pl.multiple_of((t * group + k) * BLK, BLK), BLK) for k in range(group)])
            return carry
        lax.fori_loop(0, width // BLK // group, body, 0)

    def arrived(kind, u):
        for half in range(INNER):
            wait_bytes(flow.at[kind, u, half], flow_sem.at[kind, u, half])

    def both_arrived(kind, u, v):
        arrived(kind, u)

        @pl.when(v != u)
        def _():
            arrived(kind, v)

    def pair(ref, kind, u, v):
        width = ref.shape[-1]
        return jnp.concatenate([ref[kind, u].reshape(tok, width), ref[kind, v].reshape(tok, width)], axis=0)

    def kept(u, v, fn):
        fn(u)

        @pl.when(v != u)
        def _():
            fn(v)

    def up_product(u, v, last):
        both_arrived(FWD, u, v)

        def fn(slices):
            lhs = pair(flow, FWD, u, v)
            for sl in slices:
                z = jnp.dot(lhs, wa[:, sl], preferred_element_type=F32)
                value, grad = gelu_pair(z)
                value = value.astype(BF16)
                if last:
                    act[BWD, u, :, sl] = (slope[u, :, sl] * grad[:tok]).astype(BF16)
                    act[BWD, v, :, sl] = (slope[v, :, sl] * grad[tok:]).astype(BF16)
                else:
                    slope[u, :, sl] = grad[:tok]
                    slope[v, :, sl] = grad[tok:]
                act[FWD, u, :, sl] = value[:tok]
                act[FWD, v, :, sl] = value[tok:]
        blocks(d_ff, UP_GROUP, fn)

        def out(w):
            keep(flow.at[FWD, w], h_out, w, 0)
            keep(act.at[FWD, w], a_out, w, 2)
            if last:
                keep(act.at[BWD, w], d_out, w, 3)
        kept(u, v, out)

    def across(lhs, ref, sl):
        cut = ref.shape[1] * TURN // 8
        total = lax.dot_general(lhs[:, :cut], ref[sl, :cut], NT, preferred_element_type=F32)
        for k in range(cut, ref.shape[1], TILE):
            turned = [ref[pl.ds(sl.start + q, TILE), k:k + TILE].T for q in range(0, BLK, TILE)]
            total += jnp.dot(lhs[:, k:k + TILE], jnp.concatenate(turned, axis=1), preferred_element_type=F32)
        return total

    def back_product(u, v, swapped):
        both_arrived(BWD, u, v)

        def fn(slices):
            lhs = pair(flow, BWD, u, v)
            for sl in slices:
                if swapped:
                    e = jnp.dot(lhs, wa[:, sl], preferred_element_type=F32)
                else:
                    e = across(lhs, wb, sl)
                act[BWD, u, :, sl] = (e[:tok] * slope[u, :, sl]).astype(BF16)
                act[BWD, v, :, sl] = (e[tok:] * slope[v, :, sl]).astype(BF16)
        blocks(d_ff, UP_GROUP if swapped else TURN_GROUP, fn)

        def out(w):
            keep(flow.at[BWD, w], g_out, w, 1)
            keep(act.at[BWD, w], d_out, w, 3)
        kept(u, v, out)

    def part_copy(kind, u, j):
        slot = lax.rem(u, SLOTS)
        return pltpu.make_async_remote_copy(part.at[kind, slot, j, other], recv.at[kind, u, j], part_send.at[kind, slot, j],
                                            recv_sem.at[kind, u, j], device_id=peer(stage, other), device_id_type=MESH)

    def down_product(kind, u, v, straight):
        def free(w):
            @pl.when(w >= SLOTS)
            def _():
                for j in range(n_blk):
                    part_copy(kind, w - SLOTS, j).wait_send()
        kept(u, v, free)

        def body(t, carry):
            lhs = pair(act, kind, u, v)
            for k in range(DOWN_GROUP):
                j = t * DOWN_GROUP + k
                sl = pl.ds(pl.multiple_of(j * BLK, BLK), BLK)
                if straight:
                    p = jnp.dot(lhs, wb[:, sl], preferred_element_type=F32)
                else:
                    p = across(lhs, wa, sl)
                p = p.reshape(2, INNER, rows, BLK)
                part[kind, lax.rem(u, SLOTS), j] = p[0]
                part[kind, lax.rem(v, SLOTS), j] = p[1]

            def go(w):
                for k in range(DOWN_GROUP):
                    part_copy(kind, w, t * DOWN_GROUP + k).start()
            kept(u, v, go)
            return carry
        lax.fori_loop(0, n_blk // DOWN_GROUP, body, 0)

    def hand_on(kind, first, count):
        target = stage + 1 if kind == FWD else stage - 1
        inside = stage < STAGES - 1 if kind == FWD else stage > 0
        out = STAGES - 1 if kind == FWD else 0

        def body(i, carry):
            u = first + i
            slot = lax.rem(u, SLOTS)
            for j in range(n_blk):
                sl = pl.ds(j * BLK, BLK)
                wait_bytes(recv.at[kind, u, j], recv_sem.at[kind, u, j])
                total = flow[kind, u, side, :, sl].astype(F32) + (part[kind, slot, j, side] + recv[kind, u, j])
                send[kind, u, :, sl] = total.astype(BF16)

                @pl.when(inside)
                def _():
                    for half in (side, other):
                        pltpu.make_async_remote_copy(send.at[kind, u, :, sl], flow.at[kind, u, side, :, sl], flow_send.at[kind],
                                                     flow_sem.at[kind, u, side], device_id=peer(target, half), device_id_type=MESH).start()

            @pl.when(jnp.logical_and(jnp.logical_not(inside), home_of(u) != out))
            def _():
                pltpu.make_async_remote_copy(send.at[kind, u], home.at[kind, slot_of(u)], home_send.at[kind, u],
                                             home_sem.at[kind, slot_of(u)], device_id=peer(home_of(u), side), device_id_type=MESH).start()
            return carry
        lax.fori_loop(0, count, body, 0)

    def swap_weights():
        n_i = d_model // TILE

        def body(t, carry):
            i = pl.multiple_of(lax.rem(t, n_i) * TILE, TILE)
            j = pl.multiple_of(lax.div(t, n_i) * TILE, TILE)
            up = wa[pl.ds(i, TILE), pl.ds(j, TILE)]
            down = wb[pl.ds(j, TILE), pl.ds(i, TILE)]
            wa[pl.ds(i, TILE), pl.ds(j, TILE)] = down.T
            wb[pl.ds(j, TILE), pl.ds(i, TILE)] = up.T
            return carry
        lax.fori_loop(0, n_i * (d_ff // TILE), body, 0)

    def prepare_last():
        half = UNITS // 2

        def quarter(q, carry):
            for i in range(half):
                arrived(BWD, q * half + i)
                keep(flow.at[BWD, q * half + i], g_out, q * half + i, 1)
            units = pl.ds(q * half, half)

            def fn(slices):
                lhs = flow[BWD, units].reshape(half * tok, d_model)
                for sl in slices:
                    e = lax.dot_general(lhs, wb[sl, :], NT, preferred_element_type=F32)
                    slope[units, :, sl] = e.reshape(half, tok, BLK)
            blocks(d_ff, 1, fn)
            return carry
        lax.fori_loop(0, 2, quarter, 0)
        load_a.wait()
        n_i = d_model // TILE

        def body(t, carry):
            i = pl.multiple_of(lax.rem(t, n_i) * TILE, TILE)
            j = pl.multiple_of(lax.div(t, n_i) * TILE, TILE)
            wb[pl.ds(j, TILE), pl.ds(i, TILE)] = wa[pl.ds(i, TILE), pl.ds(j, TILE)].T
            return carry
        lax.fori_loop(0, n_i * (d_ff // TILE), body, 0)

    def step(t, carry):
        group, place = lax.div(t, 3), lax.rem(t, 3)
        word = words[0]
        for i, w in enumerate(words[1:], 1):
            word = jnp.where(group == i, w, word)
        code = lax.rem(lax.div(word, jnp.where(place == 0, 1, jnp.where(place == 1, PACK, PACK * PACK))), PACK)
        op = lax.rem(code, 16)
        u = lax.rem(lax.div(code, 16), UNITS)
        count = lax.div(code, 128) + 1

        def on(want):
            return pl.when(op == want)

        v = jnp.minimum(u + count - 1, UNITS - 1)

        @on(F1)
        def _():
            up_product(u, v, False)

        @on(M1)
        def _():
            up_product(u, v, True)

        @pl.when(jnp.logical_or(op == F2, op == B2))
        def _():
            down_product(jnp.where(op == F2, FWD, BWD), u, v, True)

        @on(FR)
        def _():
            hand_on(FWD, u, count)

        @on(BR)
        def _():
            hand_on(BWD, u, count)

        @on(B1)
        def _():
            back_product(u, v, True)

        @on(T1)
        def _():
            back_product(u, v, False)

        @on(T2)
        def _():
            down_product(BWD, u, v, False)

        @on(SW)
        def _():
            swap_weights()

        @on(PR)
        def _():
            prepare_last()

        @on(YL)
        def _():
            load_b.start()
            load_b.wait()

        @on(WA)
        def _():
            load_a.wait()

        @on(WB)
        def _():
            load_b.wait()

        @on(XS)
        def _():
            for k in range(2):
                @pl.when(jnp.logical_or(stage > 1, k == 0))
                def _():
                    hand_in(FWD, x_ref, 0, k, 1)
        return carry
    lax.fori_loop(0, steps, step, 0)

    for kind, here, out in ((FWD, STAGES - 1, y_out), (BWD, 0, dx_out)):
        for k in range(2):
            @pl.when(stage == here)
            def _():
                pltpu.make_async_copy(send.at[kind, unit_of(k)], out.at[k], out_sem.at[4 + kind]).start()

            @pl.when(stage != here)
            def _():
                wait_bytes(home.at[kind, k], home_sem.at[kind, k])
                pltpu.make_async_copy(home.at[kind, k], out.at[k], out_sem.at[4 + kind]).start()

    for kind in (FWD, BWD):
        for u in range(UNITS - SLOTS, UNITS):
            for j in range(n_blk):
                part_copy(kind, u, j).wait_send()
    for kind, target, src in ((FWD, 0, x_ref), (BWD, STAGES - 1, g_ref)):
        last = STAGES - 1 - target
        for k in range(2):
            @pl.when(stage != target)
            def _():
                wait_bytes(src.at[k], in_send.at[kind, k, 0])
            wait_bytes(src.at[k], in_send.at[kind, k, 1])

        @pl.when(stage != last)
        def _():
            wait_bytes(flow.at[kind], flow_send.at[kind])

        @pl.when(stage == last)
        def _():
            for u in range(UNITS):
                if (u + 1) // 2 % STAGES != last:
                    wait_bytes(send.at[kind, u], home_send.at[kind, u])
    for lane, (ref, out) in enumerate(((flow.at[FWD], h_out), (flow.at[BWD], g_out), (act.at[FWD], a_out), (act.at[BWD], d_out),
                                       (home.at[FWD], y_out), (home.at[BWD], dx_out))):
        pltpu.make_async_copy(ref, out, out_sem.at[lane]).wait()


def run_pipeline(x_loc, g_loc, w_one, w_two):
    rows, d_model = x_loc.shape[1:]
    d_ff = w_one.shape[1]
    n_blk = d_model // BLK
    tok = INNER * rows
    hbm = pl.BlockSpec(memory_space=pl.ANY)
    out = lambda *shape: jax.ShapeDtypeStruct(shape, BF16)
    dma = lambda *shape: pltpu.SemaphoreType.DMA(shape)
    return pl.pallas_call(
        pipeline_kernel,
        name='pipeline',
        out_shape=(out(*x_loc.shape), out(*x_loc.shape), out(UNITS, INNER, rows, d_model), out(UNITS, INNER, rows, d_model),
                   out(UNITS, tok, d_ff), out(UNITS, tok, d_ff)),
        in_specs=[hbm] * 4,
        out_specs=(hbm,) * 6,
        scratch_shapes=[
            pltpu.VMEM((d_model, d_ff), BF16),
            pltpu.VMEM((d_ff, d_model), BF16),
            pltpu.VMEM((2, UNITS, INNER, rows, d_model), BF16),
            pltpu.VMEM((2, UNITS, tok, d_ff), BF16),
            pltpu.VMEM((UNITS, tok, d_ff), F32),
            pltpu.VMEM((2, SLOTS, n_blk, INNER, rows, BLK), F32),
            pltpu.VMEM((2, UNITS, n_blk, rows, BLK), F32),
            pltpu.VMEM((2, UNITS, rows, d_model), BF16),
            pltpu.VMEM((2, 2, rows, d_model), BF16),
            dma(2, UNITS, INNER), dma(2, UNITS, n_blk), dma(2, SLOTS, n_blk), dma(2), dma(2, UNITS), dma(2, 2), dma(2, 2, 2), dma(2), dma(6),
        ],
        compiler_params=pltpu.CompilerParams(collective_id=0, has_side_effects=True, vmem_limit_bytes=67043328),
    )(x_loc, g_loc, w_one, w_two)


GRAD_ROWS, GRAD_COLS = 1024, 2048


def weight_grad_kernel(h_ref, d_ref, a_ref, g_ref, y_ref, x_ref, up_ref, down_ref, y_out, x_out,
                       h, d, a, g, home, stage, in_sem, home_sem, out_sem):
    tokens, d_model = h.shape
    d_ff = d.shape[1]
    n_down, n_up = d_ff // GRAD_ROWS, d_model // GRAD_ROWS
    n_col = d_ff // GRAD_COLS

    loads = [(g_ref, g)] + [(a_ref.at[:, pl.ds(t * GRAD_ROWS, GRAD_ROWS)], a.at[:, pl.ds(t * GRAD_ROWS, GRAD_ROWS)]) for t in range(n_down)] + [(h_ref, h), (d_ref, d)]
    loads = [pltpu.make_async_copy(src, dst, in_sem.at[t]) for t, (src, dst) in enumerate(loads)]
    homes = [pltpu.make_async_copy(src, home.at[t], home_sem.at[t]) for t, src in enumerate((y_ref, x_ref))]
    for copy in loads + homes:
        copy.start()
    loads[0].wait()

    def block(t, src, first, other, second, out, pieces=1):
        slot = lax.rem(t, 2)
        size = GRAD_ROWS // pieces
        for p in range(pieces):
            rows = pl.ds(pl.multiple_of(first + p * size, size), size)
            cols = pl.ds(pl.multiple_of(second, GRAD_COLS), GRAD_COLS)
            stage[slot, pl.ds(p * size, size)] = lax.dot_general(src[:, rows], other[:, cols], (((0,), (0,)), ((), ())), preferred_element_type=F32)
            pltpu.make_async_copy(stage.at[slot, pl.ds(p * size, size)], out.at[rows, cols], out_sem.at[slot]).start()

    def freed(slot):
        pltpu.make_async_copy(stage.at[slot], stage.at[slot], out_sem.at[slot]).wait()

    def down(t, carry):
        pltpu.make_async_copy(a_ref.at[:, pl.ds(0, GRAD_ROWS)], a.at[:, pl.ds(0, GRAD_ROWS)], in_sem.at[1 + t]).wait()

        @pl.when(t >= 2)
        def _():
            freed(lax.rem(t, 2))
        block(t, a, t * GRAD_ROWS, g, 0, down_ref)
        return carry
    lax.fori_loop(0, n_down, down, 0)
    loads[1 + n_down].wait()
    loads[2 + n_down].wait()
    for copy, (src, dst) in zip(homes, ((home.at[0], y_out), (home.at[1], x_out))):
        copy.wait()
    backs = [pltpu.make_async_copy(home.at[t], dst, home_sem.at[t]) for t, dst in enumerate((y_out, x_out))]
    for copy in backs:
        copy.start()

    def up(t, carry):
        freed(lax.rem(t, 2))
        block(t, h, lax.div(t, n_col) * GRAD_ROWS, d, lax.rem(t, n_col) * GRAD_COLS, up_ref)
        return carry
    n_blocks = n_up * n_col
    lax.fori_loop(0, n_blocks - 1, up, 0)
    freed((n_blocks - 1) % 2)
    block(n_blocks - 1, h, (n_up - 1) * GRAD_ROWS, d, (n_col - 1) * GRAD_COLS, up_ref, 4)
    for slot in range(2):
        freed(slot)
    for copy in backs:
        copy.wait()


def weight_grads(h, d, a, g, y, dx):
    tokens, d_model = h.shape
    d_ff = d.shape[1]
    n_in = 3 + d_ff // GRAD_ROWS
    hbm = pl.BlockSpec(memory_space=pl.ANY)
    dma = lambda *shape: pltpu.SemaphoreType.DMA(shape)
    like = lambda v: pltpu.VMEM(v.shape, v.dtype)
    return pl.pallas_call(
        weight_grad_kernel,
        name='weight_grads',
        out_shape=(jax.ShapeDtypeStruct((d_model, d_ff), F32), jax.ShapeDtypeStruct((d_ff, d_model), F32),
                   jax.ShapeDtypeStruct(y.shape, BF16), jax.ShapeDtypeStruct(y.shape, BF16)),
        in_specs=[hbm] * 6,
        out_specs=(hbm,) * 4,
        scratch_shapes=[like(h), like(d), like(a), like(g), pltpu.VMEM((2,) + y.shape, BF16), pltpu.VMEM((2, GRAD_ROWS, GRAD_COLS), F32),
                        dma(n_in), dma(2), dma(2)],
        compiler_params=pltpu.CompilerParams(vmem_limit_bytes=60 * 1024 * 1024),
    )(h, d, a, g, y, dx)


def solution(mesh):
    tok_spec = P(('data', 'stage', 'inner'))
    up_spec = P(None, ('data', 'stage'), None, 'inner')
    down_spec = P(None, ('data', 'stage'), 'inner', None)

    def device_step(x_loc, g_loc, w_up, w_down):
        y, dx, h, g, a, d = run_pipeline(x_loc, g_loc, w_up[0, 0], w_down[0, 0])
        flat = lambda v: v.reshape(-1, v.shape[-1])
        dw_up, dw_down, y, dx = weight_grads(flat(h), flat(d), flat(a), flat(g), y, dx)
        return y, dx, dw_up[None, None], dw_down[None, None]

    return jax.shard_map(device_step, mesh=mesh, in_specs=(tok_spec, tok_spec, up_spec, down_spec), out_specs=(tok_spec, tok_spec, up_spec, down_spec), check_vma=False)
```

```python
import functools

import jax
import jax.numpy as jnp
from jax import lax
from jax.experimental import pallas as pl
from jax.experimental.pallas import tpu as pltpu
from jax.sharding import PartitionSpec as P

F32 = jnp.float32
BF16 = jnp.bfloat16
MESH = pl.DeviceIdType.MESH

STAGES = 4
INNER = 2
UNITS = 8
SLOTS = 3
DIRECT = 4
BLK = 512
TILE = 256
FWD, BWD = 0, 1
NT = (((1,), (1,)), ((), ()))

F1, F2, FR, B1, B2, BR, T1, T2, SW, PR, YL, WA, WB, XS, M1, HB, XW = range(1, 18)
PLAN = (
    ((WA, 0, 1), (F1, 0, 2), (WB, 0, 1), (XS, 0, 1), (F2, 0, 1), (F2, 1, 1), (FR, 0, 1), (F1, 2, 2),
     (FR, 1, 1), (F2, 2, 1), (F1, 4, 2), (F2, 3, 1), (F1, 6, 1), (FR, 2, 2), (F2, 4, 1), (F2, 5, 1),
     (FR, 4, 2), (F1, 7, 1), (F2, 6, 1), (F2, 7, 1), (FR, 6, 2), (SW, 0, 1), (B1, 0, 2), (B2, 0, 2),
     (B1, 2, 1), (B2, 2, 1), (BR, 0, 1), (B1, 3, 1), (B2, 3, 1), (B1, 4, 1), (BR, 1, 1), (B1, 5, 1),
     (BR, 2, 2), (B2, 4, 2), (B1, 6, 2), (B2, 6, 1), (BR, 4, 1), (B2, 7, 1), (BR, 5, 3)),
    ((WA, 0, 1), (WB, 0, 1), (F1, 0, 1), (F2, 0, 1), (F1, 1, 1), (FR, 0, 1), (F2, 1, 1), (FR, 1, 1),
     (F1, 2, 2), (F2, 2, 1), (F2, 3, 1), (FR, 2, 2), (F1, 4, 2), (F2, 4, 1), (F2, 5, 1), (FR, 4, 1),
     (F1, 6, 2), (FR, 5, 1), (F2, 6, 1), (F2, 7, 1), (FR, 6, 2), (SW, 0, 1), (HB, 0, 2), (B1, 0, 2),
     (B2, 0, 1), (HB, 2, 2), (B2, 1, 1), (BR, 0, 1), (B1, 2, 2), (BR, 1, 1), (B2, 2, 1), (B2, 3, 1),
     (BR, 2, 1), (B1, 4, 2), (BR, 3, 1), (B2, 4, 1), (B2, 5, 1), (BR, 4, 1), (B1, 6, 1), (B1, 7, 1),
     (BR, 5, 1), (B2, 6, 1), (B2, 7, 1), (BR, 6, 2)),
    ((WA, 0, 1), (WB, 0, 1), (XS, 0, 1), (XW, 0, 1), (F1, 0, 1), (F2, 0, 1), (F1, 1, 1), (FR, 0, 1),
     (F2, 1, 1), (FR, 1, 1), (F1, 2, 1), (F2, 2, 1), (FR, 2, 1), (F1, 3, 1), (F2, 3, 1), (F1, 4, 2),
     (FR, 3, 1), (F2, 4, 2), (T1, 0, 2), (T2, 0, 2), (F1, 6, 2), (FR, 4, 2), (F2, 6, 2), (T1, 2, 2),
     (FR, 6, 1), (T2, 2, 2), (FR, 7, 1), (T1, 4, 2), (T2, 4, 2), (T1, 6, 2), (BR, 4, 2), (T2, 6, 1),
     (T2, 7, 1), (BR, 6, 2)),
    ((WB, 0, 1), (XS, 0, 1), (PR, 0, 1), (XW, 0, 1), (M1, 0, 1), (B2, 0, 1), (M1, 1, 1), (BR, 0, 1),
     (B2, 1, 1), (M1, 2, 1), (BR, 1, 1), (B2, 2, 1), (M1, 3, 1), (B2, 3, 1), (BR, 2, 2), (M1, 4, 2),
     (B2, 4, 2), (M1, 6, 1), (BR, 4, 2), (B2, 6, 1), (M1, 7, 1), (B2, 7, 1), (BR, 6, 2), (YL, 0, 1),
     (F2, 0, 1), (F2, 1, 1), (FR, 0, 1), (F2, 2, 1), (FR, 1, 2), (F2, 3, 2), (F2, 5, 1), (FR, 3, 2),
     (F2, 6, 1), (FR, 5, 2), (F2, 7, 1), (FR, 7, 1)),
)


PACK = 1024
UP_GROUP = 8
TURN = 6
TURN_GROUP = 4
DOWN_GROUP = 2


def plan_words():
    rows = [[op + 32 * unit + 256 * (count - 1) for op, unit, count in row] for row in PLAN]
    steps = -(-max(len(row) for row in rows) // 3) * 3
    rows = [row + [0] * (steps - len(row)) for row in rows]
    return steps, [[row[t] + PACK * row[t + 1] + PACK * PACK * row[t + 2] for t in range(0, steps, 3)] for row in rows]


def gelu_pair(pre_act):
    root = pre_act * 0.7071067811865476
    normal_cdf = 0.5 * (1.0 + lax.erf(root))
    normal_pdf = jnp.exp2(root * root * -1.4426950408889634) * 0.3989422804014327
    return pre_act * normal_cdf, normal_cdf + pre_act * normal_pdf


def wait_bytes(ref, sem):
    pltpu.make_async_copy(ref, ref, sem).wait()


def pipeline_kernel(x_ref, g_ref, w1_ref, w2_ref,
                    y_out, dx_out, h_out, g_out, a_out, d_out,
                    wa, wb, flow, act, slope, part, recv, send, home, direct,
                    flow_sem, recv_sem, part_send, flow_send, home_send, home_sem, in_send, relay_sem, relay_send,
                    direct_sem, direct_send, cross_send, w_sem, out_sem):
    stage = lax.axis_index('stage')
    side = lax.axis_index('inner')
    other = 1 - side
    rows, d_model = flow.shape[3:]
    tok, d_ff = act.shape[2:]
    n_blk = d_model // BLK

    def peer(s, i):
        return {'stage': s, 'inner': i}

    load_a = pltpu.make_async_copy(w1_ref, wa, w_sem.at[0])
    load_b = pltpu.make_async_copy(w2_ref, wb, w_sem.at[1])

    @pl.when(stage < STAGES - 1)
    def _():
        load_a.start()
    load_b.start()

    @pl.when(stage == STAGES - 1)
    def _():
        load_a.start()

    barrier = pltpu.get_barrier_semaphore()
    for s in range(STAGES):
        for i in range(INNER):
            @pl.when(jnp.logical_or(stage != s, side != i))
            def _():
                pl.semaphore_signal(barrier, inc=1, device_id=peer(s, i), device_id_type=MESH)
    pl.semaphore_wait(barrier, STAGES * INNER - 1)

    def unit_of(k):
        return lax.rem(2 * stage + k + UNITS - 1, UNITS)

    def home_of(u):
        return lax.rem((u + 1) // 2, STAGES)

    def slot_of(u):
        return lax.rem(u + 1, 2)

    def hand_in(kind, src, target, k, lane):
        u = unit_of(k)
        if lane == 0:
            @pl.when(stage == target)
            def _():
                pltpu.make_async_copy(src.at[k], flow.at[kind, u, side], flow_sem.at[kind, u, side]).start()

            @pl.when(stage != target)
            def _():
                pltpu.make_async_remote_copy(src.at[k], flow.at[kind, u, side], in_send.at[kind, k, 0], flow_sem.at[kind, u, side],
                                             device_id=peer(target, side), device_id_type=MESH).start()
        else:
            pltpu.make_async_remote_copy(src.at[k], flow.at[kind, u, side], in_send.at[kind, k, 1], flow_sem.at[kind, u, side],
                                         device_id=peer(target, other), device_id_type=MESH).start()

    def relay(k):
        return pltpu.make_async_remote_copy(x_ref.at[k], home.at[FWD, k], in_send.at[FWD, k, 1], relay_sem.at[k],
                                            device_id=peer(stage, other), device_id_type=MESH)

    def relayed(k):
        u = unit_of(k)
        return pltpu.make_async_remote_copy(home.at[FWD, k], flow.at[FWD, u, other], relay_send.at[k], flow_sem.at[FWD, u, other],
                                            device_id=peer(0, side), device_id_type=MESH)

    for k in range(2):
        hand_in(FWD, x_ref, 0, k, 0)

        @pl.when(jnp.logical_or(stage == 1, jnp.logical_and(stage == 0, k == 1)))
        def _():
            hand_in(FWD, x_ref, 0, k, 1)

        @pl.when(stage > 1)
        def _():
            relay(k).start()
    for k in range(2):
        for lane in range(2):
            hand_in(BWD, g_ref, STAGES - 1, k, lane)

    steps, plan = plan_words()
    words = [jnp.where(stage == 0, a, jnp.where(stage == 1, b, jnp.where(stage == 2, c, d))) for a, b, c, d in zip(*plan)]

    def keep(ref, out, u, lane):
        pltpu.make_async_copy(ref, out.at[u], out_sem.at[lane]).start()

    def blocks(width, group, fn):
        def body(t, carry):
            fn([pl.ds(pl.multiple_of((t * group + k) * BLK, BLK), BLK) for k in range(group)])
            return carry
        lax.fori_loop(0, width // BLK // group, body, 0)

    def arrived(kind, u):
        for half in range(INNER):
            @pl.when(jnp.logical_not((stage == 1) & (kind == BWD) & (u < DIRECT) & (side == half)))
            def _():
                wait_bytes(flow.at[kind, u, half], flow_sem.at[kind, u, half])

    def both_arrived(kind, u, v):
        arrived(kind, u)

        @pl.when(v != u)
        def _():
            arrived(kind, v)

    def pair(ref, kind, u, v):
        width = ref.shape[-1]
        return jnp.concatenate([ref[kind, u].reshape(tok, width), ref[kind, v].reshape(tok, width)], axis=0)

    def kept(u, v, fn):
        fn(u)

        @pl.when(v != u)
        def _():
            fn(v)

    def up_product(u, v, last):
        both_arrived(FWD, u, v)

        def fn(slices):
            lhs = pair(flow, FWD, u, v)
            for sl in slices:
                z = jnp.dot(lhs, wa[:, sl], preferred_element_type=F32)
                value, grad = gelu_pair(z)
                value = value.astype(BF16)
                if last:
                    act[BWD, u, :, sl] = (slope[u, :, sl] * grad[:tok]).astype(BF16)
                    act[BWD, v, :, sl] = (slope[v, :, sl] * grad[tok:]).astype(BF16)
                else:
                    slope[u, :, sl] = grad[:tok]
                    slope[v, :, sl] = grad[tok:]
                act[FWD, u, :, sl] = value[:tok]
                act[FWD, v, :, sl] = value[tok:]
        blocks(d_ff, UP_GROUP, fn)

        def out(w):
            keep(flow.at[FWD, w], h_out, w, 0)
            keep(act.at[FWD, w], a_out, w, 2)
            if last:
                keep(act.at[BWD, w], d_out, w, 3)
        kept(u, v, out)

    def across(lhs, ref, sl):
        cut = ref.shape[1] * TURN // 8
        total = lax.dot_general(lhs[:, :cut], ref[sl, :cut], NT, preferred_element_type=F32)
        for k in range(cut, ref.shape[1], TILE):
            turned = [ref[pl.ds(sl.start + q, TILE), k:k + TILE].T for q in range(0, BLK, TILE)]
            total += jnp.dot(lhs[:, k:k + TILE], jnp.concatenate(turned, axis=1), preferred_element_type=F32)
        return total

    def back_product(u, v, swapped):
        both_arrived(BWD, u, v)

        def fn(slices):
            lhs = pair(flow, BWD, u, v)
            for sl in slices:
                if swapped:
                    e = jnp.dot(lhs, wa[:, sl], preferred_element_type=F32)
                else:
                    e = across(lhs, wb, sl)
                act[BWD, u, :, sl] = (e[:tok] * slope[u, :, sl]).astype(BF16)
                act[BWD, v, :, sl] = (e[tok:] * slope[v, :, sl]).astype(BF16)
        blocks(d_ff, UP_GROUP if swapped else TURN_GROUP, fn)

        def out(w):
            keep(flow.at[BWD, w], g_out, w, 1)
            keep(act.at[BWD, w], d_out, w, 3)
        kept(u, v, out)

    def part_copy(kind, u, j):
        slot = lax.rem(u, SLOTS)
        return pltpu.make_async_remote_copy(part.at[kind, slot, j, other], recv.at[kind, u, j], part_send.at[kind, slot, j],
                                            recv_sem.at[kind, u, j], device_id=peer(stage, other), device_id_type=MESH)

    def direct_copy(u, j, half):
        slot = lax.rem(u, SLOTS)
        if half is side:
            return pltpu.make_async_remote_copy(part.at[BWD, slot, j, side], direct.at[u, j], direct_send.at[slot, j],
                                                direct_sem.at[0, u, j], device_id=peer(stage - 1, side), device_id_type=MESH)
        return pltpu.make_async_remote_copy(part.at[BWD, slot, j, other], recv.at[FWD, u, j], part_send.at[BWD, slot, j],
                                            direct_sem.at[1, u, j], device_id=peer(stage - 1, other), device_id_type=MESH)

    def take_direct(first, count):
        def body(i, carry):
            u = first + i
            for j in range(n_blk):
                sl = pl.ds(j * BLK, BLK)
                wait_bytes(direct.at[u, j], direct_sem.at[0, u, j])
                wait_bytes(recv.at[FWD, u, j], direct_sem.at[1, u, j])
                flow[BWD, u, side, :, sl] = (direct[u, j] + recv[FWD, u, j]).astype(BF16)
                pltpu.make_async_remote_copy(flow.at[BWD, u, side, :, sl], flow.at[BWD, u, side, :, sl], cross_send.at[0],
                                             flow_sem.at[BWD, u, side], device_id=peer(stage, other), device_id_type=MESH).start()
            return carry
        lax.fori_loop(0, count, body, 0)

    def down_product(kind, u, v, straight):
        def free(w):
            @pl.when(w >= SLOTS)
            def _():
                for j in range(n_blk):
                    part_copy(kind, w - SLOTS, j).wait_send()

            if not straight:
                @pl.when((w >= SLOTS) & (w < SLOTS + DIRECT))
                def _():
                    for j in range(n_blk):
                        direct_copy(w - SLOTS, j, side).wait_send()
        kept(u, v, free)

        def body(t, carry):
            lhs = pair(act, kind, u, v)
            for k in range(DOWN_GROUP):
                j = t * DOWN_GROUP + k
                sl = pl.ds(pl.multiple_of(j * BLK, BLK), BLK)
                if straight:
                    p = jnp.dot(lhs, wb[:, sl], preferred_element_type=F32)
                else:
                    p = across(lhs, wa, sl)
                p = p.reshape(2, INNER, rows, BLK)
                part[kind, lax.rem(u, SLOTS), j] = p[0]
                part[kind, lax.rem(v, SLOTS), j] = p[1]

            def go(w):
                if straight:
                    for k in range(DOWN_GROUP):
                        part_copy(kind, w, t * DOWN_GROUP + k).start()
                    return

                @pl.when(w >= DIRECT)
                def _():
                    for k in range(DOWN_GROUP):
                        part_copy(kind, w, t * DOWN_GROUP + k).start()

                @pl.when(w < DIRECT)
                def _():
                    for k in range(DOWN_GROUP):
                        j = t * DOWN_GROUP + k
                        sl = pl.ds(pl.multiple_of(j * BLK, BLK), BLK)
                        part[BWD, lax.rem(w, SLOTS), j, side] += flow[BWD, w, side, :, sl].astype(F32)
                    for k in range(DOWN_GROUP):
                        for half in (side, other):
                            direct_copy(w, t * DOWN_GROUP + k, half).start()
            kept(u, v, go)
            return carry
        lax.fori_loop(0, n_blk // DOWN_GROUP, body, 0)

    def hand_on(kind, first, count):
        target = stage + 1 if kind == FWD else stage - 1
        inside = stage < STAGES - 1 if kind == FWD else stage > 0
        out = STAGES - 1 if kind == FWD else 0

        def body(i, carry):
            u = first + i
            slot = lax.rem(u, SLOTS)
            for j in range(n_blk):
                sl = pl.ds(j * BLK, BLK)
                wait_bytes(recv.at[kind, u, j], recv_sem.at[kind, u, j])
                total = flow[kind, u, side, :, sl].astype(F32) + (part[kind, slot, j, side] + recv[kind, u, j])
                send[kind, u, :, sl] = total.astype(BF16)

                @pl.when(inside)
                def _():
                    for half in (side, other):
                        pltpu.make_async_remote_copy(send.at[kind, u, :, sl], flow.at[kind, u, side, :, sl], flow_send.at[kind],
                                                     flow_sem.at[kind, u, side], device_id=peer(target, half), device_id_type=MESH).start()

            @pl.when(jnp.logical_and(jnp.logical_not(inside), home_of(u) != out))
            def _():
                pltpu.make_async_remote_copy(send.at[kind, u], home.at[kind, slot_of(u)], home_send.at[kind, u],
                                             home_sem.at[kind, slot_of(u)], device_id=peer(home_of(u), side), device_id_type=MESH).start()
            return carry
        lax.fori_loop(0, count, body, 0)

    def swap_weights():
        n_i = d_model // TILE

        def body(t, carry):
            i = pl.multiple_of(lax.rem(t, n_i) * TILE, TILE)
            j = pl.multiple_of(lax.div(t, n_i) * TILE, TILE)
            up = wa[pl.ds(i, TILE), pl.ds(j, TILE)]
            down = wb[pl.ds(j, TILE), pl.ds(i, TILE)]
            wa[pl.ds(i, TILE), pl.ds(j, TILE)] = down.T
            wb[pl.ds(j, TILE), pl.ds(i, TILE)] = up.T
            return carry
        lax.fori_loop(0, n_i * (d_ff // TILE), body, 0)

    def prepare_last():
        half = UNITS // 2

        def quarter(q, carry):
            for i in range(half):
                arrived(BWD, q * half + i)
                keep(flow.at[BWD, q * half + i], g_out, q * half + i, 1)
            units = pl.ds(q * half, half)

            def fn(slices):
                lhs = flow[BWD, units].reshape(half * tok, d_model)
                for sl in slices:
                    e = lax.dot_general(lhs, wb[sl, :], NT, preferred_element_type=F32)
                    slope[units, :, sl] = e.reshape(half, tok, BLK)
            blocks(d_ff, 1, fn)
            return carry
        lax.fori_loop(0, 2, quarter, 0)
        load_a.wait()
        n_i = d_model // TILE

        def body(t, carry):
            i = pl.multiple_of(lax.rem(t, n_i) * TILE, TILE)
            j = pl.multiple_of(lax.div(t, n_i) * TILE, TILE)
            wb[pl.ds(j, TILE), pl.ds(i, TILE)] = wa[pl.ds(i, TILE), pl.ds(j, TILE)].T
            return carry
        lax.fori_loop(0, n_i * (d_ff // TILE), body, 0)

    def step(t, carry):
        group, place = lax.div(t, 3), lax.rem(t, 3)
        word = words[0]
        for i, w in enumerate(words[1:], 1):
            word = jnp.where(group == i, w, word)
        code = lax.rem(lax.div(word, jnp.where(place == 0, 1, jnp.where(place == 1, PACK, PACK * PACK))), PACK)
        op = lax.rem(code, 32)
        u = lax.rem(lax.div(code, 32), UNITS)
        count = lax.div(code, 256) + 1

        def on(want):
            return pl.when(op == want)

        v = jnp.minimum(u + count - 1, UNITS - 1)

        @on(F1)
        def _():
            up_product(u, v, False)

        @on(M1)
        def _():
            up_product(u, v, True)

        @pl.when(jnp.logical_or(op == F2, op == B2))
        def _():
            down_product(jnp.where(op == F2, FWD, BWD), u, v, True)

        @on(FR)
        def _():
            hand_on(FWD, u, count)

        @on(BR)
        def _():
            hand_on(BWD, u, count)

        @on(B1)
        def _():
            back_product(u, v, True)

        @on(T1)
        def _():
            back_product(u, v, False)

        @on(T2)
        def _():
            down_product(BWD, u, v, False)

        @on(SW)
        def _():
            swap_weights()

        @on(PR)
        def _():
            prepare_last()

        @on(YL)
        def _():
            load_b.start()
            load_b.wait()

        @on(WA)
        def _():
            load_a.wait()

        @on(WB)
        def _():
            load_b.wait()

        @on(XS)
        def _():
            @pl.when(stage == 0)
            def _():
                hand_in(FWD, x_ref, 0, 0, 1)

            @pl.when(stage > 1)
            def _():
                for k in range(2):
                    wait_bytes(home.at[FWD, k], relay_sem.at[k])
                    relayed(k).start()

        @on(XW)
        def _():
            for k in range(2):
                relayed(k).wait_send()

        @on(HB)
        def _():
            take_direct(u, count)
        return carry
    lax.fori_loop(0, steps, step, 0)

    for kind, here, out in ((FWD, STAGES - 1, y_out), (BWD, 0, dx_out)):
        for k in range(2):
            @pl.when(stage == here)
            def _():
                pltpu.make_async_copy(send.at[kind, unit_of(k)], out.at[k], out_sem.at[4 + kind]).start()

            @pl.when(stage != here)
            def _():
                wait_bytes(home.at[kind, k], home_sem.at[kind, k])
                pltpu.make_async_copy(home.at[kind, k], out.at[k], out_sem.at[4 + kind]).start()

    for kind in (FWD, BWD):
        for u in range(UNITS - SLOTS, UNITS):
            for j in range(n_blk):
                part_copy(kind, u, j).wait_send()
    for kind, target, src in ((FWD, 0, x_ref), (BWD, STAGES - 1, g_ref)):
        last = STAGES - 1 - target
        for k in range(2):
            @pl.when(stage != target)
            def _():
                wait_bytes(src.at[k], in_send.at[kind, k, 0])
            wait_bytes(src.at[k], in_send.at[kind, k, 1])

        @pl.when((stage != last) & jnp.logical_not((stage == 2) & (kind == BWD)))
        def _():
            wait_bytes(flow.at[kind], flow_send.at[kind])

        @pl.when(stage == last)
        def _():
            for u in range(UNITS):
                if (u + 1) // 2 % STAGES != last:
                    wait_bytes(send.at[kind, u], home_send.at[kind, u])
    @pl.when(stage == 2)
    def _():
        wait_bytes(flow.at[BWD, pl.ds(0, UNITS - DIRECT)], flow_send.at[BWD])

    @pl.when(stage == 1)
    def _():
        wait_bytes(flow.at[BWD, pl.ds(0, DIRECT), 0], cross_send.at[0])
    for lane, (ref, out) in enumerate(((flow.at[FWD], h_out), (flow.at[BWD], g_out), (act.at[FWD], a_out), (act.at[BWD], d_out),
                                       (home.at[FWD], y_out), (home.at[BWD], dx_out))):
        pltpu.make_async_copy(ref, out, out_sem.at[lane]).wait()


def run_pipeline(x_loc, g_loc, w_one, w_two):
    rows, d_model = x_loc.shape[1:]
    d_ff = w_one.shape[1]
    n_blk = d_model // BLK
    tok = INNER * rows
    hbm = pl.BlockSpec(memory_space=pl.ANY)
    out = lambda *shape: jax.ShapeDtypeStruct(shape, BF16)
    dma = lambda *shape: pltpu.SemaphoreType.DMA(shape)
    return pl.pallas_call(
        pipeline_kernel,
        name='pipeline',
        out_shape=(out(*x_loc.shape), out(*x_loc.shape), out(UNITS, INNER, rows, d_model), out(UNITS, INNER, rows, d_model),
                   out(UNITS, tok, d_ff), out(UNITS, tok, d_ff)),
        in_specs=[hbm] * 4,
        out_specs=(hbm,) * 6,
        scratch_shapes=[
            pltpu.VMEM((d_model, d_ff), BF16),
            pltpu.VMEM((d_ff, d_model), BF16),
            pltpu.VMEM((2, UNITS, INNER, rows, d_model), BF16),
            pltpu.VMEM((2, UNITS, tok, d_ff), BF16),
            pltpu.VMEM((UNITS, tok, d_ff), F32),
            pltpu.VMEM((2, SLOTS, n_blk, INNER, rows, BLK), F32),
            pltpu.VMEM((2, UNITS, n_blk, rows, BLK), F32),
            pltpu.VMEM((2, UNITS, rows, d_model), BF16),
            pltpu.VMEM((2, 2, rows, d_model), BF16),
            pltpu.VMEM((DIRECT, n_blk, rows, BLK), F32),
            dma(2, UNITS, INNER), dma(2, UNITS, n_blk), dma(2, SLOTS, n_blk), dma(2), dma(2, UNITS), dma(2, 2), dma(2, 2, 2), dma(2), dma(2),
            dma(2, DIRECT, n_blk), dma(SLOTS, n_blk), dma(1), dma(2), dma(6),
        ],
        compiler_params=pltpu.CompilerParams(collective_id=0, has_side_effects=True, vmem_limit_bytes=67043328),
    )(x_loc, g_loc, w_one, w_two)


GRAD_ROWS, GRAD_COLS = 1024, 2048


def weight_grad_kernel(h_ref, d_ref, a_ref, g_ref, y_ref, x_ref, up_ref, down_ref, y_out, x_out,
                       h, d, a, g, home, stage, in_sem, home_sem, out_sem):
    tokens, d_model = h.shape
    d_ff = d.shape[1]
    n_down, n_up = d_ff // GRAD_ROWS, d_model // GRAD_ROWS
    n_col = d_ff // GRAD_COLS

    loads = [(g_ref, g)] + [(a_ref.at[:, pl.ds(t * GRAD_ROWS, GRAD_ROWS)], a.at[:, pl.ds(t * GRAD_ROWS, GRAD_ROWS)]) for t in range(n_down)] + [(h_ref, h), (d_ref, d)]
    loads = [pltpu.make_async_copy(src, dst, in_sem.at[t]) for t, (src, dst) in enumerate(loads)]
    homes = [pltpu.make_async_copy(src, home.at[t], home_sem.at[t]) for t, src in enumerate((y_ref, x_ref))]
    for copy in loads + homes:
        copy.start()
    loads[0].wait()

    def block(t, src, first, other, second, out, pieces=1):
        slot = lax.rem(t, 2)
        size = GRAD_ROWS // pieces
        for p in range(pieces):
            rows = pl.ds(pl.multiple_of(first + p * size, size), size)
            cols = pl.ds(pl.multiple_of(second, GRAD_COLS), GRAD_COLS)
            stage[slot, pl.ds(p * size, size)] = lax.dot_general(src[:, rows], other[:, cols], (((0,), (0,)), ((), ())), preferred_element_type=F32)
            pltpu.make_async_copy(stage.at[slot, pl.ds(p * size, size)], out.at[rows, cols], out_sem.at[slot]).start()

    def freed(slot):
        pltpu.make_async_copy(stage.at[slot], stage.at[slot], out_sem.at[slot]).wait()

    def down(t, carry):
        pltpu.make_async_copy(a_ref.at[:, pl.ds(0, GRAD_ROWS)], a.at[:, pl.ds(0, GRAD_ROWS)], in_sem.at[1 + t]).wait()

        @pl.when(t >= 2)
        def _():
            freed(lax.rem(t, 2))
        block(t, a, t * GRAD_ROWS, g, 0, down_ref)
        return carry
    lax.fori_loop(0, n_down, down, 0)
    loads[1 + n_down].wait()
    loads[2 + n_down].wait()
    for copy, (src, dst) in zip(homes, ((home.at[0], y_out), (home.at[1], x_out))):
        copy.wait()
    backs = [pltpu.make_async_copy(home.at[t], dst, home_sem.at[t]) for t, dst in enumerate((y_out, x_out))]
    for copy in backs:
        copy.start()

    def up(t, carry):
        freed(lax.rem(t, 2))
        block(t, h, lax.div(t, n_col) * GRAD_ROWS, d, lax.rem(t, n_col) * GRAD_COLS, up_ref)
        return carry
    n_blocks = n_up * n_col
    lax.fori_loop(0, n_blocks - 1, up, 0)
    freed((n_blocks - 1) % 2)
    block(n_blocks - 1, h, (n_up - 1) * GRAD_ROWS, d, (n_col - 1) * GRAD_COLS, up_ref, 4)
    for slot in range(2):
        freed(slot)
    for copy in backs:
        copy.wait()


def weight_grads(h, d, a, g, y, dx):
    tokens, d_model = h.shape
    d_ff = d.shape[1]
    n_in = 3 + d_ff // GRAD_ROWS
    hbm = pl.BlockSpec(memory_space=pl.ANY)
    dma = lambda *shape: pltpu.SemaphoreType.DMA(shape)
    like = lambda v: pltpu.VMEM(v.shape, v.dtype)
    return pl.pallas_call(
        weight_grad_kernel,
        name='weight_grads',
        out_shape=(jax.ShapeDtypeStruct((d_model, d_ff), F32), jax.ShapeDtypeStruct((d_ff, d_model), F32),
                   jax.ShapeDtypeStruct(y.shape, BF16), jax.ShapeDtypeStruct(y.shape, BF16)),
        in_specs=[hbm] * 6,
        out_specs=(hbm,) * 4,
        scratch_shapes=[like(h), like(d), like(a), like(g), pltpu.VMEM((2,) + y.shape, BF16), pltpu.VMEM((2, GRAD_ROWS, GRAD_COLS), F32),
                        dma(n_in), dma(2), dma(2)],
        compiler_params=pltpu.CompilerParams(vmem_limit_bytes=60 * 1024 * 1024),
    )(h, d, a, g, y, dx)


def solution(mesh):
    tok_spec = P(('data', 'stage', 'inner'))
    up_spec = P(None, ('data', 'stage'), None, 'inner')
    down_spec = P(None, ('data', 'stage'), 'inner', None)

    def device_step(x_loc, g_loc, w_up, w_down):
        y, dx, h, g, a, d = run_pipeline(x_loc, g_loc, w_up[0, 0], w_down[0, 0])
        flat = lambda v: v.reshape(-1, v.shape[-1])
        dw_up, dw_down, y, dx = weight_grads(flat(h), flat(d), flat(a), flat(g), y, dx)
        return y, dx, dw_up[None, None], dw_down[None, None]

    return jax.shard_map(device_step, mesh=mesh, in_specs=(tok_spec, tok_spec, up_spec, down_spec), out_specs=(tok_spec, tok_spec, up_spec, down_spec), check_vma=False)
```

```python
import functools

import jax
import jax.numpy as jnp
from jax import lax
from jax.experimental import pallas as pl
from jax.experimental.pallas import tpu as pltpu
from jax.sharding import PartitionSpec as P

F32 = jnp.float32
BF16 = jnp.bfloat16
MESH = pl.DeviceIdType.MESH

STAGES = 4
INNER = 2
UNITS = 8
SLOTS = 3
DIRECT = 3
BLK = 512
TILE = 256
FWD, BWD = 0, 1
NT = (((1,), (1,)), ((), ()))

F1, F2, FR, B1, B2, BR, T1, T2, SW, PR, YL, WA, WB, XS, M1, HB, XW = range(1, 18)
PLAN = (
    ((WA, 0, 1), (F1, 0, 2), (WB, 0, 1), (XS, 0, 1), (F2, 0, 1), (F2, 1, 1), (FR, 0, 1), (F1, 2, 2),
     (FR, 1, 1), (F2, 2, 1), (F2, 3, 1), (F1, 4, 1), (F1, 5, 2), (FR, 2, 2), (F2, 4, 1), (F2, 5, 1),
     (FR, 4, 2), (F1, 7, 1), (F2, 6, 2), (FR, 6, 2), (XW, 0, 1), (SW, 0, 1), (B1, 0, 1), (B1, 1, 1),
     (B2, 0, 1), (B2, 1, 1), (B1, 2, 2), (B2, 2, 1), (BR, 0, 1), (B2, 3, 1), (BR, 1, 1), (B1, 4, 1),
     (BR, 2, 2), (B1, 5, 1), (B2, 4, 1), (B2, 5, 1), (B1, 6, 2), (BR, 4, 1), (B2, 6, 2), (BR, 5, 3)),
    ((WA, 0, 1), (WB, 0, 1), (F1, 0, 1), (F2, 0, 1), (F1, 1, 1), (F2, 1, 1), (FR, 0, 2), (F1, 2, 2),
     (F2, 2, 1), (F2, 3, 1), (FR, 2, 1), (F1, 4, 2), (FR, 3, 1), (F2, 4, 1), (F2, 5, 1), (FR, 4, 2),
     (F1, 6, 1), (F2, 6, 1), (F1, 7, 1), (F2, 7, 1), (FR, 6, 2), (XW, 0, 1), (SW, 0, 1), (HB, 0, 2),
     (B1, 0, 2), (B2, 0, 1), (HB, 2, 1), (B2, 1, 1), (B1, 2, 1), (BR, 0, 1), (B2, 2, 1), (BR, 1, 1),
     (B1, 3, 1), (B2, 3, 1), (BR, 2, 2), (B1, 4, 2), (B2, 4, 1), (B2, 5, 1), (BR, 4, 1), (B1, 6, 2),
     (BR, 5, 1), (B2, 6, 1), (B2, 7, 1), (BR, 6, 2)),
    ((WA, 0, 1), (WB, 0, 1), (XS, 0, 1), (XW, 0, 1), (F1, 0, 1), (F2, 0, 1), (F1, 1, 1), (FR, 0, 1),
     (F2, 1, 1), (F1, 2, 1), (FR, 1, 1), (F2, 2, 1), (F1, 3, 1), (F2, 3, 1), (FR, 2, 2), (F1, 4, 2),
     (F2, 4, 2), (T1, 0, 2), (T2, 0, 2), (F1, 6, 2), (FR, 4, 2), (F2, 6, 2), (T1, 2, 2), (FR, 6, 1),
     (T2, 2, 1), (FR, 7, 1), (T2, 3, 1), (BR, 3, 1), (T1, 4, 2), (T2, 4, 2), (T1, 6, 2), (BR, 4, 2),
     (T2, 6, 1), (T2, 7, 1), (BR, 6, 2)),
    ((WB, 0, 1), (XS, 0, 1), (PR, 0, 1), (XW, 0, 1), (M1, 0, 1), (B2, 0, 1), (M1, 1, 1), (B2, 1, 1),
     (BR, 0, 2), (M1, 2, 2), (B2, 2, 2), (BR, 2, 2), (M1, 4, 2), (B2, 4, 2), (BR, 4, 2), (M1, 6, 2),
     (B2, 6, 1), (B2, 7, 1), (BR, 6, 2), (YL, 0, 1), (F2, 0, 1), (F2, 1, 2), (FR, 0, 3), (F2, 3, 1),
     (F2, 4, 1), (F2, 5, 1), (FR, 3, 3), (F2, 6, 2), (FR, 6, 2)),
)


PACK = 1024
UP_GROUP = 8
TURN = 6
TURN_GROUP = 4
DOWN_GROUP = 2


def plan_words():
    rows = [[op + 32 * unit + 256 * (count - 1) for op, unit, count in row] for row in PLAN]
    steps = -(-max(len(row) for row in rows) // 3) * 3
    rows = [row + [0] * (steps - len(row)) for row in rows]
    return steps, [[row[t] + PACK * row[t + 1] + PACK * PACK * row[t + 2] for t in range(0, steps, 3)] for row in rows]


def gelu_pair(pre_act):
    root = pre_act * 0.7071067811865476
    normal_cdf = 0.5 * (1.0 + lax.erf(root))
    normal_pdf = jnp.exp2(root * root * -1.4426950408889634) * 0.3989422804014327
    return pre_act * normal_cdf, normal_cdf + pre_act * normal_pdf


def wait_bytes(ref, sem):
    pltpu.make_async_copy(ref, ref, sem).wait()


def pipeline_kernel(x_ref, g_ref, w1_ref, w2_ref,
                    y_out, dx_out, h_out, g_out, a_out, d_out,
                    wa, wb, flow, act, slope, part, recv, send, home, direct,
                    flow_sem, recv_sem, part_send, flow_send, home_send, home_sem, in_send, relay_sem, relay_send,
                    direct_sem, direct_send, cross_send, stage_sem, w_sem, out_sem):
    stage = lax.axis_index('stage')
    side = lax.axis_index('inner')
    other = 1 - side
    rows, d_model = flow.shape[3:]
    tok, d_ff = act.shape[2:]
    n_blk = d_model // BLK

    def peer(s, i):
        return {'stage': s, 'inner': i}

    load_a = pltpu.make_async_copy(w1_ref, wa, w_sem.at[0])
    load_b = pltpu.make_async_copy(w2_ref, wb, w_sem.at[1])

    def unit_of(k):
        return lax.rem(2 * stage + k + UNITS - 1, UNITS)

    staged = (send.at[BWD, pl.ds(UNITS - 2, 2)], send.at[BWD, pl.ds(UNITS - 4, 2)])
    stagings = [pltpu.make_async_copy(src, dst, stage_sem.at[kind]) for kind, (src, dst) in enumerate(zip((x_ref, g_ref), staged))]
    for kind, target in ((FWD, 0), (BWD, STAGES - 1)):
        stagings[kind].start()

        @pl.when(stage == target)
        def _():
            for k in range(2):
                pltpu.make_async_copy((x_ref, g_ref)[kind].at[k], flow.at[kind, unit_of(k), side], flow_sem.at[kind, unit_of(k), side]).start()

    @pl.when(stage < STAGES - 1)
    def _():
        load_a.start()
    load_b.start()

    @pl.when(stage == STAGES - 1)
    def _():
        load_a.start()

    barrier = pltpu.get_barrier_semaphore()
    for s in range(STAGES):
        for i in range(INNER):
            @pl.when(jnp.logical_or(stage != s, side != i))
            def _():
                pl.semaphore_signal(barrier, inc=1, device_id=peer(s, i), device_id_type=MESH)
    pl.semaphore_wait(barrier, STAGES * INNER - 1)

    def home_of(u):
        return lax.rem((u + 1) // 2, STAGES)

    def slot_of(u):
        return lax.rem(u + 1, 2)

    def hand_in(kind, target, k, lane):
        u = unit_of(k)
        src = staged[kind]
        if lane == 0:
            @pl.when(stage != target)
            def _():
                pltpu.make_async_remote_copy(src.at[k], flow.at[kind, u, side], in_send.at[kind, k, 0], flow_sem.at[kind, u, side],
                                             device_id=peer(target, side), device_id_type=MESH).start()
        else:
            pltpu.make_async_remote_copy(src.at[k], flow.at[kind, u, side], in_send.at[kind, k, 1], flow_sem.at[kind, u, side],
                                         device_id=peer(target, other), device_id_type=MESH).start()

    def relay(k):
        return pltpu.make_async_remote_copy(staged[FWD].at[k], home.at[FWD, k], in_send.at[FWD, k, 1], relay_sem.at[k],
                                            device_id=peer(stage, other), device_id_type=MESH)

    def relayed(k):
        u = unit_of(k)
        return pltpu.make_async_remote_copy(home.at[FWD, k], flow.at[FWD, u, other], relay_send.at[k], flow_sem.at[FWD, u, other],
                                            device_id=peer(0, side), device_id_type=MESH)

    stagings[FWD].wait()
    for k in range(2):
        hand_in(FWD, 0, k, 0)

        @pl.when(jnp.logical_or(stage == 1, jnp.logical_and(stage == 0, k == 1)))
        def _():
            hand_in(FWD, 0, k, 1)

        @pl.when(stage > 1)
        def _():
            relay(k).start()
    stagings[BWD].wait()
    for k in range(2):
        for lane in range(2):
            hand_in(BWD, STAGES - 1, k, lane)

    steps, plan = plan_words()
    words = [jnp.where(stage == 0, a, jnp.where(stage == 1, b, jnp.where(stage == 2, c, d))) for a, b, c, d in zip(*plan)]

    def keep(ref, out, u, lane):
        pltpu.make_async_copy(ref, out.at[u], out_sem.at[lane]).start()

    def blocks(width, group, fn):
        def body(t, carry):
            fn([pl.ds(pl.multiple_of((t * group + k) * BLK, BLK), BLK) for k in range(group)])
            return carry
        lax.fori_loop(0, width // BLK // group, body, 0)

    def arrived(kind, u):
        for half in range(INNER):
            @pl.when(jnp.logical_not((stage == 1) & (kind == BWD) & (u < DIRECT) & (side == half)))
            def _():
                wait_bytes(flow.at[kind, u, half], flow_sem.at[kind, u, half])

    def both_arrived(kind, u, v):
        arrived(kind, u)

        @pl.when(v != u)
        def _():
            arrived(kind, v)

    def pair(ref, kind, u, v):
        width = ref.shape[-1]
        return jnp.concatenate([ref[kind, u].reshape(tok, width), ref[kind, v].reshape(tok, width)], axis=0)

    def kept(u, v, fn):
        fn(u)

        @pl.when(v != u)
        def _():
            fn(v)

    def up_product(u, v, last):
        both_arrived(FWD, u, v)

        def fn(slices):
            lhs = pair(flow, FWD, u, v)
            for sl in slices:
                z = jnp.dot(lhs, wa[:, sl], preferred_element_type=F32)
                value, grad = gelu_pair(z)
                value = value.astype(BF16)
                if last:
                    act[BWD, u, :, sl] = (slope[u, :, sl] * grad[:tok]).astype(BF16)
                    act[BWD, v, :, sl] = (slope[v, :, sl] * grad[tok:]).astype(BF16)
                else:
                    slope[u, :, sl] = grad[:tok]
                    slope[v, :, sl] = grad[tok:]
                act[FWD, u, :, sl] = value[:tok]
                act[FWD, v, :, sl] = value[tok:]
        blocks(d_ff, UP_GROUP, fn)

        def out(w):
            keep(flow.at[FWD, w], h_out, w, 0)
            keep(act.at[FWD, w], a_out, w, 2)
            if last:
                keep(act.at[BWD, w], d_out, w, 3)
        kept(u, v, out)

    def across(lhs, ref, sl):
        cut = ref.shape[1] * TURN // 8
        total = lax.dot_general(lhs[:, :cut], ref[sl, :cut], NT, preferred_element_type=F32)
        for k in range(cut, ref.shape[1], TILE):
            turned = [ref[pl.ds(sl.start + q, TILE), k:k + TILE].T for q in range(0, BLK, TILE)]
            total += jnp.dot(lhs[:, k:k + TILE], jnp.concatenate(turned, axis=1), preferred_element_type=F32)
        return total

    def back_product(u, v, swapped):
        both_arrived(BWD, u, v)

        def fn(slices):
            lhs = pair(flow, BWD, u, v)
            for sl in slices:
                if swapped:
                    e = jnp.dot(lhs, wa[:, sl], preferred_element_type=F32)
                else:
                    e = across(lhs, wb, sl)
                act[BWD, u, :, sl] = (e[:tok] * slope[u, :, sl]).astype(BF16)
                act[BWD, v, :, sl] = (e[tok:] * slope[v, :, sl]).astype(BF16)
        blocks(d_ff, UP_GROUP if swapped else TURN_GROUP, fn)

        def out(w):
            keep(flow.at[BWD, w], g_out, w, 1)
            keep(act.at[BWD, w], d_out, w, 3)
        kept(u, v, out)

    def part_copy(kind, u, j):
        slot = lax.rem(u, SLOTS)
        return pltpu.make_async_remote_copy(part.at[kind, slot, j, other], recv.at[kind, u, j], part_send.at[kind, slot, j],
                                            recv_sem.at[kind, u, j], device_id=peer(stage, other), device_id_type=MESH)

    def direct_copy(u, j, half):
        slot = lax.rem(u, SLOTS)
        if half is side:
            return pltpu.make_async_remote_copy(part.at[BWD, slot, j, side], direct.at[u, j], direct_send.at[slot, j],
                                                direct_sem.at[0, u, j], device_id=peer(stage - 1, side), device_id_type=MESH)
        return pltpu.make_async_remote_copy(part.at[BWD, slot, j, other], recv.at[FWD, u, j], part_send.at[BWD, slot, j],
                                            direct_sem.at[1, u, j], device_id=peer(stage - 1, other), device_id_type=MESH)

    def take_direct(first, count):
        def body(i, carry):
            u = first + i
            for j in range(n_blk):
                sl = pl.ds(j * BLK, BLK)
                wait_bytes(direct.at[u, j], direct_sem.at[0, u, j])
                wait_bytes(recv.at[FWD, u, j], direct_sem.at[1, u, j])
                flow[BWD, u, side, :, sl] = (direct[u, j] + recv[FWD, u, j]).astype(BF16)
                pltpu.make_async_remote_copy(flow.at[BWD, u, side, :, sl], flow.at[BWD, u, side, :, sl], cross_send.at[0],
                                             flow_sem.at[BWD, u, side], device_id=peer(stage, other), device_id_type=MESH).start()
            return carry
        lax.fori_loop(0, count, body, 0)

    def down_product(kind, u, v, straight):
        def free(w):
            @pl.when(w >= SLOTS)
            def _():
                for j in range(n_blk):
                    part_copy(kind, w - SLOTS, j).wait_send()

            if not straight:
                @pl.when((w >= SLOTS) & (w < SLOTS + DIRECT))
                def _():
                    for j in range(n_blk):
                        direct_copy(w - SLOTS, j, side).wait_send()
        kept(u, v, free)

        def body(t, carry):
            lhs = pair(act, kind, u, v)
            for k in range(DOWN_GROUP):
                j = t * DOWN_GROUP + k
                sl = pl.ds(pl.multiple_of(j * BLK, BLK), BLK)
                if straight:
                    p = jnp.dot(lhs, wb[:, sl], preferred_element_type=F32)
                else:
                    p = across(lhs, wa, sl)
                p = p.reshape(2, INNER, rows, BLK)
                part[kind, lax.rem(u, SLOTS), j] = p[0]
                part[kind, lax.rem(v, SLOTS), j] = p[1]

            def go(w):
                if straight:
                    for k in range(DOWN_GROUP):
                        part_copy(kind, w, t * DOWN_GROUP + k).start()
                    return

                @pl.when(w >= DIRECT)
                def _():
                    for k in range(DOWN_GROUP):
                        part_copy(kind, w, t * DOWN_GROUP + k).start()

                @pl.when(w < DIRECT)
                def _():
                    for k in range(DOWN_GROUP):
                        j = t * DOWN_GROUP + k
                        sl = pl.ds(pl.multiple_of(j * BLK, BLK), BLK)
                        part[BWD, lax.rem(w, SLOTS), j, side] += flow[BWD, w, side, :, sl].astype(F32)
                    for k in range(DOWN_GROUP):
                        for half in (side, other):
                            direct_copy(w, t * DOWN_GROUP + k, half).start()
            kept(u, v, go)
            return carry
        lax.fori_loop(0, n_blk // DOWN_GROUP, body, 0)

    def hand_on(kind, first, count):
        target = stage + 1 if kind == FWD else stage - 1
        inside = stage < STAGES - 1 if kind == FWD else stage > 0
        out = STAGES - 1 if kind == FWD else 0

        def body(i, carry):
            u = first + i
            slot = lax.rem(u, SLOTS)
            for j in range(n_blk):
                sl = pl.ds(j * BLK, BLK)
                wait_bytes(recv.at[kind, u, j], recv_sem.at[kind, u, j])
                total = flow[kind, u, side, :, sl].astype(F32) + (part[kind, slot, j, side] + recv[kind, u, j])
                send[kind, u, :, sl] = total.astype(BF16)

                @pl.when(inside)
                def _():
                    for half in (side, other):
                        pltpu.make_async_remote_copy(send.at[kind, u, :, sl], flow.at[kind, u, side, :, sl], flow_send.at[kind],
                                                     flow_sem.at[kind, u, side], device_id=peer(target, half), device_id_type=MESH).start()

            @pl.when(jnp.logical_and(jnp.logical_not(inside), home_of(u) != out))
            def _():
                pltpu.make_async_remote_copy(send.at[kind, u], home.at[kind, slot_of(u)], home_send.at[kind, u],
                                             home_sem.at[kind, slot_of(u)], device_id=peer(home_of(u), side), device_id_type=MESH).start()
            return carry
        lax.fori_loop(0, count, body, 0)

    def swap_weights():
        n_i = d_model // TILE

        def body(t, carry):
            i = pl.multiple_of(lax.rem(t, n_i) * TILE, TILE)
            j = pl.multiple_of(lax.div(t, n_i) * TILE, TILE)
            up = wa[pl.ds(i, TILE), pl.ds(j, TILE)]
            down = wb[pl.ds(j, TILE), pl.ds(i, TILE)]
            wa[pl.ds(i, TILE), pl.ds(j, TILE)] = down.T
            wb[pl.ds(j, TILE), pl.ds(i, TILE)] = up.T
            return carry
        lax.fori_loop(0, n_i * (d_ff // TILE), body, 0)

    def prepare_last():
        half = UNITS // 2

        def quarter(q, carry):
            for i in range(half):
                arrived(BWD, q * half + i)
                keep(flow.at[BWD, q * half + i], g_out, q * half + i, 1)
            units = pl.ds(q * half, half)

            def fn(slices):
                lhs = flow[BWD, units].reshape(half * tok, d_model)
                for sl in slices:
                    e = lax.dot_general(lhs, wb[sl, :], NT, preferred_element_type=F32)
                    slope[units, :, sl] = e.reshape(half, tok, BLK)
            blocks(d_ff, 1, fn)
            return carry
        lax.fori_loop(0, 2, quarter, 0)
        load_a.wait()
        n_i = d_model // TILE

        def body(t, carry):
            i = pl.multiple_of(lax.rem(t, n_i) * TILE, TILE)
            j = pl.multiple_of(lax.div(t, n_i) * TILE, TILE)
            wb[pl.ds(j, TILE), pl.ds(i, TILE)] = wa[pl.ds(i, TILE), pl.ds(j, TILE)].T
            return carry
        lax.fori_loop(0, n_i * (d_ff // TILE), body, 0)

    def step(t, carry):
        group, place = lax.div(t, 3), lax.rem(t, 3)
        word = words[0]
        for i, w in enumerate(words[1:], 1):
            word = jnp.where(group == i, w, word)
        code = lax.rem(lax.div(word, jnp.where(place == 0, 1, jnp.where(place == 1, PACK, PACK * PACK))), PACK)
        op = lax.rem(code, 32)
        u = lax.rem(lax.div(code, 32), UNITS)
        count = lax.div(code, 256) + 1

        def on(want):
            return pl.when(op == want)

        v = jnp.minimum(u + count - 1, UNITS - 1)

        @on(F1)
        def _():
            up_product(u, v, False)

        @on(M1)
        def _():
            up_product(u, v, True)

        @pl.when(jnp.logical_or(op == F2, op == B2))
        def _():
            down_product(jnp.where(op == F2, FWD, BWD), u, v, True)

        @on(FR)
        def _():
            hand_on(FWD, u, count)

        @on(BR)
        def _():
            hand_on(BWD, u, count)

        @on(B1)
        def _():
            back_product(u, v, True)

        @on(T1)
        def _():
            back_product(u, v, False)

        @on(T2)
        def _():
            down_product(BWD, u, v, False)

        @on(SW)
        def _():
            swap_weights()

        @on(PR)
        def _():
            prepare_last()

        @on(YL)
        def _():
            load_b.start()
            load_b.wait()

        @on(WA)
        def _():
            load_a.wait()

        @on(WB)
        def _():
            load_b.wait()

        @on(XS)
        def _():
            @pl.when(stage == 0)
            def _():
                hand_in(FWD, 0, 0, 1)

            @pl.when(stage > 1)
            def _():
                for k in range(2):
                    wait_bytes(home.at[FWD, k], relay_sem.at[k])
                    relayed(k).start()

        @on(XW)
        def _():
            for kind, target in ((FWD, 0), (BWD, STAGES - 1)):
                for k in range(2):
                    @pl.when(stage != target)
                    def _():
                        wait_bytes(staged[kind].at[k], in_send.at[kind, k, 0])
                    wait_bytes(staged[kind].at[k], in_send.at[kind, k, 1])

            @pl.when(stage > 1)
            def _():
                for k in range(2):
                    relayed(k).wait_send()

        @on(HB)
        def _():
            take_direct(u, count)
        return carry
    lax.fori_loop(0, steps, step, 0)

    for kind, here, out in ((FWD, STAGES - 1, y_out), (BWD, 0, dx_out)):
        for k in range(2):
            @pl.when(stage == here)
            def _():
                pltpu.make_async_copy(send.at[kind, unit_of(k)], out.at[k], out_sem.at[4 + kind]).start()

            @pl.when(stage != here)
            def _():
                wait_bytes(home.at[kind, k], home_sem.at[kind, k])
                pltpu.make_async_copy(home.at[kind, k], out.at[k], out_sem.at[4 + kind]).start()

    for kind in (FWD, BWD):
        for u in range(UNITS - SLOTS, UNITS):
            for j in range(n_blk):
                part_copy(kind, u, j).wait_send()
    for kind, last in ((FWD, STAGES - 1), (BWD, 0)):
        @pl.when((stage != last) & jnp.logical_not((stage == 2) & (kind == BWD)))
        def _():
            wait_bytes(flow.at[kind], flow_send.at[kind])

        @pl.when(stage == last)
        def _():
            for u in range(UNITS):
                if (u + 1) // 2 % STAGES != last:
                    wait_bytes(send.at[kind, u], home_send.at[kind, u])
    @pl.when(stage == 2)
    def _():
        wait_bytes(flow.at[BWD, pl.ds(0, UNITS - DIRECT)], flow_send.at[BWD])

    @pl.when(stage == 1)
    def _():
        wait_bytes(flow.at[BWD, pl.ds(0, DIRECT), 0], cross_send.at[0])
    for lane, (ref, out) in enumerate(((flow.at[FWD], h_out), (flow.at[BWD], g_out), (act.at[FWD], a_out), (act.at[BWD], d_out),
                                       (home.at[FWD], y_out), (home.at[BWD], dx_out))):
        pltpu.make_async_copy(ref, out, out_sem.at[lane]).wait()


def run_pipeline(x_loc, g_loc, w_one, w_two):
    rows, d_model = x_loc.shape[1:]
    d_ff = w_one.shape[1]
    n_blk = d_model // BLK
    tok = INNER * rows
    hbm = pl.BlockSpec(memory_space=pl.ANY)
    out = lambda *shape: jax.ShapeDtypeStruct(shape, BF16)
    dma = lambda *shape: pltpu.SemaphoreType.DMA(shape)
    return pl.pallas_call(
        pipeline_kernel,
        name='pipeline',
        out_shape=(out(*x_loc.shape), out(*x_loc.shape), out(UNITS, INNER, rows, d_model), out(UNITS, INNER, rows, d_model),
                   out(UNITS, tok, d_ff), out(UNITS, tok, d_ff)),
        in_specs=[hbm] * 4,
        out_specs=(hbm,) * 6,
        scratch_shapes=[
            pltpu.VMEM((d_model, d_ff), BF16),
            pltpu.VMEM((d_ff, d_model), BF16),
            pltpu.VMEM((2, UNITS, INNER, rows, d_model), BF16),
            pltpu.VMEM((2, UNITS, tok, d_ff), BF16),
            pltpu.VMEM((UNITS, tok, d_ff), F32),
            pltpu.VMEM((2, SLOTS, n_blk, INNER, rows, BLK), F32),
            pltpu.VMEM((2, UNITS, n_blk, rows, BLK), F32),
            pltpu.VMEM((2, UNITS, rows, d_model), BF16),
            pltpu.VMEM((2, 2, rows, d_model), BF16),
            pltpu.VMEM((DIRECT, n_blk, rows, BLK), F32),
            dma(2, UNITS, INNER), dma(2, UNITS, n_blk), dma(2, SLOTS, n_blk), dma(2), dma(2, UNITS), dma(2, 2), dma(2, 2, 2), dma(2), dma(2),
            dma(2, DIRECT, n_blk), dma(SLOTS, n_blk), dma(1), dma(2), dma(2), dma(6),
        ],
        compiler_params=pltpu.CompilerParams(collective_id=0, has_side_effects=True, vmem_limit_bytes=67043328),
    )(x_loc, g_loc, w_one, w_two)


GRAD_ROWS, GRAD_COLS = 1024, 2048


def weight_grad_kernel(h_ref, d_ref, a_ref, g_ref, y_ref, x_ref, up_ref, down_ref, y_out, x_out,
                       h, d, a, g, home, stage, in_sem, home_sem, out_sem):
    tokens, d_model = h.shape
    d_ff = d.shape[1]
    n_down, n_up = d_ff // GRAD_ROWS, d_model // GRAD_ROWS
    n_col = d_ff // GRAD_COLS

    loads = [(g_ref, g)] + [(a_ref.at[:, pl.ds(t * GRAD_ROWS, GRAD_ROWS)], a.at[:, pl.ds(t * GRAD_ROWS, GRAD_ROWS)]) for t in range(n_down)] + [(h_ref, h), (d_ref, d)]
    loads = [pltpu.make_async_copy(src, dst, in_sem.at[t]) for t, (src, dst) in enumerate(loads)]
    homes = [pltpu.make_async_copy(src, home.at[t], home_sem.at[t]) for t, src in enumerate((y_ref, x_ref))]
    for copy in loads + homes:
        copy.start()
    loads[0].wait()

    def block(t, src, first, other, second, out, pieces=1):
        slot = lax.rem(t, 2)
        size = GRAD_ROWS // pieces
        for p in range(pieces):
            rows = pl.ds(pl.multiple_of(first + p * size, size), size)
            cols = pl.ds(pl.multiple_of(second, GRAD_COLS), GRAD_COLS)
            stage[slot, pl.ds(p * size, size)] = lax.dot_general(src[:, rows], other[:, cols], (((0,), (0,)), ((), ())), preferred_element_type=F32)
            pltpu.make_async_copy(stage.at[slot, pl.ds(p * size, size)], out.at[rows, cols], out_sem.at[slot]).start()

    def freed(slot):
        pltpu.make_async_copy(stage.at[slot], stage.at[slot], out_sem.at[slot]).wait()

    def down(t, carry):
        pltpu.make_async_copy(a_ref.at[:, pl.ds(0, GRAD_ROWS)], a.at[:, pl.ds(0, GRAD_ROWS)], in_sem.at[1 + t]).wait()

        @pl.when(t >= 2)
        def _():
            freed(lax.rem(t, 2))
        block(t, a, t * GRAD_ROWS, g, 0, down_ref)
        return carry
    lax.fori_loop(0, n_down, down, 0)
    loads[1 + n_down].wait()
    loads[2 + n_down].wait()
    for copy, (src, dst) in zip(homes, ((home.at[0], y_out), (home.at[1], x_out))):
        copy.wait()
    backs = [pltpu.make_async_copy(home.at[t], dst, home_sem.at[t]) for t, dst in enumerate((y_out, x_out))]
    for copy in backs:
        copy.start()

    def up(t, carry):
        freed(lax.rem(t, 2))
        block(t, h, lax.div(t, n_col) * GRAD_ROWS, d, lax.rem(t, n_col) * GRAD_COLS, up_ref)
        return carry
    n_blocks = n_up * n_col
    lax.fori_loop(0, n_blocks - 1, up, 0)
    freed((n_blocks - 1) % 2)
    block(n_blocks - 1, h, (n_up - 1) * GRAD_ROWS, d, (n_col - 1) * GRAD_COLS, up_ref, 4)
    for slot in range(2):
        freed(slot)
    for copy in backs:
        copy.wait()


def weight_grads(h, d, a, g, y, dx):
    tokens, d_model = h.shape
    d_ff = d.shape[1]
    n_in = 3 + d_ff // GRAD_ROWS
    hbm = pl.BlockSpec(memory_space=pl.ANY)
    dma = lambda *shape: pltpu.SemaphoreType.DMA(shape)
    like = lambda v: pltpu.VMEM(v.shape, v.dtype)
    return pl.pallas_call(
        weight_grad_kernel,
        name='weight_grads',
        out_shape=(jax.ShapeDtypeStruct((d_model, d_ff), F32), jax.ShapeDtypeStruct((d_ff, d_model), F32),
                   jax.ShapeDtypeStruct(y.shape, BF16), jax.ShapeDtypeStruct(y.shape, BF16)),
        in_specs=[hbm] * 6,
        out_specs=(hbm,) * 4,
        scratch_shapes=[like(h), like(d), like(a), like(g), pltpu.VMEM((2,) + y.shape, BF16), pltpu.VMEM((2, GRAD_ROWS, GRAD_COLS), F32),
                        dma(n_in), dma(2), dma(2)],
        compiler_params=pltpu.CompilerParams(vmem_limit_bytes=60 * 1024 * 1024),
    )(h, d, a, g, y, dx)


def solution(mesh):
    tok_spec = P(('data', 'stage', 'inner'))
    up_spec = P(None, ('data', 'stage'), None, 'inner')
    down_spec = P(None, ('data', 'stage'), 'inner', None)

    def device_step(x_loc, g_loc, w_up, w_down):
        y, dx, h, g, a, d = run_pipeline(x_loc, g_loc, w_up[0, 0], w_down[0, 0])
        flat = lambda v: v.reshape(-1, v.shape[-1])
        dw_up, dw_down, y, dx = weight_grads(flat(h), flat(d), flat(a), flat(g), y, dx)
        return y, dx, dw_up[None, None], dw_down[None, None]

    return jax.shard_map(device_step, mesh=mesh, in_specs=(tok_spec, tok_spec, up_spec, down_spec), out_specs=(tok_spec, tok_spec, up_spec, down_spec), check_vma=False)
```

```python
import functools

import jax
import jax.numpy as jnp
from jax import lax
from jax.experimental import pallas as pl
from jax.experimental.pallas import tpu as pltpu
from jax.sharding import PartitionSpec as P

F32 = jnp.float32
BF16 = jnp.bfloat16
MESH = pl.DeviceIdType.MESH

STAGES = 4
INNER = 2
UNITS = 8
SLOTS = 3
DIRECT = 3
BLK = 512
TILE = 256
FWD, BWD = 0, 1
NT = (((1,), (1,)), ((), ()))

F1, F2, FR, B1, B2, BR, T1, T2, SW, PR, YL, WA, WB, XS, M1, HB, XW = range(1, 18)
PLAN = (
    ((WA, 0, 1), (F1, 0, 2), (WB, 0, 1), (XS, 0, 1), (F2, 0, 1), (F2, 1, 1), (FR, 0, 1), (F1, 2, 2),
     (FR, 1, 1), (F2, 2, 1), (F2, 3, 1), (F1, 4, 1), (F1, 5, 2), (FR, 2, 2), (F2, 4, 1), (F2, 5, 1),
     (FR, 4, 2), (F1, 7, 1), (F2, 6, 2), (FR, 6, 2), (XW, 0, 1), (SW, 0, 1), (B1, 0, 1), (B1, 1, 1),
     (B2, 0, 1), (B2, 1, 1), (B1, 2, 2), (B2, 2, 1), (BR, 0, 1), (B2, 3, 1), (BR, 1, 1), (B1, 4, 1),
     (BR, 2, 2), (B1, 5, 1), (B2, 4, 1), (B2, 5, 1), (B1, 6, 2), (BR, 4, 1), (B2, 6, 2), (BR, 5, 3)),
    ((WA, 0, 1), (WB, 0, 1), (XS, 0, 1), (F1, 0, 1), (F2, 0, 1), (F1, 1, 1), (F2, 1, 1), (FR, 0, 2),
     (F1, 2, 2), (F2, 2, 1), (F2, 3, 1), (FR, 2, 1), (F1, 4, 2), (FR, 3, 1), (F2, 4, 1), (F2, 5, 1),
     (FR, 4, 2), (F1, 6, 1), (F2, 6, 1), (F1, 7, 1), (F2, 7, 1), (FR, 6, 2), (XW, 0, 1), (SW, 0, 1),
     (HB, 0, 2), (B1, 0, 2), (B2, 0, 1), (HB, 2, 1), (B2, 1, 1), (B1, 2, 1), (BR, 0, 1), (B2, 2, 1),
     (BR, 1, 1), (B1, 3, 1), (B2, 3, 1), (BR, 2, 2), (B1, 4, 2), (B2, 4, 1), (B2, 5, 1), (BR, 4, 1),
     (B1, 6, 2), (BR, 5, 1), (B2, 6, 1), (B2, 7, 1), (BR, 6, 2)),
    ((WA, 0, 1), (WB, 0, 1), (XS, 0, 1), (XW, 0, 1), (F1, 0, 1), (F2, 0, 1), (F1, 1, 1), (FR, 0, 1),
     (F2, 1, 1), (F1, 2, 1), (FR, 1, 1), (F2, 2, 1), (F1, 3, 1), (F2, 3, 1), (FR, 2, 2), (F1, 4, 2),
     (F2, 4, 2), (T1, 0, 2), (T2, 0, 2), (F1, 6, 2), (FR, 4, 2), (F2, 6, 2), (T1, 2, 2), (FR, 6, 1),
     (T2, 2, 1), (FR, 7, 1), (T2, 3, 1), (BR, 3, 1), (T1, 4, 2), (T2, 4, 2), (T1, 6, 2), (BR, 4, 2),
     (T2, 6, 1), (T2, 7, 1), (BR, 6, 2)),
    ((WB, 0, 1), (XS, 0, 1), (PR, 0, 1), (XW, 0, 1), (M1, 0, 1), (B2, 0, 1), (M1, 1, 1), (B2, 1, 1),
     (BR, 0, 2), (M1, 2, 2), (B2, 2, 2), (BR, 2, 2), (M1, 4, 2), (B2, 4, 2), (BR, 4, 2), (M1, 6, 2),
     (B2, 6, 1), (B2, 7, 1), (BR, 6, 2), (YL, 0, 1), (F2, 0, 1), (F2, 1, 2), (FR, 0, 3), (F2, 3, 1),
     (F2, 4, 1), (F2, 5, 1), (FR, 3, 3), (F2, 6, 2), (FR, 6, 2)),
)


PACK = 1024
UP_GROUP = 8
TURN = 6
TURN_GROUP = 4
DOWN_GROUP = 2


def plan_words():
    rows = [[op + 32 * unit + 256 * (count - 1) for op, unit, count in row] for row in PLAN]
    steps = -(-max(len(row) for row in rows) // 3) * 3
    rows = [row + [0] * (steps - len(row)) for row in rows]
    return steps, [[row[t] + PACK * row[t + 1] + PACK * PACK * row[t + 2] for t in range(0, steps, 3)] for row in rows]


def gelu_pair(pre_act):
    root = pre_act * 0.7071067811865476
    normal_cdf = 0.5 * (1.0 + lax.erf(root))
    normal_pdf = jnp.exp2(root * root * -1.4426950408889634) * 0.3989422804014327
    return pre_act * normal_cdf, normal_cdf + pre_act * normal_pdf


def wait_bytes(ref, sem):
    pltpu.make_async_copy(ref, ref, sem).wait()


def pipeline_kernel(x_ref, g_ref, w1_ref, w2_ref,
                    y_out, dx_out, h_out, g_out, a_out, d_out,
                    wa, wb, flow, act, slope, part, recv, send, home, direct,
                    flow_sem, recv_sem, part_send, flow_send, home_send, home_sem, in_send, relay_sem, relay_send,
                    direct_sem, direct_send, cross_send, stage_sem, w_sem, out_sem):
    stage = lax.axis_index('stage')
    side = lax.axis_index('inner')
    other = 1 - side
    rows, d_model = flow.shape[3:]
    tok, d_ff = act.shape[2:]
    n_blk = d_model // BLK

    def peer(s, i):
        return {'stage': s, 'inner': i}

    load_a = pltpu.make_async_copy(w1_ref, wa, w_sem.at[0])
    load_b = pltpu.make_async_copy(w2_ref, wb, w_sem.at[1])

    def unit_of(k):
        return lax.rem(2 * stage + k + UNITS - 1, UNITS)

    staged = (send.at[BWD, pl.ds(UNITS - 2, 2)], send.at[BWD, pl.ds(UNITS - 4, 2)])
    stagings = [pltpu.make_async_copy(src, dst, stage_sem.at[kind]) for kind, (src, dst) in enumerate(zip((x_ref, g_ref), staged))]
    for kind, target in ((FWD, 0), (BWD, STAGES - 1)):
        stagings[kind].start()

        @pl.when(stage == target)
        def _():
            for k in range(2):
                pltpu.make_async_copy((x_ref, g_ref)[kind].at[k], flow.at[kind, unit_of(k), side], flow_sem.at[kind, unit_of(k), side]).start()

    @pl.when(stage < STAGES - 1)
    def _():
        load_a.start()
    load_b.start()

    @pl.when(stage == STAGES - 1)
    def _():
        load_a.start()

    barrier = pltpu.get_barrier_semaphore()
    for s in range(STAGES):
        for i in range(INNER):
            @pl.when(jnp.logical_or(stage != s, side != i))
            def _():
                pl.semaphore_signal(barrier, inc=1, device_id=peer(s, i), device_id_type=MESH)
    pl.semaphore_wait(barrier, STAGES * INNER - 1)

    def home_of(u):
        return lax.rem((u + 1) // 2, STAGES)

    def slot_of(u):
        return lax.rem(u + 1, 2)

    def hand_in(kind, target, k, lane):
        u = unit_of(k)
        src = staged[kind]
        if lane == 0:
            @pl.when(stage != target)
            def _():
                pltpu.make_async_remote_copy(src.at[k], flow.at[kind, u, side], in_send.at[kind, k, 0], flow_sem.at[kind, u, side],
                                             device_id=peer(target, side), device_id_type=MESH).start()
        else:
            pltpu.make_async_remote_copy(src.at[k], flow.at[kind, u, side], in_send.at[kind, k, 1], flow_sem.at[kind, u, side],
                                         device_id=peer(target, other), device_id_type=MESH).start()

    def relay(k):
        return pltpu.make_async_remote_copy(staged[FWD].at[k], home.at[FWD, k], in_send.at[FWD, k, 1], relay_sem.at[k],
                                            device_id=peer(stage, other), device_id_type=MESH)

    def relayed(k):
        u = unit_of(k)
        return pltpu.make_async_remote_copy(home.at[FWD, k], flow.at[FWD, u, other], relay_send.at[k], flow_sem.at[FWD, u, other],
                                            device_id=peer(0, side), device_id_type=MESH)

    stagings[FWD].wait()
    for k in range(2):
        hand_in(FWD, 0, k, 0)

        @pl.when(jnp.logical_or(stage == 1, jnp.logical_and(stage == 0, k == 1)))
        def _():
            hand_in(FWD, 0, k, 1)

        @pl.when(stage > 1)
        def _():
            relay(k).start()
    steps, plan = plan_words()
    words = [jnp.where(stage == 0, a, jnp.where(stage == 1, b, jnp.where(stage == 2, c, d))) for a, b, c, d in zip(*plan)]

    def keep(ref, out, u, lane):
        pltpu.make_async_copy(ref, out.at[u], out_sem.at[lane]).start()

    def blocks(width, group, fn):
        def body(t, carry):
            fn([pl.ds(pl.multiple_of((t * group + k) * BLK, BLK), BLK) for k in range(group)])
            return carry
        lax.fori_loop(0, width // BLK // group, body, 0)

    def arrived(kind, u):
        for half in range(INNER):
            @pl.when(jnp.logical_not((stage == 1) & (kind == BWD) & (u < DIRECT) & (side == half)))
            def _():
                wait_bytes(flow.at[kind, u, half], flow_sem.at[kind, u, half])

    def both_arrived(kind, u, v):
        arrived(kind, u)

        @pl.when(v != u)
        def _():
            arrived(kind, v)

    def pair(ref, kind, u, v):
        width = ref.shape[-1]
        return jnp.concatenate([ref[kind, u].reshape(tok, width), ref[kind, v].reshape(tok, width)], axis=0)

    def kept(u, v, fn):
        fn(u)

        @pl.when(v != u)
        def _():
            fn(v)

    def up_product(u, v, last):
        both_arrived(FWD, u, v)

        def fn(slices):
            lhs = pair(flow, FWD, u, v)
            for sl in slices:
                z = jnp.dot(lhs, wa[:, sl], preferred_element_type=F32)
                value, grad = gelu_pair(z)
                value = value.astype(BF16)
                if last:
                    act[BWD, u, :, sl] = (slope[u, :, sl] * grad[:tok]).astype(BF16)
                    act[BWD, v, :, sl] = (slope[v, :, sl] * grad[tok:]).astype(BF16)
                else:
                    slope[u, :, sl] = grad[:tok]
                    slope[v, :, sl] = grad[tok:]
                act[FWD, u, :, sl] = value[:tok]
                act[FWD, v, :, sl] = value[tok:]
        blocks(d_ff, UP_GROUP, fn)

        def out(w):
            keep(flow.at[FWD, w], h_out, w, 0)
            keep(act.at[FWD, w], a_out, w, 2)
            if last:
                keep(act.at[BWD, w], d_out, w, 3)
        kept(u, v, out)

    def across(lhs, ref, sl):
        cut = ref.shape[1] * TURN // 8
        total = lax.dot_general(lhs[:, :cut], ref[sl, :cut], NT, preferred_element_type=F32)
        for k in range(cut, ref.shape[1], TILE):
            turned = [ref[pl.ds(sl.start + q, TILE), k:k + TILE].T for q in range(0, BLK, TILE)]
            total += jnp.dot(lhs[:, k:k + TILE], jnp.concatenate(turned, axis=1), preferred_element_type=F32)
        return total

    def back_product(u, v, swapped):
        both_arrived(BWD, u, v)

        def fn(slices):
            lhs = pair(flow, BWD, u, v)
            for sl in slices:
                if swapped:
                    e = jnp.dot(lhs, wa[:, sl], preferred_element_type=F32)
                else:
                    e = across(lhs, wb, sl)
                act[BWD, u, :, sl] = (e[:tok] * slope[u, :, sl]).astype(BF16)
                act[BWD, v, :, sl] = (e[tok:] * slope[v, :, sl]).astype(BF16)
        blocks(d_ff, UP_GROUP if swapped else TURN_GROUP, fn)

        def out(w):
            keep(flow.at[BWD, w], g_out, w, 1)
            keep(act.at[BWD, w], d_out, w, 3)
        kept(u, v, out)

    def part_copy(kind, u, j):
        slot = lax.rem(u, SLOTS)
        return pltpu.make_async_remote_copy(part.at[kind, slot, j, other], recv.at[kind, u, j], part_send.at[kind, slot, j],
                                            recv_sem.at[kind, u, j], device_id=peer(stage, other), device_id_type=MESH)

    def direct_copy(u, j, half):
        slot = lax.rem(u, SLOTS)
        if half is side:
            return pltpu.make_async_remote_copy(part.at[BWD, slot, j, side], direct.at[u, j], direct_send.at[slot, j],
                                                direct_sem.at[0, u, j], device_id=peer(stage - 1, side), device_id_type=MESH)
        return pltpu.make_async_remote_copy(part.at[BWD, slot, j, other], recv.at[FWD, u, j], part_send.at[BWD, slot, j],
                                            direct_sem.at[1, u, j], device_id=peer(stage - 1, other), device_id_type=MESH)

    def take_direct(first, count):
        def body(i, carry):
            u = first + i
            for j in range(n_blk):
                sl = pl.ds(j * BLK, BLK)
                wait_bytes(direct.at[u, j], direct_sem.at[0, u, j])
                wait_bytes(recv.at[FWD, u, j], direct_sem.at[1, u, j])
                flow[BWD, u, side, :, sl] = (direct[u, j] + recv[FWD, u, j]).astype(BF16)
                pltpu.make_async_remote_copy(flow.at[BWD, u, side, :, sl], flow.at[BWD, u, side, :, sl], cross_send.at[0],
                                             flow_sem.at[BWD, u, side], device_id=peer(stage, other), device_id_type=MESH).start()
            return carry
        lax.fori_loop(0, count, body, 0)

    def down_product(kind, u, v, straight):
        def free(w):
            @pl.when(w >= SLOTS)
            def _():
                for j in range(n_blk):
                    part_copy(kind, w - SLOTS, j).wait_send()

            if not straight:
                @pl.when((w >= SLOTS) & (w < SLOTS + DIRECT))
                def _():
                    for j in range(n_blk):
                        direct_copy(w - SLOTS, j, side).wait_send()
        kept(u, v, free)

        def body(t, carry):
            lhs = pair(act, kind, u, v)
            for k in range(DOWN_GROUP):
                j = t * DOWN_GROUP + k
                sl = pl.ds(pl.multiple_of(j * BLK, BLK), BLK)
                if straight:
                    p = jnp.dot(lhs, wb[:, sl], preferred_element_type=F32)
                else:
                    p = across(lhs, wa, sl)
                p = p.reshape(2, INNER, rows, BLK)
                part[kind, lax.rem(u, SLOTS), j] = p[0]
                part[kind, lax.rem(v, SLOTS), j] = p[1]

            def go(w):
                if straight:
                    for k in range(DOWN_GROUP):
                        part_copy(kind, w, t * DOWN_GROUP + k).start()
                    return

                @pl.when(w >= DIRECT)
                def _():
                    for k in range(DOWN_GROUP):
                        part_copy(kind, w, t * DOWN_GROUP + k).start()

                @pl.when(w < DIRECT)
                def _():
                    for k in range(DOWN_GROUP):
                        j = t * DOWN_GROUP + k
                        sl = pl.ds(pl.multiple_of(j * BLK, BLK), BLK)
                        part[BWD, lax.rem(w, SLOTS), j, side] += flow[BWD, w, side, :, sl].astype(F32)
                    for k in range(DOWN_GROUP):
                        for half in (side, other):
                            direct_copy(w, t * DOWN_GROUP + k, half).start()
            kept(u, v, go)
            return carry
        lax.fori_loop(0, n_blk // DOWN_GROUP, body, 0)

    def hand_on(kind, first, count):
        target = stage + 1 if kind == FWD else stage - 1
        inside = stage < STAGES - 1 if kind == FWD else stage > 0
        out = STAGES - 1 if kind == FWD else 0

        def body(i, carry):
            u = first + i
            slot = lax.rem(u, SLOTS)
            for j in range(n_blk):
                sl = pl.ds(j * BLK, BLK)
                wait_bytes(recv.at[kind, u, j], recv_sem.at[kind, u, j])
                total = flow[kind, u, side, :, sl].astype(F32) + (part[kind, slot, j, side] + recv[kind, u, j])
                send[kind, u, :, sl] = total.astype(BF16)

                @pl.when(inside)
                def _():
                    for half in (side, other):
                        pltpu.make_async_remote_copy(send.at[kind, u, :, sl], flow.at[kind, u, side, :, sl], flow_send.at[kind],
                                                     flow_sem.at[kind, u, side], device_id=peer(target, half), device_id_type=MESH).start()

            @pl.when(jnp.logical_and(jnp.logical_not(inside), home_of(u) != out))
            def _():
                pltpu.make_async_remote_copy(send.at[kind, u], home.at[kind, slot_of(u)], home_send.at[kind, u],
                                             home_sem.at[kind, slot_of(u)], device_id=peer(home_of(u), side), device_id_type=MESH).start()
            return carry
        lax.fori_loop(0, count, body, 0)

    def swap_weights():
        n_i = d_model // TILE

        def body(t, carry):
            i = pl.multiple_of(lax.rem(t, n_i) * TILE, TILE)
            j = pl.multiple_of(lax.div(t, n_i) * TILE, TILE)
            up = wa[pl.ds(i, TILE), pl.ds(j, TILE)]
            down = wb[pl.ds(j, TILE), pl.ds(i, TILE)]
            wa[pl.ds(i, TILE), pl.ds(j, TILE)] = down.T
            wb[pl.ds(j, TILE), pl.ds(i, TILE)] = up.T
            return carry
        lax.fori_loop(0, n_i * (d_ff // TILE), body, 0)

    def prepare_last():
        half = UNITS // 2

        def quarter(q, carry):
            for i in range(half):
                arrived(BWD, q * half + i)
                keep(flow.at[BWD, q * half + i], g_out, q * half + i, 1)
            units = pl.ds(q * half, half)

            def fn(slices):
                lhs = flow[BWD, units].reshape(half * tok, d_model)
                for sl in slices:
                    e = lax.dot_general(lhs, wb[sl, :], NT, preferred_element_type=F32)
                    slope[units, :, sl] = e.reshape(half, tok, BLK)
            blocks(d_ff, 1, fn)
            return carry
        lax.fori_loop(0, 2, quarter, 0)
        load_a.wait()
        n_i = d_model // TILE

        def body(t, carry):
            i = pl.multiple_of(lax.rem(t, n_i) * TILE, TILE)
            j = pl.multiple_of(lax.div(t, n_i) * TILE, TILE)
            wb[pl.ds(j, TILE), pl.ds(i, TILE)] = wa[pl.ds(i, TILE), pl.ds(j, TILE)].T
            return carry
        lax.fori_loop(0, n_i * (d_ff // TILE), body, 0)

    def step(t, carry):
        group, place = lax.div(t, 3), lax.rem(t, 3)
        word = words[0]
        for i, w in enumerate(words[1:], 1):
            word = jnp.where(group == i, w, word)
        code = lax.rem(lax.div(word, jnp.where(place == 0, 1, jnp.where(place == 1, PACK, PACK * PACK))), PACK)
        op = lax.rem(code, 32)
        u = lax.rem(lax.div(code, 32), UNITS)
        count = lax.div(code, 256) + 1

        def on(want):
            return pl.when(op == want)

        v = jnp.minimum(u + count - 1, UNITS - 1)

        @on(F1)
        def _():
            up_product(u, v, False)

        @on(M1)
        def _():
            up_product(u, v, True)

        @pl.when(jnp.logical_or(op == F2, op == B2))
        def _():
            down_product(jnp.where(op == F2, FWD, BWD), u, v, True)

        @on(FR)
        def _():
            hand_on(FWD, u, count)

        @on(BR)
        def _():
            hand_on(BWD, u, count)

        @on(B1)
        def _():
            back_product(u, v, True)

        @on(T1)
        def _():
            back_product(u, v, False)

        @on(T2)
        def _():
            down_product(BWD, u, v, False)

        @on(SW)
        def _():
            swap_weights()

        @on(PR)
        def _():
            prepare_last()

        @on(YL)
        def _():
            load_b.start()
            load_b.wait()

        @on(WA)
        def _():
            load_a.wait()

        @on(WB)
        def _():
            load_b.wait()

        @on(XS)
        def _():
            stagings[BWD].wait()
            for k in range(2):
                for lane in range(2):
                    hand_in(BWD, STAGES - 1, k, lane)

            @pl.when(stage == 0)
            def _():
                hand_in(FWD, 0, 0, 1)

            @pl.when(stage > 1)
            def _():
                for k in range(2):
                    wait_bytes(home.at[FWD, k], relay_sem.at[k])
                    relayed(k).start()

        @on(XW)
        def _():
            for kind, target in ((FWD, 0), (BWD, STAGES - 1)):
                for k in range(2):
                    @pl.when(stage != target)
                    def _():
                        wait_bytes(staged[kind].at[k], in_send.at[kind, k, 0])
                    wait_bytes(staged[kind].at[k], in_send.at[kind, k, 1])

            @pl.when(stage > 1)
            def _():
                for k in range(2):
                    relayed(k).wait_send()

        @on(HB)
        def _():
            take_direct(u, count)
        return carry
    lax.fori_loop(0, steps, step, 0)

    for kind, here, out in ((FWD, STAGES - 1, y_out), (BWD, 0, dx_out)):
        for k in range(2):
            @pl.when(stage == here)
            def _():
                pltpu.make_async_copy(send.at[kind, unit_of(k)], out.at[k], out_sem.at[4 + kind]).start()

            @pl.when(stage != here)
            def _():
                wait_bytes(home.at[kind, k], home_sem.at[kind, k])
                pltpu.make_async_copy(home.at[kind, k], out.at[k], out_sem.at[4 + kind]).start()

    for kind in (FWD, BWD):
        for u in range(UNITS - SLOTS, UNITS):
            for j in range(n_blk):
                part_copy(kind, u, j).wait_send()
    for kind, last in ((FWD, STAGES - 1), (BWD, 0)):
        @pl.when((stage != last) & jnp.logical_not((stage == 2) & (kind == BWD)))
        def _():
            wait_bytes(flow.at[kind], flow_send.at[kind])

        @pl.when(stage == last)
        def _():
            for u in range(UNITS):
                if (u + 1) // 2 % STAGES != last:
                    wait_bytes(send.at[kind, u], home_send.at[kind, u])
    @pl.when(stage == 2)
    def _():
        wait_bytes(flow.at[BWD, pl.ds(0, UNITS - DIRECT)], flow_send.at[BWD])

    @pl.when(stage == 1)
    def _():
        wait_bytes(flow.at[BWD, pl.ds(0, DIRECT), 0], cross_send.at[0])
    for lane, (ref, out) in enumerate(((flow.at[FWD], h_out), (flow.at[BWD], g_out), (act.at[FWD], a_out), (act.at[BWD], d_out),
                                       (home.at[FWD], y_out), (home.at[BWD], dx_out))):
        pltpu.make_async_copy(ref, out, out_sem.at[lane]).wait()


def run_pipeline(x_loc, g_loc, w_one, w_two):
    rows, d_model = x_loc.shape[1:]
    d_ff = w_one.shape[1]
    n_blk = d_model // BLK
    tok = INNER * rows
    hbm = pl.BlockSpec(memory_space=pl.ANY)
    out = lambda *shape: jax.ShapeDtypeStruct(shape, BF16)
    dma = lambda *shape: pltpu.SemaphoreType.DMA(shape)
    return pl.pallas_call(
        pipeline_kernel,
        name='pipeline',
        out_shape=(out(*x_loc.shape), out(*x_loc.shape), out(UNITS, INNER, rows, d_model), out(UNITS, INNER, rows, d_model),
                   out(UNITS, tok, d_ff), out(UNITS, tok, d_ff)),
        in_specs=[hbm] * 4,
        out_specs=(hbm,) * 6,
        scratch_shapes=[
            pltpu.VMEM((d_model, d_ff), BF16),
            pltpu.VMEM((d_ff, d_model), BF16),
            pltpu.VMEM((2, UNITS, INNER, rows, d_model), BF16),
            pltpu.VMEM((2, UNITS, tok, d_ff), BF16),
            pltpu.VMEM((UNITS, tok, d_ff), F32),
            pltpu.VMEM((2, SLOTS, n_blk, INNER, rows, BLK), F32),
            pltpu.VMEM((2, UNITS, n_blk, rows, BLK), F32),
            pltpu.VMEM((2, UNITS, rows, d_model), BF16),
            pltpu.VMEM((2, 2, rows, d_model), BF16),
            pltpu.VMEM((DIRECT, n_blk, rows, BLK), F32),
            dma(2, UNITS, INNER), dma(2, UNITS, n_blk), dma(2, SLOTS, n_blk), dma(2), dma(2, UNITS), dma(2, 2), dma(2, 2, 2), dma(2), dma(2),
            dma(2, DIRECT, n_blk), dma(SLOTS, n_blk), dma(1), dma(2), dma(2), dma(6),
        ],
        compiler_params=pltpu.CompilerParams(collective_id=0, has_side_effects=True, vmem_limit_bytes=67043328),
    )(x_loc, g_loc, w_one, w_two)


GRAD_ROWS, GRAD_COLS = 1024, 2048


def weight_grad_kernel(h_ref, d_ref, a_ref, g_ref, y_ref, x_ref, up_ref, down_ref, y_out, x_out,
                       h, d, a, g, home, stage, in_sem, home_sem, out_sem):
    tokens, d_model = h.shape
    d_ff = d.shape[1]
    n_down, n_up = d_ff // GRAD_ROWS, d_model // GRAD_ROWS
    n_col = d_ff // GRAD_COLS

    loads = [(g_ref, g)] + [(a_ref.at[:, pl.ds(t * GRAD_ROWS, GRAD_ROWS)], a.at[:, pl.ds(t * GRAD_ROWS, GRAD_ROWS)]) for t in range(n_down)] + [(h_ref, h), (d_ref, d)]
    loads = [pltpu.make_async_copy(src, dst, in_sem.at[t]) for t, (src, dst) in enumerate(loads)]
    homes = [pltpu.make_async_copy(src, home.at[t], home_sem.at[t]) for t, src in enumerate((y_ref, x_ref))]
    for copy in loads + homes:
        copy.start()
    loads[0].wait()

    def block(t, src, first, other, second, out, pieces=1):
        slot = lax.rem(t, 2)
        size = GRAD_ROWS // pieces
        for p in range(pieces):
            rows = pl.ds(pl.multiple_of(first + p * size, size), size)
            cols = pl.ds(pl.multiple_of(second, GRAD_COLS), GRAD_COLS)
            stage[slot, pl.ds(p * size, size)] = lax.dot_general(src[:, rows], other[:, cols], (((0,), (0,)), ((), ())), preferred_element_type=F32)
            pltpu.make_async_copy(stage.at[slot, pl.ds(p * size, size)], out.at[rows, cols], out_sem.at[slot]).start()

    def freed(slot):
        pltpu.make_async_copy(stage.at[slot], stage.at[slot], out_sem.at[slot]).wait()

    def down(t, carry):
        pltpu.make_async_copy(a_ref.at[:, pl.ds(0, GRAD_ROWS)], a.at[:, pl.ds(0, GRAD_ROWS)], in_sem.at[1 + t]).wait()

        @pl.when(t >= 2)
        def _():
            freed(lax.rem(t, 2))
        block(t, a, t * GRAD_ROWS, g, 0, down_ref)
        return carry
    lax.fori_loop(0, n_down, down, 0)
    loads[1 + n_down].wait()
    loads[2 + n_down].wait()
    for copy, (src, dst) in zip(homes, ((home.at[0], y_out), (home.at[1], x_out))):
        copy.wait()
    backs = [pltpu.make_async_copy(home.at[t], dst, home_sem.at[t]) for t, dst in enumerate((y_out, x_out))]
    for copy in backs:
        copy.start()

    def up(t, carry):
        freed(lax.rem(t, 2))
        block(t, h, lax.div(t, n_col) * GRAD_ROWS, d, lax.rem(t, n_col) * GRAD_COLS, up_ref)
        return carry
    n_blocks = n_up * n_col
    lax.fori_loop(0, n_blocks - 1, up, 0)
    freed((n_blocks - 1) % 2)
    block(n_blocks - 1, h, (n_up - 1) * GRAD_ROWS, d, (n_col - 1) * GRAD_COLS, up_ref, 4)
    for slot in range(2):
        freed(slot)
    for copy in backs:
        copy.wait()


def weight_grads(h, d, a, g, y, dx):
    tokens, d_model = h.shape
    d_ff = d.shape[1]
    n_in = 3 + d_ff // GRAD_ROWS
    hbm = pl.BlockSpec(memory_space=pl.ANY)
    dma = lambda *shape: pltpu.SemaphoreType.DMA(shape)
    like = lambda v: pltpu.VMEM(v.shape, v.dtype)
    return pl.pallas_call(
        weight_grad_kernel,
        name='weight_grads',
        out_shape=(jax.ShapeDtypeStruct((d_model, d_ff), F32), jax.ShapeDtypeStruct((d_ff, d_model), F32),
                   jax.ShapeDtypeStruct(y.shape, BF16), jax.ShapeDtypeStruct(y.shape, BF16)),
        in_specs=[hbm] * 6,
        out_specs=(hbm,) * 4,
        scratch_shapes=[like(h), like(d), like(a), like(g), pltpu.VMEM((2,) + y.shape, BF16), pltpu.VMEM((2, GRAD_ROWS, GRAD_COLS), F32),
                        dma(n_in), dma(2), dma(2)],
        compiler_params=pltpu.CompilerParams(vmem_limit_bytes=60 * 1024 * 1024),
    )(h, d, a, g, y, dx)


def solution(mesh):
    tok_spec = P(('data', 'stage', 'inner'))
    up_spec = P(None, ('data', 'stage'), None, 'inner')
    down_spec = P(None, ('data', 'stage'), 'inner', None)

    def device_step(x_loc, g_loc, w_up, w_down):
        y, dx, h, g, a, d = run_pipeline(x_loc, g_loc, w_up[0, 0], w_down[0, 0])
        flat = lambda v: v.reshape(-1, v.shape[-1])
        dw_up, dw_down, y, dx = weight_grads(flat(h), flat(d), flat(a), flat(g), y, dx)
        return y, dx, dw_up[None, None], dw_down[None, None]

    return jax.shard_map(device_step, mesh=mesh, in_specs=(tok_spec, tok_spec, up_spec, down_spec), out_specs=(tok_spec, tok_spec, up_spec, down_spec), check_vma=False)
```

```python
import functools

import jax
import jax.numpy as jnp
from jax import lax
from jax.experimental import pallas as pl
from jax.experimental.pallas import tpu as pltpu
from jax.sharding import PartitionSpec as P

F32 = jnp.float32
BF16 = jnp.bfloat16
MESH = pl.DeviceIdType.MESH

STAGES = 4
INNER = 2
UNITS = 8
SLOTS = 3
DIRECT = 3
BLK = 512
TILE = 256
FWD, BWD = 0, 1
NT = (((1,), (1,)), ((), ()))

F1, F2, FR, B1, B2, BR, T1, T2, SW, PR, YL, WA, WB, XS, M1, HB, XW = range(1, 18)
PLAN = (
    ((WA, 0, 1), (F1, 0, 2), (WB, 0, 1), (XS, 0, 1), (F2, 0, 1), (F2, 1, 1), (FR, 0, 1), (F1, 2, 2),
     (FR, 1, 1), (F2, 2, 1), (F1, 4, 2), (F2, 3, 1), (F1, 6, 2), (FR, 2, 2), (F2, 4, 2), (FR, 4, 2),
     (F2, 6, 2), (XW, 0, 1), (SW, 0, 1), (FR, 6, 2), (B1, 0, 2), (B2, 0, 2), (B1, 2, 1), (B2, 2, 1),
     (BR, 0, 3), (B1, 3, 1), (B1, 4, 2), (B2, 3, 1), (B2, 4, 1), (B2, 5, 1), (B1, 6, 2), (BR, 3, 1),
     (B2, 6, 1), (BR, 4, 1), (B2, 7, 1), (BR, 5, 3)),
    ((WA, 0, 1), (WB, 0, 1), (XS, 0, 1), (F1, 0, 1), (F2, 0, 1), (F1, 1, 1), (FR, 0, 1), (F2, 1, 1),
     (FR, 1, 1), (F1, 2, 2), (F2, 2, 1), (F2, 3, 1), (FR, 2, 1), (F1, 4, 2), (FR, 3, 1), (F2, 4, 1),
     (F2, 5, 1), (FR, 4, 2), (F1, 6, 2), (F2, 6, 1), (F2, 7, 1), (FR, 6, 2), (XW, 0, 1), (SW, 0, 1),
     (HB, 0, 2), (B1, 0, 1), (B2, 0, 1), (B1, 1, 1), (B2, 1, 1), (HB, 2, 1), (BR, 0, 2), (B1, 2, 2),
     (B2, 2, 1), (BR, 2, 1), (B2, 3, 1), (B1, 4, 1), (B2, 4, 1), (B1, 5, 1), (B2, 5, 1), (BR, 3, 2),
     (B1, 6, 2), (BR, 5, 1), (B2, 6, 1), (B2, 7, 1), (BR, 6, 2)),
    ((WA, 0, 1), (WB, 0, 1), (XS, 0, 1), (XW, 0, 1), (F1, 0, 1), (F2, 0, 1), (F1, 1, 1), (FR, 0, 1),
     (F2, 1, 1), (FR, 1, 1), (F1, 2, 1), (F2, 2, 1), (F1, 3, 1), (F2, 3, 1), (FR, 2, 1), (F1, 4, 2),
     (FR, 3, 1), (F2, 4, 2), (T1, 0, 2), (T2, 0, 2), (FR, 4, 1), (F1, 6, 2), (FR, 5, 1), (F2, 6, 2),
     (T1, 2, 2), (FR, 6, 2), (T2, 2, 2), (BR, 3, 1), (T1, 4, 2), (T2, 4, 2), (T1, 6, 2), (BR, 4, 1),
     (T2, 6, 2), (BR, 5, 3)),
    ((WB, 0, 1), (XS, 0, 1), (PR, 0, 1), (XW, 0, 1), (M1, 0, 1), (B2, 0, 1), (BR, 0, 1), (M1, 1, 1),
     (B2, 1, 1), (BR, 1, 1), (M1, 2, 1), (B2, 2, 1), (M1, 3, 1), (B2, 3, 1), (BR, 2, 2), (M1, 4, 1),
     (B2, 4, 1), (M1, 5, 1), (B2, 5, 1), (BR, 4, 2), (M1, 6, 2), (B2, 6, 1), (B2, 7, 1), (BR, 6, 2),
     (YL, 0, 1), (F2, 0, 1), (F2, 1, 1), (FR, 0, 2), (F2, 2, 1), (F2, 3, 1), (FR, 2, 2), (F2, 4, 2),
     (FR, 4, 1), (F2, 6, 2), (FR, 5, 3)),
)


PACK = 1024
UP_GROUP = 8
TURN = 6
TURN_GROUP = 4
DOWN_GROUP = 2


def plan_words():
    rows = [[op + 32 * unit + 256 * (count - 1) for op, unit, count in row] for row in PLAN]
    steps = -(-max(len(row) for row in rows) // 3) * 3
    rows = [row + [0] * (steps - len(row)) for row in rows]
    return steps, [[row[t] + PACK * row[t + 1] + PACK * PACK * row[t + 2] for t in range(0, steps, 3)] for row in rows]


def gelu_pair(pre_act):
    root = pre_act * 0.7071067811865476
    normal_cdf = 0.5 * (1.0 + lax.erf(root))
    normal_pdf = jnp.exp2(root * root * -1.4426950408889634) * 0.3989422804014327
    return pre_act * normal_cdf, normal_cdf + pre_act * normal_pdf


def wait_bytes(ref, sem):
    pltpu.make_async_copy(ref, ref, sem).wait()


def pipeline_kernel(x_ref, g_ref, w1_ref, w2_ref,
                    y_out, dx_out, h_out, g_out, a_out, d_out,
                    wa, wb, flow, act, slope, part, recv, send, home, direct,
                    flow_sem, recv_sem, part_send, flow_send, home_send, home_sem, in_send, relay_sem, relay_send,
                    direct_sem, direct_send, cross_send, stage_sem, w_sem, out_sem):
    stage = lax.axis_index('stage')
    side = lax.axis_index('inner')
    other = 1 - side
    rows, d_model = flow.shape[3:]
    tok, d_ff = act.shape[2:]
    n_blk = d_model // BLK

    def peer(s, i):
        return {'stage': s, 'inner': i}

    load_a = pltpu.make_async_copy(w1_ref, wa, w_sem.at[0])
    load_b = pltpu.make_async_copy(w2_ref, wb, w_sem.at[1])

    def unit_of(k):
        return lax.rem(2 * stage + k + UNITS - 1, UNITS)

    staged = (send.at[BWD, pl.ds(UNITS - 2, 2)], send.at[BWD, pl.ds(UNITS - 4, 2)])
    stagings = [pltpu.make_async_copy(src, dst, stage_sem.at[kind]) for kind, (src, dst) in enumerate(zip((x_ref, g_ref), staged))]
    for kind, target in ((FWD, 0), (BWD, STAGES - 1)):
        stagings[kind].start()

        @pl.when(stage == target)
        def _():
            for k in range(2):
                pltpu.make_async_copy((x_ref, g_ref)[kind].at[k], flow.at[kind, unit_of(k), side], flow_sem.at[kind, unit_of(k), side]).start()

    @pl.when(stage < STAGES - 1)
    def _():
        load_a.start()
    load_b.start()

    @pl.when(stage == STAGES - 1)
    def _():
        load_a.start()

    barrier = pltpu.get_barrier_semaphore()
    for s in range(STAGES):
        for i in range(INNER):
            @pl.when(jnp.logical_or(stage != s, side != i))
            def _():
                pl.semaphore_signal(barrier, inc=1, device_id=peer(s, i), device_id_type=MESH)
    pl.semaphore_wait(barrier, STAGES * INNER - 1)

    def home_of(u):
        return lax.rem((u + 1) // 2, STAGES)

    def slot_of(u):
        return lax.rem(u + 1, 2)

    def hand_in(kind, target, k, lane):
        u = unit_of(k)
        src = staged[kind]
        if lane == 0:
            @pl.when(stage != target)
            def _():
                pltpu.make_async_remote_copy(src.at[k], flow.at[kind, u, side], in_send.at[kind, k, 0], flow_sem.at[kind, u, side],
                                             device_id=peer(target, side), device_id_type=MESH).start()
        else:
            pltpu.make_async_remote_copy(src.at[k], flow.at[kind, u, side], in_send.at[kind, k, 1], flow_sem.at[kind, u, side],
                                         device_id=peer(target, other), device_id_type=MESH).start()

    def relay(k):
        return pltpu.make_async_remote_copy(staged[FWD].at[k], home.at[FWD, k], in_send.at[FWD, k, 1], relay_sem.at[k],
                                            device_id=peer(stage, other), device_id_type=MESH)

    def relayed(k):
        u = unit_of(k)
        return pltpu.make_async_remote_copy(home.at[FWD, k], flow.at[FWD, u, other], relay_send.at[k], flow_sem.at[FWD, u, other],
                                            device_id=peer(0, side), device_id_type=MESH)

    stagings[FWD].wait()
    for k in range(2):
        hand_in(FWD, 0, k, 0)

        @pl.when(jnp.logical_or(stage == 1, jnp.logical_and(stage == 0, k == 1)))
        def _():
            hand_in(FWD, 0, k, 1)

        @pl.when(stage > 1)
        def _():
            relay(k).start()
    steps, plan = plan_words()
    words = [jnp.where(stage == 0, a, jnp.where(stage == 1, b, jnp.where(stage == 2, c, d))) for a, b, c, d in zip(*plan)]

    def keep(ref, out, u, lane):
        pltpu.make_async_copy(ref, out.at[u], out_sem.at[lane]).start()

    def blocks(width, group, fn):
        def body(t, carry):
            fn([pl.ds(pl.multiple_of((t * group + k) * BLK, BLK), BLK) for k in range(group)])
            return carry
        lax.fori_loop(0, width // BLK // group, body, 0)

    def arrived(kind, u):
        for half in range(INNER):
            @pl.when(jnp.logical_not((stage == 1) & (kind == BWD) & (u < DIRECT) & (side == half)))
            def _():
                wait_bytes(flow.at[kind, u, half], flow_sem.at[kind, u, half])

    def both_arrived(kind, u, v):
        arrived(kind, u)

        @pl.when(v != u)
        def _():
            arrived(kind, v)

    def pair(ref, kind, u, v):
        width = ref.shape[-1]
        return jnp.concatenate([ref[kind, u].reshape(tok, width), ref[kind, v].reshape(tok, width)], axis=0)

    def kept(u, v, fn):
        fn(u)

        @pl.when(v != u)
        def _():
            fn(v)

    def up_product(u, v, last):
        both_arrived(FWD, u, v)

        def fn(slices):
            lhs = pair(flow, FWD, u, v)
            for sl in slices:
                z = jnp.dot(lhs, wa[:, sl], preferred_element_type=F32)
                value, grad = gelu_pair(z)
                value = value.astype(BF16)
                if last:
                    act[BWD, u, :, sl] = (slope[u, :, sl] * grad[:tok]).astype(BF16)
                    act[BWD, v, :, sl] = (slope[v, :, sl] * grad[tok:]).astype(BF16)
                else:
                    slope[u, :, sl] = grad[:tok]
                    slope[v, :, sl] = grad[tok:]
                act[FWD, u, :, sl] = value[:tok]
                act[FWD, v, :, sl] = value[tok:]
        blocks(d_ff, UP_GROUP, fn)

        def out(w):
            keep(flow.at[FWD, w], h_out, w, 0)
            keep(act.at[FWD, w], a_out, w, 2)
            if last:
                keep(act.at[BWD, w], d_out, w, 3)
        kept(u, v, out)

    def across(lhs, ref, sl):
        cut = ref.shape[1] * TURN // 8
        total = lax.dot_general(lhs[:, :cut], ref[sl, :cut], NT, preferred_element_type=F32)
        for k in range(cut, ref.shape[1], TILE):
            turned = [ref[pl.ds(sl.start + q, TILE), k:k + TILE].T for q in range(0, BLK, TILE)]
            total += jnp.dot(lhs[:, k:k + TILE], jnp.concatenate(turned, axis=1), preferred_element_type=F32)
        return total

    def back_product(u, v, swapped):
        both_arrived(BWD, u, v)

        def fn(slices):
            lhs = pair(flow, BWD, u, v)
            for sl in slices:
                if swapped:
                    e = jnp.dot(lhs, wa[:, sl], preferred_element_type=F32)
                else:
                    e = across(lhs, wb, sl)
                act[BWD, u, :, sl] = (e[:tok] * slope[u, :, sl]).astype(BF16)
                act[BWD, v, :, sl] = (e[tok:] * slope[v, :, sl]).astype(BF16)
        blocks(d_ff, UP_GROUP if swapped else TURN_GROUP, fn)

        def out(w):
            keep(flow.at[BWD, w], g_out, w, 1)
            keep(act.at[BWD, w], d_out, w, 3)
        kept(u, v, out)

    def part_copy(kind, u, j):
        slot = lax.rem(u, SLOTS)
        return pltpu.make_async_remote_copy(part.at[kind, slot, j, other], recv.at[kind, u, j], part_send.at[kind, slot, j],
                                            recv_sem.at[kind, u, j], device_id=peer(stage, other), device_id_type=MESH)

    def direct_copy(u, j, half):
        slot = lax.rem(u, SLOTS)
        if half is side:
            return pltpu.make_async_remote_copy(part.at[BWD, slot, j, side], direct.at[u, j], direct_send.at[slot, j],
                                                direct_sem.at[0, u, j], device_id=peer(stage - 1, side), device_id_type=MESH)
        return pltpu.make_async_remote_copy(part.at[BWD, slot, j, other], recv.at[FWD, u, j], part_send.at[BWD, slot, j],
                                            direct_sem.at[1, u, j], device_id=peer(stage - 1, other), device_id_type=MESH)

    def take_direct(first, count):
        def body(i, carry):
            u = first + i
            for j in range(n_blk):
                sl = pl.ds(j * BLK, BLK)
                wait_bytes(direct.at[u, j], direct_sem.at[0, u, j])
                wait_bytes(recv.at[FWD, u, j], direct_sem.at[1, u, j])
                flow[BWD, u, side, :, sl] = (direct[u, j] + recv[FWD, u, j]).astype(BF16)
                pltpu.make_async_remote_copy(flow.at[BWD, u, side, :, sl], flow.at[BWD, u, side, :, sl], cross_send.at[0],
                                             flow_sem.at[BWD, u, side], device_id=peer(stage, other), device_id_type=MESH).start()
            return carry
        lax.fori_loop(0, count, body, 0)

    def down_product(kind, u, v, straight):
        def free(w):
            @pl.when(w >= SLOTS)
            def _():
                for j in range(n_blk):
                    part_copy(kind, w - SLOTS, j).wait_send()

            if not straight:
                @pl.when((w >= SLOTS) & (w < SLOTS + DIRECT))
                def _():
                    for j in range(n_blk):
                        direct_copy(w - SLOTS, j, side).wait_send()
        kept(u, v, free)

        def body(t, carry):
            lhs = pair(act, kind, u, v)
            for k in range(DOWN_GROUP):
                j = t * DOWN_GROUP + k
                sl = pl.ds(pl.multiple_of(j * BLK, BLK), BLK)
                if straight:
                    p = jnp.dot(lhs, wb[:, sl], preferred_element_type=F32)
                else:
                    p = across(lhs, wa, sl)
                p = p.reshape(2, INNER, rows, BLK)
                part[kind, lax.rem(u, SLOTS), j] = p[0]
                part[kind, lax.rem(v, SLOTS), j] = p[1]

            def go(w):
                if straight:
                    for k in range(DOWN_GROUP):
                        part_copy(kind, w, t * DOWN_GROUP + k).start()
                    return

                @pl.when(w >= DIRECT)
                def _():
                    for k in range(DOWN_GROUP):
                        part_copy(kind, w, t * DOWN_GROUP + k).start()

                @pl.when(w < DIRECT)
                def _():
                    for k in range(DOWN_GROUP):
                        j = t * DOWN_GROUP + k
                        sl = pl.ds(pl.multiple_of(j * BLK, BLK), BLK)
                        part[BWD, lax.rem(w, SLOTS), j, side] += flow[BWD, w, side, :, sl].astype(F32)
                    for k in range(DOWN_GROUP):
                        for half in (side, other):
                            direct_copy(w, t * DOWN_GROUP + k, half).start()
            kept(u, v, go)
            return carry
        lax.fori_loop(0, n_blk // DOWN_GROUP, body, 0)

    def hand_on(kind, first, count):
        target = stage + 1 if kind == FWD else stage - 1
        inside = stage < STAGES - 1 if kind == FWD else stage > 0
        out = STAGES - 1 if kind == FWD else 0

        def body(i, carry):
            u = first + i
            slot = lax.rem(u, SLOTS)
            for j in range(n_blk):
                sl = pl.ds(j * BLK, BLK)
                wait_bytes(recv.at[kind, u, j], recv_sem.at[kind, u, j])
                total = flow[kind, u, side, :, sl].astype(F32) + (part[kind, slot, j, side] + recv[kind, u, j])
                send[kind, u, :, sl] = total.astype(BF16)

                @pl.when(inside)
                def _():
                    for half in (side, other):
                        pltpu.make_async_remote_copy(send.at[kind, u, :, sl], flow.at[kind, u, side, :, sl], flow_send.at[kind],
                                                     flow_sem.at[kind, u, side], device_id=peer(target, half), device_id_type=MESH).start()

            @pl.when(jnp.logical_and(jnp.logical_not(inside), home_of(u) != out))
            def _():
                pltpu.make_async_remote_copy(send.at[kind, u], home.at[kind, slot_of(u)], home_send.at[kind, u],
                                             home_sem.at[kind, slot_of(u)], device_id=peer(home_of(u), side), device_id_type=MESH).start()
            return carry
        lax.fori_loop(0, count, body, 0)

    def swap_weights():
        n_i = d_model // TILE

        def body(t, carry):
            i = pl.multiple_of(lax.rem(t, n_i) * TILE, TILE)
            j = pl.multiple_of(lax.div(t, n_i) * TILE, TILE)
            up = wa[pl.ds(i, TILE), pl.ds(j, TILE)]
            down = wb[pl.ds(j, TILE), pl.ds(i, TILE)]
            wa[pl.ds(i, TILE), pl.ds(j, TILE)] = down.T
            wb[pl.ds(j, TILE), pl.ds(i, TILE)] = up.T
            return carry
        lax.fori_loop(0, n_i * (d_ff // TILE), body, 0)

    def prepare_last():
        half = UNITS // 2

        def quarter(q, carry):
            for i in range(half):
                arrived(BWD, q * half + i)
                keep(flow.at[BWD, q * half + i], g_out, q * half + i, 1)
            units = pl.ds(q * half, half)

            def fn(slices):
                lhs = flow[BWD, units].reshape(half * tok, d_model)
                for sl in slices:
                    e = lax.dot_general(lhs, wb[sl, :], NT, preferred_element_type=F32)
                    slope[units, :, sl] = e.reshape(half, tok, BLK)
            blocks(d_ff, 1, fn)
            return carry
        lax.fori_loop(0, 2, quarter, 0)
        load_a.wait()
        n_i = d_model // TILE

        def body(t, carry):
            i = pl.multiple_of(lax.rem(t, n_i) * TILE, TILE)
            j = pl.multiple_of(lax.div(t, n_i) * TILE, TILE)
            wb[pl.ds(j, TILE), pl.ds(i, TILE)] = wa[pl.ds(i, TILE), pl.ds(j, TILE)].T
            return carry
        lax.fori_loop(0, n_i * (d_ff // TILE), body, 0)

    def step(t, carry):
        group, place = lax.div(t, 3), lax.rem(t, 3)
        word = words[0]
        for i, w in enumerate(words[1:], 1):
            word = jnp.where(group == i, w, word)
        code = lax.rem(lax.div(word, jnp.where(place == 0, 1, jnp.where(place == 1, PACK, PACK * PACK))), PACK)
        op = lax.rem(code, 32)
        u = lax.rem(lax.div(code, 32), UNITS)
        count = lax.div(code, 256) + 1

        def on(want):
            return pl.when(op == want)

        v = jnp.minimum(u + count - 1, UNITS - 1)

        @on(F1)
        def _():
            up_product(u, v, False)

        @on(M1)
        def _():
            up_product(u, v, True)

        @pl.when(jnp.logical_or(op == F2, op == B2))
        def _():
            down_product(jnp.where(op == F2, FWD, BWD), u, v, True)

        @on(FR)
        def _():
            hand_on(FWD, u, count)

        @on(BR)
        def _():
            hand_on(BWD, u, count)

        @on(B1)
        def _():
            back_product(u, v, True)

        @on(T1)
        def _():
            back_product(u, v, False)

        @on(T2)
        def _():
            down_product(BWD, u, v, False)

        @on(SW)
        def _():
            swap_weights()

        @on(PR)
        def _():
            prepare_last()

        @on(YL)
        def _():
            load_b.start()
            load_b.wait()

        @on(WA)
        def _():
            load_a.wait()

        @on(WB)
        def _():
            load_b.wait()

        @on(XS)
        def _():
            stagings[BWD].wait()
            for k in range(2):
                for lane in range(2):
                    hand_in(BWD, STAGES - 1, k, lane)

            @pl.when(stage == 0)
            def _():
                hand_in(FWD, 0, 0, 1)

            @pl.when(stage > 1)
            def _():
                for k in range(2):
                    wait_bytes(home.at[FWD, k], relay_sem.at[k])
                    relayed(k).start()

        @on(XW)
        def _():
            for kind, target in ((FWD, 0), (BWD, STAGES - 1)):
                for k in range(2):
                    @pl.when(stage != target)
                    def _():
                        wait_bytes(staged[kind].at[k], in_send.at[kind, k, 0])
                    wait_bytes(staged[kind].at[k], in_send.at[kind, k, 1])

            @pl.when(stage > 1)
            def _():
                for k in range(2):
                    relayed(k).wait_send()

        @on(HB)
        def _():
            take_direct(u, count)
        return carry
    lax.fori_loop(0, steps, step, 0)

    for kind, here, out in ((FWD, STAGES - 1, y_out), (BWD, 0, dx_out)):
        for k in range(2):
            @pl.when(stage == here)
            def _():
                pltpu.make_async_copy(send.at[kind, unit_of(k)], out.at[k], out_sem.at[4 + kind]).start()

            @pl.when(stage != here)
            def _():
                wait_bytes(home.at[kind, k], home_sem.at[kind, k])
                pltpu.make_async_copy(home.at[kind, k], out.at[k], out_sem.at[4 + kind]).start()

    for kind in (FWD, BWD):
        for u in range(UNITS - SLOTS, UNITS):
            for j in range(n_blk):
                part_copy(kind, u, j).wait_send()
    for kind, last in ((FWD, STAGES - 1), (BWD, 0)):
        @pl.when((stage != last) & jnp.logical_not((stage == 2) & (kind == BWD)))
        def _():
            wait_bytes(flow.at[kind], flow_send.at[kind])

        @pl.when(stage == last)
        def _():
            for u in range(UNITS):
                if (u + 1) // 2 % STAGES != last:
                    wait_bytes(send.at[kind, u], home_send.at[kind, u])
    @pl.when(stage == 2)
    def _():
        wait_bytes(flow.at[BWD, pl.ds(0, UNITS - DIRECT)], flow_send.at[BWD])

    @pl.when(stage == 1)
    def _():
        wait_bytes(flow.at[BWD, pl.ds(0, DIRECT), 0], cross_send.at[0])
    for lane, (ref, out) in enumerate(((flow.at[FWD], h_out), (flow.at[BWD], g_out), (act.at[FWD], a_out), (act.at[BWD], d_out),
                                       (home.at[FWD], y_out), (home.at[BWD], dx_out))):
        pltpu.make_async_copy(ref, out, out_sem.at[lane]).wait()


def run_pipeline(x_loc, g_loc, w_one, w_two):
    rows, d_model = x_loc.shape[1:]
    d_ff = w_one.shape[1]
    n_blk = d_model // BLK
    tok = INNER * rows
    hbm = pl.BlockSpec(memory_space=pl.ANY)
    out = lambda *shape: jax.ShapeDtypeStruct(shape, BF16)
    dma = lambda *shape: pltpu.SemaphoreType.DMA(shape)
    return pl.pallas_call(
        pipeline_kernel,
        name='pipeline',
        out_shape=(out(*x_loc.shape), out(*x_loc.shape), out(UNITS, INNER, rows, d_model), out(UNITS, INNER, rows, d_model),
                   out(UNITS, tok, d_ff), out(UNITS, tok, d_ff)),
        in_specs=[hbm] * 4,
        out_specs=(hbm,) * 6,
        scratch_shapes=[
            pltpu.VMEM((d_model, d_ff), BF16),
            pltpu.VMEM((d_ff, d_model), BF16),
            pltpu.VMEM((2, UNITS, INNER, rows, d_model), BF16),
            pltpu.VMEM((2, UNITS, tok, d_ff), BF16),
            pltpu.VMEM((UNITS, tok, d_ff), F32),
            pltpu.VMEM((2, SLOTS, n_blk, INNER, rows, BLK), F32),
            pltpu.VMEM((2, UNITS, n_blk, rows, BLK), F32),
            pltpu.VMEM((2, UNITS, rows, d_model), BF16),
            pltpu.VMEM((2, 2, rows, d_model), BF16),
            pltpu.VMEM((DIRECT, n_blk, rows, BLK), F32),
            dma(2, UNITS, INNER), dma(2, UNITS, n_blk), dma(2, SLOTS, n_blk), dma(2), dma(2, UNITS), dma(2, 2), dma(2, 2, 2), dma(2), dma(2),
            dma(2, DIRECT, n_blk), dma(SLOTS, n_blk), dma(1), dma(2), dma(2), dma(6),
        ],
        compiler_params=pltpu.CompilerParams(collective_id=0, has_side_effects=True, vmem_limit_bytes=67043328),
    )(x_loc, g_loc, w_one, w_two)


GRAD_ROWS, GRAD_COLS = 1024, 2048


def weight_grad_kernel(h_ref, d_ref, a_ref, g_ref, y_ref, x_ref, up_ref, down_ref, y_out, x_out,
                       h, d, a, g, home, left, right, stage, in_sem, home_sem, out_sem):
    d_model, d_ff = h.shape[1], d.shape[1]
    n_down, n_up, n_col = d_ff // GRAD_ROWS, d_model // GRAD_ROWS, d_ff // GRAD_COLS

    pieces = [a.at[:, pl.ds(t * GRAD_ROWS, GRAD_ROWS)] for t in range(n_down)]
    loads = [(g_ref, g)] + [(a_ref.at[:, pl.ds(t * GRAD_ROWS, GRAD_ROWS)], piece) for t, piece in enumerate(pieces)] + [(h_ref, h), (d_ref, d)]
    loads = [pltpu.make_async_copy(src, dst, in_sem.at[t]) for t, (src, dst) in enumerate(loads)]
    homes = [pltpu.make_async_copy(src, home.at[t], home_sem.at[t]) for t, src in enumerate((y_ref, x_ref))]
    backs = [pltpu.make_async_copy(home.at[t], dst, home_sem.at[t]) for t, dst in enumerate((y_out, x_out))]
    for copy in loads + homes:
        copy.start()

    rows_of = lambda t: pl.ds(t * GRAD_ROWS, GRAD_ROWS)
    blocks = [(a, t, g, 0, down_ref) for t in range(n_down)] + [(h, t, d, c, up_ref) for t in range(n_up) for c in range(n_col)]
    turned = (left, right)
    loads[0].wait()
    loads[1].wait()
    arrived = 2
    turn = -1
    for t, (src, row, other, col, out) in enumerate(blocks):
        slot = t % 2
        cols = pl.ds(col * GRAD_COLS, GRAD_COLS)
        after = blocks[t + 1] if t + 1 < len(blocks) else None
        need = (1 + n_down if after is None or after[0] is h else t + 2) + (1 if src is h or (after is not None and after[0] is h) else 0)
        need = min(need, len(loads) - 1) + (1 if src is h else 0)
        while arrived < min(need + 1, len(loads)):
            loads[arrived].wait()
            arrived += 1
        if t >= 2:
            pltpu.make_async_copy(stage.at[slot], stage.at[slot], out_sem.at[slot]).wait()
        last = after is None
        size = GRAD_ROWS // 4 if last else GRAD_ROWS
        for p in range(0, GRAD_ROWS, size):
            if t == 0:
                value = lax.dot_general(src[:, rows_of(0)], other[:, cols], (((0,), (0,)), ((), ())), preferred_element_type=F32)
            else:
                value = jnp.dot(turned[turn % 2][p:p + size], other[:, cols], preferred_element_type=F32)
            stage[slot, p:p + size] = value
            if not last and (after[0] is not src or after[1] != row):
                turn += 1
                turned[turn % 2][...] = after[0][:, rows_of(after[1])].T
            pltpu.make_async_copy(stage.at[slot, pl.ds(p, size)], out.at[pl.ds(row * GRAD_ROWS + p, size), cols], out_sem.at[slot]).start()
        if t == 1:
            for copy, back in zip(homes, backs):
                copy.wait()
                back.start()
    for slot in range(2):
        pltpu.make_async_copy(stage.at[slot], stage.at[slot], out_sem.at[slot]).wait()
    for copy in backs:
        copy.wait()


def weight_grads(h, d, a, g, y, dx):
    tokens, d_model = h.shape
    d_ff = d.shape[1]
    n_in = 3 + d_ff // GRAD_ROWS
    hbm = pl.BlockSpec(memory_space=pl.ANY)
    dma = lambda *shape: pltpu.SemaphoreType.DMA(shape)
    like = lambda v: pltpu.VMEM(v.shape, v.dtype)
    return pl.pallas_call(
        weight_grad_kernel,
        name='weight_grads',
        out_shape=(jax.ShapeDtypeStruct((d_model, d_ff), F32), jax.ShapeDtypeStruct((d_ff, d_model), F32),
                   jax.ShapeDtypeStruct(y.shape, BF16), jax.ShapeDtypeStruct(y.shape, BF16)),
        in_specs=[hbm] * 6,
        out_specs=(hbm,) * 4,
        scratch_shapes=[like(h), like(d), like(a), like(g), pltpu.VMEM((2,) + y.shape, BF16), pltpu.VMEM((GRAD_ROWS, tokens), BF16), pltpu.VMEM((GRAD_ROWS, tokens), BF16),
                        pltpu.VMEM((2, GRAD_ROWS, GRAD_COLS), F32),
                        dma(n_in), dma(2), dma(2)],
        compiler_params=pltpu.CompilerParams(vmem_limit_bytes=60 * 1024 * 1024),
    )(h, d, a, g, y, dx)


def solution(mesh):
    tok_spec = P(('data', 'stage', 'inner'))
    up_spec = P(None, ('data', 'stage'), None, 'inner')
    down_spec = P(None, ('data', 'stage'), 'inner', None)

    def device_step(x_loc, g_loc, w_up, w_down):
        y, dx, h, g, a, d = run_pipeline(x_loc, g_loc, w_up[0, 0], w_down[0, 0])
        flat = lambda v: v.reshape(-1, v.shape[-1])
        dw_up, dw_down, y, dx = weight_grads(flat(h), flat(d), flat(a), flat(g), y, dx)
        return y, dx, dw_up[None, None], dw_down[None, None]

    return jax.shard_map(device_step, mesh=mesh, in_specs=(tok_spec, tok_spec, up_spec, down_spec), out_specs=(tok_spec, tok_spec, up_spec, down_spec), check_vma=False)
```

```python
import functools

import jax
import jax.numpy as jnp
from jax import lax
from jax.experimental import pallas as pl
from jax.experimental.pallas import tpu as pltpu
from jax.sharding import PartitionSpec as P

F32 = jnp.float32
BF16 = jnp.bfloat16
MESH = pl.DeviceIdType.MESH

STAGES = 4
INNER = 2
UNITS = 8
SLOTS = 3
DIRECT = 3
BLK = 512
TILE = 256
FWD, BWD = 0, 1
NT = (((1,), (1,)), ((), ()))

F1, F2, FR, B1, B2, BR, T1, T2, SW, PR, YL, WA, WB, XS, M1, HB, XW = range(1, 18)
PLAN = (
    ((WA, 0, 1), (F1, 0, 2), (WB, 0, 1), (XS, 0, 1), (F2, 0, 2), (F1, 2, 2), (FR, 0, 2), (F2, 2, 2),
     (FR, 2, 1), (F1, 4, 2), (FR, 3, 1), (F2, 4, 2), (FR, 4, 2), (F1, 6, 2), (F2, 6, 1), (F2, 7, 1),
     (FR, 6, 2), (XW, 0, 1), (SW, 0, 1), (B1, 0, 2), (B2, 0, 1), (B2, 1, 1), (B1, 2, 1), (B2, 2, 1),
     (B1, 3, 1), (BR, 0, 2), (B2, 3, 1), (BR, 2, 1), (B1, 4, 2), (B2, 4, 2), (BR, 3, 1), (B1, 6, 2),
     (B2, 6, 1), (BR, 4, 1), (B2, 7, 1), (BR, 5, 3)),
    ((WA, 0, 1), (WB, 0, 1), (XS, 0, 1), (F1, 0, 2), (F2, 0, 1), (F2, 1, 1), (FR, 0, 2), (F1, 2, 2),
     (F2, 2, 1), (F2, 3, 1), (FR, 2, 1), (F1, 4, 2), (FR, 3, 1), (F2, 4, 1), (F2, 5, 1), (FR, 4, 2),
     (F1, 6, 2), (F2, 6, 2), (FR, 6, 2), (XW, 0, 1), (SW, 0, 1), (HB, 0, 2), (B1, 0, 2), (B2, 0, 1),
     (HB, 2, 1), (B2, 1, 1), (BR, 0, 1), (B1, 2, 2), (BR, 1, 1), (B2, 2, 2), (BR, 2, 2), (B1, 4, 1),
     (B1, 5, 1), (B2, 4, 2), (B1, 6, 1), (B2, 6, 1), (BR, 4, 1), (B1, 7, 1), (BR, 5, 1), (B2, 7, 1),
     (BR, 6, 2)),
    ((WA, 0, 1), (WB, 0, 1), (XS, 0, 1), (XW, 0, 1), (F1, 0, 1), (F2, 0, 1), (F1, 1, 1), (FR, 0, 1),
     (F2, 1, 1), (FR, 1, 1), (F1, 2, 1), (F2, 2, 1), (F1, 3, 1), (F2, 3, 1), (FR, 2, 1), (F1, 4, 1),
     (F1, 5, 1), (FR, 3, 1), (F2, 4, 2), (T1, 0, 2), (F1, 6, 2), (T2, 0, 2), (FR, 4, 1), (F2, 6, 2),
     (FR, 5, 1), (T1, 2, 2), (FR, 6, 2), (T2, 2, 2), (BR, 3, 1), (T1, 4, 2), (T2, 4, 2), (T1, 6, 2),
     (BR, 4, 1), (T2, 6, 2), (BR, 5, 3)),
    ((WB, 0, 1), (XS, 0, 1), (PR, 0, 1), (XW, 0, 1), (M1, 0, 1), (B2, 0, 1), (BR, 0, 1), (M1, 1, 1),
     (B2, 1, 1), (BR, 1, 1), (M1, 2, 2), (B2, 2, 1), (B2, 3, 1), (BR, 2, 2), (M1, 4, 1), (B2, 4, 1),
     (M1, 5, 1), (B2, 5, 1), (BR, 4, 1), (M1, 6, 2), (BR, 5, 1), (B2, 6, 2), (BR, 6, 2), (YL, 0, 1),
     (F2, 0, 2), (FR, 0, 2), (F2, 2, 1), (F2, 3, 2), (FR, 2, 1), (F2, 5, 1), (FR, 3, 2), (F2, 6, 1),
     (FR, 5, 1), (F2, 7, 1), (FR, 6, 2)),
)


PACK = 1024
UP_GROUP = 8
TURN = 6
TURN_GROUP = 4
DOWN_GROUP = 2


def plan_words():
    rows = [[op + 32 * unit + 256 * (count - 1) for op, unit, count in row] for row in PLAN]
    steps = -(-max(len(row) for row in rows) // 3) * 3
    rows = [row + [0] * (steps - len(row)) for row in rows]
    return steps, [[row[t] + PACK * row[t + 1] + PACK * PACK * row[t + 2] for t in range(0, steps, 3)] for row in rows]


def gelu_pair(pre_act):
    root = pre_act * 0.7071067811865476
    normal_cdf = 0.5 * (1.0 + lax.erf(root))
    normal_pdf = jnp.exp2(root * root * -1.4426950408889634) * 0.3989422804014327
    return pre_act * normal_cdf, normal_cdf + pre_act * normal_pdf


def wait_bytes(ref, sem):
    pltpu.make_async_copy(ref, ref, sem).wait()


def pipeline_kernel(x_ref, g_ref, w1_ref, w2_ref,
                    y_out, dx_out, h_out, g_out, a_out, d_out,
                    wa, wb, flow, act, slope, part, recv, send, home, direct,
                    flow_sem, recv_sem, part_send, flow_send, home_send, home_sem, in_send, relay_sem, relay_send,
                    direct_sem, direct_send, cross_send, stage_sem, w_sem, out_sem):
    stage = lax.axis_index('stage')
    side = lax.axis_index('inner')
    other = 1 - side
    rows, d_model = flow.shape[3:]
    tok, d_ff = act.shape[2:]
    n_blk = d_model // BLK

    def peer(s, i):
        return {'stage': s, 'inner': i}

    load_a = pltpu.make_async_copy(w1_ref, wa, w_sem.at[0])
    load_b = pltpu.make_async_copy(w2_ref, wb, w_sem.at[1])

    def unit_of(k):
        return lax.rem(2 * stage + k + UNITS - 1, UNITS)

    staged = (send.at[BWD, pl.ds(UNITS - 2, 2)], send.at[BWD, pl.ds(UNITS - 4, 2)])
    stagings = [pltpu.make_async_copy(src, dst, stage_sem.at[kind]) for kind, (src, dst) in enumerate(zip((x_ref, g_ref), staged))]
    for kind, target in ((FWD, 0), (BWD, STAGES - 1)):
        stagings[kind].start()

        @pl.when(stage == target)
        def _():
            for k in range(2):
                pltpu.make_async_copy((x_ref, g_ref)[kind].at[k], flow.at[kind, unit_of(k), side], flow_sem.at[kind, unit_of(k), side]).start()

    @pl.when(stage < STAGES - 1)
    def _():
        load_a.start()
    load_b.start()

    @pl.when(stage == STAGES - 1)
    def _():
        load_a.start()

    barrier = pltpu.get_barrier_semaphore()
    for s in range(STAGES):
        for i in range(INNER):
            @pl.when(jnp.logical_or(stage != s, side != i))
            def _():
                pl.semaphore_signal(barrier, inc=1, device_id=peer(s, i), device_id_type=MESH)
    pl.semaphore_wait(barrier, STAGES * INNER - 1)

    def home_of(u):
        return lax.rem((u + 1) // 2, STAGES)

    def slot_of(u):
        return lax.rem(u + 1, 2)

    def hand_in(kind, target, k, lane):
        u = unit_of(k)
        src = staged[kind]
        if lane == 0:
            @pl.when(stage != target)
            def _():
                pltpu.make_async_remote_copy(src.at[k], flow.at[kind, u, side], in_send.at[kind, k, 0], flow_sem.at[kind, u, side],
                                             device_id=peer(target, side), device_id_type=MESH).start()
        else:
            pltpu.make_async_remote_copy(src.at[k], flow.at[kind, u, side], in_send.at[kind, k, 1], flow_sem.at[kind, u, side],
                                         device_id=peer(target, other), device_id_type=MESH).start()

    def relay(k):
        return pltpu.make_async_remote_copy(staged[FWD].at[k], home.at[FWD, k], in_send.at[FWD, k, 1], relay_sem.at[k],
                                            device_id=peer(stage, other), device_id_type=MESH)

    def relayed(k):
        u = unit_of(k)
        return pltpu.make_async_remote_copy(home.at[FWD, k], flow.at[FWD, u, other], relay_send.at[k], flow_sem.at[FWD, u, other],
                                            device_id=peer(0, side), device_id_type=MESH)

    stagings[FWD].wait()
    for k in range(2):
        hand_in(FWD, 0, k, 0)

        @pl.when(jnp.logical_or(stage == 1, jnp.logical_and(stage == 0, k == 1)))
        def _():
            hand_in(FWD, 0, k, 1)

        @pl.when(stage > 1)
        def _():
            relay(k).start()
    steps, plan = plan_words()
    words = [jnp.where(stage == 0, a, jnp.where(stage == 1, b, jnp.where(stage == 2, c, d))) for a, b, c, d in zip(*plan)]

    def keep(ref, out, u, lane):
        pltpu.make_async_copy(ref, out.at[u], out_sem.at[lane]).start()

    def blocks(width, group, fn):
        def body(t, carry):
            fn([pl.ds(pl.multiple_of((t * group + k) * BLK, BLK), BLK) for k in range(group)])
            return carry
        lax.fori_loop(0, width // BLK // group, body, 0)

    def arrived(kind, u):
        for half in range(INNER):
            @pl.when(jnp.logical_not((stage == 1) & (kind == BWD) & (u < DIRECT) & (side == half)))
            def _():
                wait_bytes(flow.at[kind, u, half], flow_sem.at[kind, u, half])

    def both_arrived(kind, u, v):
        arrived(kind, u)

        @pl.when(v != u)
        def _():
            arrived(kind, v)

    def pair(ref, kind, u, v):
        width = ref.shape[-1]
        return jnp.concatenate([ref[kind, u].reshape(tok, width), ref[kind, v].reshape(tok, width)], axis=0)

    def kept(u, v, fn):
        fn(u)

        @pl.when(v != u)
        def _():
            fn(v)

    def up_product(u, v, last):
        both_arrived(FWD, u, v)

        def fn(slices):
            lhs = pair(flow, FWD, u, v)
            for sl in slices:
                z = jnp.dot(lhs, wa[:, sl], preferred_element_type=F32)
                value, grad = gelu_pair(z)
                value = value.astype(BF16)
                if last:
                    act[BWD, u, :, sl] = (slope[u, :, sl] * grad[:tok]).astype(BF16)
                    act[BWD, v, :, sl] = (slope[v, :, sl] * grad[tok:]).astype(BF16)
                else:
                    slope[u, :, sl] = grad[:tok]
                    slope[v, :, sl] = grad[tok:]
                act[FWD, u, :, sl] = value[:tok]
                act[FWD, v, :, sl] = value[tok:]
        blocks(d_ff, UP_GROUP, fn)

        def out(w):
            keep(flow.at[FWD, w], h_out, w, 0)
            keep(act.at[FWD, w], a_out, w, 2)
            if last:
                keep(act.at[BWD, w], d_out, w, 3)
        kept(u, v, out)

    def across(lhs, ref, sl):
        cut = ref.shape[1] * TURN // 8
        total = lax.dot_general(lhs[:, :cut], ref[sl, :cut], NT, preferred_element_type=F32)
        for k in range(cut, ref.shape[1], TILE):
            turned = [ref[pl.ds(sl.start + q, TILE), k:k + TILE].T for q in range(0, BLK, TILE)]
            total += jnp.dot(lhs[:, k:k + TILE], jnp.concatenate(turned, axis=1), preferred_element_type=F32)
        return total

    def back_product(u, v, swapped):
        both_arrived(BWD, u, v)

        def fn(slices):
            lhs = pair(flow, BWD, u, v)
            for sl in slices:
                if swapped:
                    e = jnp.dot(lhs, wa[:, sl], preferred_element_type=F32)
                else:
                    e = across(lhs, wb, sl)
                act[BWD, u, :, sl] = (e[:tok] * slope[u, :, sl]).astype(BF16)
                act[BWD, v, :, sl] = (e[tok:] * slope[v, :, sl]).astype(BF16)
        blocks(d_ff, UP_GROUP if swapped else TURN_GROUP, fn)

        def out(w):
            keep(flow.at[BWD, w], g_out, w, 1)
            keep(act.at[BWD, w], d_out, w, 3)
        kept(u, v, out)

    def part_copy(kind, u, j):
        slot = lax.rem(u, SLOTS)
        return pltpu.make_async_remote_copy(part.at[kind, slot, j, other], recv.at[kind, u, j], part_send.at[kind, slot, j],
                                            recv_sem.at[kind, u, j], device_id=peer(stage, other), device_id_type=MESH)

    def direct_copy(u, j, half):
        slot = lax.rem(u, SLOTS)
        if half is side:
            return pltpu.make_async_remote_copy(part.at[BWD, slot, j, side], direct.at[u, j], direct_send.at[slot, j],
                                                direct_sem.at[0, u, j], device_id=peer(stage - 1, side), device_id_type=MESH)
        return pltpu.make_async_remote_copy(part.at[BWD, slot, j, other], recv.at[FWD, u, j], part_send.at[BWD, slot, j],
                                            direct_sem.at[1, u, j], device_id=peer(stage - 1, other), device_id_type=MESH)

    def take_direct(first, count):
        def body(i, carry):
            u = first + i
            for j in range(n_blk):
                sl = pl.ds(j * BLK, BLK)
                wait_bytes(direct.at[u, j], direct_sem.at[0, u, j])
                wait_bytes(recv.at[FWD, u, j], direct_sem.at[1, u, j])
                flow[BWD, u, side, :, sl] = (direct[u, j] + recv[FWD, u, j]).astype(BF16)
                pltpu.make_async_remote_copy(flow.at[BWD, u, side, :, sl], flow.at[BWD, u, side, :, sl], cross_send.at[0],
                                             flow_sem.at[BWD, u, side], device_id=peer(stage, other), device_id_type=MESH).start()
            return carry
        lax.fori_loop(0, count, body, 0)

    def down_product(kind, u, v, straight):
        def free(w):
            @pl.when(w >= SLOTS)
            def _():
                for j in range(n_blk):
                    part_copy(kind, w - SLOTS, j).wait_send()

            if not straight:
                @pl.when((w >= SLOTS) & (w < SLOTS + DIRECT))
                def _():
                    for j in range(n_blk):
                        direct_copy(w - SLOTS, j, side).wait_send()
        kept(u, v, free)

        def body(t, carry):
            lhs = pair(act, kind, u, v)
            for k in range(DOWN_GROUP):
                j = t * DOWN_GROUP + k
                sl = pl.ds(pl.multiple_of(j * BLK, BLK), BLK)
                if straight:
                    p = jnp.dot(lhs, wb[:, sl], preferred_element_type=F32)
                else:
                    p = across(lhs, wa, sl)
                p = p.reshape(2, INNER, rows, BLK)
                part[kind, lax.rem(u, SLOTS), j] = p[0]
                part[kind, lax.rem(v, SLOTS), j] = p[1]

            def go(w):
                if straight:
                    for k in range(DOWN_GROUP):
                        part_copy(kind, w, t * DOWN_GROUP + k).start()
                    return

                @pl.when(w >= DIRECT)
                def _():
                    for k in range(DOWN_GROUP):
                        part_copy(kind, w, t * DOWN_GROUP + k).start()

                @pl.when(w < DIRECT)
                def _():
                    for k in range(DOWN_GROUP):
                        j = t * DOWN_GROUP + k
                        sl = pl.ds(pl.multiple_of(j * BLK, BLK), BLK)
                        part[BWD, lax.rem(w, SLOTS), j, side] += flow[BWD, w, side, :, sl].astype(F32)
                    for k in range(DOWN_GROUP):
                        for half in (side, other):
                            direct_copy(w, t * DOWN_GROUP + k, half).start()
            kept(u, v, go)
            return carry
        lax.fori_loop(0, n_blk // DOWN_GROUP, body, 0)

    def hand_on(kind, first, count):
        target = stage + 1 if kind == FWD else stage - 1
        inside = stage < STAGES - 1 if kind == FWD else stage > 0
        out = STAGES - 1 if kind == FWD else 0

        def body(i, carry):
            u = first + i
            slot = lax.rem(u, SLOTS)
            for j in range(n_blk):
                sl = pl.ds(j * BLK, BLK)
                wait_bytes(recv.at[kind, u, j], recv_sem.at[kind, u, j])
                total = flow[kind, u, side, :, sl].astype(F32) + (part[kind, slot, j, side] + recv[kind, u, j])
                send[kind, u, :, sl] = total.astype(BF16)

                @pl.when(inside)
                def _():
                    for half in (side, other):
                        pltpu.make_async_remote_copy(send.at[kind, u, :, sl], flow.at[kind, u, side, :, sl], flow_send.at[kind],
                                                     flow_sem.at[kind, u, side], device_id=peer(target, half), device_id_type=MESH).start()

            @pl.when(jnp.logical_and(jnp.logical_not(inside), home_of(u) != out))
            def _():
                pltpu.make_async_remote_copy(send.at[kind, u], home.at[kind, slot_of(u)], home_send.at[kind, u],
                                             home_sem.at[kind, slot_of(u)], device_id=peer(home_of(u), side), device_id_type=MESH).start()
            return carry
        lax.fori_loop(0, count, body, 0)

    def swap_weights():
        n_i = d_model // TILE

        def body(t, carry):
            i = pl.multiple_of(lax.rem(t, n_i) * TILE, TILE)
            j = pl.multiple_of(lax.div(t, n_i) * TILE, TILE)
            up = wa[pl.ds(i, TILE), pl.ds(j, TILE)]
            down = wb[pl.ds(j, TILE), pl.ds(i, TILE)]
            wa[pl.ds(i, TILE), pl.ds(j, TILE)] = down.T
            wb[pl.ds(j, TILE), pl.ds(i, TILE)] = up.T
            return carry
        lax.fori_loop(0, n_i * (d_ff // TILE), body, 0)

    def prepare_last():
        half = UNITS // 2

        def quarter(q, carry):
            for i in range(half):
                arrived(BWD, q * half + i)
                keep(flow.at[BWD, q * half + i], g_out, q * half + i, 1)
            units = pl.ds(q * half, half)

            def fn(slices):
                lhs = flow[BWD, units].reshape(half * tok, d_model)
                for sl in slices:
                    e = lax.dot_general(lhs, wb[sl, :], NT, preferred_element_type=F32)
                    slope[units, :, sl] = e.reshape(half, tok, BLK)
            blocks(d_ff, 1, fn)
            return carry
        lax.fori_loop(0, 2, quarter, 0)
        load_a.wait()
        n_i = d_model // TILE

        def body(t, carry):
            i = pl.multiple_of(lax.rem(t, n_i) * TILE, TILE)
            j = pl.multiple_of(lax.div(t, n_i) * TILE, TILE)
            wb[pl.ds(j, TILE), pl.ds(i, TILE)] = wa[pl.ds(i, TILE), pl.ds(j, TILE)].T
            return carry
        lax.fori_loop(0, n_i * (d_ff // TILE), body, 0)

    def step(t, carry):
        group, place = lax.div(t, 3), lax.rem(t, 3)
        word = words[0]
        for i, w in enumerate(words[1:], 1):
            word = jnp.where(group == i, w, word)
        code = lax.rem(lax.div(word, jnp.where(place == 0, 1, jnp.where(place == 1, PACK, PACK * PACK))), PACK)
        op = lax.rem(code, 32)
        u = lax.rem(lax.div(code, 32), UNITS)
        count = lax.div(code, 256) + 1

        def on(want):
            return pl.when(op == want)

        v = jnp.minimum(u + count - 1, UNITS - 1)

        @on(F1)
        def _():
            up_product(u, v, False)

        @on(M1)
        def _():
            up_product(u, v, True)

        @pl.when(jnp.logical_or(op == F2, op == B2))
        def _():
            down_product(jnp.where(op == F2, FWD, BWD), u, v, True)

        @on(FR)
        def _():
            hand_on(FWD, u, count)

        @on(BR)
        def _():
            hand_on(BWD, u, count)

        @on(B1)
        def _():
            back_product(u, v, True)

        @on(T1)
        def _():
            back_product(u, v, False)

        @on(T2)
        def _():
            down_product(BWD, u, v, False)

        @on(SW)
        def _():
            swap_weights()

        @on(PR)
        def _():
            prepare_last()

        @on(YL)
        def _():
            load_b.start()
            load_b.wait()

        @on(WA)
        def _():
            load_a.wait()

        @on(WB)
        def _():
            load_b.wait()

        @on(XS)
        def _():
            stagings[BWD].wait()
            for k in range(2):
                for lane in range(2):
                    hand_in(BWD, STAGES - 1, k, lane)

            @pl.when(stage == 0)
            def _():
                hand_in(FWD, 0, 0, 1)

            @pl.when(stage > 1)
            def _():
                for k in range(2):
                    wait_bytes(home.at[FWD, k], relay_sem.at[k])
                    relayed(k).start()

        @on(XW)
        def _():
            for kind, target in ((FWD, 0), (BWD, STAGES - 1)):
                for k in range(2):
                    @pl.when(stage != target)
                    def _():
                        wait_bytes(staged[kind].at[k], in_send.at[kind, k, 0])
                    wait_bytes(staged[kind].at[k], in_send.at[kind, k, 1])

            @pl.when(stage > 1)
            def _():
                for k in range(2):
                    relayed(k).wait_send()

        @on(HB)
        def _():
            take_direct(u, count)
        return carry
    lax.fori_loop(0, steps, step, 0)

    for kind, here, out in ((FWD, STAGES - 1, y_out), (BWD, 0, dx_out)):
        for k in range(2):
            @pl.when(stage == here)
            def _():
                pltpu.make_async_copy(send.at[kind, unit_of(k)], out.at[k], out_sem.at[4 + kind]).start()

            @pl.when(stage != here)
            def _():
                wait_bytes(home.at[kind, k], home_sem.at[kind, k])
                pltpu.make_async_copy(home.at[kind, k], out.at[k], out_sem.at[4 + kind]).start()

    for kind in (FWD, BWD):
        for u in range(UNITS - SLOTS, UNITS):
            for j in range(n_blk):
                part_copy(kind, u, j).wait_send()
    for kind, last in ((FWD, STAGES - 1), (BWD, 0)):
        @pl.when((stage != last) & jnp.logical_not((stage == 2) & (kind == BWD)))
        def _():
            wait_bytes(flow.at[kind], flow_send.at[kind])

        @pl.when(stage == last)
        def _():
            for u in range(UNITS):
                if (u + 1) // 2 % STAGES != last:
                    wait_bytes(send.at[kind, u], home_send.at[kind, u])
    @pl.when(stage == 2)
    def _():
        wait_bytes(flow.at[BWD, pl.ds(0, UNITS - DIRECT)], flow_send.at[BWD])

    @pl.when(stage == 1)
    def _():
        wait_bytes(flow.at[BWD, pl.ds(0, DIRECT), 0], cross_send.at[0])
    for lane, (ref, out) in enumerate(((flow.at[FWD], h_out), (flow.at[BWD], g_out), (act.at[FWD], a_out), (act.at[BWD], d_out),
                                       (home.at[FWD], y_out), (home.at[BWD], dx_out))):
        pltpu.make_async_copy(ref, out, out_sem.at[lane]).wait()


def run_pipeline(x_loc, g_loc, w_one, w_two):
    rows, d_model = x_loc.shape[1:]
    d_ff = w_one.shape[1]
    n_blk = d_model // BLK
    tok = INNER * rows
    hbm = pl.BlockSpec(memory_space=pl.ANY)
    out = lambda *shape: jax.ShapeDtypeStruct(shape, BF16)
    dma = lambda *shape: pltpu.SemaphoreType.DMA(shape)
    return pl.pallas_call(
        pipeline_kernel,
        name='pipeline',
        out_shape=(out(*x_loc.shape), out(*x_loc.shape), out(UNITS, INNER, rows, d_model), out(UNITS, INNER, rows, d_model),
                   out(UNITS, tok, d_ff), out(UNITS, tok, d_ff)),
        in_specs=[hbm] * 4,
        out_specs=(hbm,) * 6,
        scratch_shapes=[
            pltpu.VMEM((d_model, d_ff), BF16),
            pltpu.VMEM((d_ff, d_model), BF16),
            pltpu.VMEM((2, UNITS, INNER, rows, d_model), BF16),
            pltpu.VMEM((2, UNITS, tok, d_ff), BF16),
            pltpu.VMEM((UNITS, tok, d_ff), F32),
            pltpu.VMEM((2, SLOTS, n_blk, INNER, rows, BLK), F32),
            pltpu.VMEM((2, UNITS, n_blk, rows, BLK), F32),
            pltpu.VMEM((2, UNITS, rows, d_model), BF16),
            pltpu.VMEM((2, 2, rows, d_model), BF16),
            pltpu.VMEM((DIRECT, n_blk, rows, BLK), F32),
            dma(2, UNITS, INNER), dma(2, UNITS, n_blk), dma(2, SLOTS, n_blk), dma(2), dma(2, UNITS), dma(2, 2), dma(2, 2, 2), dma(2), dma(2),
            dma(2, DIRECT, n_blk), dma(SLOTS, n_blk), dma(1), dma(2), dma(2), dma(6),
        ],
        compiler_params=pltpu.CompilerParams(collective_id=0, has_side_effects=True, vmem_limit_bytes=67043328),
    )(x_loc, g_loc, w_one, w_two)


GRAD_ROWS, GRAD_COLS, GRAD_PART = 1024, 2048, 512


def weight_grad_kernel(h_ref, d_ref, a_ref, g_ref, y_ref, x_ref, up_ref, down_ref, y_out, x_out,
                       h, d, a, g, home, left, right, stage, in_sem, home_sem, out_sem):
    d_model, d_ff = h.shape[1], d.shape[1]
    n_down, n_up, n_col = d_ff // GRAD_ROWS, d_model // GRAD_ROWS, d_ff // GRAD_COLS

    pieces = [a.at[:, pl.ds(t * GRAD_ROWS, GRAD_ROWS)] for t in range(n_down)]
    loads = [(g_ref, g)] + [(a_ref.at[:, pl.ds(t * GRAD_ROWS, GRAD_ROWS)], piece) for t, piece in enumerate(pieces)] + [(h_ref, h), (d_ref, d)]
    loads = [pltpu.make_async_copy(src, dst, in_sem.at[t]) for t, (src, dst) in enumerate(loads)]
    homes = [pltpu.make_async_copy(src, home.at[t], home_sem.at[t]) for t, src in enumerate((y_ref, x_ref))]
    backs = [pltpu.make_async_copy(home.at[t], dst, home_sem.at[t]) for t, dst in enumerate((y_out, x_out))]
    for copy in loads + homes:
        copy.start()

    rows_of = lambda t: pl.ds(t * GRAD_ROWS, GRAD_ROWS)
    blocks = [(a, t, g, 0, down_ref) for t in range(n_down)] + [(h, t, d, c, up_ref) for t in range(n_up) for c in range(n_col)]
    turned = (left, right)
    loads[0].wait()
    loads[1].wait()
    arrived = 2
    turn = -1
    for t, (src, row, other, col, out) in enumerate(blocks):
        slot = t % 2
        cols = pl.ds(col * GRAD_COLS, GRAD_COLS)
        after = blocks[t + 1] if t + 1 < len(blocks) else None
        need = (1 + n_down if after is None or after[0] is h else t + 2) + (1 if src is h or (after is not None and after[0] is h) else 0)
        need = min(need, len(loads) - 1) + (1 if src is h else 0)
        while arrived < min(need + 1, len(loads)):
            loads[arrived].wait()
            arrived += 1
        if t >= 2:
            pltpu.make_async_copy(stage.at[slot], stage.at[slot], out_sem.at[slot]).wait()
        last = after is None
        size = GRAD_ROWS // 4 if last else GRAD_ROWS
        for p in range(0, GRAD_ROWS, size):
            if t == 0:
                value = lax.dot_general(src[:, rows_of(0)], other[:, cols], (((0,), (0,)), ((), ())), preferred_element_type=F32)
                stage[slot] = value
            else:
                for q in range(p, p + size, min(size, GRAD_PART)):
                    part = slice(q, q + min(size, GRAD_PART))
                    stage[slot, part] = jnp.dot(turned[turn % 2][part], other[:, cols], preferred_element_type=F32)
            if not last and (after[0] is not src or after[1] != row):
                turn += 1
                turned[turn % 2][...] = after[0][:, rows_of(after[1])].T
            pltpu.make_async_copy(stage.at[slot, pl.ds(p, size)], out.at[pl.ds(row * GRAD_ROWS + p, size), cols], out_sem.at[slot]).start()
        if t == 1:
            for copy, back in zip(homes, backs):
                copy.wait()
                back.start()
    for slot in range(2):
        pltpu.make_async_copy(stage.at[slot], stage.at[slot], out_sem.at[slot]).wait()
    for copy in backs:
        copy.wait()


def weight_grads(h, d, a, g, y, dx):
    tokens, d_model = h.shape
    d_ff = d.shape[1]
    n_in = 3 + d_ff // GRAD_ROWS
    hbm = pl.BlockSpec(memory_space=pl.ANY)
    dma = lambda *shape: pltpu.SemaphoreType.DMA(shape)
    like = lambda v: pltpu.VMEM(v.shape, v.dtype)
    return pl.pallas_call(
        weight_grad_kernel,
        name='weight_grads',
        out_shape=(jax.ShapeDtypeStruct((d_model, d_ff), F32), jax.ShapeDtypeStruct((d_ff, d_model), F32),
                   jax.ShapeDtypeStruct(y.shape, BF16), jax.ShapeDtypeStruct(y.shape, BF16)),
        in_specs=[hbm] * 6,
        out_specs=(hbm,) * 4,
        scratch_shapes=[like(h), like(d), like(a), like(g), pltpu.VMEM((2,) + y.shape, BF16), pltpu.VMEM((GRAD_ROWS, tokens), BF16), pltpu.VMEM((GRAD_ROWS, tokens), BF16),
                        pltpu.VMEM((2, GRAD_ROWS, GRAD_COLS), F32),
                        dma(n_in), dma(2), dma(2)],
        compiler_params=pltpu.CompilerParams(vmem_limit_bytes=60 * 1024 * 1024),
    )(h, d, a, g, y, dx)


def solution(mesh):
    tok_spec = P(('data', 'stage', 'inner'))
    up_spec = P(None, ('data', 'stage'), None, 'inner')
    down_spec = P(None, ('data', 'stage'), 'inner', None)

    def device_step(x_loc, g_loc, w_up, w_down):
        y, dx, h, g, a, d = run_pipeline(x_loc, g_loc, w_up[0, 0], w_down[0, 0])
        flat = lambda v: v.reshape(-1, v.shape[-1])
        dw_up, dw_down, y, dx = weight_grads(flat(h), flat(d), flat(a), flat(g), y, dx)
        return y, dx, dw_up[None, None], dw_down[None, None]

    return jax.shard_map(device_step, mesh=mesh, in_specs=(tok_spec, tok_spec, up_spec, down_spec), out_specs=(tok_spec, tok_spec, up_spec, down_spec), check_vma=False)
```

```python
import functools

import jax
import jax.numpy as jnp
from jax import lax
from jax.experimental import pallas as pl
from jax.experimental.pallas import tpu as pltpu
from jax.sharding import PartitionSpec as P

F32 = jnp.float32
BF16 = jnp.bfloat16
MESH = pl.DeviceIdType.MESH

STAGES = 4
INNER = 2
UNITS = 8
SLOTS = 3
DIRECT = 3
BLK = 512
TILE = 256
FWD, BWD = 0, 1
NT = (((1,), (1,)), ((), ()))

F1, F2, FR, B1, B2, BR, T1, T2, SW, PR, YL, WA, WB, XS, M1, HB, XW, XR = range(1, 19)
PLAN = (
    ((WA, 0, 1), (F1, 0, 2), (WB, 0, 1), (XS, 0, 1), (F2, 0, 2), (F1, 2, 2), (FR, 0, 2), (F2, 2, 2),
     (FR, 2, 1), (F1, 4, 2), (FR, 3, 1), (F2, 4, 2), (FR, 4, 2), (F1, 6, 2), (F2, 6, 1), (F2, 7, 1),
     (FR, 6, 2), (XW, 0, 1), (SW, 0, 1), (B1, 0, 2), (B2, 0, 1), (B2, 1, 1), (B1, 2, 1), (B2, 2, 1),
     (B1, 3, 1), (BR, 0, 2), (B2, 3, 1), (BR, 2, 1), (B1, 4, 2), (B2, 4, 2), (BR, 3, 1), (B1, 6, 2),
     (B2, 6, 1), (BR, 4, 1), (B2, 7, 1), (BR, 5, 3)),
    ((WA, 0, 1), (WB, 0, 1), (XS, 0, 1), (F1, 0, 2), (F2, 0, 1), (F2, 1, 1), (FR, 0, 2), (F1, 2, 2),
     (F2, 2, 1), (F2, 3, 1), (FR, 2, 1), (F1, 4, 2), (FR, 3, 1), (F2, 4, 1), (F2, 5, 1), (FR, 4, 2),
     (F1, 6, 2), (F2, 6, 2), (FR, 6, 2), (XW, 0, 1), (SW, 0, 1), (HB, 0, 2), (B1, 0, 2), (B2, 0, 1),
     (HB, 2, 1), (B2, 1, 1), (BR, 0, 1), (B1, 2, 2), (BR, 1, 1), (B2, 2, 2), (BR, 2, 2), (B1, 4, 1),
     (B1, 5, 1), (B2, 4, 2), (B1, 6, 1), (B2, 6, 1), (BR, 4, 1), (B1, 7, 1), (BR, 5, 1), (B2, 7, 1),
     (BR, 6, 2)),
    ((XR, 0, 1), (WA, 0, 1), (WB, 0, 1), (XS, 0, 1), (XW, 0, 1), (F1, 0, 1), (F2, 0, 1), (F1, 1, 1),
     (FR, 0, 1), (F2, 1, 1), (FR, 1, 1), (F1, 2, 1), (F2, 2, 1), (F1, 3, 1), (F2, 3, 1), (FR, 2, 1),
     (F1, 4, 1), (F1, 5, 1), (FR, 3, 1), (F2, 4, 2), (T1, 0, 2), (F1, 6, 2), (T2, 0, 2), (FR, 4, 1),
     (F2, 6, 2), (FR, 5, 1), (T1, 2, 2), (FR, 6, 2), (T2, 2, 2), (BR, 3, 1), (T1, 4, 2), (T2, 4, 2),
     (T1, 6, 2), (BR, 4, 1), (T2, 6, 2), (BR, 5, 3)),
    ((XR, 0, 1), (WB, 0, 1), (XS, 0, 1), (PR, 0, 1), (XW, 0, 1), (M1, 0, 1), (B2, 0, 1), (BR, 0, 1),
     (M1, 1, 1), (B2, 1, 1), (BR, 1, 1), (M1, 2, 2), (B2, 2, 1), (B2, 3, 1), (BR, 2, 2), (M1, 4, 1),
     (B2, 4, 1), (M1, 5, 1), (B2, 5, 1), (BR, 4, 1), (M1, 6, 2), (BR, 5, 1), (B2, 6, 2), (BR, 6, 2),
     (YL, 0, 1), (F2, 0, 2), (FR, 0, 2), (F2, 2, 1), (F2, 3, 2), (FR, 2, 1), (F2, 5, 1), (FR, 3, 2),
     (F2, 6, 1), (FR, 5, 1), (F2, 7, 1), (FR, 6, 2)),
)


PACK = 1024
UP_GROUP = 8
TURN = 6
TURN_GROUP = 4
DOWN_GROUP = 2


def plan_words():
    rows = [[op + 32 * unit + 256 * (count - 1) for op, unit, count in row] for row in PLAN]
    steps = -(-max(len(row) for row in rows) // 3) * 3
    rows = [row + [0] * (steps - len(row)) for row in rows]
    return steps, [[row[t] + PACK * row[t + 1] + PACK * PACK * row[t + 2] for t in range(0, steps, 3)] for row in rows]


def gelu_pair(pre_act):
    root = pre_act * 0.7071067811865476
    normal_cdf = 0.5 * (1.0 + lax.erf(root))
    normal_pdf = jnp.exp2(root * root * -1.4426950408889634) * 0.3989422804014327
    return pre_act * normal_cdf, normal_cdf + pre_act * normal_pdf


def wait_bytes(ref, sem):
    pltpu.make_async_copy(ref, ref, sem).wait()


def pipeline_kernel(x_ref, g_ref, w1_ref, w2_ref,
                    y_out, dx_out, h_out, g_out, a_out, d_out,
                    wa, wb, flow, act, slope, part, recv, send, home, direct,
                    flow_sem, recv_sem, part_send, flow_send, home_send, home_sem, in_send, relay_sem, relay_send,
                    direct_sem, direct_send, cross_send, stage_sem, w_sem, out_sem):
    stage = lax.axis_index('stage')
    side = lax.axis_index('inner')
    other = 1 - side
    rows, d_model = flow.shape[3:]
    tok, d_ff = act.shape[2:]
    n_blk = d_model // BLK

    def peer(s, i):
        return {'stage': s, 'inner': i}

    load_a = pltpu.make_async_copy(w1_ref, wa, w_sem.at[0])
    load_b = pltpu.make_async_copy(w2_ref, wb, w_sem.at[1])

    def unit_of(k):
        return lax.rem(2 * stage + k + UNITS - 1, UNITS)

    staged = (send.at[BWD, pl.ds(UNITS - 2, 2)], send.at[BWD, pl.ds(UNITS - 4, 2)])
    stagings = [pltpu.make_async_copy(src, dst, stage_sem.at[kind]) for kind, (src, dst) in enumerate(zip((x_ref, g_ref), staged))]
    for kind, target in ((FWD, 0), (BWD, STAGES - 1)):
        stagings[kind].start()

        @pl.when(stage == target)
        def _():
            for k in range(2):
                pltpu.make_async_copy((x_ref, g_ref)[kind].at[k], flow.at[kind, unit_of(k), side], flow_sem.at[kind, unit_of(k), side]).start()

    @pl.when(stage < STAGES - 1)
    def _():
        load_a.start()
    load_b.start()

    @pl.when(stage == STAGES - 1)
    def _():
        load_a.start()

    barrier = pltpu.get_barrier_semaphore()
    for s in range(STAGES):
        for i in range(INNER):
            @pl.when(jnp.logical_or(stage != s, side != i))
            def _():
                pl.semaphore_signal(barrier, inc=1, device_id=peer(s, i), device_id_type=MESH)
    pl.semaphore_wait(barrier, STAGES * INNER - 1)

    def home_of(u):
        return lax.rem((u + 1) // 2, STAGES)

    def slot_of(u):
        return lax.rem(u + 1, 2)

    def hand_in(kind, target, k, lane):
        u = unit_of(k)
        src = staged[kind]
        if lane == 0:
            @pl.when(stage != target)
            def _():
                pltpu.make_async_remote_copy(src.at[k], flow.at[kind, u, side], in_send.at[kind, k, 0], flow_sem.at[kind, u, side],
                                             device_id=peer(target, side), device_id_type=MESH).start()
        else:
            pltpu.make_async_remote_copy(src.at[k], flow.at[kind, u, side], in_send.at[kind, k, 1], flow_sem.at[kind, u, side],
                                         device_id=peer(target, other), device_id_type=MESH).start()

    def relay(k):
        return pltpu.make_async_remote_copy(staged[FWD].at[k], home.at[FWD, k], in_send.at[FWD, k, 1], relay_sem.at[k],
                                            device_id=peer(stage, other), device_id_type=MESH)

    def relayed(k):
        u = unit_of(k)
        return pltpu.make_async_remote_copy(home.at[FWD, k], flow.at[FWD, u, other], relay_send.at[k], flow_sem.at[FWD, u, other],
                                            device_id=peer(0, side), device_id_type=MESH)

    stagings[FWD].wait()
    for k in range(2):
        hand_in(FWD, 0, k, 0)

        @pl.when(jnp.logical_or(stage == 1, jnp.logical_and(stage == 0, k == 1)))
        def _():
            hand_in(FWD, 0, k, 1)

        @pl.when(stage > 1)
        def _():
            relay(k).start()
    steps, plan = plan_words()
    words = [jnp.where(stage == 0, a, jnp.where(stage == 1, b, jnp.where(stage == 2, c, d))) for a, b, c, d in zip(*plan)]

    def keep(ref, out, u, lane):
        pltpu.make_async_copy(ref, out.at[u], out_sem.at[lane]).start()

    def blocks(width, group, fn):
        def body(t, carry):
            fn([pl.ds(pl.multiple_of((t * group + k) * BLK, BLK), BLK) for k in range(group)])
            return carry
        lax.fori_loop(0, width // BLK // group, body, 0)

    def arrived(kind, u):
        for half in range(INNER):
            @pl.when(jnp.logical_not((stage == 1) & (kind == BWD) & (u < DIRECT) & (side == half)))
            def _():
                wait_bytes(flow.at[kind, u, half], flow_sem.at[kind, u, half])

    def both_arrived(kind, u, v):
        arrived(kind, u)

        @pl.when(v != u)
        def _():
            arrived(kind, v)

    def pair(ref, kind, u, v):
        width = ref.shape[-1]
        return jnp.concatenate([ref[kind, u].reshape(tok, width), ref[kind, v].reshape(tok, width)], axis=0)

    def kept(u, v, fn):
        fn(u)

        @pl.when(v != u)
        def _():
            fn(v)

    def up_product(u, v, last):
        both_arrived(FWD, u, v)

        def fn(slices):
            lhs = pair(flow, FWD, u, v)
            for sl in slices:
                z = jnp.dot(lhs, wa[:, sl], preferred_element_type=F32)
                value, grad = gelu_pair(z)
                value = value.astype(BF16)
                if last:
                    act[BWD, u, :, sl] = (slope[u, :, sl] * grad[:tok]).astype(BF16)
                    act[BWD, v, :, sl] = (slope[v, :, sl] * grad[tok:]).astype(BF16)
                else:
                    slope[u, :, sl] = grad[:tok]
                    slope[v, :, sl] = grad[tok:]
                act[FWD, u, :, sl] = value[:tok]
                act[FWD, v, :, sl] = value[tok:]
        blocks(d_ff, UP_GROUP, fn)

        def out(w):
            keep(flow.at[FWD, w], h_out, w, 0)
            keep(act.at[FWD, w], a_out, w, 2)
            if last:
                keep(act.at[BWD, w], d_out, w, 3)
        kept(u, v, out)

    def across(lhs, ref, sl):
        cut = ref.shape[1] * TURN // 8
        total = lax.dot_general(lhs[:, :cut], ref[sl, :cut], NT, preferred_element_type=F32)
        for k in range(cut, ref.shape[1], TILE):
            turned = [ref[pl.ds(sl.start + q, TILE), k:k + TILE].T for q in range(0, BLK, TILE)]
            total += jnp.dot(lhs[:, k:k + TILE], jnp.concatenate(turned, axis=1), preferred_element_type=F32)
        return total

    def back_product(u, v, swapped):
        both_arrived(BWD, u, v)

        def fn(slices):
            lhs = pair(flow, BWD, u, v)
            for sl in slices:
                if swapped:
                    e = jnp.dot(lhs, wa[:, sl], preferred_element_type=F32)
                else:
                    e = across(lhs, wb, sl)
                act[BWD, u, :, sl] = (e[:tok] * slope[u, :, sl]).astype(BF16)
                act[BWD, v, :, sl] = (e[tok:] * slope[v, :, sl]).astype(BF16)
        blocks(d_ff, UP_GROUP if swapped else TURN_GROUP, fn)

        def out(w):
            keep(flow.at[BWD, w], g_out, w, 1)
            keep(act.at[BWD, w], d_out, w, 3)
        kept(u, v, out)

    def part_copy(kind, u, j):
        slot = lax.rem(u, SLOTS)
        return pltpu.make_async_remote_copy(part.at[kind, slot, j, other], recv.at[kind, u, j], part_send.at[kind, slot, j],
                                            recv_sem.at[kind, u, j], device_id=peer(stage, other), device_id_type=MESH)

    def direct_copy(u, j, half):
        slot = lax.rem(u, SLOTS)
        if half is side:
            return pltpu.make_async_remote_copy(part.at[BWD, slot, j, side], direct.at[u, j], direct_send.at[slot, j],
                                                direct_sem.at[0, u, j], device_id=peer(stage - 1, side), device_id_type=MESH)
        return pltpu.make_async_remote_copy(part.at[BWD, slot, j, other], recv.at[FWD, u, j], part_send.at[BWD, slot, j],
                                            direct_sem.at[1, u, j], device_id=peer(stage - 1, other), device_id_type=MESH)

    def take_direct(first, count):
        def body(i, carry):
            u = first + i
            for j in range(n_blk):
                sl = pl.ds(j * BLK, BLK)
                wait_bytes(direct.at[u, j], direct_sem.at[0, u, j])
                wait_bytes(recv.at[FWD, u, j], direct_sem.at[1, u, j])
                flow[BWD, u, side, :, sl] = (direct[u, j] + recv[FWD, u, j]).astype(BF16)
                pltpu.make_async_remote_copy(flow.at[BWD, u, side, :, sl], flow.at[BWD, u, side, :, sl], cross_send.at[0],
                                             flow_sem.at[BWD, u, side], device_id=peer(stage, other), device_id_type=MESH).start()
            return carry
        lax.fori_loop(0, count, body, 0)

    def down_product(kind, u, v, straight):
        def free(w):
            @pl.when(w >= SLOTS)
            def _():
                for j in range(n_blk):
                    part_copy(kind, w - SLOTS, j).wait_send()

            if not straight:
                @pl.when((w >= SLOTS) & (w < SLOTS + DIRECT))
                def _():
                    for j in range(n_blk):
                        direct_copy(w - SLOTS, j, side).wait_send()
        kept(u, v, free)

        def body(t, carry):
            lhs = pair(act, kind, u, v)
            for k in range(DOWN_GROUP):
                j = t * DOWN_GROUP + k
                sl = pl.ds(pl.multiple_of(j * BLK, BLK), BLK)
                if straight:
                    p = jnp.dot(lhs, wb[:, sl], preferred_element_type=F32)
                else:
                    p = across(lhs, wa, sl)
                p = p.reshape(2, INNER, rows, BLK)
                part[kind, lax.rem(u, SLOTS), j] = p[0]
                part[kind, lax.rem(v, SLOTS), j] = p[1]

            def go(w):
                if straight:
                    for k in range(DOWN_GROUP):
                        part_copy(kind, w, t * DOWN_GROUP + k).start()
                    return

                @pl.when(w >= DIRECT)
                def _():
                    for k in range(DOWN_GROUP):
                        part_copy(kind, w, t * DOWN_GROUP + k).start()

                @pl.when(w < DIRECT)
                def _():
                    for k in range(DOWN_GROUP):
                        j = t * DOWN_GROUP + k
                        sl = pl.ds(pl.multiple_of(j * BLK, BLK), BLK)
                        part[BWD, lax.rem(w, SLOTS), j, side] += flow[BWD, w, side, :, sl].astype(F32)
                    for k in range(DOWN_GROUP):
                        for half in (side, other):
                            direct_copy(w, t * DOWN_GROUP + k, half).start()
            kept(u, v, go)
            return carry
        lax.fori_loop(0, n_blk // DOWN_GROUP, body, 0)

    def hand_on(kind, first, count):
        target = stage + 1 if kind == FWD else stage - 1
        inside = stage < STAGES - 1 if kind == FWD else stage > 0
        out = STAGES - 1 if kind == FWD else 0

        def body(i, carry):
            u = first + i
            slot = lax.rem(u, SLOTS)
            for j in range(n_blk):
                sl = pl.ds(j * BLK, BLK)
                wait_bytes(recv.at[kind, u, j], recv_sem.at[kind, u, j])
                total = flow[kind, u, side, :, sl].astype(F32) + (part[kind, slot, j, side] + recv[kind, u, j])
                send[kind, u, :, sl] = total.astype(BF16)

                @pl.when(inside)
                def _():
                    for half in (side, other):
                        pltpu.make_async_remote_copy(send.at[kind, u, :, sl], flow.at[kind, u, side, :, sl], flow_send.at[kind],
                                                     flow_sem.at[kind, u, side], device_id=peer(target, half), device_id_type=MESH).start()

            @pl.when(jnp.logical_and(jnp.logical_not(inside), home_of(u) != out))
            def _():
                pltpu.make_async_remote_copy(send.at[kind, u], home.at[kind, slot_of(u)], home_send.at[kind, u],
                                             home_sem.at[kind, slot_of(u)], device_id=peer(home_of(u), side), device_id_type=MESH).start()
            return carry
        lax.fori_loop(0, count, body, 0)

    def swap_weights():
        n_i = d_model // TILE

        def body(t, carry):
            i = pl.multiple_of(lax.rem(t, n_i) * TILE, TILE)
            j = pl.multiple_of(lax.div(t, n_i) * TILE, TILE)
            up = wa[pl.ds(i, TILE), pl.ds(j, TILE)]
            down = wb[pl.ds(j, TILE), pl.ds(i, TILE)]
            wa[pl.ds(i, TILE), pl.ds(j, TILE)] = down.T
            wb[pl.ds(j, TILE), pl.ds(i, TILE)] = up.T
            return carry
        lax.fori_loop(0, n_i * (d_ff // TILE), body, 0)

    def prepare_last():
        half = UNITS // 2

        def quarter(q, carry):
            for i in range(half):
                arrived(BWD, q * half + i)
                keep(flow.at[BWD, q * half + i], g_out, q * half + i, 1)
            units = pl.ds(q * half, half)

            def fn(slices):
                lhs = flow[BWD, units].reshape(half * tok, d_model)
                for sl in slices:
                    e = lax.dot_general(lhs, wb[sl, :], NT, preferred_element_type=F32)
                    slope[units, :, sl] = e.reshape(half, tok, BLK)
            blocks(d_ff, 1, fn)
            return carry
        lax.fori_loop(0, 2, quarter, 0)
        load_a.wait()
        n_i = d_model // TILE

        def body(t, carry):
            i = pl.multiple_of(lax.rem(t, n_i) * TILE, TILE)
            j = pl.multiple_of(lax.div(t, n_i) * TILE, TILE)
            wb[pl.ds(j, TILE), pl.ds(i, TILE)] = wa[pl.ds(i, TILE), pl.ds(j, TILE)].T
            return carry
        lax.fori_loop(0, n_i * (d_ff // TILE), body, 0)

    def step(t, carry):
        group, place = lax.div(t, 3), lax.rem(t, 3)
        word = words[0]
        for i, w in enumerate(words[1:], 1):
            word = jnp.where(group == i, w, word)
        code = lax.rem(lax.div(word, jnp.where(place == 0, 1, jnp.where(place == 1, PACK, PACK * PACK))), PACK)
        op = lax.rem(code, 32)
        u = lax.rem(lax.div(code, 32), UNITS)
        count = lax.div(code, 256) + 1

        def on(want):
            return pl.when(op == want)

        v = jnp.minimum(u + count - 1, UNITS - 1)

        @on(F1)
        def _():
            up_product(u, v, False)

        @on(M1)
        def _():
            up_product(u, v, True)

        @pl.when(jnp.logical_or(op == F2, op == B2))
        def _():
            down_product(jnp.where(op == F2, FWD, BWD), u, v, True)

        @on(FR)
        def _():
            hand_on(FWD, u, count)

        @on(BR)
        def _():
            hand_on(BWD, u, count)

        @on(B1)
        def _():
            back_product(u, v, True)

        @on(T1)
        def _():
            back_product(u, v, False)

        @on(T2)
        def _():
            down_product(BWD, u, v, False)

        @on(SW)
        def _():
            swap_weights()

        @on(PR)
        def _():
            prepare_last()

        @on(YL)
        def _():
            load_b.start()
            load_b.wait()

        @on(WA)
        def _():
            load_a.wait()

        @on(WB)
        def _():
            load_b.wait()

        @on(XS)
        def _():
            stagings[BWD].wait()
            for k in range(2):
                for lane in range(2):
                    hand_in(BWD, STAGES - 1, k, lane)

            @pl.when(stage == 0)
            def _():
                hand_in(FWD, 0, 0, 1)

        @on(XR)
        def _():
            for k in range(2):
                wait_bytes(home.at[FWD, k], relay_sem.at[k])
                relayed(k).start()

        @on(XW)
        def _():
            for kind, target in ((FWD, 0), (BWD, STAGES - 1)):
                for k in range(2):
                    @pl.when(stage != target)
                    def _():
                        wait_bytes(staged[kind].at[k], in_send.at[kind, k, 0])
                    wait_bytes(staged[kind].at[k], in_send.at[kind, k, 1])

            @pl.when(stage > 1)
            def _():
                for k in range(2):
                    relayed(k).wait_send()

        @on(HB)
        def _():
            take_direct(u, count)
        return carry
    lax.fori_loop(0, steps, step, 0)

    for kind, here, out in ((FWD, STAGES - 1, y_out), (BWD, 0, dx_out)):
        for k in range(2):
            @pl.when(stage == here)
            def _():
                pltpu.make_async_copy(send.at[kind, unit_of(k)], out.at[k], out_sem.at[4 + kind]).start()

            @pl.when(stage != here)
            def _():
                wait_bytes(home.at[kind, k], home_sem.at[kind, k])
                pltpu.make_async_copy(home.at[kind, k], out.at[k], out_sem.at[4 + kind]).start()

    for kind in (FWD, BWD):
        for u in range(UNITS - SLOTS, UNITS):
            for j in range(n_blk):
                part_copy(kind, u, j).wait_send()
    for kind, last in ((FWD, STAGES - 1), (BWD, 0)):
        @pl.when((stage != last) & jnp.logical_not((stage == 2) & (kind == BWD)))
        def _():
            wait_bytes(flow.at[kind], flow_send.at[kind])

        @pl.when(stage == last)
        def _():
            for u in range(UNITS):
                if (u + 1) // 2 % STAGES != last:
                    wait_bytes(send.at[kind, u], home_send.at[kind, u])
    @pl.when(stage == 2)
    def _():
        wait_bytes(flow.at[BWD, pl.ds(0, UNITS - DIRECT)], flow_send.at[BWD])

    @pl.when(stage == 1)
    def _():
        wait_bytes(flow.at[BWD, pl.ds(0, DIRECT), 0], cross_send.at[0])
    for lane, (ref, out) in enumerate(((flow.at[FWD], h_out), (flow.at[BWD], g_out), (act.at[FWD], a_out), (act.at[BWD], d_out),
                                       (home.at[FWD], y_out), (home.at[BWD], dx_out))):
        pltpu.make_async_copy(ref, out, out_sem.at[lane]).wait()


def run_pipeline(x_loc, g_loc, w_one, w_two):
    rows, d_model = x_loc.shape[1:]
    d_ff = w_one.shape[1]
    n_blk = d_model // BLK
    tok = INNER * rows
    hbm = pl.BlockSpec(memory_space=pl.ANY)
    out = lambda *shape: jax.ShapeDtypeStruct(shape, BF16)
    dma = lambda *shape: pltpu.SemaphoreType.DMA(shape)
    return pl.pallas_call(
        pipeline_kernel,
        name='pipeline',
        out_shape=(out(*x_loc.shape), out(*x_loc.shape), out(UNITS, INNER, rows, d_model), out(UNITS, INNER, rows, d_model),
                   out(UNITS, tok, d_ff), out(UNITS, tok, d_ff)),
        in_specs=[hbm] * 4,
        out_specs=(hbm,) * 6,
        scratch_shapes=[
            pltpu.VMEM((d_model, d_ff), BF16),
            pltpu.VMEM((d_ff, d_model), BF16),
            pltpu.VMEM((2, UNITS, INNER, rows, d_model), BF16),
            pltpu.VMEM((2, UNITS, tok, d_ff), BF16),
            pltpu.VMEM((UNITS, tok, d_ff), F32),
            pltpu.VMEM((2, SLOTS, n_blk, INNER, rows, BLK), F32),
            pltpu.VMEM((2, UNITS, n_blk, rows, BLK), F32),
            pltpu.VMEM((2, UNITS, rows, d_model), BF16),
            pltpu.VMEM((2, 2, rows, d_model), BF16),
            pltpu.VMEM((DIRECT, n_blk, rows, BLK), F32),
            dma(2, UNITS, INNER), dma(2, UNITS, n_blk), dma(2, SLOTS, n_blk), dma(2), dma(2, UNITS), dma(2, 2), dma(2, 2, 2), dma(2), dma(2),
            dma(2, DIRECT, n_blk), dma(SLOTS, n_blk), dma(1), dma(2), dma(2), dma(6),
        ],
        compiler_params=pltpu.CompilerParams(collective_id=0, has_side_effects=True, vmem_limit_bytes=67043328),
    )(x_loc, g_loc, w_one, w_two)


GRAD_ROWS, GRAD_COLS, GRAD_PART, GRAD_SLOTS = 1024, 2048, 256, 4


def weight_grad_kernel(h_ref, d_ref, a_ref, g_ref, y_ref, x_ref, up_ref, down_ref, y_out, x_out,
                       h, d, a, g, home, left, right, stage, in_sem, home_sem, out_sem):
    d_model, d_ff = h.shape[1], d.shape[1]
    n_down, n_up, n_col = d_ff // GRAD_ROWS, d_model // GRAD_ROWS, d_ff // GRAD_COLS

    pieces = [a.at[:, pl.ds(t * GRAD_ROWS, GRAD_ROWS)] for t in range(n_down)]
    loads = [(g_ref, g)] + [(a_ref.at[:, pl.ds(t * GRAD_ROWS, GRAD_ROWS)], piece) for t, piece in enumerate(pieces)] + [(h_ref, h), (d_ref, d)]
    loads = [pltpu.make_async_copy(src, dst, in_sem.at[t]) for t, (src, dst) in enumerate(loads)]
    homes = [pltpu.make_async_copy(src, home.at[t], home_sem.at[t]) for t, src in enumerate((y_ref, x_ref))]
    backs = [pltpu.make_async_copy(home.at[t], dst, home_sem.at[t]) for t, dst in enumerate((y_out, x_out))]
    for copy in loads + homes:
        copy.start()

    rows_of = lambda t: pl.ds(t * GRAD_ROWS, GRAD_ROWS)
    blocks = [(a, t, g, 0, down_ref) for t in range(n_down)] + [(h, t, d, c, up_ref) for t in range(n_up) for c in range(n_col)]
    turned = (left, right)
    loads[0].wait()
    loads[1].wait()
    arrived = 2
    turn = -1
    for t, (src, row, other, col, out) in enumerate(blocks):
        slot = t % GRAD_SLOTS
        cols = pl.ds(col * GRAD_COLS, GRAD_COLS)
        after = blocks[t + 1] if t + 1 < len(blocks) else None
        need = (1 + n_down if after is None or after[0] is h else t + 2) + (1 if src is h or (after is not None and after[0] is h) else 0)
        need = min(need, len(loads) - 1) + (1 if src is h else 0)
        while arrived < min(need + 1, len(loads)):
            loads[arrived].wait()
            arrived += 1
        if t >= GRAD_SLOTS:
            pltpu.make_async_copy(stage.at[slot], stage.at[slot], out_sem.at[slot]).wait()
        size = GRAD_PART if after is None or t == 0 else GRAD_ROWS
        for p in range(0, GRAD_ROWS, size):
            if t == 0:
                stage[slot, p:p + size] = lax.dot_general(src[:, p:p + size], other[:, cols], (((0,), (0,)), ((), ())), preferred_element_type=F32)
            else:
                stage[slot, p:p + size] = jnp.dot(turned[turn % 2][p:p + size], other[:, cols], preferred_element_type=F32)
            if p + size == GRAD_ROWS and after is not None and (after[0] is not src or after[1] != row):
                turn += 1
                turned[turn % 2][...] = after[0][:, rows_of(after[1])].T
            for q in range(p, p + size, GRAD_PART):
                pltpu.make_async_copy(stage.at[slot, pl.ds(q, GRAD_PART)], out.at[pl.ds(row * GRAD_ROWS + q, GRAD_PART), cols], out_sem.at[slot]).start()
        if t == 1:
            for copy, back in zip(homes, backs):
                copy.wait()
                back.start()
    for slot in range(GRAD_SLOTS):
        pltpu.make_async_copy(stage.at[slot], stage.at[slot], out_sem.at[slot]).wait()
    for copy in backs:
        copy.wait()


def weight_grads(h, d, a, g, y, dx):
    tokens, d_model = h.shape
    d_ff = d.shape[1]
    n_in = 3 + d_ff // GRAD_ROWS
    hbm = pl.BlockSpec(memory_space=pl.ANY)
    dma = lambda *shape: pltpu.SemaphoreType.DMA(shape)
    like = lambda v: pltpu.VMEM(v.shape, v.dtype)
    return pl.pallas_call(
        weight_grad_kernel,
        name='weight_grads',
        out_shape=(jax.ShapeDtypeStruct((d_model, d_ff), F32), jax.ShapeDtypeStruct((d_ff, d_model), F32),
                   jax.ShapeDtypeStruct(y.shape, BF16), jax.ShapeDtypeStruct(y.shape, BF16)),
        in_specs=[hbm] * 6,
        out_specs=(hbm,) * 4,
        scratch_shapes=[like(h), like(d), like(a), like(g), pltpu.VMEM((2,) + y.shape, BF16), pltpu.VMEM((GRAD_ROWS, tokens), BF16), pltpu.VMEM((GRAD_ROWS, tokens), BF16),
                        pltpu.VMEM((GRAD_SLOTS, GRAD_ROWS, GRAD_COLS), F32),
                        dma(n_in), dma(2), dma(GRAD_SLOTS)],
        compiler_params=pltpu.CompilerParams(vmem_limit_bytes=60 * 1024 * 1024),
    )(h, d, a, g, y, dx)


def solution(mesh):
    tok_spec = P(('data', 'stage', 'inner'))
    up_spec = P(None, ('data', 'stage'), None, 'inner')
    down_spec = P(None, ('data', 'stage'), 'inner', None)

    def device_step(x_loc, g_loc, w_up, w_down):
        y, dx, h, g, a, d = run_pipeline(x_loc, g_loc, w_up[0, 0], w_down[0, 0])
        flat = lambda v: v.reshape(-1, v.shape[-1])
        dw_up, dw_down, y, dx = weight_grads(flat(h), flat(d), flat(a), flat(g), y, dx)
        return y, dx, dw_up[None, None], dw_down[None, None]

    return jax.shard_map(device_step, mesh=mesh, in_specs=(tok_spec, tok_spec, up_spec, down_spec), out_specs=(tok_spec, tok_spec, up_spec, down_spec), check_vma=False)
```

```python
import functools

import jax
import jax.numpy as jnp
from jax import lax
from jax.experimental import pallas as pl
from jax.experimental.pallas import tpu as pltpu
from jax.sharding import PartitionSpec as P

F32 = jnp.float32
BF16 = jnp.bfloat16
MESH = pl.DeviceIdType.MESH

STAGES = 4
INNER = 2
UNITS = 8
SLOTS = 3
DIRECT = 3
BLK = 512
TILE = 256
FWD, BWD = 0, 1
NT = (((1,), (1,)), ((), ()))

F1, F2, FR, B1, B2, BR, T1, T2, SW, PR, YL, WA, WB, XS, M1, HB, XW, XR = range(1, 19)
PLAN = (
    ((WA, 0, 1), (F1, 0, 2), (WB, 0, 1), (XS, 0, 1), (F2, 0, 2), (F1, 2, 2), (FR, 0, 2), (F2, 2, 2),
     (FR, 2, 1), (F1, 4, 2), (FR, 3, 1), (F2, 4, 2), (FR, 4, 2), (F1, 6, 2), (F2, 6, 1), (F2, 7, 1),
     (FR, 6, 2), (XW, 0, 1), (SW, 0, 1), (B1, 0, 2), (B2, 0, 1), (B2, 1, 1), (B1, 2, 1), (B2, 2, 1),
     (B1, 3, 1), (BR, 0, 2), (B2, 3, 1), (BR, 2, 1), (B1, 4, 2), (B2, 4, 2), (BR, 3, 1), (B1, 6, 2),
     (B2, 6, 1), (BR, 4, 1), (B2, 7, 1), (BR, 5, 3)),
    ((WA, 0, 1), (WB, 0, 1), (XS, 0, 1), (F1, 0, 2), (F2, 0, 1), (F2, 1, 1), (FR, 0, 2), (F1, 2, 2),
     (F2, 2, 1), (F2, 3, 1), (FR, 2, 1), (F1, 4, 2), (FR, 3, 1), (F2, 4, 1), (F2, 5, 1), (FR, 4, 2),
     (F1, 6, 2), (F2, 6, 2), (FR, 6, 2), (XW, 0, 1), (SW, 0, 1), (HB, 0, 2), (B1, 0, 2), (B2, 0, 1),
     (HB, 2, 1), (B2, 1, 1), (BR, 0, 1), (B1, 2, 2), (BR, 1, 1), (B2, 2, 2), (BR, 2, 2), (B1, 4, 1),
     (B1, 5, 1), (B2, 4, 2), (B1, 6, 1), (B2, 6, 1), (BR, 4, 1), (B1, 7, 1), (BR, 5, 1), (B2, 7, 1),
     (BR, 6, 2)),
    ((XR, 0, 1), (WA, 0, 1), (WB, 0, 1), (XS, 0, 1), (XW, 0, 1), (F1, 0, 1), (F2, 0, 1), (F1, 1, 1),
     (FR, 0, 1), (F2, 1, 1), (FR, 1, 1), (F1, 2, 1), (F2, 2, 1), (F1, 3, 1), (F2, 3, 1), (FR, 2, 1),
     (F1, 4, 1), (F1, 5, 1), (FR, 3, 1), (F2, 4, 2), (T1, 0, 2), (F1, 6, 2), (T2, 0, 2), (FR, 4, 1),
     (F2, 6, 2), (FR, 5, 1), (T1, 2, 2), (FR, 6, 2), (T2, 2, 2), (BR, 3, 1), (T1, 4, 2), (T2, 4, 2),
     (T1, 6, 2), (BR, 4, 1), (T2, 6, 2), (BR, 5, 3)),
    ((XR, 0, 1), (WB, 0, 1), (XS, 0, 1), (PR, 0, 1), (XW, 0, 1), (M1, 0, 1), (B2, 0, 1), (BR, 0, 1),
     (M1, 1, 1), (B2, 1, 1), (BR, 1, 1), (M1, 2, 2), (B2, 2, 1), (B2, 3, 1), (BR, 2, 2), (M1, 4, 1),
     (B2, 4, 1), (M1, 5, 1), (B2, 5, 1), (BR, 4, 1), (M1, 6, 2), (BR, 5, 1), (B2, 6, 2), (BR, 6, 2),
     (YL, 0, 1), (F2, 0, 2), (FR, 0, 2), (F2, 2, 1), (F2, 3, 2), (FR, 2, 1), (F2, 5, 1), (FR, 3, 2),
     (F2, 6, 1), (FR, 5, 1), (F2, 7, 1), (FR, 6, 2)),
)


PACK = 1024
UP_GROUP = 8
TURN = 5
TURN_GROUP = 4
DOWN_GROUP = 2


def plan_words():
    rows = [[op + 32 * unit + 256 * (count - 1) for op, unit, count in row] for row in PLAN]
    steps = -(-max(len(row) for row in rows) // 3) * 3
    rows = [row + [0] * (steps - len(row)) for row in rows]
    return steps, [[row[t] + PACK * row[t + 1] + PACK * PACK * row[t + 2] for t in range(0, steps, 3)] for row in rows]


def gelu_pair(pre_act):
    root = pre_act * 0.7071067811865476
    normal_cdf = 0.5 * (1.0 + lax.erf(root))
    normal_pdf = jnp.exp2(root * root * -1.4426950408889634) * 0.3989422804014327
    return pre_act * normal_cdf, normal_cdf + pre_act * normal_pdf


def wait_bytes(ref, sem):
    pltpu.make_async_copy(ref, ref, sem).wait()


def pipeline_kernel(x_ref, g_ref, w1_ref, w2_ref,
                    y_out, dx_out, h_out, g_out, a_out, d_out,
                    wa, wb, flow, act, slope, part, recv, send, home, direct,
                    flow_sem, recv_sem, part_send, flow_send, home_send, home_sem, in_send, relay_sem, relay_send,
                    direct_sem, direct_send, cross_send, stage_sem, w_sem, out_sem):
    stage = lax.axis_index('stage')
    side = lax.axis_index('inner')
    other = 1 - side
    rows, d_model = flow.shape[3:]
    tok, d_ff = act.shape[2:]
    n_blk = d_model // BLK

    def peer(s, i):
        return {'stage': s, 'inner': i}

    load_a = pltpu.make_async_copy(w1_ref, wa, w_sem.at[0])
    load_b = pltpu.make_async_copy(w2_ref, wb, w_sem.at[1])

    def unit_of(k):
        return lax.rem(2 * stage + k + UNITS - 1, UNITS)

    staged = (send.at[BWD, pl.ds(UNITS - 2, 2)], send.at[BWD, pl.ds(UNITS - 4, 2)])
    stagings = [pltpu.make_async_copy(src, dst, stage_sem.at[kind]) for kind, (src, dst) in enumerate(zip((x_ref, g_ref), staged))]
    for kind, target in ((FWD, 0), (BWD, STAGES - 1)):
        stagings[kind].start()

        @pl.when(stage == target)
        def _():
            for k in range(2):
                pltpu.make_async_copy((x_ref, g_ref)[kind].at[k], flow.at[kind, unit_of(k), side], flow_sem.at[kind, unit_of(k), side]).start()

    @pl.when(stage < STAGES - 1)
    def _():
        load_a.start()
    load_b.start()

    @pl.when(stage == STAGES - 1)
    def _():
        load_a.start()

    barrier = pltpu.get_barrier_semaphore()
    for s in range(STAGES):
        for i in range(INNER):
            @pl.when(jnp.logical_or(stage != s, side != i))
            def _():
                pl.semaphore_signal(barrier, inc=1, device_id=peer(s, i), device_id_type=MESH)
    pl.semaphore_wait(barrier, STAGES * INNER - 1)

    def home_of(u):
        return lax.rem((u + 1) // 2, STAGES)

    def slot_of(u):
        return lax.rem(u + 1, 2)

    def hand_in(kind, target, k, lane):
        u = unit_of(k)
        src = staged[kind]
        if lane == 0:
            @pl.when(stage != target)
            def _():
                pltpu.make_async_remote_copy(src.at[k], flow.at[kind, u, side], in_send.at[kind, k, 0], flow_sem.at[kind, u, side],
                                             device_id=peer(target, side), device_id_type=MESH).start()
        else:
            pltpu.make_async_remote_copy(src.at[k], flow.at[kind, u, side], in_send.at[kind, k, 1], flow_sem.at[kind, u, side],
                                         device_id=peer(target, other), device_id_type=MESH).start()

    def relay(k):
        return pltpu.make_async_remote_copy(staged[FWD].at[k], home.at[FWD, k], in_send.at[FWD, k, 1], relay_sem.at[k],
                                            device_id=peer(stage, other), device_id_type=MESH)

    def relayed(k):
        u = unit_of(k)
        return pltpu.make_async_remote_copy(home.at[FWD, k], flow.at[FWD, u, other], relay_send.at[k], flow_sem.at[FWD, u, other],
                                            device_id=peer(0, side), device_id_type=MESH)

    stagings[FWD].wait()
    for k in range(2):
        hand_in(FWD, 0, k, 0)

        @pl.when(jnp.logical_or(stage == 1, jnp.logical_and(stage == 0, k == 1)))
        def _():
            hand_in(FWD, 0, k, 1)

        @pl.when(stage > 1)
        def _():
            relay(k).start()
    steps, plan = plan_words()
    words = [jnp.where(stage == 0, a, jnp.where(stage == 1, b, jnp.where(stage == 2, c, d))) for a, b, c, d in zip(*plan)]

    def keep(ref, out, u, lane):
        pltpu.make_async_copy(ref, out.at[u], out_sem.at[lane]).start()

    def blocks(width, group, fn):
        def body(t, carry):
            fn([pl.ds(pl.multiple_of((t * group + k) * BLK, BLK), BLK) for k in range(group)])
            return carry
        lax.fori_loop(0, width // BLK // group, body, 0)

    def arrived(kind, u):
        for half in range(INNER):
            @pl.when(jnp.logical_not((stage == 1) & (kind == BWD) & (u < DIRECT) & (side == half)))
            def _():
                wait_bytes(flow.at[kind, u, half], flow_sem.at[kind, u, half])

    def both_arrived(kind, u, v):
        arrived(kind, u)

        @pl.when(v != u)
        def _():
            arrived(kind, v)

    def pair(ref, kind, u, v):
        width = ref.shape[-1]
        return jnp.concatenate([ref[kind, u].reshape(tok, width), ref[kind, v].reshape(tok, width)], axis=0)

    def kept(u, v, fn):
        fn(u)

        @pl.when(v != u)
        def _():
            fn(v)

    def up_product(u, v, last):
        both_arrived(FWD, u, v)

        def fn(slices):
            lhs = pair(flow, FWD, u, v)
            for sl in slices:
                z = jnp.dot(lhs, wa[:, sl], preferred_element_type=F32)
                value, grad = gelu_pair(z)
                value = value.astype(BF16)
                if last:
                    act[BWD, u, :, sl] = (slope[u, :, sl] * grad[:tok]).astype(BF16)
                    act[BWD, v, :, sl] = (slope[v, :, sl] * grad[tok:]).astype(BF16)
                else:
                    slope[u, :, sl] = grad[:tok]
                    slope[v, :, sl] = grad[tok:]
                act[FWD, u, :, sl] = value[:tok]
                act[FWD, v, :, sl] = value[tok:]
        blocks(d_ff, UP_GROUP, fn)

        def out(w):
            keep(flow.at[FWD, w], h_out, w, 0)
            keep(act.at[FWD, w], a_out, w, 2)
            if last:
                keep(act.at[BWD, w], d_out, w, 3)
        kept(u, v, out)

    def across(lhs, ref, sl):
        cut = ref.shape[1] * TURN // 8
        total = lax.dot_general(lhs[:, :cut], ref[sl, :cut], NT, preferred_element_type=F32)
        for k in range(cut, ref.shape[1], TILE):
            turned = [ref[pl.ds(sl.start + q, TILE), k:k + TILE].T for q in range(0, BLK, TILE)]
            total += jnp.dot(lhs[:, k:k + TILE], jnp.concatenate(turned, axis=1), preferred_element_type=F32)
        return total

    def back_product(u, v, swapped):
        both_arrived(BWD, u, v)

        def fn(slices):
            lhs = pair(flow, BWD, u, v)
            for sl in slices:
                if swapped:
                    e = jnp.dot(lhs, wa[:, sl], preferred_element_type=F32)
                else:
                    e = across(lhs, wb, sl)
                act[BWD, u, :, sl] = (e[:tok] * slope[u, :, sl]).astype(BF16)
                act[BWD, v, :, sl] = (e[tok:] * slope[v, :, sl]).astype(BF16)
        blocks(d_ff, UP_GROUP if swapped else TURN_GROUP, fn)

        def out(w):
            keep(flow.at[BWD, w], g_out, w, 1)
            keep(act.at[BWD, w], d_out, w, 3)
        kept(u, v, out)

    def part_copy(kind, u, j):
        slot = lax.rem(u, SLOTS)
        return pltpu.make_async_remote_copy(part.at[kind, slot, j, other], recv.at[kind, u, j], part_send.at[kind, slot, j],
                                            recv_sem.at[kind, u, j], device_id=peer(stage, other), device_id_type=MESH)

    def direct_copy(u, j, half):
        slot = lax.rem(u, SLOTS)
        if half is side:
            return pltpu.make_async_remote_copy(part.at[BWD, slot, j, side], direct.at[u, j], direct_send.at[slot, j],
                                                direct_sem.at[0, u, j], device_id=peer(stage - 1, side), device_id_type=MESH)
        return pltpu.make_async_remote_copy(part.at[BWD, slot, j, other], recv.at[FWD, u, j], part_send.at[BWD, slot, j],
                                            direct_sem.at[1, u, j], device_id=peer(stage - 1, other), device_id_type=MESH)

    def take_direct(first, count):
        def body(i, carry):
            u = first + i
            for j in range(n_blk):
                sl = pl.ds(j * BLK, BLK)
                wait_bytes(direct.at[u, j], direct_sem.at[0, u, j])
                wait_bytes(recv.at[FWD, u, j], direct_sem.at[1, u, j])
                flow[BWD, u, side, :, sl] = (direct[u, j] + recv[FWD, u, j]).astype(BF16)
                pltpu.make_async_remote_copy(flow.at[BWD, u, side, :, sl], flow.at[BWD, u, side, :, sl], cross_send.at[0],
                                             flow_sem.at[BWD, u, side], device_id=peer(stage, other), device_id_type=MESH).start()
            return carry
        lax.fori_loop(0, count, body, 0)

    def down_product(kind, u, v, straight):
        def free(w):
            @pl.when(w >= SLOTS)
            def _():
                for j in range(n_blk):
                    part_copy(kind, w - SLOTS, j).wait_send()

            if not straight:
                @pl.when((w >= SLOTS) & (w < SLOTS + DIRECT))
                def _():
                    for j in range(n_blk):
                        direct_copy(w - SLOTS, j, side).wait_send()
        kept(u, v, free)

        def body(t, carry):
            lhs = pair(act, kind, u, v)
            for k in range(DOWN_GROUP):
                j = t * DOWN_GROUP + k
                sl = pl.ds(pl.multiple_of(j * BLK, BLK), BLK)
                if straight:
                    p = jnp.dot(lhs, wb[:, sl], preferred_element_type=F32)
                else:
                    p = across(lhs, wa, sl)
                p = p.reshape(2, INNER, rows, BLK)
                part[kind, lax.rem(u, SLOTS), j] = p[0]
                part[kind, lax.rem(v, SLOTS), j] = p[1]

            def go(w):
                if straight:
                    for k in range(DOWN_GROUP):
                        part_copy(kind, w, t * DOWN_GROUP + k).start()
                    return

                @pl.when(w >= DIRECT)
                def _():
                    for k in range(DOWN_GROUP):
                        part_copy(kind, w, t * DOWN_GROUP + k).start()

                @pl.when(w < DIRECT)
                def _():
                    for k in range(DOWN_GROUP):
                        j = t * DOWN_GROUP + k
                        sl = pl.ds(pl.multiple_of(j * BLK, BLK), BLK)
                        part[BWD, lax.rem(w, SLOTS), j, side] += flow[BWD, w, side, :, sl].astype(F32)
                    for k in range(DOWN_GROUP):
                        for half in (side, other):
                            direct_copy(w, t * DOWN_GROUP + k, half).start()
            kept(u, v, go)
            return carry
        lax.fori_loop(0, n_blk // DOWN_GROUP, body, 0)

    def hand_on(kind, first, count):
        target = stage + 1 if kind == FWD else stage - 1
        inside = stage < STAGES - 1 if kind == FWD else stage > 0
        out = STAGES - 1 if kind == FWD else 0

        def body(i, carry):
            u = first + i
            slot = lax.rem(u, SLOTS)
            for j in range(n_blk):
                sl = pl.ds(j * BLK, BLK)
                wait_bytes(recv.at[kind, u, j], recv_sem.at[kind, u, j])
                total = flow[kind, u, side, :, sl].astype(F32) + (part[kind, slot, j, side] + recv[kind, u, j])
                send[kind, u, :, sl] = total.astype(BF16)

                @pl.when(inside)
                def _():
                    for half in (side, other):
                        pltpu.make_async_remote_copy(send.at[kind, u, :, sl], flow.at[kind, u, side, :, sl], flow_send.at[kind],
                                                     flow_sem.at[kind, u, side], device_id=peer(target, half), device_id_type=MESH).start()

            @pl.when(jnp.logical_and(jnp.logical_not(inside), home_of(u) != out))
            def _():
                pltpu.make_async_remote_copy(send.at[kind, u], home.at[kind, slot_of(u)], home_send.at[kind, u],
                                             home_sem.at[kind, slot_of(u)], device_id=peer(home_of(u), side), device_id_type=MESH).start()
            return carry
        lax.fori_loop(0, count, body, 0)

    def swap_weights():
        n_i = d_model // TILE

        def body(t, carry):
            i = pl.multiple_of(lax.rem(t, n_i) * TILE, TILE)
            j = pl.multiple_of(lax.div(t, n_i) * TILE, TILE)
            up = wa[pl.ds(i, TILE), pl.ds(j, TILE)]
            down = wb[pl.ds(j, TILE), pl.ds(i, TILE)]
            wa[pl.ds(i, TILE), pl.ds(j, TILE)] = down.T
            wb[pl.ds(j, TILE), pl.ds(i, TILE)] = up.T
            return carry
        lax.fori_loop(0, n_i * (d_ff // TILE), body, 0)

    def prepare_last():
        half = UNITS // 2

        def quarter(q, carry):
            for i in range(half):
                arrived(BWD, q * half + i)
                keep(flow.at[BWD, q * half + i], g_out, q * half + i, 1)
            units = pl.ds(q * half, half)

            def fn(slices):
                lhs = flow[BWD, units].reshape(half * tok, d_model)
                for sl in slices:
                    e = lax.dot_general(lhs, wb[sl, :], NT, preferred_element_type=F32)
                    slope[units, :, sl] = e.reshape(half, tok, BLK)
            blocks(d_ff, 1, fn)
            return carry
        lax.fori_loop(0, 2, quarter, 0)
        load_a.wait()
        n_i = d_model // TILE

        def body(t, carry):
            i = pl.multiple_of(lax.rem(t, n_i) * TILE, TILE)
            j = pl.multiple_of(lax.div(t, n_i) * TILE, TILE)
            wb[pl.ds(j, TILE), pl.ds(i, TILE)] = wa[pl.ds(i, TILE), pl.ds(j, TILE)].T
            return carry
        lax.fori_loop(0, n_i * (d_ff // TILE), body, 0)

    def step(t, carry):
        group, place = lax.div(t, 3), lax.rem(t, 3)
        word = words[0]
        for i, w in enumerate(words[1:], 1):
            word = jnp.where(group == i, w, word)
        code = lax.rem(lax.div(word, jnp.where(place == 0, 1, jnp.where(place == 1, PACK, PACK * PACK))), PACK)
        op = lax.rem(code, 32)
        u = lax.rem(lax.div(code, 32), UNITS)
        count = lax.div(code, 256) + 1

        def on(want):
            return pl.when(op == want)

        v = jnp.minimum(u + count - 1, UNITS - 1)

        @on(F1)
        def _():
            up_product(u, v, False)

        @on(M1)
        def _():
            up_product(u, v, True)

        @pl.when(jnp.logical_or(op == F2, op == B2))
        def _():
            down_product(jnp.where(op == F2, FWD, BWD), u, v, True)

        @on(FR)
        def _():
            hand_on(FWD, u, count)

        @on(BR)
        def _():
            hand_on(BWD, u, count)

        @on(B1)
        def _():
            back_product(u, v, True)

        @on(T1)
        def _():
            back_product(u, v, False)

        @on(T2)
        def _():
            down_product(BWD, u, v, False)

        @on(SW)
        def _():
            swap_weights()

        @on(PR)
        def _():
            prepare_last()

        @on(YL)
        def _():
            load_b.start()
            load_b.wait()

        @on(WA)
        def _():
            load_a.wait()

        @on(WB)
        def _():
            load_b.wait()

        @on(XS)
        def _():
            stagings[BWD].wait()
            for k in range(2):
                for lane in range(2):
                    hand_in(BWD, STAGES - 1, k, lane)

            @pl.when(stage == 0)
            def _():
                hand_in(FWD, 0, 0, 1)

        @on(XR)
        def _():
            for k in range(2):
                wait_bytes(home.at[FWD, k], relay_sem.at[k])
                relayed(k).start()

        @on(XW)
        def _():
            for kind, target in ((FWD, 0), (BWD, STAGES - 1)):
                for k in range(2):
                    @pl.when(stage != target)
                    def _():
                        wait_bytes(staged[kind].at[k], in_send.at[kind, k, 0])
                    wait_bytes(staged[kind].at[k], in_send.at[kind, k, 1])

            @pl.when(stage > 1)
            def _():
                for k in range(2):
                    relayed(k).wait_send()

        @on(HB)
        def _():
            take_direct(u, count)
        return carry
    lax.fori_loop(0, steps, step, 0)

    for kind, here, out in ((FWD, STAGES - 1, y_out), (BWD, 0, dx_out)):
        for k in range(2):
            @pl.when(stage == here)
            def _():
                pltpu.make_async_copy(send.at[kind, unit_of(k)], out.at[k], out_sem.at[4 + kind]).start()

            @pl.when(stage != here)
            def _():
                wait_bytes(home.at[kind, k], home_sem.at[kind, k])
                pltpu.make_async_copy(home.at[kind, k], out.at[k], out_sem.at[4 + kind]).start()

    for kind in (FWD, BWD):
        for u in range(UNITS - SLOTS, UNITS):
            for j in range(n_blk):
                part_copy(kind, u, j).wait_send()
    for kind, last in ((FWD, STAGES - 1), (BWD, 0)):
        @pl.when((stage != last) & jnp.logical_not((stage == 2) & (kind == BWD)))
        def _():
            wait_bytes(flow.at[kind], flow_send.at[kind])

        @pl.when(stage == last)
        def _():
            for u in range(UNITS):
                if (u + 1) // 2 % STAGES != last:
                    wait_bytes(send.at[kind, u], home_send.at[kind, u])
    @pl.when(stage == 2)
    def _():
        wait_bytes(flow.at[BWD, pl.ds(0, UNITS - DIRECT)], flow_send.at[BWD])

    @pl.when(stage == 1)
    def _():
        wait_bytes(flow.at[BWD, pl.ds(0, DIRECT), 0], cross_send.at[0])
    for lane, (ref, out) in enumerate(((flow.at[FWD], h_out), (flow.at[BWD], g_out), (act.at[FWD], a_out), (act.at[BWD], d_out),
                                       (home.at[FWD], y_out), (home.at[BWD], dx_out))):
        pltpu.make_async_copy(ref, out, out_sem.at[lane]).wait()


def run_pipeline(x_loc, g_loc, w_one, w_two):
    rows, d_model = x_loc.shape[1:]
    d_ff = w_one.shape[1]
    n_blk = d_model // BLK
    tok = INNER * rows
    hbm = pl.BlockSpec(memory_space=pl.ANY)
    out = lambda *shape: jax.ShapeDtypeStruct(shape, BF16)
    dma = lambda *shape: pltpu.SemaphoreType.DMA(shape)
    return pl.pallas_call(
        pipeline_kernel,
        name='pipeline',
        out_shape=(out(*x_loc.shape), out(*x_loc.shape), out(UNITS, INNER, rows, d_model), out(UNITS, INNER, rows, d_model),
                   out(UNITS, tok, d_ff), out(UNITS, tok, d_ff)),
        in_specs=[hbm] * 4,
        out_specs=(hbm,) * 6,
        scratch_shapes=[
            pltpu.VMEM((d_model, d_ff), BF16),
            pltpu.VMEM((d_ff, d_model), BF16),
            pltpu.VMEM((2, UNITS, INNER, rows, d_model), BF16),
            pltpu.VMEM((2, UNITS, tok, d_ff), BF16),
            pltpu.VMEM((UNITS, tok, d_ff), F32),
            pltpu.VMEM((2, SLOTS, n_blk, INNER, rows, BLK), F32),
            pltpu.VMEM((2, UNITS, n_blk, rows, BLK), F32),
            pltpu.VMEM((2, UNITS, rows, d_model), BF16),
            pltpu.VMEM((2, 2, rows, d_model), BF16),
            pltpu.VMEM((DIRECT, n_blk, rows, BLK), F32),
            dma(2, UNITS, INNER), dma(2, UNITS, n_blk), dma(2, SLOTS, n_blk), dma(2), dma(2, UNITS), dma(2, 2), dma(2, 2, 2), dma(2), dma(2),
            dma(2, DIRECT, n_blk), dma(SLOTS, n_blk), dma(1), dma(2), dma(2), dma(6),
        ],
        compiler_params=pltpu.CompilerParams(collective_id=0, has_side_effects=True, vmem_limit_bytes=67043328),
    )(x_loc, g_loc, w_one, w_two)


GRAD_ROWS, GRAD_COLS, GRAD_PART, GRAD_SLOTS = 1024, 2048, 256, 4


def weight_grad_kernel(h_ref, d_ref, a_ref, g_ref, y_ref, x_ref, up_ref, down_ref, y_out, x_out,
                       h, d, a, g, home, left, right, stage, in_sem, home_sem, out_sem):
    d_model, d_ff = h.shape[1], d.shape[1]
    n_down, n_up, n_col = d_ff // GRAD_ROWS, d_model // GRAD_ROWS, d_ff // GRAD_COLS

    pieces = [a.at[:, pl.ds(t * GRAD_ROWS, GRAD_ROWS)] for t in range(n_down)]
    loads = [(g_ref, g)] + [(a_ref.at[:, pl.ds(t * GRAD_ROWS, GRAD_ROWS)], piece) for t, piece in enumerate(pieces)] + [(h_ref, h), (d_ref, d)]
    loads = [pltpu.make_async_copy(src, dst, in_sem.at[t]) for t, (src, dst) in enumerate(loads)]
    homes = [pltpu.make_async_copy(src, home.at[t], home_sem.at[t]) for t, src in enumerate((y_ref, x_ref))]
    backs = [pltpu.make_async_copy(home.at[t], dst, home_sem.at[t]) for t, dst in enumerate((y_out, x_out))]
    for copy in loads + homes:
        copy.start()

    rows_of = lambda t: pl.ds(t * GRAD_ROWS, GRAD_ROWS)
    blocks = [(a, t, g, 0, down_ref) for t in range(n_down)] + [(h, t, d, c, up_ref) for t in range(n_up) for c in range(n_col)]
    turned = (left, right)
    loads[0].wait()
    loads[1].wait()
    arrived = 2
    turn = -1
    for t, (src, row, other, col, out) in enumerate(blocks):
        slot = t % GRAD_SLOTS
        cols = pl.ds(col * GRAD_COLS, GRAD_COLS)
        after = blocks[t + 1] if t + 1 < len(blocks) else None
        need = (1 + n_down if after is None or after[0] is h else t + 2) + (1 if src is h or (after is not None and after[0] is h) else 0)
        need = min(need, len(loads) - 1) + (1 if src is h else 0)
        while arrived < min(need + 1, len(loads)):
            loads[arrived].wait()
            arrived += 1
        if t >= GRAD_SLOTS:
            pltpu.make_async_copy(stage.at[slot], stage.at[slot], out_sem.at[slot]).wait()
        size = GRAD_PART if after is None or t == 0 else GRAD_ROWS
        for p in range(0, GRAD_ROWS, size):
            if t == 0:
                stage[slot, p:p + size] = lax.dot_general(src[:, p:p + size], other[:, cols], (((0,), (0,)), ((), ())), preferred_element_type=F32)
            else:
                stage[slot, p:p + size] = jnp.dot(turned[turn % 2][p:p + size], other[:, cols], preferred_element_type=F32)
            if p + size == GRAD_ROWS and after is not None and (after[0] is not src or after[1] != row):
                turn += 1
                turned[turn % 2][...] = after[0][:, rows_of(after[1])].T
            for q in range(p, p + size, GRAD_PART):
                pltpu.make_async_copy(stage.at[slot, pl.ds(q, GRAD_PART)], out.at[pl.ds(row * GRAD_ROWS + q, GRAD_PART), cols], out_sem.at[slot]).start()
        if t == 1:
            for copy, back in zip(homes, backs):
                copy.wait()
                back.start()
    for slot in range(GRAD_SLOTS):
        pltpu.make_async_copy(stage.at[slot], stage.at[slot], out_sem.at[slot]).wait()
    for copy in backs:
        copy.wait()


def weight_grads(h, d, a, g, y, dx):
    tokens, d_model = h.shape
    d_ff = d.shape[1]
    n_in = 3 + d_ff // GRAD_ROWS
    hbm = pl.BlockSpec(memory_space=pl.ANY)
    dma = lambda *shape: pltpu.SemaphoreType.DMA(shape)
    like = lambda v: pltpu.VMEM(v.shape, v.dtype)
    return pl.pallas_call(
        weight_grad_kernel,
        name='weight_grads',
        out_shape=(jax.ShapeDtypeStruct((d_model, d_ff), F32), jax.ShapeDtypeStruct((d_ff, d_model), F32),
                   jax.ShapeDtypeStruct(y.shape, BF16), jax.ShapeDtypeStruct(y.shape, BF16)),
        in_specs=[hbm] * 6,
        out_specs=(hbm,) * 4,
        scratch_shapes=[like(h), like(d), like(a), like(g), pltpu.VMEM((2,) + y.shape, BF16), pltpu.VMEM((GRAD_ROWS, tokens), BF16), pltpu.VMEM((GRAD_ROWS, tokens), BF16),
                        pltpu.VMEM((GRAD_SLOTS, GRAD_ROWS, GRAD_COLS), F32),
                        dma(n_in), dma(2), dma(GRAD_SLOTS)],
        compiler_params=pltpu.CompilerParams(vmem_limit_bytes=60 * 1024 * 1024),
    )(h, d, a, g, y, dx)


def solution(mesh):
    tok_spec = P(('data', 'stage', 'inner'))
    up_spec = P(None, ('data', 'stage'), None, 'inner')
    down_spec = P(None, ('data', 'stage'), 'inner', None)

    def device_step(x_loc, g_loc, w_up, w_down):
        y, dx, h, g, a, d = run_pipeline(x_loc, g_loc, w_up[0, 0], w_down[0, 0])
        flat = lambda v: v.reshape(-1, v.shape[-1])
        dw_up, dw_down, y, dx = weight_grads(flat(h), flat(d), flat(a), flat(g), y, dx)
        return y, dx, dw_up[None, None], dw_down[None, None]

    return jax.shard_map(device_step, mesh=mesh, in_specs=(tok_spec, tok_spec, up_spec, down_spec), out_specs=(tok_spec, tok_spec, up_spec, down_spec), check_vma=False)
```

```python
import functools

import jax
import jax.numpy as jnp
from jax import lax
from jax.experimental import pallas as pl
from jax.experimental.pallas import tpu as pltpu
from jax.sharding import PartitionSpec as P

F32 = jnp.float32
BF16 = jnp.bfloat16
MESH = pl.DeviceIdType.MESH

STAGES = 4
INNER = 2
UNITS = 8
SLOTS = 3
DIRECT = 3
BLK = 512
TILE = 256
FWD, BWD = 0, 1
HOMES = (0, 1, 2, 2, 3, 3, 1, 0)
NT = (((1,), (1,)), ((), ()))

F1, F2, FR, B1, B2, BR, T1, T2, SW, PR, YL, WA, WB, XS, M1, HB, XW, XR = range(1, 19)
PLAN = (
    ((WA, 0, 1), (F1, 0, 2), (WB, 0, 1), (XS, 0, 1), (F2, 0, 2), (F1, 2, 2), (FR, 0, 2), (F2, 2, 2),
     (FR, 2, 1), (F1, 4, 2), (FR, 3, 1), (F2, 4, 2), (FR, 4, 2), (F1, 6, 2), (F2, 6, 1), (F2, 7, 1),
     (FR, 6, 2), (XW, 0, 1), (SW, 0, 1), (B1, 0, 2), (B2, 0, 1), (B2, 1, 1), (B1, 2, 1), (B2, 2, 1),
     (B1, 3, 1), (BR, 0, 2), (B2, 3, 1), (BR, 2, 1), (B1, 4, 2), (B2, 4, 2), (BR, 3, 1), (B1, 6, 2),
     (B2, 6, 1), (BR, 4, 1), (B2, 7, 1), (BR, 5, 3)),
    ((WA, 0, 1), (WB, 0, 1), (XS, 0, 1), (F1, 0, 2), (F2, 0, 1), (F2, 1, 1), (FR, 0, 2), (F1, 2, 2),
     (F2, 2, 1), (F2, 3, 1), (FR, 2, 1), (F1, 4, 2), (FR, 3, 1), (F2, 4, 1), (F2, 5, 1), (FR, 4, 2),
     (F1, 6, 2), (F2, 6, 2), (FR, 6, 2), (XW, 0, 1), (SW, 0, 1), (HB, 0, 2), (B1, 0, 2), (B2, 0, 1),
     (HB, 2, 1), (B2, 1, 1), (BR, 0, 1), (B1, 2, 2), (BR, 1, 1), (B2, 2, 2), (BR, 2, 2), (B1, 4, 1),
     (B1, 5, 1), (B2, 4, 2), (B1, 6, 1), (B2, 6, 1), (BR, 4, 1), (B1, 7, 1), (BR, 5, 1), (B2, 7, 1),
     (BR, 6, 2)),
    ((XR, 0, 1), (WA, 0, 1), (WB, 0, 1), (XS, 0, 1), (XW, 0, 1), (F1, 0, 1), (F2, 0, 1), (F1, 1, 1),
     (FR, 0, 1), (F2, 1, 1), (FR, 1, 1), (F1, 2, 1), (F2, 2, 1), (F1, 3, 1), (F2, 3, 1), (FR, 2, 1),
     (F1, 4, 1), (F1, 5, 1), (FR, 3, 1), (F2, 4, 2), (T1, 0, 2), (F1, 6, 2), (T2, 0, 2), (FR, 4, 1),
     (F2, 6, 2), (FR, 5, 1), (T1, 2, 2), (FR, 6, 2), (T2, 2, 2), (BR, 3, 1), (T1, 4, 2), (T2, 4, 2),
     (T1, 6, 2), (BR, 4, 1), (T2, 6, 2), (BR, 5, 3)),
    ((WB, 0, 1), (XS, 0, 1), (XR, 0, 1), (PR, 0, 1), (XW, 0, 1), (M1, 0, 1), (B2, 0, 1), (BR, 0, 1),
     (M1, 1, 1), (B2, 1, 1), (BR, 1, 1), (M1, 2, 2), (B2, 2, 1), (B2, 3, 1), (BR, 2, 2), (M1, 4, 1),
     (B2, 4, 1), (M1, 5, 1), (B2, 5, 1), (BR, 4, 1), (M1, 6, 2), (BR, 5, 1), (B2, 6, 2), (BR, 6, 2),
     (YL, 0, 1), (F2, 0, 2), (FR, 0, 2), (F2, 2, 1), (F2, 3, 2), (FR, 2, 1), (F2, 5, 1), (FR, 3, 2),
     (F2, 6, 1), (FR, 5, 1), (F2, 7, 1), (FR, 6, 2)),
)


PACK = 1024
UP_GROUP = 8
TURN = 5
TURN_GROUP = 4
DOWN_GROUP = 2


def plan_words():
    rows = [[op + 32 * unit + 256 * (count - 1) for op, unit, count in row] for row in PLAN]
    steps = -(-max(len(row) for row in rows) // 3) * 3
    rows = [row + [0] * (steps - len(row)) for row in rows]
    return steps, [[row[t] + PACK * row[t + 1] + PACK * PACK * row[t + 2] for t in range(0, steps, 3)] for row in rows]


def gelu_pair(pre_act):
    root = pre_act * 0.7071067811865476
    normal_cdf = 0.5 * (1.0 + lax.erf(root))
    normal_pdf = jnp.exp2(root * root * -1.4426950408889634) * 0.3989422804014327
    return pre_act * normal_cdf, normal_cdf + pre_act * normal_pdf


def wait_bytes(ref, sem):
    pltpu.make_async_copy(ref, ref, sem).wait()


def pipeline_kernel(x_ref, g_ref, w1_ref, w2_ref,
                    y_out, dx_out, h_out, g_out, a_out, d_out,
                    wa, wb, flow, act, slope, part, recv, send, home, direct,
                    flow_sem, recv_sem, part_send, flow_send, home_send, home_sem, in_send, relay_sem, relay_send,
                    direct_sem, direct_send, cross_send, stage_sem, w_sem, out_sem):
    stage = lax.axis_index('stage')
    side = lax.axis_index('inner')
    other = 1 - side
    rows, d_model = flow.shape[3:]
    tok, d_ff = act.shape[2:]
    n_blk = d_model // BLK

    def peer(s, i):
        return {'stage': s, 'inner': i}

    load_a = pltpu.make_async_copy(w1_ref, wa, w_sem.at[0])
    load_b = pltpu.make_async_copy(w2_ref, wb, w_sem.at[1])

    def unit_of(k):
        return jnp.where(stage < 2, stage + (7 - 2 * stage) * k, 2 * stage - 2 + k)

    staged = (send.at[BWD, pl.ds(UNITS - 2, 2)], send.at[BWD, pl.ds(UNITS - 4, 2)])
    stagings = [pltpu.make_async_copy(src, dst, stage_sem.at[kind]) for kind, (src, dst) in enumerate(zip((x_ref, g_ref), staged))]
    for kind, target in ((FWD, 0), (BWD, STAGES - 1)):
        stagings[kind].start()

        @pl.when(stage == target)
        def _():
            for k in range(2):
                pltpu.make_async_copy((x_ref, g_ref)[kind].at[k], flow.at[kind, unit_of(k), side], flow_sem.at[kind, unit_of(k), side]).start()

    @pl.when(stage < STAGES - 1)
    def _():
        load_a.start()
    load_b.start()

    @pl.when(stage == STAGES - 1)
    def _():
        load_a.start()

    barrier = pltpu.get_barrier_semaphore()
    for s in range(STAGES):
        for i in range(INNER):
            @pl.when(jnp.logical_or(stage != s, side != i))
            def _():
                pl.semaphore_signal(barrier, inc=1, device_id=peer(s, i), device_id_type=MESH)
    pl.semaphore_wait(barrier, STAGES * INNER - 1)

    def home_of(u):
        return jnp.where(u < 2, u, jnp.where(u > 5, 7 - u, (u + 2) // 2))

    def slot_of(u):
        return jnp.where(u < 2, 0, jnp.where(u > 5, 1, lax.rem(u, 2)))

    def hand_in(kind, target, k, lane):
        u = unit_of(k)
        src = staged[kind]
        if lane == 0:
            @pl.when(stage != target)
            def _():
                pltpu.make_async_remote_copy(src.at[k], flow.at[kind, u, side], in_send.at[kind, k, 0], flow_sem.at[kind, u, side],
                                             device_id=peer(target, side), device_id_type=MESH).start()
        else:
            pltpu.make_async_remote_copy(src.at[k], flow.at[kind, u, side], in_send.at[kind, k, 1], flow_sem.at[kind, u, side],
                                         device_id=peer(target, other), device_id_type=MESH).start()

    def relay(k):
        return pltpu.make_async_remote_copy(staged[FWD].at[k], home.at[FWD, k], in_send.at[FWD, k, 1], relay_sem.at[k],
                                            device_id=peer(stage, other), device_id_type=MESH)

    def relayed(k):
        u = unit_of(k)
        return pltpu.make_async_remote_copy(home.at[FWD, k], flow.at[FWD, u, other], relay_send.at[k], flow_sem.at[FWD, u, other],
                                            device_id=peer(0, side), device_id_type=MESH)

    stagings[FWD].wait()
    for k in range(2):
        hand_in(FWD, 0, k, 0)

        if k == 0:
            @pl.when(stage < 2)
            def _():
                hand_in(FWD, 0, k, 1)

        @pl.when(stage == 2)
        def _():
            relay(k).start()
    steps, plan = plan_words()
    words = [jnp.where(stage == 0, a, jnp.where(stage == 1, b, jnp.where(stage == 2, c, d))) for a, b, c, d in zip(*plan)]

    def keep(ref, out, u, lane):
        pltpu.make_async_copy(ref, out.at[u], out_sem.at[lane]).start()

    def blocks(width, group, fn):
        def body(t, carry):
            fn([pl.ds(pl.multiple_of((t * group + k) * BLK, BLK), BLK) for k in range(group)])
            return carry
        lax.fori_loop(0, width // BLK // group, body, 0)

    def arrived(kind, u):
        for half in range(INNER):
            @pl.when(jnp.logical_not((stage == 1) & (kind == BWD) & (u < DIRECT) & (side == half)))
            def _():
                wait_bytes(flow.at[kind, u, half], flow_sem.at[kind, u, half])

    def both_arrived(kind, u, v):
        arrived(kind, u)

        @pl.when(v != u)
        def _():
            arrived(kind, v)

    def pair(ref, kind, u, v):
        width = ref.shape[-1]
        return jnp.concatenate([ref[kind, u].reshape(tok, width), ref[kind, v].reshape(tok, width)], axis=0)

    def kept(u, v, fn):
        fn(u)

        @pl.when(v != u)
        def _():
            fn(v)

    def up_product(u, v, last):
        both_arrived(FWD, u, v)

        def fn(slices):
            lhs = pair(flow, FWD, u, v)
            for sl in slices:
                z = jnp.dot(lhs, wa[:, sl], preferred_element_type=F32)
                value, grad = gelu_pair(z)
                value = value.astype(BF16)
                if last:
                    act[BWD, u, :, sl] = (slope[u, :, sl] * grad[:tok]).astype(BF16)
                    act[BWD, v, :, sl] = (slope[v, :, sl] * grad[tok:]).astype(BF16)
                else:
                    slope[u, :, sl] = grad[:tok]
                    slope[v, :, sl] = grad[tok:]
                act[FWD, u, :, sl] = value[:tok]
                act[FWD, v, :, sl] = value[tok:]
        blocks(d_ff, UP_GROUP, fn)

        def out(w):
            keep(flow.at[FWD, w], h_out, w, 0)
            keep(act.at[FWD, w], a_out, w, 2)
            if last:
                keep(act.at[BWD, w], d_out, w, 3)
        kept(u, v, out)

    def across(lhs, ref, sl):
        cut = ref.shape[1] * TURN // 8
        total = lax.dot_general(lhs[:, :cut], ref[sl, :cut], NT, preferred_element_type=F32)
        for k in range(cut, ref.shape[1], TILE):
            turned = [ref[pl.ds(sl.start + q, TILE), k:k + TILE].T for q in range(0, BLK, TILE)]
            total += jnp.dot(lhs[:, k:k + TILE], jnp.concatenate(turned, axis=1), preferred_element_type=F32)
        return total

    def back_product(u, v, swapped):
        both_arrived(BWD, u, v)

        def fn(slices):
            lhs = pair(flow, BWD, u, v)
            for sl in slices:
                if swapped:
                    e = jnp.dot(lhs, wa[:, sl], preferred_element_type=F32)
                else:
                    e = across(lhs, wb, sl)
                act[BWD, u, :, sl] = (e[:tok] * slope[u, :, sl]).astype(BF16)
                act[BWD, v, :, sl] = (e[tok:] * slope[v, :, sl]).astype(BF16)
        blocks(d_ff, UP_GROUP if swapped else TURN_GROUP, fn)

        def out(w):
            keep(flow.at[BWD, w], g_out, w, 1)
            keep(act.at[BWD, w], d_out, w, 3)
        kept(u, v, out)

    def part_copy(kind, u, j):
        slot = lax.rem(u, SLOTS)
        return pltpu.make_async_remote_copy(part.at[kind, slot, j, other], recv.at[kind, u, j], part_send.at[kind, slot, j],
                                            recv_sem.at[kind, u, j], device_id=peer(stage, other), device_id_type=MESH)

    def direct_copy(u, j, half):
        slot = lax.rem(u, SLOTS)
        if half is side:
            return pltpu.make_async_remote_copy(part.at[BWD, slot, j, side], direct.at[u, j], direct_send.at[slot, j],
                                                direct_sem.at[0, u, j], device_id=peer(stage - 1, side), device_id_type=MESH)
        return pltpu.make_async_remote_copy(part.at[BWD, slot, j, other], recv.at[FWD, u, j], part_send.at[BWD, slot, j],
                                            direct_sem.at[1, u, j], device_id=peer(stage - 1, other), device_id_type=MESH)

    def take_direct(first, count):
        def body(i, carry):
            u = first + i
            for j in range(n_blk):
                sl = pl.ds(j * BLK, BLK)
                wait_bytes(direct.at[u, j], direct_sem.at[0, u, j])
                wait_bytes(recv.at[FWD, u, j], direct_sem.at[1, u, j])
                flow[BWD, u, side, :, sl] = (direct[u, j] + recv[FWD, u, j]).astype(BF16)
                pltpu.make_async_remote_copy(flow.at[BWD, u, side, :, sl], flow.at[BWD, u, side, :, sl], cross_send.at[0],
                                             flow_sem.at[BWD, u, side], device_id=peer(stage, other), device_id_type=MESH).start()
            return carry
        lax.fori_loop(0, count, body, 0)

    def down_product(kind, u, v, straight):
        def free(w):
            @pl.when(w >= SLOTS)
            def _():
                for j in range(n_blk):
                    part_copy(kind, w - SLOTS, j).wait_send()

            if not straight:
                @pl.when((w >= SLOTS) & (w < SLOTS + DIRECT))
                def _():
                    for j in range(n_blk):
                        direct_copy(w - SLOTS, j, side).wait_send()
        kept(u, v, free)

        def body(t, carry):
            lhs = pair(act, kind, u, v)
            for k in range(DOWN_GROUP):
                j = t * DOWN_GROUP + k
                sl = pl.ds(pl.multiple_of(j * BLK, BLK), BLK)
                if straight:
                    p = jnp.dot(lhs, wb[:, sl], preferred_element_type=F32)
                else:
                    p = across(lhs, wa, sl)
                p = p.reshape(2, INNER, rows, BLK)
                part[kind, lax.rem(u, SLOTS), j] = p[0]
                part[kind, lax.rem(v, SLOTS), j] = p[1]

            def go(w):
                if straight:
                    for k in range(DOWN_GROUP):
                        part_copy(kind, w, t * DOWN_GROUP + k).start()
                    return

                @pl.when(w >= DIRECT)
                def _():
                    for k in range(DOWN_GROUP):
                        part_copy(kind, w, t * DOWN_GROUP + k).start()

                @pl.when(w < DIRECT)
                def _():
                    for k in range(DOWN_GROUP):
                        j = t * DOWN_GROUP + k
                        sl = pl.ds(pl.multiple_of(j * BLK, BLK), BLK)
                        part[BWD, lax.rem(w, SLOTS), j, side] += flow[BWD, w, side, :, sl].astype(F32)
                    for k in range(DOWN_GROUP):
                        for half in (side, other):
                            direct_copy(w, t * DOWN_GROUP + k, half).start()
            kept(u, v, go)
            return carry
        lax.fori_loop(0, n_blk // DOWN_GROUP, body, 0)

    def hand_on(kind, first, count):
        target = stage + 1 if kind == FWD else stage - 1
        inside = stage < STAGES - 1 if kind == FWD else stage > 0
        out = STAGES - 1 if kind == FWD else 0

        def body(i, carry):
            u = first + i
            slot = lax.rem(u, SLOTS)
            for j in range(n_blk):
                sl = pl.ds(j * BLK, BLK)
                wait_bytes(recv.at[kind, u, j], recv_sem.at[kind, u, j])
                total = flow[kind, u, side, :, sl].astype(F32) + (part[kind, slot, j, side] + recv[kind, u, j])
                send[kind, u, :, sl] = total.astype(BF16)

                @pl.when(inside)
                def _():
                    for half in (side, other):
                        pltpu.make_async_remote_copy(send.at[kind, u, :, sl], flow.at[kind, u, side, :, sl], flow_send.at[kind],
                                                     flow_sem.at[kind, u, side], device_id=peer(target, half), device_id_type=MESH).start()

            @pl.when(jnp.logical_and(jnp.logical_not(inside), home_of(u) != out))
            def _():
                pltpu.make_async_remote_copy(send.at[kind, u], home.at[kind, slot_of(u)], home_send.at[kind, u],
                                             home_sem.at[kind, slot_of(u)], device_id=peer(home_of(u), side), device_id_type=MESH).start()
            return carry
        lax.fori_loop(0, count, body, 0)

    def swap_weights():
        n_i = d_model // TILE

        def body(t, carry):
            i = pl.multiple_of(lax.rem(t, n_i) * TILE, TILE)
            j = pl.multiple_of(lax.div(t, n_i) * TILE, TILE)
            up = wa[pl.ds(i, TILE), pl.ds(j, TILE)]
            down = wb[pl.ds(j, TILE), pl.ds(i, TILE)]
            wa[pl.ds(i, TILE), pl.ds(j, TILE)] = down.T
            wb[pl.ds(j, TILE), pl.ds(i, TILE)] = up.T
            return carry
        lax.fori_loop(0, n_i * (d_ff // TILE), body, 0)

    def prepare_last():
        half = UNITS // 2

        def quarter(q, carry):
            for i in range(half):
                arrived(BWD, q * half + i)
                keep(flow.at[BWD, q * half + i], g_out, q * half + i, 1)
            units = pl.ds(q * half, half)

            def fn(slices):
                lhs = flow[BWD, units].reshape(half * tok, d_model)
                for sl in slices:
                    e = lax.dot_general(lhs, wb[sl, :], NT, preferred_element_type=F32)
                    slope[units, :, sl] = e.reshape(half, tok, BLK)
            blocks(d_ff, 1, fn)
            return carry
        lax.fori_loop(0, 2, quarter, 0)
        load_a.wait()
        n_i = d_model // TILE

        def body(t, carry):
            i = pl.multiple_of(lax.rem(t, n_i) * TILE, TILE)
            j = pl.multiple_of(lax.div(t, n_i) * TILE, TILE)
            wb[pl.ds(j, TILE), pl.ds(i, TILE)] = wa[pl.ds(i, TILE), pl.ds(j, TILE)].T
            return carry
        lax.fori_loop(0, n_i * (d_ff // TILE), body, 0)

    def step(t, carry):
        group, place = lax.div(t, 3), lax.rem(t, 3)
        word = words[0]
        for i, w in enumerate(words[1:], 1):
            word = jnp.where(group == i, w, word)
        code = lax.rem(lax.div(word, jnp.where(place == 0, 1, jnp.where(place == 1, PACK, PACK * PACK))), PACK)
        op = lax.rem(code, 32)
        u = lax.rem(lax.div(code, 32), UNITS)
        count = lax.div(code, 256) + 1

        def on(want):
            return pl.when(op == want)

        v = jnp.minimum(u + count - 1, UNITS - 1)

        @on(F1)
        def _():
            up_product(u, v, False)

        @on(M1)
        def _():
            up_product(u, v, True)

        @pl.when(jnp.logical_or(op == F2, op == B2))
        def _():
            down_product(jnp.where(op == F2, FWD, BWD), u, v, True)

        @on(FR)
        def _():
            hand_on(FWD, u, count)

        @on(BR)
        def _():
            hand_on(BWD, u, count)

        @on(B1)
        def _():
            back_product(u, v, True)

        @on(T1)
        def _():
            back_product(u, v, False)

        @on(T2)
        def _():
            down_product(BWD, u, v, False)

        @on(SW)
        def _():
            swap_weights()

        @on(PR)
        def _():
            prepare_last()

        @on(YL)
        def _():
            load_b.start()
            load_b.wait()

        @on(WA)
        def _():
            load_a.wait()

        @on(WB)
        def _():
            load_b.wait()

        @on(XS)
        def _():
            stagings[BWD].wait()
            for k in range(2):
                for lane in range(2):
                    hand_in(BWD, STAGES - 1, k, lane)

            @pl.when(stage < 2)
            def _():
                hand_in(FWD, 0, 1, 1)

            @pl.when(stage == STAGES - 1)
            def _():
                for k in range(2):
                    relay(k).start()

        @on(XR)
        def _():
            for k in range(2):
                wait_bytes(home.at[FWD, k], relay_sem.at[k])
                relayed(k).start()

        @on(XW)
        def _():
            for kind, target in ((FWD, 0), (BWD, STAGES - 1)):
                for k in range(2):
                    @pl.when(stage != target)
                    def _():
                        wait_bytes(staged[kind].at[k], in_send.at[kind, k, 0])
                    wait_bytes(staged[kind].at[k], in_send.at[kind, k, 1])

            @pl.when(stage > 1)
            def _():
                for k in range(2):
                    relayed(k).wait_send()

        @on(HB)
        def _():
            take_direct(u, count)
        return carry
    lax.fori_loop(0, steps, step, 0)

    for kind, here, out in ((FWD, STAGES - 1, y_out), (BWD, 0, dx_out)):
        for k in range(2):
            @pl.when(stage == here)
            def _():
                pltpu.make_async_copy(send.at[kind, unit_of(k)], out.at[k], out_sem.at[4 + kind]).start()

            @pl.when(stage != here)
            def _():
                wait_bytes(home.at[kind, k], home_sem.at[kind, k])
                pltpu.make_async_copy(home.at[kind, k], out.at[k], out_sem.at[4 + kind]).start()

    for kind in (FWD, BWD):
        for u in range(UNITS - SLOTS, UNITS):
            for j in range(n_blk):
                part_copy(kind, u, j).wait_send()
    for kind, last in ((FWD, STAGES - 1), (BWD, 0)):
        @pl.when((stage != last) & jnp.logical_not((stage == 2) & (kind == BWD)))
        def _():
            wait_bytes(flow.at[kind], flow_send.at[kind])

        @pl.when(stage == last)
        def _():
            for u in range(UNITS):
                if HOMES[u] != last:
                    wait_bytes(send.at[kind, u], home_send.at[kind, u])
    @pl.when(stage == 2)
    def _():
        wait_bytes(flow.at[BWD, pl.ds(0, UNITS - DIRECT)], flow_send.at[BWD])

    @pl.when(stage == 1)
    def _():
        wait_bytes(flow.at[BWD, pl.ds(0, DIRECT), 0], cross_send.at[0])
    for lane, (ref, out) in enumerate(((flow.at[FWD], h_out), (flow.at[BWD], g_out), (act.at[FWD], a_out), (act.at[BWD], d_out),
                                       (home.at[FWD], y_out), (home.at[BWD], dx_out))):
        pltpu.make_async_copy(ref, out, out_sem.at[lane]).wait()


def run_pipeline(x_loc, g_loc, w_one, w_two):
    rows, d_model = x_loc.shape[1:]
    d_ff = w_one.shape[1]
    n_blk = d_model // BLK
    tok = INNER * rows
    hbm = pl.BlockSpec(memory_space=pl.ANY)
    out = lambda *shape: jax.ShapeDtypeStruct(shape, BF16)
    dma = lambda *shape: pltpu.SemaphoreType.DMA(shape)
    return pl.pallas_call(
        pipeline_kernel,
        name='pipeline',
        out_shape=(out(*x_loc.shape), out(*x_loc.shape), out(UNITS, INNER, rows, d_model), out(UNITS, INNER, rows, d_model),
                   out(UNITS, tok, d_ff), out(UNITS, tok, d_ff)),
        in_specs=[hbm] * 4,
        out_specs=(hbm,) * 6,
        scratch_shapes=[
            pltpu.VMEM((d_model, d_ff), BF16),
            pltpu.VMEM((d_ff, d_model), BF16),
            pltpu.VMEM((2, UNITS, INNER, rows, d_model), BF16),
            pltpu.VMEM((2, UNITS, tok, d_ff), BF16),
            pltpu.VMEM((UNITS, tok, d_ff), F32),
            pltpu.VMEM((2, SLOTS, n_blk, INNER, rows, BLK), F32),
            pltpu.VMEM((2, UNITS, n_blk, rows, BLK), F32),
            pltpu.VMEM((2, UNITS, rows, d_model), BF16),
            pltpu.VMEM((2, 2, rows, d_model), BF16),
            pltpu.VMEM((DIRECT, n_blk, rows, BLK), F32),
            dma(2, UNITS, INNER), dma(2, UNITS, n_blk), dma(2, SLOTS, n_blk), dma(2), dma(2, UNITS), dma(2, 2), dma(2, 2, 2), dma(2), dma(2),
            dma(2, DIRECT, n_blk), dma(SLOTS, n_blk), dma(1), dma(2), dma(2), dma(6),
        ],
        compiler_params=pltpu.CompilerParams(collective_id=0, has_side_effects=True, vmem_limit_bytes=67043328),
    )(x_loc, g_loc, w_one, w_two)


GRAD_ROWS, GRAD_COLS, GRAD_PART, GRAD_SLOTS = 1024, 2048, 256, 4


def weight_grad_kernel(h_ref, d_ref, a_ref, g_ref, y_ref, x_ref, up_ref, down_ref, y_out, x_out,
                       h, d, a, g, home, left, right, stage, in_sem, home_sem, out_sem):
    d_model, d_ff = h.shape[1], d.shape[1]
    n_down, n_up, n_col = d_ff // GRAD_ROWS, d_model // GRAD_ROWS, d_ff // GRAD_COLS

    pieces = [a.at[:, pl.ds(t * GRAD_ROWS, GRAD_ROWS)] for t in range(n_down)]
    loads = [(g_ref, g)] + [(a_ref.at[:, pl.ds(t * GRAD_ROWS, GRAD_ROWS)], piece) for t, piece in enumerate(pieces)] + [(h_ref, h), (d_ref, d)]
    loads = [pltpu.make_async_copy(src, dst, in_sem.at[t]) for t, (src, dst) in enumerate(loads)]
    homes = [pltpu.make_async_copy(src, home.at[t], home_sem.at[t]) for t, src in enumerate((y_ref, x_ref))]
    backs = [pltpu.make_async_copy(home.at[t], dst, home_sem.at[t]) for t, dst in enumerate((y_out, x_out))]
    for copy in loads + homes:
        copy.start()

    rows_of = lambda t: pl.ds(t * GRAD_ROWS, GRAD_ROWS)
    blocks = [(a, t, g, 0, down_ref) for t in range(n_down)] + [(h, t, d, c, up_ref) for t in range(n_up) for c in range(n_col)]
    turned = (left, right)
    loads[0].wait()
    loads[1].wait()
    arrived = 2
    turn = -1
    for t, (src, row, other, col, out) in enumerate(blocks):
        slot = t % GRAD_SLOTS
        cols = pl.ds(col * GRAD_COLS, GRAD_COLS)
        after = blocks[t + 1] if t + 1 < len(blocks) else None
        need = (1 + n_down if after is None or after[0] is h else t + 2) + (1 if src is h or (after is not None and after[0] is h) else 0)
        need = min(need, len(loads) - 1) + (1 if src is h else 0)
        while arrived < min(need + 1, len(loads)):
            loads[arrived].wait()
            arrived += 1
        if t >= GRAD_SLOTS:
            pltpu.make_async_copy(stage.at[slot], stage.at[slot], out_sem.at[slot]).wait()
        size = GRAD_PART if after is None or t == 0 else GRAD_ROWS
        for p in range(0, GRAD_ROWS, size):
            if t == 0:
                stage[slot, p:p + size] = lax.dot_general(src[:, p:p + size], other[:, cols], (((0,), (0,)), ((), ())), preferred_element_type=F32)
            else:
                stage[slot, p:p + size] = jnp.dot(turned[turn % 2][p:p + size], other[:, cols], preferred_element_type=F32)
            if p + size == GRAD_ROWS and after is not None and (after[0] is not src or after[1] != row):
                turn += 1
                turned[turn % 2][...] = after[0][:, rows_of(after[1])].T
            for q in range(p, p + size, GRAD_PART):
                pltpu.make_async_copy(stage.at[slot, pl.ds(q, GRAD_PART)], out.at[pl.ds(row * GRAD_ROWS + q, GRAD_PART), cols], out_sem.at[slot]).start()
        if t == 1:
            for copy, back in zip(homes, backs):
                copy.wait()
                back.start()
    for slot in range(GRAD_SLOTS):
        pltpu.make_async_copy(stage.at[slot], stage.at[slot], out_sem.at[slot]).wait()
    for copy in backs:
        copy.wait()


def weight_grads(h, d, a, g, y, dx):
    tokens, d_model = h.shape
    d_ff = d.shape[1]
    n_in = 3 + d_ff // GRAD_ROWS
    hbm = pl.BlockSpec(memory_space=pl.ANY)
    dma = lambda *shape: pltpu.SemaphoreType.DMA(shape)
    like = lambda v: pltpu.VMEM(v.shape, v.dtype)
    return pl.pallas_call(
        weight_grad_kernel,
        name='weight_grads',
        out_shape=(jax.ShapeDtypeStruct((d_model, d_ff), F32), jax.ShapeDtypeStruct((d_ff, d_model), F32),
                   jax.ShapeDtypeStruct(y.shape, BF16), jax.ShapeDtypeStruct(y.shape, BF16)),
        in_specs=[hbm] * 6,
        out_specs=(hbm,) * 4,
        scratch_shapes=[like(h), like(d), like(a), like(g), pltpu.VMEM((2,) + y.shape, BF16), pltpu.VMEM((GRAD_ROWS, tokens), BF16), pltpu.VMEM((GRAD_ROWS, tokens), BF16),
                        pltpu.VMEM((GRAD_SLOTS, GRAD_ROWS, GRAD_COLS), F32),
                        dma(n_in), dma(2), dma(GRAD_SLOTS)],
        compiler_params=pltpu.CompilerParams(vmem_limit_bytes=60 * 1024 * 1024),
    )(h, d, a, g, y, dx)


def solution(mesh):
    tok_spec = P(('data', 'stage', 'inner'))
    up_spec = P(None, ('data', 'stage'), None, 'inner')
    down_spec = P(None, ('data', 'stage'), 'inner', None)

    def device_step(x_loc, g_loc, w_up, w_down):
        y, dx, h, g, a, d = run_pipeline(x_loc, g_loc, w_up[0, 0], w_down[0, 0])
        flat = lambda v: v.reshape(-1, v.shape[-1])
        dw_up, dw_down, y, dx = weight_grads(flat(h), flat(d), flat(a), flat(g), y, dx)
        return y, dx, dw_up[None, None], dw_down[None, None]

    return jax.shard_map(device_step, mesh=mesh, in_specs=(tok_spec, tok_spec, up_spec, down_spec), out_specs=(tok_spec, tok_spec, up_spec, down_spec), check_vma=False)
```

```python
import functools

import jax
import jax.numpy as jnp
from jax import lax
from jax.experimental import pallas as pl
from jax.experimental.pallas import tpu as pltpu
from jax.sharding import PartitionSpec as P

F32 = jnp.float32
BF16 = jnp.bfloat16
MESH = pl.DeviceIdType.MESH

STAGES = 4
INNER = 2
UNITS = 8
SLOTS = 3
DIRECT = 3
BLK = 512
TILE = 256
FWD, BWD = 0, 1
HOMES = (0, 1, 2, 2, 3, 3, 1, 0)
NT = (((1,), (1,)), ((), ()))

F1, M1, B1, T1, F2, B2, T2, FR, BR, HB, SW, PR, YL, WA, WB, XS, XW, XR = range(1, 19)
PLAN = (
    ((WA, 0, 1), (F1, 0, 2), (WB, 0, 1), (XS, 0, 1), (F2, 0, 2), (F1, 2, 2), (FR, 0, 2), (F2, 2, 2),
     (FR, 2, 1), (F1, 4, 2), (FR, 3, 1), (F2, 4, 2), (FR, 4, 2), (F1, 6, 2), (F2, 6, 1), (F2, 7, 1),
     (FR, 6, 2), (XW, 0, 1), (SW, 0, 1), (B1, 0, 2), (B2, 0, 1), (B2, 1, 1), (B1, 2, 1), (B2, 2, 1),
     (B1, 3, 1), (BR, 0, 2), (B2, 3, 1), (BR, 2, 1), (B1, 4, 2), (B2, 4, 2), (BR, 3, 1), (B1, 6, 2),
     (B2, 6, 1), (BR, 4, 1), (B2, 7, 1), (BR, 5, 3)),
    ((WA, 0, 1), (WB, 0, 1), (XS, 0, 1), (F1, 0, 2), (F2, 0, 1), (F2, 1, 1), (FR, 0, 2), (F1, 2, 2),
     (F2, 2, 1), (F2, 3, 1), (FR, 2, 1), (F1, 4, 2), (FR, 3, 1), (F2, 4, 1), (F2, 5, 1), (FR, 4, 2),
     (F1, 6, 2), (F2, 6, 2), (FR, 6, 2), (XW, 0, 1), (SW, 0, 1), (HB, 0, 2), (B1, 0, 2), (B2, 0, 1),
     (HB, 2, 1), (B2, 1, 1), (BR, 0, 1), (B1, 2, 2), (BR, 1, 1), (B2, 2, 2), (BR, 2, 2), (B1, 4, 1),
     (B1, 5, 1), (B2, 4, 2), (B1, 6, 1), (B2, 6, 1), (BR, 4, 1), (B1, 7, 1), (BR, 5, 1), (B2, 7, 1),
     (BR, 6, 2)),
    ((XR, 0, 1), (WA, 0, 1), (WB, 0, 1), (XS, 0, 1), (XW, 0, 1), (F1, 0, 1), (F2, 0, 1), (F1, 1, 1),
     (FR, 0, 1), (F2, 1, 1), (FR, 1, 1), (F1, 2, 1), (F2, 2, 1), (F1, 3, 1), (F2, 3, 1), (FR, 2, 1),
     (F1, 4, 1), (F1, 5, 1), (FR, 3, 1), (F2, 4, 2), (T1, 0, 2), (F1, 6, 2), (T2, 0, 2), (FR, 4, 1),
     (F2, 6, 2), (FR, 5, 1), (T1, 2, 2), (FR, 6, 2), (T2, 2, 2), (BR, 3, 1), (T1, 4, 2), (T2, 4, 2),
     (T1, 6, 2), (BR, 4, 1), (T2, 6, 2), (BR, 5, 3)),
    ((WB, 0, 1), (XS, 0, 1), (XR, 0, 1), (PR, 0, 1), (XW, 0, 1), (M1, 0, 1), (B2, 0, 1), (BR, 0, 1),
     (M1, 1, 1), (B2, 1, 1), (BR, 1, 1), (M1, 2, 2), (B2, 2, 1), (B2, 3, 1), (BR, 2, 2), (M1, 4, 1),
     (B2, 4, 1), (M1, 5, 1), (B2, 5, 1), (BR, 4, 1), (M1, 6, 2), (BR, 5, 1), (B2, 6, 2), (BR, 6, 2),
     (YL, 0, 1), (F2, 0, 2), (FR, 0, 2), (F2, 2, 1), (F2, 3, 2), (FR, 2, 1), (F2, 5, 1), (FR, 3, 2),
     (F2, 6, 1), (FR, 5, 1), (F2, 7, 1), (FR, 6, 2)),
)


PACK = 1024
UP_GROUP = 8
TURN = 5
TURN_GROUP = 4
DOWN_GROUP = 2


def plan_words():
    rows = [[op + 32 * unit + 256 * (count - 1) for op, unit, count in row] for row in PLAN]
    steps = -(-max(len(row) for row in rows) // 3) * 3
    rows = [row + [0] * (steps - len(row)) for row in rows]
    return [[row[t] + PACK * row[t + 1] + PACK * PACK * row[t + 2] for t in range(0, steps, 3)] for row in rows]


def gelu_pair(pre_act):
    root = pre_act * 0.7071067811865476
    normal_cdf = 0.5 * (1.0 + lax.erf(root))
    normal_pdf = jnp.exp2(root * root * -1.4426950408889634) * 0.3989422804014327
    return pre_act * normal_cdf, normal_cdf + pre_act * normal_pdf


def wait_bytes(ref, sem):
    pltpu.make_async_copy(ref, ref, sem).wait()


def pipeline_kernel(x_ref, g_ref, w1_ref, w2_ref,
                    y_out, dx_out, h_out, g_out, a_out, d_out,
                    wa, wb, flow, act, slope, part, recv, send, home, direct,
                    flow_sem, recv_sem, part_send, flow_send, home_send, home_sem, in_send, relay_sem, relay_send,
                    direct_sem, direct_send, cross_send, stage_sem, w_sem, out_sem):
    stage = lax.axis_index('stage')
    side = lax.axis_index('inner')
    other = 1 - side
    rows, d_model = flow.shape[3:]
    tok, d_ff = act.shape[2:]
    n_blk = d_model // BLK

    def peer(s, i):
        return {'stage': s, 'inner': i}

    load_a = pltpu.make_async_copy(w1_ref, wa, w_sem.at[0])
    load_b = pltpu.make_async_copy(w2_ref, wb, w_sem.at[1])

    def unit_of(k):
        return jnp.where(stage < 2, stage + (7 - 2 * stage) * k, 2 * stage - 2 + k)

    staged = (send.at[BWD, pl.ds(UNITS - 2, 2)], send.at[BWD, pl.ds(UNITS - 4, 2)])
    stagings = [pltpu.make_async_copy(src, dst, stage_sem.at[kind]) for kind, (src, dst) in enumerate(zip((x_ref, g_ref), staged))]
    for kind, target in ((FWD, 0), (BWD, STAGES - 1)):
        stagings[kind].start()

        @pl.when(stage == target)
        def _():
            for k in range(2):
                pltpu.make_async_copy((x_ref, g_ref)[kind].at[k], flow.at[kind, unit_of(k), side], flow_sem.at[kind, unit_of(k), side]).start()

    @pl.when(stage < STAGES - 1)
    def _():
        load_a.start()
    load_b.start()

    @pl.when(stage == STAGES - 1)
    def _():
        load_a.start()

    barrier = pltpu.get_barrier_semaphore()
    for s in range(STAGES):
        for i in range(INNER):
            @pl.when(jnp.logical_or(stage != s, side != i))
            def _():
                pl.semaphore_signal(barrier, inc=1, device_id=peer(s, i), device_id_type=MESH)
    pl.semaphore_wait(barrier, STAGES * INNER - 1)

    def home_of(u):
        return jnp.where(u < 2, u, jnp.where(u > 5, 7 - u, (u + 2) // 2))

    def slot_of(u):
        return jnp.where(u < 2, 0, jnp.where(u > 5, 1, lax.rem(u, 2)))

    def hand_in(kind, target, k, lane):
        u = unit_of(k)
        src = staged[kind]
        if lane == 0:
            @pl.when(stage != target)
            def _():
                pltpu.make_async_remote_copy(src.at[k], flow.at[kind, u, side], in_send.at[kind, k, 0], flow_sem.at[kind, u, side],
                                             device_id=peer(target, side), device_id_type=MESH).start()
        else:
            pltpu.make_async_remote_copy(src.at[k], flow.at[kind, u, side], in_send.at[kind, k, 1], flow_sem.at[kind, u, side],
                                         device_id=peer(target, other), device_id_type=MESH).start()

    def relay(k):
        return pltpu.make_async_remote_copy(staged[FWD].at[k], home.at[FWD, k], in_send.at[FWD, k, 1], relay_sem.at[k],
                                            device_id=peer(stage, other), device_id_type=MESH)

    def relayed(k):
        u = unit_of(k)
        return pltpu.make_async_remote_copy(home.at[FWD, k], flow.at[FWD, u, other], relay_send.at[k], flow_sem.at[FWD, u, other],
                                            device_id=peer(0, side), device_id_type=MESH)

    stagings[FWD].wait()
    for k in range(2):
        hand_in(FWD, 0, k, 0)

        if k == 0:
            @pl.when(stage < 2)
            def _():
                hand_in(FWD, 0, k, 1)

        @pl.when(stage == 2)
        def _():
            relay(k).start()
    plan = plan_words()
    words = [jnp.where(stage == 0, a, jnp.where(stage == 1, b, jnp.where(stage == 2, c, d))) for a, b, c, d in zip(*plan)]

    def keep(ref, out, u, lane):
        pltpu.make_async_copy(ref, out.at[u], out_sem.at[lane]).start()

    def blocks(width, group, fn):
        def body(t, carry):
            fn([pl.ds(pl.multiple_of((t * group + k) * BLK, BLK), BLK) for k in range(group)])
            return carry
        lax.fori_loop(0, width // BLK // group, body, 0)

    def arrived(kind, u):
        for half in range(INNER):
            @pl.when(jnp.logical_not((stage == 1) & (kind == BWD) & (u < DIRECT) & (side == half)))
            def _():
                wait_bytes(flow.at[kind, u, half], flow_sem.at[kind, u, half])

    def both_arrived(kind, u, v):
        arrived(kind, u)

        @pl.when(v != u)
        def _():
            arrived(kind, v)

    def pair(ref, kind, u, v):
        width = ref.shape[-1]
        return jnp.concatenate([ref[kind, u].reshape(tok, width), ref[kind, v].reshape(tok, width)], axis=0)

    def kept(u, v, fn):
        fn(u)

        @pl.when(v != u)
        def _():
            fn(v)

    def up_product(u, v, last):
        both_arrived(FWD, u, v)

        def fn(slices):
            lhs = pair(flow, FWD, u, v)
            for sl in slices:
                z = jnp.dot(lhs, wa[:, sl], preferred_element_type=F32)
                value, grad = gelu_pair(z)
                value = value.astype(BF16)
                if last:
                    act[BWD, u, :, sl] = (slope[u, :, sl] * grad[:tok]).astype(BF16)
                    act[BWD, v, :, sl] = (slope[v, :, sl] * grad[tok:]).astype(BF16)
                else:
                    slope[u, :, sl] = grad[:tok]
                    slope[v, :, sl] = grad[tok:]
                act[FWD, u, :, sl] = value[:tok]
                act[FWD, v, :, sl] = value[tok:]
        blocks(d_ff, UP_GROUP, fn)

        def out(w):
            keep(flow.at[FWD, w], h_out, w, 0)
            keep(act.at[FWD, w], a_out, w, 2)
            if last:
                keep(act.at[BWD, w], d_out, w, 3)
        kept(u, v, out)

    def across(lhs, ref, sl):
        cut = ref.shape[1] * TURN // 8
        total = lax.dot_general(lhs[:, :cut], ref[sl, :cut], NT, preferred_element_type=F32)
        for k in range(cut, ref.shape[1], TILE):
            turned = [ref[pl.ds(sl.start + q, TILE), k:k + TILE].T for q in range(0, BLK, TILE)]
            total += jnp.dot(lhs[:, k:k + TILE], jnp.concatenate(turned, axis=1), preferred_element_type=F32)
        return total

    def back_product(u, v, swapped):
        both_arrived(BWD, u, v)

        def fn(slices):
            lhs = pair(flow, BWD, u, v)
            for sl in slices:
                if swapped:
                    e = jnp.dot(lhs, wa[:, sl], preferred_element_type=F32)
                else:
                    e = across(lhs, wb, sl)
                act[BWD, u, :, sl] = (e[:tok] * slope[u, :, sl]).astype(BF16)
                act[BWD, v, :, sl] = (e[tok:] * slope[v, :, sl]).astype(BF16)
        blocks(d_ff, UP_GROUP if swapped else TURN_GROUP, fn)

        def out(w):
            keep(flow.at[BWD, w], g_out, w, 1)
            keep(act.at[BWD, w], d_out, w, 3)
        kept(u, v, out)

    def part_copy(kind, u, j):
        slot = lax.rem(u, SLOTS)
        return pltpu.make_async_remote_copy(part.at[kind, slot, j, other], recv.at[kind, u, j], part_send.at[kind, slot, j],
                                            recv_sem.at[kind, u, j], device_id=peer(stage, other), device_id_type=MESH)

    def direct_copy(u, j, half):
        slot = lax.rem(u, SLOTS)
        if half is side:
            return pltpu.make_async_remote_copy(part.at[BWD, slot, j, side], direct.at[u, j], direct_send.at[slot, j],
                                                direct_sem.at[0, u, j], device_id=peer(stage - 1, side), device_id_type=MESH)
        return pltpu.make_async_remote_copy(part.at[BWD, slot, j, other], recv.at[FWD, u, j], part_send.at[BWD, slot, j],
                                            direct_sem.at[1, u, j], device_id=peer(stage - 1, other), device_id_type=MESH)

    def take_direct(first, count):
        def body(i, carry):
            u = first + i
            for j in range(n_blk):
                sl = pl.ds(j * BLK, BLK)
                wait_bytes(direct.at[u, j], direct_sem.at[0, u, j])
                wait_bytes(recv.at[FWD, u, j], direct_sem.at[1, u, j])
                flow[BWD, u, side, :, sl] = (direct[u, j] + recv[FWD, u, j]).astype(BF16)
                pltpu.make_async_remote_copy(flow.at[BWD, u, side, :, sl], flow.at[BWD, u, side, :, sl], cross_send.at[0],
                                             flow_sem.at[BWD, u, side], device_id=peer(stage, other), device_id_type=MESH).start()
            return carry
        lax.fori_loop(0, count, body, 0)

    def down_product(kind, u, v, straight):
        def free(w):
            @pl.when(w >= SLOTS)
            def _():
                for j in range(n_blk):
                    part_copy(kind, w - SLOTS, j).wait_send()

            if not straight:
                @pl.when((w >= SLOTS) & (w < SLOTS + DIRECT))
                def _():
                    for j in range(n_blk):
                        direct_copy(w - SLOTS, j, side).wait_send()
        kept(u, v, free)

        def body(t, carry):
            lhs = pair(act, kind, u, v)
            for k in range(DOWN_GROUP):
                j = t * DOWN_GROUP + k
                sl = pl.ds(pl.multiple_of(j * BLK, BLK), BLK)
                if straight:
                    p = jnp.dot(lhs, wb[:, sl], preferred_element_type=F32)
                else:
                    p = across(lhs, wa, sl)
                p = p.reshape(2, INNER, rows, BLK)
                part[kind, lax.rem(u, SLOTS), j] = p[0]
                part[kind, lax.rem(v, SLOTS), j] = p[1]

            def go(w):
                if straight:
                    for k in range(DOWN_GROUP):
                        part_copy(kind, w, t * DOWN_GROUP + k).start()
                    return

                @pl.when(w >= DIRECT)
                def _():
                    for k in range(DOWN_GROUP):
                        part_copy(kind, w, t * DOWN_GROUP + k).start()

                @pl.when(w < DIRECT)
                def _():
                    for k in range(DOWN_GROUP):
                        j = t * DOWN_GROUP + k
                        sl = pl.ds(pl.multiple_of(j * BLK, BLK), BLK)
                        part[BWD, lax.rem(w, SLOTS), j, side] += flow[BWD, w, side, :, sl].astype(F32)
                    for k in range(DOWN_GROUP):
                        for half in (side, other):
                            direct_copy(w, t * DOWN_GROUP + k, half).start()
            kept(u, v, go)
            return carry
        lax.fori_loop(0, n_blk // DOWN_GROUP, body, 0)

    def hand_on(kind, first, count):
        target = stage + 1 if kind == FWD else stage - 1
        inside = stage < STAGES - 1 if kind == FWD else stage > 0
        out = STAGES - 1 if kind == FWD else 0

        def body(i, carry):
            u = first + i
            slot = lax.rem(u, SLOTS)
            for j in range(n_blk):
                sl = pl.ds(j * BLK, BLK)
                wait_bytes(recv.at[kind, u, j], recv_sem.at[kind, u, j])
                total = flow[kind, u, side, :, sl].astype(F32) + (part[kind, slot, j, side] + recv[kind, u, j])
                send[kind, u, :, sl] = total.astype(BF16)

                @pl.when(inside)
                def _():
                    for half in (side, other):
                        pltpu.make_async_remote_copy(send.at[kind, u, :, sl], flow.at[kind, u, side, :, sl], flow_send.at[kind],
                                                     flow_sem.at[kind, u, side], device_id=peer(target, half), device_id_type=MESH).start()

            @pl.when(jnp.logical_and(jnp.logical_not(inside), home_of(u) != out))
            def _():
                pltpu.make_async_remote_copy(send.at[kind, u], home.at[kind, slot_of(u)], home_send.at[kind, u],
                                             home_sem.at[kind, slot_of(u)], device_id=peer(home_of(u), side), device_id_type=MESH).start()
            return carry
        lax.fori_loop(0, count, body, 0)

    def swap_weights():
        n_i = d_model // TILE

        def body(t, carry):
            i = pl.multiple_of(lax.rem(t, n_i) * TILE, TILE)
            j = pl.multiple_of(lax.div(t, n_i) * TILE, TILE)
            up = wa[pl.ds(i, TILE), pl.ds(j, TILE)]
            down = wb[pl.ds(j, TILE), pl.ds(i, TILE)]
            wa[pl.ds(i, TILE), pl.ds(j, TILE)] = down.T
            wb[pl.ds(j, TILE), pl.ds(i, TILE)] = up.T
            return carry
        lax.fori_loop(0, n_i * (d_ff // TILE), body, 0)

    def prepare_last():
        half = UNITS // 2

        def quarter(q, carry):
            for i in range(half):
                arrived(BWD, q * half + i)
                keep(flow.at[BWD, q * half + i], g_out, q * half + i, 1)
            units = pl.ds(q * half, half)

            def fn(slices):
                lhs = flow[BWD, units].reshape(half * tok, d_model)
                for sl in slices:
                    e = lax.dot_general(lhs, wb[sl, :], NT, preferred_element_type=F32)
                    slope[units, :, sl] = e.reshape(half, tok, BLK)
            blocks(d_ff, 1, fn)
            return carry
        lax.fori_loop(0, 2, quarter, 0)
        load_a.wait()
        n_i = d_model // TILE

        def body(t, carry):
            i = pl.multiple_of(lax.rem(t, n_i) * TILE, TILE)
            j = pl.multiple_of(lax.div(t, n_i) * TILE, TILE)
            wb[pl.ds(j, TILE), pl.ds(i, TILE)] = wa[pl.ds(i, TILE), pl.ds(j, TILE)].T
            return carry
        lax.fori_loop(0, n_i * (d_ff // TILE), body, 0)

    def step(t, carry):
        group, place = lax.div(t, 3), lax.rem(t, 3)
        word = words[0]
        for i, w in enumerate(words[1:], 1):
            word = jnp.where(group == i, w, word)
        code = lax.rem(lax.div(word, jnp.where(place == 0, 1, jnp.where(place == 1, PACK, PACK * PACK))), PACK)
        op = lax.rem(code, 32)
        u = lax.rem(lax.div(code, 32), UNITS)
        count = lax.div(code, 256) + 1

        def on(want):
            return pl.when(op == want)

        v = jnp.minimum(u + count - 1, UNITS - 1)

        @pl.when(op <= T1)
        def _():
            @on(F1)
            def _():
                up_product(u, v, False)

            @on(M1)
            def _():
                up_product(u, v, True)

            @on(B1)
            def _():
                back_product(u, v, True)

            @on(T1)
            def _():
                back_product(u, v, False)

        @pl.when((op > T1) & (op <= T2))
        def _():
            @pl.when(op < T2)
            def _():
                down_product(jnp.where(op == F2, FWD, BWD), u, v, True)

            @on(T2)
            def _():
                down_product(BWD, u, v, False)

        @pl.when((op > T2) & (op <= HB))
        def _():
            @on(FR)
            def _():
                hand_on(FWD, u, count)

            @on(BR)
            def _():
                hand_on(BWD, u, count)

            @on(HB)
            def _():
                take_direct(u, count)

        @pl.when(op > HB)
        def _():
            @on(SW)
            def _():
                swap_weights()

            @on(PR)
            def _():
                prepare_last()

            @on(YL)
            def _():
                load_b.start()
                load_b.wait()

            @on(WA)
            def _():
                load_a.wait()

            @on(WB)
            def _():
                load_b.wait()

            @on(XS)
            def _():
                stagings[BWD].wait()
                for k in range(2):
                    for lane in range(2):
                        hand_in(BWD, STAGES - 1, k, lane)

                @pl.when(stage < 2)
                def _():
                    hand_in(FWD, 0, 1, 1)

                @pl.when(stage == STAGES - 1)
                def _():
                    for k in range(2):
                        relay(k).start()

            @on(XR)
            def _():
                for k in range(2):
                    wait_bytes(home.at[FWD, k], relay_sem.at[k])
                    relayed(k).start()

            @on(XW)
            def _():
                for kind, target in ((FWD, 0), (BWD, STAGES - 1)):
                    for k in range(2):
                        @pl.when(stage != target)
                        def _():
                            wait_bytes(staged[kind].at[k], in_send.at[kind, k, 0])
                        wait_bytes(staged[kind].at[k], in_send.at[kind, k, 1])

                @pl.when(stage > 1)
                def _():
                    for k in range(2):
                        relayed(k).wait_send()
        return carry
    lengths = [len(row) for row in PLAN]
    lax.fori_loop(0, jnp.where(stage == 0, lengths[0], jnp.where(stage == 1, lengths[1], jnp.where(stage == 2, lengths[2], lengths[3]))), step, 0)

    for kind, here, out in ((FWD, STAGES - 1, y_out), (BWD, 0, dx_out)):
        for k in range(2):
            @pl.when(stage == here)
            def _():
                pltpu.make_async_copy(send.at[kind, unit_of(k)], out.at[k], out_sem.at[4 + kind]).start()

            @pl.when(stage != here)
            def _():
                wait_bytes(home.at[kind, k], home_sem.at[kind, k])
                pltpu.make_async_copy(home.at[kind, k], out.at[k], out_sem.at[4 + kind]).start()

    for kind in (FWD, BWD):
        for u in range(UNITS - SLOTS, UNITS):
            for j in range(n_blk):
                part_copy(kind, u, j).wait_send()
    for kind, last in ((FWD, STAGES - 1), (BWD, 0)):
        @pl.when((stage != last) & jnp.logical_not((stage == 2) & (kind == BWD)))
        def _():
            wait_bytes(flow.at[kind], flow_send.at[kind])

        @pl.when(stage == last)
        def _():
            for u in range(UNITS):
                if HOMES[u] != last:
                    wait_bytes(send.at[kind, u], home_send.at[kind, u])
    @pl.when(stage == 2)
    def _():
        wait_bytes(flow.at[BWD, pl.ds(0, UNITS - DIRECT)], flow_send.at[BWD])

    @pl.when(stage == 1)
    def _():
        wait_bytes(flow.at[BWD, pl.ds(0, DIRECT), 0], cross_send.at[0])
    for lane, (ref, out) in enumerate(((flow.at[FWD], h_out), (flow.at[BWD], g_out), (act.at[FWD], a_out), (act.at[BWD], d_out),
                                       (home.at[FWD], y_out), (home.at[BWD], dx_out))):
        pltpu.make_async_copy(ref, out, out_sem.at[lane]).wait()


def run_pipeline(x_loc, g_loc, w_one, w_two):
    rows, d_model = x_loc.shape[1:]
    d_ff = w_one.shape[1]
    n_blk = d_model // BLK
    tok = INNER * rows
    hbm = pl.BlockSpec(memory_space=pl.ANY)
    out = lambda *shape: jax.ShapeDtypeStruct(shape, BF16)
    dma = lambda *shape: pltpu.SemaphoreType.DMA(shape)
    return pl.pallas_call(
        pipeline_kernel,
        name='pipeline',
        out_shape=(out(*x_loc.shape), out(*x_loc.shape), out(UNITS, INNER, rows, d_model), out(UNITS, INNER, rows, d_model),
                   out(UNITS, tok, d_ff), out(UNITS, tok, d_ff)),
        in_specs=[hbm] * 4,
        out_specs=(hbm,) * 6,
        scratch_shapes=[
            pltpu.VMEM((d_model, d_ff), BF16),
            pltpu.VMEM((d_ff, d_model), BF16),
            pltpu.VMEM((2, UNITS, INNER, rows, d_model), BF16),
            pltpu.VMEM((2, UNITS, tok, d_ff), BF16),
            pltpu.VMEM((UNITS, tok, d_ff), F32),
            pltpu.VMEM((2, SLOTS, n_blk, INNER, rows, BLK), F32),
            pltpu.VMEM((2, UNITS, n_blk, rows, BLK), F32),
            pltpu.VMEM((2, UNITS, rows, d_model), BF16),
            pltpu.VMEM((2, 2, rows, d_model), BF16),
            pltpu.VMEM((DIRECT, n_blk, rows, BLK), F32),
            dma(2, UNITS, INNER), dma(2, UNITS, n_blk), dma(2, SLOTS, n_blk), dma(2), dma(2, UNITS), dma(2, 2), dma(2, 2, 2), dma(2), dma(2),
            dma(2, DIRECT, n_blk), dma(SLOTS, n_blk), dma(1), dma(2), dma(2), dma(6),
        ],
        compiler_params=pltpu.CompilerParams(collective_id=0, has_side_effects=True, vmem_limit_bytes=67043328),
    )(x_loc, g_loc, w_one, w_two)


GRAD_ROWS, GRAD_COLS, GRAD_PART, GRAD_SLOTS = 1024, 2048, 256, 4


def weight_grad_kernel(h_ref, d_ref, a_ref, g_ref, y_ref, x_ref, up_ref, down_ref, y_out, x_out,
                       h, d, a, g, home, left, right, stage, in_sem, home_sem, out_sem):
    d_model, d_ff = h.shape[1], d.shape[1]
    n_down, n_up, n_col = d_ff // GRAD_ROWS, d_model // GRAD_ROWS, d_ff // GRAD_COLS

    pieces = [a.at[:, pl.ds(t * GRAD_ROWS, GRAD_ROWS)] for t in range(n_down)]
    loads = [(g_ref, g)] + [(a_ref.at[:, pl.ds(t * GRAD_ROWS, GRAD_ROWS)], piece) for t, piece in enumerate(pieces)] + [(h_ref, h), (d_ref, d)]
    loads = [pltpu.make_async_copy(src, dst, in_sem.at[t]) for t, (src, dst) in enumerate(loads)]
    homes = [pltpu.make_async_copy(src, home.at[t], home_sem.at[t]) for t, src in enumerate((y_ref, x_ref))]
    backs = [pltpu.make_async_copy(home.at[t], dst, home_sem.at[t]) for t, dst in enumerate((y_out, x_out))]
    for copy in loads + homes:
        copy.start()

    rows_of = lambda t: pl.ds(t * GRAD_ROWS, GRAD_ROWS)
    blocks = [(a, t, g, 0, down_ref) for t in range(n_down)] + [(h, t, d, c, up_ref) for t in range(n_up) for c in range(n_col)]
    turned = (left, right)
    loads[0].wait()
    loads[1].wait()
    arrived = 2
    turn = -1
    for t, (src, row, other, col, out) in enumerate(blocks):
        slot = t % GRAD_SLOTS
        cols = pl.ds(col * GRAD_COLS, GRAD_COLS)
        after = blocks[t + 1] if t + 1 < len(blocks) else None
        need = (1 + n_down if after is None or after[0] is h else t + 2) + (1 if src is h or (after is not None and after[0] is h) else 0)
        need = min(need, len(loads) - 1) + (1 if src is h else 0)
        while arrived < min(need + 1, len(loads)):
            loads[arrived].wait()
            arrived += 1
        if t >= GRAD_SLOTS:
            pltpu.make_async_copy(stage.at[slot], stage.at[slot], out_sem.at[slot]).wait()
        size = GRAD_PART if after is None or t == 0 else GRAD_ROWS
        for p in range(0, GRAD_ROWS, size):
            if t == 0:
                stage[slot, p:p + size] = lax.dot_general(src[:, p:p + size], other[:, cols], (((0,), (0,)), ((), ())), preferred_element_type=F32)
            else:
                stage[slot, p:p + size] = jnp.dot(turned[turn % 2][p:p + size], other[:, cols], preferred_element_type=F32)
            if p + size == GRAD_ROWS and after is not None and (after[0] is not src or after[1] != row):
                turn += 1
                turned[turn % 2][...] = after[0][:, rows_of(after[1])].T
            for q in range(p, p + size, GRAD_PART):
                pltpu.make_async_copy(stage.at[slot, pl.ds(q, GRAD_PART)], out.at[pl.ds(row * GRAD_ROWS + q, GRAD_PART), cols], out_sem.at[slot]).start()
        if t == 1:
            for copy, back in zip(homes, backs):
                copy.wait()
                back.start()
    for slot in range(GRAD_SLOTS):
        pltpu.make_async_copy(stage.at[slot], stage.at[slot], out_sem.at[slot]).wait()
    for copy in backs:
        copy.wait()


def weight_grads(h, d, a, g, y, dx):
    tokens, d_model = h.shape
    d_ff = d.shape[1]
    n_in = 3 + d_ff // GRAD_ROWS
    hbm = pl.BlockSpec(memory_space=pl.ANY)
    dma = lambda *shape: pltpu.SemaphoreType.DMA(shape)
    like = lambda v: pltpu.VMEM(v.shape, v.dtype)
    return pl.pallas_call(
        weight_grad_kernel,
        name='weight_grads',
        out_shape=(jax.ShapeDtypeStruct((d_model, d_ff), F32), jax.ShapeDtypeStruct((d_ff, d_model), F32),
                   jax.ShapeDtypeStruct(y.shape, BF16), jax.ShapeDtypeStruct(y.shape, BF16)),
        in_specs=[hbm] * 6,
        out_specs=(hbm,) * 4,
        scratch_shapes=[like(h), like(d), like(a), like(g), pltpu.VMEM((2,) + y.shape, BF16), pltpu.VMEM((GRAD_ROWS, tokens), BF16), pltpu.VMEM((GRAD_ROWS, tokens), BF16),
                        pltpu.VMEM((GRAD_SLOTS, GRAD_ROWS, GRAD_COLS), F32),
                        dma(n_in), dma(2), dma(GRAD_SLOTS)],
        compiler_params=pltpu.CompilerParams(vmem_limit_bytes=60 * 1024 * 1024),
    )(h, d, a, g, y, dx)


def solution(mesh):
    tok_spec = P(('data', 'stage', 'inner'))
    up_spec = P(None, ('data', 'stage'), None, 'inner')
    down_spec = P(None, ('data', 'stage'), 'inner', None)

    def device_step(x_loc, g_loc, w_up, w_down):
        y, dx, h, g, a, d = run_pipeline(x_loc, g_loc, w_up[0, 0], w_down[0, 0])
        flat = lambda v: v.reshape(-1, v.shape[-1])
        dw_up, dw_down, y, dx = weight_grads(flat(h), flat(d), flat(a), flat(g), y, dx)
        return y, dx, dw_up[None, None], dw_down[None, None]

    return jax.shard_map(device_step, mesh=mesh, in_specs=(tok_spec, tok_spec, up_spec, down_spec), out_specs=(tok_spec, tok_spec, up_spec, down_spec), check_vma=False)
```

```python
import functools

import jax
import jax.numpy as jnp
from jax import lax
from jax.experimental import pallas as pl
from jax.experimental.pallas import tpu as pltpu
from jax.sharding import PartitionSpec as P

F32 = jnp.float32
BF16 = jnp.bfloat16
MESH = pl.DeviceIdType.MESH

STAGES = 4
INNER = 2
UNITS = 8
SLOTS = 3
DIRECT = 3
BLK = 512
TILE = 256
FWD, BWD = 0, 1
HOMES = (0, 1, 2, 2, 3, 3, 1, 0)
NT = (((1,), (1,)), ((), ()))

F1, M1, B1, T1, F2, B2, T2, FR, BR, HB, SW, PR, YL, WA, WB, XS, XW, XR = range(1, 19)
PLAN = (
    ((WA, 0, 1), (F1, 0, 2), (WB, 0, 1), (XS, 0, 1), (F2, 0, 2), (F1, 2, 2), (FR, 0, 2), (F2, 2, 2),
     (FR, 2, 1), (F1, 4, 2), (FR, 3, 1), (F2, 4, 2), (FR, 4, 2), (F1, 6, 2), (F2, 6, 1), (F2, 7, 1),
     (FR, 6, 2), (XW, 0, 1), (SW, 0, 1), (B1, 0, 2), (B2, 0, 1), (B2, 1, 1), (B1, 2, 1), (B2, 2, 1),
     (B1, 3, 1), (BR, 0, 2), (B2, 3, 1), (BR, 2, 1), (B1, 4, 2), (B2, 4, 2), (BR, 3, 1), (B1, 6, 2),
     (B2, 6, 1), (BR, 4, 1), (B2, 7, 1), (BR, 5, 3)),
    ((WA, 0, 1), (WB, 0, 1), (XS, 0, 1), (F1, 0, 2), (F2, 0, 1), (F2, 1, 1), (FR, 0, 2), (F1, 2, 2),
     (F2, 2, 1), (F2, 3, 1), (FR, 2, 1), (F1, 4, 2), (FR, 3, 1), (F2, 4, 1), (F2, 5, 1), (FR, 4, 2),
     (F1, 6, 2), (F2, 6, 2), (FR, 6, 2), (XW, 0, 1), (SW, 0, 1), (HB, 0, 2), (B1, 0, 2), (B2, 0, 1),
     (HB, 2, 1), (B2, 1, 1), (BR, 0, 1), (B1, 2, 2), (BR, 1, 1), (B2, 2, 2), (BR, 2, 2), (B1, 4, 1),
     (B1, 5, 1), (B2, 4, 2), (B1, 6, 1), (B2, 6, 1), (BR, 4, 1), (B1, 7, 1), (BR, 5, 1), (B2, 7, 1),
     (BR, 6, 2)),
    ((XR, 0, 1), (WA, 0, 1), (WB, 0, 1), (XS, 0, 1), (XW, 0, 1), (F1, 0, 1), (F2, 0, 1), (F1, 1, 1),
     (FR, 0, 1), (F2, 1, 1), (FR, 1, 1), (F1, 2, 1), (F2, 2, 1), (F1, 3, 1), (F2, 3, 1), (FR, 2, 1),
     (F1, 4, 1), (F1, 5, 1), (FR, 3, 1), (F2, 4, 2), (T1, 0, 2), (F1, 6, 2), (T2, 0, 2), (FR, 4, 1),
     (F2, 6, 2), (FR, 5, 1), (T1, 2, 2), (FR, 6, 2), (T2, 2, 2), (BR, 3, 1), (T1, 4, 2), (T2, 4, 2),
     (T1, 6, 2), (BR, 4, 1), (T2, 6, 2), (BR, 5, 3)),
    ((WB, 0, 1), (XS, 0, 1), (XR, 0, 1), (PR, 0, 1), (XW, 0, 1), (M1, 0, 1), (B2, 0, 1), (BR, 0, 1),
     (M1, 1, 1), (B2, 1, 1), (BR, 1, 1), (M1, 2, 2), (B2, 2, 1), (B2, 3, 1), (BR, 2, 2), (M1, 4, 1),
     (B2, 4, 1), (M1, 5, 1), (B2, 5, 1), (BR, 4, 1), (M1, 6, 2), (BR, 5, 1), (B2, 6, 2), (BR, 6, 2),
     (YL, 0, 1), (F2, 0, 2), (FR, 0, 2), (F2, 2, 1), (F2, 3, 2), (FR, 2, 1), (F2, 5, 1), (FR, 3, 2),
     (F2, 6, 1), (FR, 5, 1), (F2, 7, 1), (FR, 6, 2)),
)


PACK = 1024
UP_GROUP = 8
TURN = 5
TURN_GROUP = 4
DOWN_GROUP = 2


def plan_words():
    rows = [[op + 32 * unit + 256 * (count - 1) for op, unit, count in row] for row in PLAN]
    steps = -(-max(len(row) for row in rows) // 3) * 3
    rows = [row + [0] * (steps - len(row)) for row in rows]
    return [[row[t] + PACK * row[t + 1] + PACK * PACK * row[t + 2] for t in range(0, steps, 3)] for row in rows]


def gelu_pair(pre_act):
    root = pre_act * 0.7071067811865476
    normal_cdf = 0.5 * (1.0 + lax.erf(root))
    normal_pdf = jnp.exp2(root * root * -1.4426950408889634) * 0.3989422804014327
    return pre_act * normal_cdf, normal_cdf + pre_act * normal_pdf


def wait_bytes(ref, sem):
    pltpu.make_async_copy(ref, ref, sem).wait()


def pipeline_kernel(x_ref, g_ref, w1_ref, w2_ref,
                    y_out, dx_out, h_out, g_out, a_out, d_out,
                    wa, wb, flow, act, slope, part, recv, send, home, direct,
                    flow_sem, recv_sem, part_send, flow_send, home_send, home_sem, in_send, relay_sem, relay_send,
                    direct_sem, direct_send, cross_send, stage_sem, w_sem, out_sem):
    stage = lax.axis_index('stage')
    side = lax.axis_index('inner')
    other = 1 - side
    rows, d_model = flow.shape[3:]
    tok, d_ff = act.shape[2:]
    n_blk = d_model // BLK

    def peer(s, i):
        return {'stage': s, 'inner': i}

    load_a = pltpu.make_async_copy(w1_ref, wa, w_sem.at[0])
    load_b = pltpu.make_async_copy(w2_ref, wb, w_sem.at[1])

    def unit_of(k):
        return jnp.where(stage < 2, stage + (7 - 2 * stage) * k, 2 * stage - 2 + k)

    staged = (send.at[BWD, pl.ds(UNITS - 2, 2)], send.at[BWD, pl.ds(UNITS - 4, 2)])
    stagings = [pltpu.make_async_copy(src, dst, stage_sem.at[kind]) for kind, (src, dst) in enumerate(zip((x_ref, g_ref), staged))]
    for kind, target in ((FWD, 0), (BWD, STAGES - 1)):
        stagings[kind].start()

        @pl.when(stage == target)
        def _():
            for k in range(2):
                pltpu.make_async_copy((x_ref, g_ref)[kind].at[k], flow.at[kind, unit_of(k), side], flow_sem.at[kind, unit_of(k), side]).start()

    @pl.when(stage < STAGES - 1)
    def _():
        load_a.start()
    load_b.start()

    @pl.when(stage == STAGES - 1)
    def _():
        load_a.start()

    barrier = pltpu.get_barrier_semaphore()
    for s in range(STAGES):
        for i in range(INNER):
            @pl.when(jnp.logical_or(stage != s, side != i))
            def _():
                pl.semaphore_signal(barrier, inc=1, device_id=peer(s, i), device_id_type=MESH)
    pl.semaphore_wait(barrier, STAGES * INNER - 1)

    def home_of(u):
        return jnp.where(u < 2, u, jnp.where(u > 5, 7 - u, (u + 2) // 2))

    def slot_of(u):
        return jnp.where(u < 2, 0, jnp.where(u > 5, 1, lax.rem(u, 2)))

    def hand_in(kind, target, k, lane):
        u = unit_of(k)
        src = staged[kind]
        if lane == 0:
            @pl.when(stage != target)
            def _():
                pltpu.make_async_remote_copy(src.at[k], flow.at[kind, u, side], in_send.at[kind, k, 0], flow_sem.at[kind, u, side],
                                             device_id=peer(target, side), device_id_type=MESH).start()
        else:
            pltpu.make_async_remote_copy(src.at[k], flow.at[kind, u, side], in_send.at[kind, k, 1], flow_sem.at[kind, u, side],
                                         device_id=peer(target, other), device_id_type=MESH).start()

    def relay(k):
        return pltpu.make_async_remote_copy(staged[FWD].at[k], home.at[FWD, k], in_send.at[FWD, k, 1], relay_sem.at[k],
                                            device_id=peer(stage, other), device_id_type=MESH)

    def relayed(k):
        u = unit_of(k)
        return pltpu.make_async_remote_copy(home.at[FWD, k], flow.at[FWD, u, other], relay_send.at[k], flow_sem.at[FWD, u, other],
                                            device_id=peer(0, side), device_id_type=MESH)

    stagings[FWD].wait()
    for k in range(2):
        hand_in(FWD, 0, k, 0)

        if k == 0:
            @pl.when(stage < 2)
            def _():
                hand_in(FWD, 0, k, 1)

        @pl.when(stage == 2)
        def _():
            relay(k).start()
    plan = plan_words()
    words = [jnp.where(stage == 0, a, jnp.where(stage == 1, b, jnp.where(stage == 2, c, d))) for a, b, c, d in zip(*plan)]

    def keep(ref, out, u, lane):
        pltpu.make_async_copy(ref, out.at[u], out_sem.at[lane]).start()

    def blocks(width, group, fn):
        def body(t, carry):
            fn([pl.ds(pl.multiple_of((t * group + k) * BLK, BLK), BLK) for k in range(group)])
            return carry
        lax.fori_loop(0, width // BLK // group, body, 0)

    def arrived(kind, u):
        for half in range(INNER):
            @pl.when(jnp.logical_not((stage == 1) & (kind == BWD) & (u < DIRECT) & (side == half)))
            def _():
                wait_bytes(flow.at[kind, u, half], flow_sem.at[kind, u, half])

    def both_arrived(kind, u, v):
        arrived(kind, u)

        @pl.when(v != u)
        def _():
            arrived(kind, v)

    def pair(ref, kind, u, v):
        width = ref.shape[-1]
        return jnp.concatenate([ref[kind, u].reshape(tok, width), ref[kind, v].reshape(tok, width)], axis=0)

    def kept(u, v, fn):
        fn(u)

        @pl.when(v != u)
        def _():
            fn(v)

    def up_product(u, v, last):
        both_arrived(FWD, u, v)

        def fn(slices):
            lhs = pair(flow, FWD, u, v)
            for sl in slices:
                z = jnp.dot(lhs, wa[:, sl], preferred_element_type=F32)
                value, grad = gelu_pair(z)
                value = value.astype(BF16)
                if last:
                    act[BWD, u, :, sl] = (slope[u, :, sl] * grad[:tok]).astype(BF16)
                    act[BWD, v, :, sl] = (slope[v, :, sl] * grad[tok:]).astype(BF16)
                else:
                    slope[u, :, sl] = grad[:tok]
                    slope[v, :, sl] = grad[tok:]
                act[FWD, u, :, sl] = value[:tok]
                act[FWD, v, :, sl] = value[tok:]
        blocks(d_ff, UP_GROUP, fn)

        def out(w):
            keep(flow.at[FWD, w], h_out, w, 0)
            keep(act.at[FWD, w], a_out, w, 2)
            if last:
                keep(act.at[BWD, w], d_out, w, 3)
        kept(u, v, out)

    def across(lhs, ref, sl):
        cut = ref.shape[1] * TURN // 8
        total = lax.dot_general(lhs[:, :cut], ref[sl, :cut], NT, preferred_element_type=F32)
        for k in range(cut, ref.shape[1], TILE):
            turned = [ref[pl.ds(sl.start + q, TILE), k:k + TILE].T for q in range(0, BLK, TILE)]
            total += jnp.dot(lhs[:, k:k + TILE], jnp.concatenate(turned, axis=1), preferred_element_type=F32)
        return total

    def back_product(u, v, swapped):
        both_arrived(BWD, u, v)

        def fn(slices):
            lhs = pair(flow, BWD, u, v)
            for sl in slices:
                if swapped:
                    e = jnp.dot(lhs, wa[:, sl], preferred_element_type=F32)
                else:
                    e = across(lhs, wb, sl)
                act[BWD, u, :, sl] = (e[:tok] * slope[u, :, sl]).astype(BF16)
                act[BWD, v, :, sl] = (e[tok:] * slope[v, :, sl]).astype(BF16)
        blocks(d_ff, UP_GROUP if swapped else TURN_GROUP, fn)

        def out(w):
            keep(flow.at[BWD, w], g_out, w, 1)
            keep(act.at[BWD, w], d_out, w, 3)
        kept(u, v, out)

    def part_copy(kind, u, j):
        slot = lax.rem(u, SLOTS)
        return pltpu.make_async_remote_copy(part.at[kind, slot, j, other], recv.at[kind, u, j], part_send.at[kind, slot, j],
                                            recv_sem.at[kind, u, j], device_id=peer(stage, other), device_id_type=MESH)

    def direct_copy(u, j, half):
        slot = lax.rem(u, SLOTS)
        if half is side:
            return pltpu.make_async_remote_copy(part.at[BWD, slot, j, side], direct.at[u, j], direct_send.at[slot, j],
                                                direct_sem.at[0, u, j], device_id=peer(stage - 1, side), device_id_type=MESH)
        return pltpu.make_async_remote_copy(part.at[BWD, slot, j, other], recv.at[FWD, u, j], part_send.at[BWD, slot, j],
                                            direct_sem.at[1, u, j], device_id=peer(stage - 1, other), device_id_type=MESH)

    def take_direct(first, count):
        def body(i, carry):
            u = first + i
            for j in range(n_blk):
                sl = pl.ds(j * BLK, BLK)
                wait_bytes(direct.at[u, j], direct_sem.at[0, u, j])
                wait_bytes(recv.at[FWD, u, j], direct_sem.at[1, u, j])
                flow[BWD, u, side, :, sl] = (direct[u, j] + recv[FWD, u, j]).astype(BF16)
                pltpu.make_async_remote_copy(flow.at[BWD, u, side, :, sl], flow.at[BWD, u, side, :, sl], cross_send.at[0],
                                             flow_sem.at[BWD, u, side], device_id=peer(stage, other), device_id_type=MESH).start()
            return carry
        lax.fori_loop(0, count, body, 0)

    def down_product(kind, u, v, straight):
        def free(w):
            @pl.when(w >= SLOTS)
            def _():
                for j in range(n_blk):
                    part_copy(kind, w - SLOTS, j).wait_send()

            if not straight:
                @pl.when((w >= SLOTS) & (w < SLOTS + DIRECT))
                def _():
                    for j in range(n_blk):
                        direct_copy(w - SLOTS, j, side).wait_send()
        kept(u, v, free)

        def body(t, carry):
            lhs = pair(act, kind, u, v)
            for k in range(DOWN_GROUP):
                j = t * DOWN_GROUP + k
                sl = pl.ds(pl.multiple_of(j * BLK, BLK), BLK)
                if straight:
                    p = jnp.dot(lhs, wb[:, sl], preferred_element_type=F32)
                else:
                    p = across(lhs, wa, sl)
                p = p.reshape(2, INNER, rows, BLK)
                part[kind, lax.rem(u, SLOTS), j] = p[0]
                part[kind, lax.rem(v, SLOTS), j] = p[1]

            def go(w):
                if straight:
                    for k in range(DOWN_GROUP):
                        part_copy(kind, w, t * DOWN_GROUP + k).start()
                    return

                @pl.when(w >= DIRECT)
                def _():
                    for k in range(DOWN_GROUP):
                        part_copy(kind, w, t * DOWN_GROUP + k).start()

                @pl.when(w < DIRECT)
                def _():
                    for k in range(DOWN_GROUP):
                        j = t * DOWN_GROUP + k
                        sl = pl.ds(pl.multiple_of(j * BLK, BLK), BLK)
                        part[BWD, lax.rem(w, SLOTS), j, side] += flow[BWD, w, side, :, sl].astype(F32)
                    for k in range(DOWN_GROUP):
                        for half in (side, other):
                            direct_copy(w, t * DOWN_GROUP + k, half).start()
            kept(u, v, go)
            return carry
        lax.fori_loop(0, n_blk // DOWN_GROUP, body, 0)

    def hand_on(kind, first, count):
        target = stage + 1 if kind == FWD else stage - 1
        inside = stage < STAGES - 1 if kind == FWD else stage > 0
        out = STAGES - 1 if kind == FWD else 0

        def body(i, carry):
            u = first + i
            slot = lax.rem(u, SLOTS)
            for j in range(n_blk):
                sl = pl.ds(j * BLK, BLK)
                wait_bytes(recv.at[kind, u, j], recv_sem.at[kind, u, j])
                total = flow[kind, u, side, :, sl].astype(F32) + (part[kind, slot, j, side] + recv[kind, u, j])
                send[kind, u, :, sl] = total.astype(BF16)

                @pl.when(inside)
                def _():
                    for half in (other, side):
                        pltpu.make_async_remote_copy(send.at[kind, u, :, sl], flow.at[kind, u, side, :, sl], flow_send.at[kind],
                                                     flow_sem.at[kind, u, side], device_id=peer(target, half), device_id_type=MESH).start()

            @pl.when(jnp.logical_and(jnp.logical_not(inside), home_of(u) != out))
            def _():
                pltpu.make_async_remote_copy(send.at[kind, u], home.at[kind, slot_of(u)], home_send.at[kind, u],
                                             home_sem.at[kind, slot_of(u)], device_id=peer(home_of(u), side), device_id_type=MESH).start()
            return carry
        lax.fori_loop(0, count, body, 0)

    def swap_weights():
        n_i = d_model // TILE

        def body(t, carry):
            i = pl.multiple_of(lax.rem(t, n_i) * TILE, TILE)
            j = pl.multiple_of(lax.div(t, n_i) * TILE, TILE)
            up = wa[pl.ds(i, TILE), pl.ds(j, TILE)]
            down = wb[pl.ds(j, TILE), pl.ds(i, TILE)]
            wa[pl.ds(i, TILE), pl.ds(j, TILE)] = down.T
            wb[pl.ds(j, TILE), pl.ds(i, TILE)] = up.T
            return carry
        lax.fori_loop(0, n_i * (d_ff // TILE), body, 0)

    def prepare_last():
        half = UNITS // 2

        def quarter(q, carry):
            for i in range(half):
                arrived(BWD, q * half + i)
                keep(flow.at[BWD, q * half + i], g_out, q * half + i, 1)
            units = pl.ds(q * half, half)

            def fn(slices):
                lhs = flow[BWD, units].reshape(half * tok, d_model)
                for sl in slices:
                    e = lax.dot_general(lhs, wb[sl, :], NT, preferred_element_type=F32)
                    slope[units, :, sl] = e.reshape(half, tok, BLK)
            blocks(d_ff, 1, fn)
            return carry
        lax.fori_loop(0, 2, quarter, 0)
        load_a.wait()
        n_i = d_model // TILE

        def body(t, carry):
            i = pl.multiple_of(lax.rem(t, n_i) * TILE, TILE)
            j = pl.multiple_of(lax.div(t, n_i) * TILE, TILE)
            wb[pl.ds(j, TILE), pl.ds(i, TILE)] = wa[pl.ds(i, TILE), pl.ds(j, TILE)].T
            return carry
        lax.fori_loop(0, n_i * (d_ff // TILE), body, 0)

    def step(t, carry):
        group, place = lax.div(t, 3), lax.rem(t, 3)
        word = words[0]
        for i, w in enumerate(words[1:], 1):
            word = jnp.where(group == i, w, word)
        code = lax.rem(lax.div(word, jnp.where(place == 0, 1, jnp.where(place == 1, PACK, PACK * PACK))), PACK)
        op = lax.rem(code, 32)
        u = lax.rem(lax.div(code, 32), UNITS)
        count = lax.div(code, 256) + 1

        def on(want):
            return pl.when(op == want)

        v = jnp.minimum(u + count - 1, UNITS - 1)

        @pl.when(op <= T1)
        def _():
            @on(F1)
            def _():
                up_product(u, v, False)

            @on(M1)
            def _():
                up_product(u, v, True)

            @on(B1)
            def _():
                back_product(u, v, True)

            @on(T1)
            def _():
                back_product(u, v, False)

        @pl.when((op > T1) & (op <= T2))
        def _():
            @pl.when(op < T2)
            def _():
                down_product(jnp.where(op == F2, FWD, BWD), u, v, True)

            @on(T2)
            def _():
                down_product(BWD, u, v, False)

        @pl.when((op > T2) & (op <= HB))
        def _():
            @on(FR)
            def _():
                hand_on(FWD, u, count)

            @on(BR)
            def _():
                hand_on(BWD, u, count)

            @on(HB)
            def _():
                take_direct(u, count)

        @pl.when(op > HB)
        def _():
            @on(SW)
            def _():
                swap_weights()

            @on(PR)
            def _():
                prepare_last()

            @on(YL)
            def _():
                load_b.start()
                load_b.wait()

            @on(WA)
            def _():
                load_a.wait()

            @on(WB)
            def _():
                load_b.wait()

            @on(XS)
            def _():
                @pl.when(stage == STAGES - 1)
                def _():
                    for k in range(2):
                        relay(k).start()

                @pl.when(stage < 2)
                def _():
                    hand_in(FWD, 0, 1, 1)
                stagings[BWD].wait()
                for k in range(2):
                    for lane in range(2):
                        hand_in(BWD, STAGES - 1, k, lane)

            @on(XR)
            def _():
                for k in range(2):
                    wait_bytes(home.at[FWD, k], relay_sem.at[k])
                    relayed(k).start()

            @on(XW)
            def _():
                for kind, target in ((FWD, 0), (BWD, STAGES - 1)):
                    for k in range(2):
                        @pl.when(stage != target)
                        def _():
                            wait_bytes(staged[kind].at[k], in_send.at[kind, k, 0])
                        wait_bytes(staged[kind].at[k], in_send.at[kind, k, 1])

                @pl.when(stage > 1)
                def _():
                    for k in range(2):
                        relayed(k).wait_send()
        return carry
    lengths = [len(row) for row in PLAN]
    lax.fori_loop(0, jnp.where(stage == 0, lengths[0], jnp.where(stage == 1, lengths[1], jnp.where(stage == 2, lengths[2], lengths[3]))), step, 0)

    for kind, here, out in ((FWD, STAGES - 1, y_out), (BWD, 0, dx_out)):
        for k in range(2):
            @pl.when(stage == here)
            def _():
                pltpu.make_async_copy(send.at[kind, unit_of(k)], out.at[k], out_sem.at[4 + kind]).start()

            @pl.when(stage != here)
            def _():
                wait_bytes(home.at[kind, k], home_sem.at[kind, k])
                pltpu.make_async_copy(home.at[kind, k], out.at[k], out_sem.at[4 + kind]).start()

    for kind in (FWD, BWD):
        for u in range(UNITS - SLOTS, UNITS):
            for j in range(n_blk):
                part_copy(kind, u, j).wait_send()
    for kind, last in ((FWD, STAGES - 1), (BWD, 0)):
        @pl.when((stage != last) & jnp.logical_not((stage == 2) & (kind == BWD)))
        def _():
            wait_bytes(flow.at[kind], flow_send.at[kind])

        @pl.when(stage == last)
        def _():
            for u in range(UNITS):
                if HOMES[u] != last:
                    wait_bytes(send.at[kind, u], home_send.at[kind, u])
    @pl.when(stage == 2)
    def _():
        wait_bytes(flow.at[BWD, pl.ds(0, UNITS - DIRECT)], flow_send.at[BWD])

    @pl.when(stage == 1)
    def _():
        wait_bytes(flow.at[BWD, pl.ds(0, DIRECT), 0], cross_send.at[0])
    for lane, (ref, out) in enumerate(((flow.at[FWD], h_out), (flow.at[BWD], g_out), (act.at[FWD], a_out), (act.at[BWD], d_out),
                                       (home.at[FWD], y_out), (home.at[BWD], dx_out))):
        pltpu.make_async_copy(ref, out, out_sem.at[lane]).wait()


def run_pipeline(x_loc, g_loc, w_one, w_two):
    rows, d_model = x_loc.shape[1:]
    d_ff = w_one.shape[1]
    n_blk = d_model // BLK
    tok = INNER * rows
    hbm = pl.BlockSpec(memory_space=pl.ANY)
    out = lambda *shape: jax.ShapeDtypeStruct(shape, BF16)
    dma = lambda *shape: pltpu.SemaphoreType.DMA(shape)
    return pl.pallas_call(
        pipeline_kernel,
        name='pipeline',
        out_shape=(out(*x_loc.shape), out(*x_loc.shape), out(UNITS, INNER, rows, d_model), out(UNITS, INNER, rows, d_model),
                   out(UNITS, tok, d_ff), out(UNITS, tok, d_ff)),
        in_specs=[hbm] * 4,
        out_specs=(hbm,) * 6,
        scratch_shapes=[
            pltpu.VMEM((d_model, d_ff), BF16),
            pltpu.VMEM((d_ff, d_model), BF16),
            pltpu.VMEM((2, UNITS, INNER, rows, d_model), BF16),
            pltpu.VMEM((2, UNITS, tok, d_ff), BF16),
            pltpu.VMEM((UNITS, tok, d_ff), F32),
            pltpu.VMEM((2, SLOTS, n_blk, INNER, rows, BLK), F32),
            pltpu.VMEM((2, UNITS, n_blk, rows, BLK), F32),
            pltpu.VMEM((2, UNITS, rows, d_model), BF16),
            pltpu.VMEM((2, 2, rows, d_model), BF16),
            pltpu.VMEM((DIRECT, n_blk, rows, BLK), F32),
            dma(2, UNITS, INNER), dma(2, UNITS, n_blk), dma(2, SLOTS, n_blk), dma(2), dma(2, UNITS), dma(2, 2), dma(2, 2, 2), dma(2), dma(2),
            dma(2, DIRECT, n_blk), dma(SLOTS, n_blk), dma(1), dma(2), dma(2), dma(6),
        ],
        compiler_params=pltpu.CompilerParams(collective_id=0, has_side_effects=True, vmem_limit_bytes=67043328),
    )(x_loc, g_loc, w_one, w_two)


GRAD_ROWS, GRAD_COLS, GRAD_PART, GRAD_SLOTS = 1024, 2048, 256, 4


def weight_grad_kernel(h_ref, d_ref, a_ref, g_ref, y_ref, x_ref, up_ref, down_ref, y_out, x_out,
                       h, d, a, g, home, left, right, stage, in_sem, home_sem, out_sem):
    d_model, d_ff = h.shape[1], d.shape[1]
    n_down, n_up, n_col = d_ff // GRAD_ROWS, d_model // GRAD_ROWS, d_ff // GRAD_COLS

    pieces = [a.at[:, pl.ds(t * GRAD_ROWS, GRAD_ROWS)] for t in range(n_down)]
    loads = [(g_ref, g)] + [(a_ref.at[:, pl.ds(t * GRAD_ROWS, GRAD_ROWS)], piece) for t, piece in enumerate(pieces)] + [(h_ref, h), (d_ref, d)]
    loads = [pltpu.make_async_copy(src, dst, in_sem.at[t]) for t, (src, dst) in enumerate(loads)]
    homes = [pltpu.make_async_copy(src, home.at[t], home_sem.at[t]) for t, src in enumerate((y_ref, x_ref))]
    backs = [pltpu.make_async_copy(home.at[t], dst, home_sem.at[t]) for t, dst in enumerate((y_out, x_out))]
    for copy in loads + homes:
        copy.start()

    rows_of = lambda t: pl.ds(t * GRAD_ROWS, GRAD_ROWS)
    blocks = [(a, t, g, 0, down_ref) for t in range(n_down)] + [(h, t, d, c, up_ref) for t in range(n_up) for c in range(n_col)]
    turned = (left, right)
    loads[0].wait()
    loads[1].wait()
    arrived = 2
    turn = -1
    for t, (src, row, other, col, out) in enumerate(blocks):
        slot = t % GRAD_SLOTS
        cols = pl.ds(col * GRAD_COLS, GRAD_COLS)
        after = blocks[t + 1] if t + 1 < len(blocks) else None
        need = (1 + n_down if after is None or after[0] is h else t + 2) + (1 if src is h or (after is not None and after[0] is h) else 0)
        need = min(need, len(loads) - 1) + (1 if src is h else 0)
        while arrived < min(need + 1, len(loads)):
            loads[arrived].wait()
            arrived += 1
        if t >= GRAD_SLOTS:
            pltpu.make_async_copy(stage.at[slot], stage.at[slot], out_sem.at[slot]).wait()
        size = GRAD_PART if after is None or t == 0 else GRAD_ROWS
        for p in range(0, GRAD_ROWS, size):
            if t == 0:
                stage[slot, p:p + size] = lax.dot_general(src[:, p:p + size], other[:, cols], (((0,), (0,)), ((), ())), preferred_element_type=F32)
            else:
                stage[slot, p:p + size] = jnp.dot(turned[turn % 2][p:p + size], other[:, cols], preferred_element_type=F32)
            if p + size == GRAD_ROWS and after is not None and (after[0] is not src or after[1] != row):
                turn += 1
                turned[turn % 2][...] = after[0][:, rows_of(after[1])].T
            for q in range(p, p + size, GRAD_PART):
                pltpu.make_async_copy(stage.at[slot, pl.ds(q, GRAD_PART)], out.at[pl.ds(row * GRAD_ROWS + q, GRAD_PART), cols], out_sem.at[slot]).start()
        if t == 1:
            for copy, back in zip(homes, backs):
                copy.wait()
                back.start()
    for slot in range(GRAD_SLOTS):
        pltpu.make_async_copy(stage.at[slot], stage.at[slot], out_sem.at[slot]).wait()
    for copy in backs:
        copy.wait()


def weight_grads(h, d, a, g, y, dx):
    tokens, d_model = h.shape
    d_ff = d.shape[1]
    n_in = 3 + d_ff // GRAD_ROWS
    hbm = pl.BlockSpec(memory_space=pl.ANY)
    dma = lambda *shape: pltpu.SemaphoreType.DMA(shape)
    like = lambda v: pltpu.VMEM(v.shape, v.dtype)
    return pl.pallas_call(
        weight_grad_kernel,
        name='weight_grads',
        out_shape=(jax.ShapeDtypeStruct((d_model, d_ff), F32), jax.ShapeDtypeStruct((d_ff, d_model), F32),
                   jax.ShapeDtypeStruct(y.shape, BF16), jax.ShapeDtypeStruct(y.shape, BF16)),
        in_specs=[hbm] * 6,
        out_specs=(hbm,) * 4,
        scratch_shapes=[like(h), like(d), like(a), like(g), pltpu.VMEM((2,) + y.shape, BF16), pltpu.VMEM((GRAD_ROWS, tokens), BF16), pltpu.VMEM((GRAD_ROWS, tokens), BF16),
                        pltpu.VMEM((GRAD_SLOTS, GRAD_ROWS, GRAD_COLS), F32),
                        dma(n_in), dma(2), dma(GRAD_SLOTS)],
        compiler_params=pltpu.CompilerParams(vmem_limit_bytes=60 * 1024 * 1024),
    )(h, d, a, g, y, dx)


def solution(mesh):
    tok_spec = P(('data', 'stage', 'inner'))
    up_spec = P(None, ('data', 'stage'), None, 'inner')
    down_spec = P(None, ('data', 'stage'), 'inner', None)

    def device_step(x_loc, g_loc, w_up, w_down):
        y, dx, h, g, a, d = run_pipeline(x_loc, g_loc, w_up[0, 0], w_down[0, 0])
        flat = lambda v: v.reshape(-1, v.shape[-1])
        dw_up, dw_down, y, dx = weight_grads(flat(h), flat(d), flat(a), flat(g), y, dx)
        return y, dx, dw_up[None, None], dw_down[None, None]

    return jax.shard_map(device_step, mesh=mesh, in_specs=(tok_spec, tok_spec, up_spec, down_spec), out_specs=(tok_spec, tok_spec, up_spec, down_spec), check_vma=False)
```

```python
import functools

import jax
import jax.numpy as jnp
from jax import lax
from jax.experimental import pallas as pl
from jax.experimental.pallas import tpu as pltpu
from jax.sharding import PartitionSpec as P

F32 = jnp.float32
BF16 = jnp.bfloat16
MESH = pl.DeviceIdType.MESH

STAGES = 4
INNER = 2
UNITS = 8
SLOTS = 3
DIRECT = 3
BLK = 512
TILE = 256
FWD, BWD = 0, 1
NT = (((1,), (1,)), ((), ()))

F1, M1, B1, T1, F2, B2, T2, FR, BR, HB, SW, PR, YL, WA, WB, XS, XW, XR = range(1, 19)
PLAN = (
    ((WA, 0, 1), (F1, 0, 2), (WB, 0, 1), (XS, 0, 1), (F2, 0, 2), (F1, 2, 2), (FR, 0, 2), (F2, 2, 1),
     (F2, 3, 1), (FR, 2, 1), (F1, 4, 2), (FR, 3, 1), (F2, 4, 2), (FR, 4, 2), (F1, 6, 2), (F2, 6, 1),
     (F2, 7, 1), (FR, 6, 2), (XW, 0, 1), (SW, 0, 1), (B1, 0, 2), (B2, 0, 1), (B2, 1, 1), (B1, 2, 1),
     (B2, 2, 1), (B1, 3, 1), (BR, 0, 2), (B2, 3, 1), (BR, 2, 1), (B1, 4, 2), (B2, 4, 2), (BR, 3, 1),
     (B1, 6, 2), (B2, 6, 1), (BR, 4, 1), (B2, 7, 1), (BR, 5, 3)),
    ((WA, 0, 1), (WB, 0, 1), (XS, 0, 1), (F1, 0, 2), (F2, 0, 1), (F2, 1, 1), (FR, 0, 2), (F1, 2, 2),
     (F2, 2, 1), (F2, 3, 1), (FR, 2, 1), (F1, 4, 2), (FR, 3, 1), (F2, 4, 1), (F2, 5, 1), (FR, 4, 2),
     (F1, 6, 2), (F2, 6, 2), (FR, 6, 2), (XW, 0, 1), (SW, 0, 1), (HB, 0, 2), (B1, 0, 2), (B2, 0, 1),
     (HB, 2, 1), (B2, 1, 1), (BR, 0, 1), (B1, 2, 2), (BR, 1, 1), (B2, 2, 2), (BR, 2, 2), (B1, 4, 1),
     (B1, 5, 1), (B2, 4, 2), (B1, 6, 1), (B2, 6, 1), (BR, 4, 1), (B1, 7, 1), (BR, 5, 1), (B2, 7, 1),
     (BR, 6, 2)),
    ((XR, 0, 1), (WA, 0, 1), (WB, 0, 1), (XS, 0, 1), (XW, 0, 1), (F1, 0, 1), (F2, 0, 1), (F1, 1, 1),
     (FR, 0, 1), (F2, 1, 1), (FR, 1, 1), (F1, 2, 1), (F2, 2, 1), (F1, 3, 1), (F2, 3, 1), (FR, 2, 1),
     (F1, 4, 1), (F1, 5, 1), (FR, 3, 1), (F2, 4, 2), (T1, 0, 2), (F1, 6, 2), (T2, 0, 2), (FR, 4, 1),
     (F2, 6, 2), (FR, 5, 1), (T1, 2, 2), (FR, 6, 2), (T2, 2, 2), (BR, 3, 1), (T1, 4, 2), (T2, 4, 2),
     (T1, 6, 2), (BR, 4, 1), (T2, 6, 2), (BR, 5, 3)),
    ((WB, 0, 1), (XS, 0, 1), (XR, 0, 1), (PR, 0, 1), (XW, 0, 1), (M1, 0, 1), (B2, 0, 1), (BR, 0, 1),
     (M1, 1, 1), (B2, 1, 1), (BR, 1, 1), (M1, 2, 2), (B2, 2, 1), (B2, 3, 1), (BR, 2, 2), (M1, 4, 1),
     (B2, 4, 1), (M1, 5, 1), (B2, 5, 1), (BR, 4, 1), (M1, 6, 2), (BR, 5, 1), (B2, 6, 2), (BR, 6, 2),
     (YL, 0, 1), (F2, 0, 2), (FR, 0, 2), (F2, 2, 1), (F2, 3, 2), (FR, 2, 1), (F2, 5, 1), (FR, 3, 2),
     (F2, 6, 1), (FR, 5, 1), (F2, 7, 1), (FR, 6, 2)),
)


PACK = 1024
UP_GROUP = 8
TURN = 5
TURN_GROUP = 4
DOWN_GROUP = 2


def plan_words():
    rows = [[op + 32 * unit + 256 * (count - 1) for op, unit, count in row] for row in PLAN]
    steps = -(-max(len(row) for row in rows) // 3) * 3
    rows = [row + [0] * (steps - len(row)) for row in rows]
    return [[row[t] + PACK * row[t + 1] + PACK * PACK * row[t + 2] for t in range(0, steps, 3)] for row in rows]


def gelu_pair(pre_act):
    root = pre_act * 0.7071067811865476
    normal_cdf = 0.5 * (1.0 + lax.erf(root))
    normal_pdf = jnp.exp2(root * root * -1.4426950408889634) * 0.3989422804014327
    return pre_act * normal_cdf, normal_cdf + pre_act * normal_pdf


def wait_bytes(ref, sem):
    pltpu.make_async_copy(ref, ref, sem).wait()


def pipeline_kernel(x_ref, g_ref, w1_ref, w2_ref,
                    y_out, dx_out, h_out, g_out, a_out, d_out,
                    wa, wb, flow, act, slope, part, recv, send, home, direct,
                    flow_sem, recv_sem, part_send, flow_send, home_send, home_sem, in_send, relay_sem, relay_send,
                    direct_sem, direct_send, cross_send, stage_sem, w_sem, out_sem):
    stage = lax.axis_index('stage')
    side = lax.axis_index('inner')
    other = 1 - side
    rows, d_model = flow.shape[3:]
    tok, d_ff = act.shape[2:]
    n_blk = d_model // BLK

    def peer(s, i):
        return {'stage': s, 'inner': i}

    load_a = pltpu.make_async_copy(w1_ref, wa, w_sem.at[0])
    load_b = pltpu.make_async_copy(w2_ref, wb, w_sem.at[1])

    def unit_of(k):
        return jnp.where(stage < 2, stage + (7 - 2 * stage) * k, 2 * stage - 2 + k)

    staged = (send.at[BWD, pl.ds(UNITS - 2, 2)], send.at[BWD, pl.ds(UNITS - 4, 2)])
    stagings = [pltpu.make_async_copy(src, dst, stage_sem.at[kind]) for kind, (src, dst) in enumerate(zip((x_ref, g_ref), staged))]
    for kind, target in ((FWD, 0), (BWD, STAGES - 1)):
        stagings[kind].start()

        @pl.when(stage == target)
        def _():
            for k in range(2):
                pltpu.make_async_copy((x_ref, g_ref)[kind].at[k], flow.at[kind, unit_of(k), side], flow_sem.at[kind, unit_of(k)]).start()

    @pl.when(stage < STAGES - 1)
    def _():
        load_a.start()
    load_b.start()

    @pl.when(stage == STAGES - 1)
    def _():
        load_a.start()

    barrier = pltpu.get_barrier_semaphore()
    for s in range(STAGES):
        for i in range(INNER):
            @pl.when(jnp.logical_or(stage != s, side != i))
            def _():
                pl.semaphore_signal(barrier, inc=1, device_id=peer(s, i), device_id_type=MESH)
    pl.semaphore_wait(barrier, STAGES * INNER - 1)

    def home_of(u):
        return jnp.where(u < 2, u, jnp.where(u > 5, 7 - u, (u + 2) // 2))

    def slot_of(u):
        return jnp.where(u < 2, 0, jnp.where(u > 5, 1, lax.rem(u, 2)))

    def hand_in(kind, target, k, lane):
        u = unit_of(k)
        src = staged[kind]
        if lane == 0:
            @pl.when(stage != target)
            def _():
                pltpu.make_async_remote_copy(src.at[k], flow.at[kind, u, side], in_send.at[kind], flow_sem.at[kind, u],
                                             device_id=peer(target, side), device_id_type=MESH).start()
        else:
            pltpu.make_async_remote_copy(src.at[k], flow.at[kind, u, side], in_send.at[kind], flow_sem.at[kind, u],
                                         device_id=peer(target, other), device_id_type=MESH).start()

    def relay(k):
        return pltpu.make_async_remote_copy(staged[FWD].at[k], home.at[FWD, k], in_send.at[FWD], relay_sem.at[k],
                                            device_id=peer(stage, other), device_id_type=MESH)

    def relayed(k):
        u = unit_of(k)
        return pltpu.make_async_remote_copy(home.at[FWD, k], flow.at[FWD, u, other], relay_send.at[k], flow_sem.at[FWD, u],
                                            device_id=peer(0, side), device_id_type=MESH)

    stagings[FWD].wait()
    for k in range(2):
        hand_in(FWD, 0, k, 0)

        if k == 0:
            @pl.when(stage < 2)
            def _():
                hand_in(FWD, 0, k, 1)

        @pl.when(stage == 2)
        def _():
            relay(k).start()
    plan = plan_words()
    words = [jnp.where(stage == 0, a, jnp.where(stage == 1, b, jnp.where(stage == 2, c, d))) for a, b, c, d in zip(*plan)]

    def keep(ref, out, u, lane):
        pltpu.make_async_copy(ref, out.at[u], out_sem.at[lane]).start()

    def blocks(width, group, fn):
        def body(t, carry):
            fn([pl.ds(pl.multiple_of((t * group + k) * BLK, BLK), BLK) for k in range(group)])
            return carry
        lax.fori_loop(0, width // BLK // group, body, 0)

    def arrived(kind, u):
        taken = (stage == 1) & (kind == BWD) & (u < DIRECT)

        @pl.when(jnp.logical_not(taken))
        def _():
            wait_bytes(flow.at[kind, u], flow_sem.at[kind, u])

        @pl.when(taken)
        def _():
            wait_bytes(flow.at[kind, u, other], flow_sem.at[kind, u])

    def both_arrived(kind, u, v):
        arrived(kind, u)

        @pl.when(v != u)
        def _():
            arrived(kind, v)

    def pair(ref, kind, u, v):
        width = ref.shape[-1]
        return jnp.concatenate([ref[kind, u].reshape(tok, width), ref[kind, v].reshape(tok, width)], axis=0)

    def kept(u, v, fn):
        fn(u)

        @pl.when(v != u)
        def _():
            fn(v)

    def up_product(u, v, last):
        both_arrived(FWD, u, v)

        def fn(slices):
            lhs = pair(flow, FWD, u, v)
            for sl in slices:
                z = jnp.dot(lhs, wa[:, sl], preferred_element_type=F32)
                value, grad = gelu_pair(z)
                value = value.astype(BF16)
                if last:
                    act[BWD, u, :, sl] = (slope[u, :, sl] * grad[:tok]).astype(BF16)
                    act[BWD, v, :, sl] = (slope[v, :, sl] * grad[tok:]).astype(BF16)
                else:
                    slope[u, :, sl] = grad[:tok]
                    slope[v, :, sl] = grad[tok:]
                act[FWD, u, :, sl] = value[:tok]
                act[FWD, v, :, sl] = value[tok:]
        blocks(d_ff, UP_GROUP, fn)

        def out(w):
            keep(flow.at[FWD, w], h_out, w, 0)
            keep(act.at[FWD, w], a_out, w, 2)
            if last:
                keep(act.at[BWD, w], d_out, w, 3)
        kept(u, v, out)

    def across(lhs, ref, sl):
        cut = ref.shape[1] * TURN // 8
        total = lax.dot_general(lhs[:, :cut], ref[sl, :cut], NT, preferred_element_type=F32)
        for k in range(cut, ref.shape[1], TILE):
            turned = [ref[pl.ds(sl.start + q, TILE), k:k + TILE].T for q in range(0, BLK, TILE)]
            total += jnp.dot(lhs[:, k:k + TILE], jnp.concatenate(turned, axis=1), preferred_element_type=F32)
        return total

    def back_product(u, v, swapped):
        both_arrived(BWD, u, v)

        def fn(slices):
            lhs = pair(flow, BWD, u, v)
            for sl in slices:
                if swapped:
                    e = jnp.dot(lhs, wa[:, sl], preferred_element_type=F32)
                else:
                    e = across(lhs, wb, sl)
                act[BWD, u, :, sl] = (e[:tok] * slope[u, :, sl]).astype(BF16)
                act[BWD, v, :, sl] = (e[tok:] * slope[v, :, sl]).astype(BF16)
        blocks(d_ff, UP_GROUP if swapped else TURN_GROUP, fn)

        def out(w):
            keep(flow.at[BWD, w], g_out, w, 1)
            keep(act.at[BWD, w], d_out, w, 3)
        kept(u, v, out)

    def group(t):
        return pl.ds(t * DOWN_GROUP, DOWN_GROUP)

    def part_copy(kind, u, t):
        slot = lax.rem(u, SLOTS)
        return pltpu.make_async_remote_copy(part.at[kind, slot, group(t), other], recv.at[kind, u, group(t)], part_send.at[kind, slot],
                                            recv_sem.at[kind, u, t], device_id=peer(stage, other), device_id_type=MESH)

    def direct_copy(u, t, half):
        slot = lax.rem(u, SLOTS)
        if half is side:
            return pltpu.make_async_remote_copy(part.at[BWD, slot, group(t), side], direct.at[u, group(t)], direct_send.at[slot],
                                                direct_sem.at[0, u, t], device_id=peer(stage - 1, side), device_id_type=MESH)
        return pltpu.make_async_remote_copy(part.at[BWD, slot, group(t), other], recv.at[FWD, u, group(t)], part_send.at[BWD, slot],
                                            direct_sem.at[1, u, t], device_id=peer(stage - 1, other), device_id_type=MESH)

    def take_direct(first, count):
        def body(i, carry):
            u = first + i
            for j in range(n_blk):
                sl = pl.ds(j * BLK, BLK)
                if j % DOWN_GROUP == 0:
                    t = j // DOWN_GROUP
                    wait_bytes(direct.at[u, group(t)], direct_sem.at[0, u, t])
                    wait_bytes(recv.at[FWD, u, group(t)], direct_sem.at[1, u, t])
                flow[BWD, u, side, :, sl] = (direct[u, j] + recv[FWD, u, j]).astype(BF16)
                pltpu.make_async_remote_copy(flow.at[BWD, u, side, :, sl], flow.at[BWD, u, side, :, sl], cross_send.at[0],
                                             flow_sem.at[BWD, u], device_id=peer(stage, other), device_id_type=MESH).start()
            return carry
        lax.fori_loop(0, count, body, 0)

    def down_product(kind, u, v, straight):
        def free(w):
            @pl.when(w >= SLOTS)
            def _():
                wait_bytes(recv.at[kind, w - SLOTS], part_send.at[kind, lax.rem(w, SLOTS)])

            if not straight:
                @pl.when((w >= SLOTS) & (w < SLOTS + DIRECT))
                def _():
                    wait_bytes(direct.at[w - SLOTS], direct_send.at[lax.rem(w, SLOTS)])
        kept(u, v, free)

        def body(t, carry):
            lhs = pair(act, kind, u, v)
            for k in range(DOWN_GROUP):
                j = t * DOWN_GROUP + k
                sl = pl.ds(pl.multiple_of(j * BLK, BLK), BLK)
                if straight:
                    p = jnp.dot(lhs, wb[:, sl], preferred_element_type=F32)
                else:
                    p = across(lhs, wa, sl)
                p = p.reshape(2, INNER, rows, BLK)
                part[kind, lax.rem(u, SLOTS), j] = p[0]
                part[kind, lax.rem(v, SLOTS), j] = p[1]

            def go(w):
                if straight:
                    part_copy(kind, w, t).start()
                    return

                @pl.when(w >= DIRECT)
                def _():
                    part_copy(kind, w, t).start()

                @pl.when(w < DIRECT)
                def _():
                    for k in range(DOWN_GROUP):
                        j = t * DOWN_GROUP + k
                        sl = pl.ds(pl.multiple_of(j * BLK, BLK), BLK)
                        part[BWD, lax.rem(w, SLOTS), j, side] += flow[BWD, w, side, :, sl].astype(F32)
                    for half in (side, other):
                        direct_copy(w, t, half).start()
            kept(u, v, go)
            return carry
        lax.fori_loop(0, n_blk // DOWN_GROUP, body, 0)

    def hand_on(kind, first, count):
        target = stage + 1 if kind == FWD else stage - 1
        inside = stage < STAGES - 1 if kind == FWD else stage > 0
        out = STAGES - 1 if kind == FWD else 0

        def body(i, carry):
            u = first + i
            slot = lax.rem(u, SLOTS)
            for j in range(n_blk):
                sl = pl.ds(j * BLK, BLK)
                if j % DOWN_GROUP == 0:
                    wait_bytes(recv.at[kind, u, group(j // DOWN_GROUP)], recv_sem.at[kind, u, j // DOWN_GROUP])
                total = flow[kind, u, side, :, sl].astype(F32) + (part[kind, slot, j, side] + recv[kind, u, j])
                send[kind, u, :, sl] = total.astype(BF16)

                @pl.when(inside)
                def _():
                    for half in (other, side):
                        pltpu.make_async_remote_copy(send.at[kind, u, :, sl], flow.at[kind, u, side, :, sl], flow_send.at[kind],
                                                     flow_sem.at[kind, u], device_id=peer(target, half), device_id_type=MESH).start()

            @pl.when(jnp.logical_and(jnp.logical_not(inside), home_of(u) != out))
            def _():
                pltpu.make_async_remote_copy(send.at[kind, u], home.at[kind, slot_of(u)], home_send.at[kind],
                                             home_sem.at[kind, slot_of(u)], device_id=peer(home_of(u), side), device_id_type=MESH).start()
            return carry
        lax.fori_loop(0, count, body, 0)

    def swap_weights():
        n_i = d_model // TILE

        def body(t, carry):
            i = pl.multiple_of(lax.rem(t, n_i) * TILE, TILE)
            j = pl.multiple_of(lax.div(t, n_i) * TILE, TILE)
            up = wa[pl.ds(i, TILE), pl.ds(j, TILE)]
            down = wb[pl.ds(j, TILE), pl.ds(i, TILE)]
            wa[pl.ds(i, TILE), pl.ds(j, TILE)] = down.T
            wb[pl.ds(j, TILE), pl.ds(i, TILE)] = up.T
            return carry
        lax.fori_loop(0, n_i * (d_ff // TILE), body, 0)

    def prepare_last():
        half = UNITS // 2

        def quarter(q, carry):
            for i in range(half):
                arrived(BWD, q * half + i)
                keep(flow.at[BWD, q * half + i], g_out, q * half + i, 1)
            units = pl.ds(q * half, half)

            def fn(slices):
                lhs = flow[BWD, units].reshape(half * tok, d_model)
                for sl in slices:
                    e = lax.dot_general(lhs, wb[sl, :], NT, preferred_element_type=F32)
                    slope[units, :, sl] = e.reshape(half, tok, BLK)
            blocks(d_ff, 1, fn)
            return carry
        lax.fori_loop(0, 2, quarter, 0)
        load_a.wait()
        n_i = d_model // TILE

        def body(t, carry):
            i = pl.multiple_of(lax.rem(t, n_i) * TILE, TILE)
            j = pl.multiple_of(lax.div(t, n_i) * TILE, TILE)
            wb[pl.ds(j, TILE), pl.ds(i, TILE)] = wa[pl.ds(i, TILE), pl.ds(j, TILE)].T
            return carry
        lax.fori_loop(0, n_i * (d_ff // TILE), body, 0)

    def step(t, carry):
        group, place = lax.div(t, 3), lax.rem(t, 3)
        word = words[0]
        for i, w in enumerate(words[1:], 1):
            word = jnp.where(group == i, w, word)
        code = lax.rem(lax.div(word, jnp.where(place == 0, 1, jnp.where(place == 1, PACK, PACK * PACK))), PACK)
        op = lax.rem(code, 32)
        u = lax.rem(lax.div(code, 32), UNITS)
        count = lax.div(code, 256) + 1

        def on(want):
            return pl.when(op == want)

        v = jnp.minimum(u + count - 1, UNITS - 1)

        @pl.when(op <= T1)
        def _():
            @on(F1)
            def _():
                up_product(u, v, False)

            @on(M1)
            def _():
                up_product(u, v, True)

            @on(B1)
            def _():
                back_product(u, v, True)

            @on(T1)
            def _():
                back_product(u, v, False)

        @pl.when((op > T1) & (op <= T2))
        def _():
            @pl.when(op < T2)
            def _():
                down_product(jnp.where(op == F2, FWD, BWD), u, v, True)

            @on(T2)
            def _():
                down_product(BWD, u, v, False)

        @pl.when((op > T2) & (op <= HB))
        def _():
            @on(FR)
            def _():
                hand_on(FWD, u, count)

            @on(BR)
            def _():
                hand_on(BWD, u, count)

            @on(HB)
            def _():
                take_direct(u, count)

        @pl.when(op > HB)
        def _():
            @on(SW)
            def _():
                swap_weights()

            @on(PR)
            def _():
                prepare_last()

            @on(YL)
            def _():
                load_b.start()
                load_b.wait()

            @on(WA)
            def _():
                load_a.wait()

            @on(WB)
            def _():
                load_b.wait()

            @on(XS)
            def _():
                @pl.when(stage == STAGES - 1)
                def _():
                    for k in range(2):
                        relay(k).start()

                @pl.when(stage < 2)
                def _():
                    hand_in(FWD, 0, 1, 1)
                stagings[BWD].wait()
                for k in range(2):
                    for lane in range(2):
                        hand_in(BWD, STAGES - 1, k, lane)

            @on(XR)
            def _():
                for k in range(2):
                    wait_bytes(home.at[FWD, k], relay_sem.at[k])
                    relayed(k).start()

            @on(XW)
            def _():
                for kind, target in ((FWD, 0), (BWD, STAGES - 1)):
                    @pl.when(stage != target)
                    def _():
                        wait_bytes(send.at[BWD, pl.ds(UNITS - 4, 4)], in_send.at[kind])

                    @pl.when(stage == target)
                    def _():
                        wait_bytes(staged[kind], in_send.at[kind])

                @pl.when(stage > 1)
                def _():
                    for k in range(2):
                        relayed(k).wait_send()
        return carry
    lengths = [len(row) for row in PLAN]
    lax.fori_loop(0, jnp.where(stage == 0, lengths[0], jnp.where(stage == 1, lengths[1], jnp.where(stage == 2, lengths[2], lengths[3]))), step, 0)

    for kind, here, out in ((FWD, STAGES - 1, y_out), (BWD, 0, dx_out)):
        for k in range(2):
            @pl.when(stage == here)
            def _():
                pltpu.make_async_copy(send.at[kind, unit_of(k)], out.at[k], out_sem.at[4 + kind]).start()

            @pl.when(stage != here)
            def _():
                wait_bytes(home.at[kind, k], home_sem.at[kind, k])
                pltpu.make_async_copy(home.at[kind, k], out.at[k], out_sem.at[4 + kind]).start()

    for kind in (FWD, BWD):
        for u in range(UNITS - SLOTS, UNITS):
            wait_bytes(recv.at[kind, u], part_send.at[kind, u % SLOTS])
    for kind, last in ((FWD, STAGES - 1), (BWD, 0)):
        @pl.when((stage != last) & jnp.logical_not((stage == 2) & (kind == BWD)))
        def _():
            wait_bytes(flow.at[kind], flow_send.at[kind])

        @pl.when(stage == last)
        def _():
            wait_bytes(send.at[kind, pl.ds(0, UNITS - 2)], home_send.at[kind])

    @pl.when(stage == 2)
    def _():
        wait_bytes(flow.at[BWD, pl.ds(0, UNITS - DIRECT)], flow_send.at[BWD])

    @pl.when(stage == 1)
    def _():
        wait_bytes(flow.at[BWD, pl.ds(0, DIRECT), 0], cross_send.at[0])
    for lane, (ref, out) in enumerate(((flow.at[FWD], h_out), (flow.at[BWD], g_out), (act.at[FWD], a_out), (act.at[BWD], d_out),
                                       (home.at[FWD], y_out), (home.at[BWD], dx_out))):
        pltpu.make_async_copy(ref, out, out_sem.at[lane]).wait()


def run_pipeline(x_loc, g_loc, w_one, w_two):
    rows, d_model = x_loc.shape[1:]
    d_ff = w_one.shape[1]
    n_blk = d_model // BLK
    tok = INNER * rows
    hbm = pl.BlockSpec(memory_space=pl.ANY)
    out = lambda *shape: jax.ShapeDtypeStruct(shape, BF16)
    dma = lambda *shape: pltpu.SemaphoreType.DMA(shape)
    return pl.pallas_call(
        pipeline_kernel,
        name='pipeline',
        out_shape=(out(*x_loc.shape), out(*x_loc.shape), out(UNITS, INNER, rows, d_model), out(UNITS, INNER, rows, d_model),
                   out(UNITS, tok, d_ff), out(UNITS, tok, d_ff)),
        in_specs=[hbm] * 4,
        out_specs=(hbm,) * 6,
        scratch_shapes=[
            pltpu.VMEM((d_model, d_ff), BF16),
            pltpu.VMEM((d_ff, d_model), BF16),
            pltpu.VMEM((2, UNITS, INNER, rows, d_model), BF16),
            pltpu.VMEM((2, UNITS, tok, d_ff), BF16),
            pltpu.VMEM((UNITS, tok, d_ff), F32),
            pltpu.VMEM((2, SLOTS, n_blk, INNER, rows, BLK), F32),
            pltpu.VMEM((2, UNITS, n_blk, rows, BLK), F32),
            pltpu.VMEM((2, UNITS, rows, d_model), BF16),
            pltpu.VMEM((2, 2, rows, d_model), BF16),
            pltpu.VMEM((DIRECT, n_blk, rows, BLK), F32),
            dma(2, UNITS), dma(2, UNITS, n_blk // DOWN_GROUP), dma(2, SLOTS), dma(2), dma(2), dma(2, 2), dma(2), dma(2), dma(2),
            dma(2, DIRECT, n_blk // DOWN_GROUP), dma(SLOTS), dma(1), dma(2), dma(2), dma(6),
        ],
        compiler_params=pltpu.CompilerParams(collective_id=0, has_side_effects=True, vmem_limit_bytes=67043328),
    )(x_loc, g_loc, w_one, w_two)


GRAD_ROWS, GRAD_COLS, GRAD_PART, GRAD_SLOTS = 1024, 2048, 256, 4


def weight_grad_kernel(h_ref, d_ref, a_ref, g_ref, y_ref, x_ref, up_ref, down_ref, y_out, x_out,
                       h, d, a, g, home, left, right, stage, in_sem, home_sem, out_sem):
    d_model, d_ff = h.shape[1], d.shape[1]
    n_down, n_up, n_col = d_ff // GRAD_ROWS, d_model // GRAD_ROWS, d_ff // GRAD_COLS

    pieces = [a.at[:, pl.ds(t * GRAD_ROWS, GRAD_ROWS)] for t in range(n_down)]
    loads = [(g_ref, g)] + [(a_ref.at[:, pl.ds(t * GRAD_ROWS, GRAD_ROWS)], piece) for t, piece in enumerate(pieces)] + [(h_ref, h), (d_ref, d)]
    loads = [pltpu.make_async_copy(src, dst, in_sem.at[t]) for t, (src, dst) in enumerate(loads)]
    homes = [pltpu.make_async_copy(src, home.at[t], home_sem.at[t]) for t, src in enumerate((y_ref, x_ref))]
    backs = [pltpu.make_async_copy(home.at[t], dst, home_sem.at[t]) for t, dst in enumerate((y_out, x_out))]
    for copy in loads + homes:
        copy.start()

    rows_of = lambda t: pl.ds(t * GRAD_ROWS, GRAD_ROWS)
    blocks = [(a, t, g, 0, down_ref) for t in range(n_down)] + [(h, t, d, c, up_ref) for t in range(n_up) for c in range(n_col)]
    turned = (left, right)
    loads[0].wait()
    loads[1].wait()
    arrived = 2
    turn = -1
    for t, (src, row, other, col, out) in enumerate(blocks):
        slot = t % GRAD_SLOTS
        cols = pl.ds(col * GRAD_COLS, GRAD_COLS)
        after = blocks[t + 1] if t + 1 < len(blocks) else None
        need = (1 + n_down if after is None or after[0] is h else t + 2) + (1 if src is h or (after is not None and after[0] is h) else 0)
        need = min(need, len(loads) - 1) + (1 if src is h else 0)
        while arrived < min(need + 1, len(loads)):
            loads[arrived].wait()
            arrived += 1
        if t >= GRAD_SLOTS:
            pltpu.make_async_copy(stage.at[slot], stage.at[slot], out_sem.at[slot]).wait()
        size = GRAD_PART if after is None or t == 0 else GRAD_ROWS
        for p in range(0, GRAD_ROWS, size):
            if t == 0:
                stage[slot, p:p + size] = lax.dot_general(src[:, p:p + size], other[:, cols], (((0,), (0,)), ((), ())), preferred_element_type=F32)
            else:
                stage[slot, p:p + size] = jnp.dot(turned[turn % 2][p:p + size], other[:, cols], preferred_element_type=F32)
            if p + size == GRAD_ROWS and after is not None and (after[0] is not src or after[1] != row):
                turn += 1
                turned[turn % 2][...] = after[0][:, rows_of(after[1])].T
            for q in range(p, p + size, GRAD_PART):
                pltpu.make_async_copy(stage.at[slot, pl.ds(q, GRAD_PART)], out.at[pl.ds(row * GRAD_ROWS + q, GRAD_PART), cols], out_sem.at[slot]).start()
        if t == 1:
            for copy, back in zip(homes, backs):
                copy.wait()
                back.start()
    for slot in range(GRAD_SLOTS):
        pltpu.make_async_copy(stage.at[slot], stage.at[slot], out_sem.at[slot]).wait()
    for copy in backs:
        copy.wait()


def weight_grads(h, d, a, g, y, dx):
    tokens, d_model = h.shape
    d_ff = d.shape[1]
    n_in = 3 + d_ff // GRAD_ROWS
    hbm = pl.BlockSpec(memory_space=pl.ANY)
    dma = lambda *shape: pltpu.SemaphoreType.DMA(shape)
    like = lambda v: pltpu.VMEM(v.shape, v.dtype)
    return pl.pallas_call(
        weight_grad_kernel,
        name='weight_grads',
        out_shape=(jax.ShapeDtypeStruct((d_model, d_ff), F32), jax.ShapeDtypeStruct((d_ff, d_model), F32),
                   jax.ShapeDtypeStruct(y.shape, BF16), jax.ShapeDtypeStruct(y.shape, BF16)),
        in_specs=[hbm] * 6,
        out_specs=(hbm,) * 4,
        scratch_shapes=[like(h), like(d), like(a), like(g), pltpu.VMEM((2,) + y.shape, BF16), pltpu.VMEM((GRAD_ROWS, tokens), BF16), pltpu.VMEM((GRAD_ROWS, tokens), BF16),
                        pltpu.VMEM((GRAD_SLOTS, GRAD_ROWS, GRAD_COLS), F32),
                        dma(n_in), dma(2), dma(GRAD_SLOTS)],
        compiler_params=pltpu.CompilerParams(vmem_limit_bytes=60 * 1024 * 1024),
    )(h, d, a, g, y, dx)


def solution(mesh):
    tok_spec = P(('data', 'stage', 'inner'))
    up_spec = P(None, ('data', 'stage'), None, 'inner')
    down_spec = P(None, ('data', 'stage'), 'inner', None)

    def device_step(x_loc, g_loc, w_up, w_down):
        y, dx, h, g, a, d = run_pipeline(x_loc, g_loc, w_up[0, 0], w_down[0, 0])
        flat = lambda v: v.reshape(-1, v.shape[-1])
        dw_up, dw_down, y, dx = weight_grads(flat(h), flat(d), flat(a), flat(g), y, dx)
        return y, dx, dw_up[None, None], dw_down[None, None]

    return jax.shard_map(device_step, mesh=mesh, in_specs=(tok_spec, tok_spec, up_spec, down_spec), out_specs=(tok_spec, tok_spec, up_spec, down_spec), check_vma=False)
```

```python
import functools

import jax
import jax.numpy as jnp
from jax import lax
from jax.experimental import pallas as pl
from jax.experimental.pallas import tpu as pltpu
from jax.sharding import PartitionSpec as P

F32 = jnp.float32
BF16 = jnp.bfloat16
MESH = pl.DeviceIdType.MESH

STAGES = 4
INNER = 2
UNITS = 8
SLOTS = 3
DIRECT = 3
BLK = 512
TILE = 256
FWD, BWD = 0, 1
NT = (((1,), (1,)), ((), ()))

F1, M1, B1, T1, F2, B2, T2, FR, BR, HB, SW, PR, YL, WA, WB, XS, XW, XR = range(1, 19)
PLAN = (
    ((WA, 0, 1), (F1, 0, 2), (WB, 0, 1), (XS, 0, 1), (F2, 0, 2), (F1, 2, 2), (FR, 0, 2), (F2, 2, 2),
     (FR, 2, 1), (F1, 4, 2), (FR, 3, 1), (F2, 4, 2), (FR, 4, 2), (F1, 6, 2), (F2, 6, 1), (F2, 7, 1),
     (FR, 6, 2), (XW, 0, 1), (SW, 0, 1), (B1, 0, 2), (B2, 0, 1), (B2, 1, 1), (B1, 2, 1), (B2, 2, 1),
     (B1, 3, 1), (BR, 0, 2), (B2, 3, 1), (BR, 2, 1), (B1, 4, 2), (B2, 4, 2), (BR, 3, 1), (B1, 6, 2),
     (B2, 6, 1), (BR, 4, 1), (B2, 7, 1), (BR, 5, 3)),
    ((WA, 0, 1), (WB, 0, 1), (XS, 0, 1), (F1, 0, 2), (F2, 0, 1), (F2, 1, 1), (FR, 0, 2), (F1, 2, 2),
     (F2, 2, 1), (F2, 3, 1), (FR, 2, 1), (F1, 4, 2), (FR, 3, 1), (F2, 4, 1), (F2, 5, 1), (FR, 4, 2),
     (F1, 6, 2), (F2, 6, 2), (FR, 6, 2), (XW, 0, 1), (SW, 0, 1), (HB, 0, 2), (B1, 0, 2), (B2, 0, 1),
     (HB, 2, 1), (B2, 1, 1), (BR, 0, 1), (B1, 2, 2), (BR, 1, 1), (B2, 2, 2), (BR, 2, 2), (B1, 4, 1),
     (B1, 5, 1), (B2, 4, 2), (B1, 6, 1), (B2, 6, 1), (BR, 4, 1), (B1, 7, 1), (BR, 5, 1), (B2, 7, 1),
     (BR, 6, 2)),
    ((XR, 0, 1), (WA, 0, 1), (WB, 0, 1), (XS, 0, 1), (XW, 0, 1), (F1, 0, 1), (F2, 0, 1), (F1, 1, 1),
     (FR, 0, 1), (F2, 1, 1), (FR, 1, 1), (F1, 2, 1), (F2, 2, 1), (F1, 3, 1), (F2, 3, 1), (FR, 2, 1),
     (F1, 4, 1), (F1, 5, 1), (FR, 3, 1), (F2, 4, 2), (T1, 0, 2), (F1, 6, 2), (T2, 0, 2), (FR, 4, 1),
     (F2, 6, 2), (FR, 5, 1), (T1, 2, 2), (FR, 6, 2), (T2, 2, 2), (BR, 3, 1), (T1, 4, 2), (T2, 4, 2),
     (T1, 6, 2), (BR, 4, 1), (T2, 6, 2), (BR, 5, 3)),
    ((WB, 0, 1), (XS, 0, 1), (XR, 0, 1), (PR, 0, 1), (XW, 0, 1), (M1, 0, 1), (B2, 0, 1), (BR, 0, 1),
     (M1, 1, 1), (B2, 1, 1), (BR, 1, 1), (M1, 2, 2), (B2, 2, 1), (B2, 3, 1), (BR, 2, 2), (M1, 4, 1),
     (B2, 4, 1), (M1, 5, 1), (B2, 5, 1), (BR, 4, 1), (M1, 6, 2), (BR, 5, 1), (B2, 6, 2), (BR, 6, 2),
     (YL, 0, 1), (F2, 0, 2), (FR, 0, 2), (F2, 2, 1), (F2, 3, 2), (FR, 2, 1), (F2, 5, 1), (FR, 3, 2),
     (F2, 6, 1), (FR, 5, 1), (F2, 7, 1), (FR, 6, 2)),
)


PACK = 1024
UP_GROUP = 8
TURN = 5
TURN_GROUP = 4
DOWN_GROUP = 2


def plan_words():
    rows = [[op + 32 * unit + 256 * (count - 1) for op, unit, count in row] for row in PLAN]
    steps = -(-max(len(row) for row in rows) // 3) * 3
    rows = [row + [0] * (steps - len(row)) for row in rows]
    return [[row[t] + PACK * row[t + 1] + PACK * PACK * row[t + 2] for t in range(0, steps, 3)] for row in rows]


def gelu_pair(pre_act):
    root = pre_act * 0.7071067811865476
    normal_cdf = 0.5 * (1.0 + lax.erf(root))
    normal_pdf = jnp.exp2(root * root * -1.4426950408889634) * 0.3989422804014327
    return pre_act * normal_cdf, normal_cdf + pre_act * normal_pdf


def wait_bytes(ref, sem):
    pltpu.make_async_copy(ref, ref, sem).wait()


def pipeline_kernel(x_ref, g_ref, w1_ref, w2_ref,
                    y_out, dx_out, h_out, g_out, a_out, d_out,
                    wa, wb, flow, act, slope, part, recv, send, home, direct,
                    flow_sem, recv_sem, part_send, flow_send, home_send, home_sem, in_send, relay_sem, relay_send,
                    direct_sem, direct_send, cross_send, stage_sem, w_sem, out_sem):
    stage = lax.axis_index('stage')
    side = lax.axis_index('inner')
    other = 1 - side
    rows, d_model = flow.shape[3:]
    tok, d_ff = act.shape[2:]
    n_blk = d_model // BLK

    def peer(s, i):
        return {'stage': s, 'inner': i}

    load_a = pltpu.make_async_copy(w1_ref, wa, w_sem.at[0])
    load_b = pltpu.make_async_copy(w2_ref, wb, w_sem.at[1])

    def unit_of(k):
        return jnp.where(stage < 2, stage + (7 - 2 * stage) * k, 2 * stage - 2 + k)

    staged = (send.at[BWD, pl.ds(UNITS - 2, 2)], send.at[BWD, pl.ds(UNITS - 4, 2)])
    stagings = [pltpu.make_async_copy(src, dst, stage_sem.at[kind]) for kind, (src, dst) in enumerate(zip((x_ref, g_ref), staged))]
    for kind, target in ((FWD, 0), (BWD, STAGES - 1)):
        stagings[kind].start()

        @pl.when(stage == target)
        def _():
            for k in range(2):
                pltpu.make_async_copy((x_ref, g_ref)[kind].at[k], flow.at[kind, unit_of(k), side], flow_sem.at[kind, unit_of(k)]).start()

    @pl.when(stage < STAGES - 1)
    def _():
        load_a.start()
    load_b.start()

    @pl.when(stage == STAGES - 1)
    def _():
        load_a.start()

    barrier = pltpu.get_barrier_semaphore()
    for s in range(STAGES):
        for i in range(INNER):
            @pl.when(jnp.logical_or(stage != s, side != i))
            def _():
                pl.semaphore_signal(barrier, inc=1, device_id=peer(s, i), device_id_type=MESH)
    pl.semaphore_wait(barrier, STAGES * INNER - 1)

    def home_of(u):
        return jnp.where(u < 2, u, jnp.where(u > 5, 7 - u, (u + 2) // 2))

    def slot_of(u):
        return jnp.where(u < 2, 0, jnp.where(u > 5, 1, lax.rem(u, 2)))

    def hand_in(kind, target, k, lane):
        u = unit_of(k)
        src = staged[kind]
        if lane == 0:
            @pl.when(stage != target)
            def _():
                pltpu.make_async_remote_copy(src.at[k], flow.at[kind, u, side], in_send.at[kind], flow_sem.at[kind, u],
                                             device_id=peer(target, side), device_id_type=MESH).start()
        else:
            pltpu.make_async_remote_copy(src.at[k], flow.at[kind, u, side], in_send.at[kind], flow_sem.at[kind, u],
                                         device_id=peer(target, other), device_id_type=MESH).start()

    def relay(k):
        return pltpu.make_async_remote_copy(staged[FWD].at[k], home.at[FWD, k], in_send.at[FWD], relay_sem.at[k],
                                            device_id=peer(stage, other), device_id_type=MESH)

    def relayed(k):
        u = unit_of(k)
        return pltpu.make_async_remote_copy(home.at[FWD, k], flow.at[FWD, u, other], relay_send.at[k], flow_sem.at[FWD, u],
                                            device_id=peer(0, side), device_id_type=MESH)

    stagings[FWD].wait()
    for k in range(2):
        hand_in(FWD, 0, k, 0)

        if k == 0:
            @pl.when(stage < 2)
            def _():
                hand_in(FWD, 0, k, 1)

        @pl.when(stage == 2)
        def _():
            relay(k).start()
    plan = plan_words()
    words = [jnp.where(stage == 0, a, jnp.where(stage == 1, b, jnp.where(stage == 2, c, d))) for a, b, c, d in zip(*plan)]

    def keep(ref, out, u, lane):
        pltpu.make_async_copy(ref, out.at[u], out_sem.at[lane]).start()

    def blocks(width, group, fn):
        def body(t, carry):
            fn([pl.ds(pl.multiple_of((t * group + k) * BLK, BLK), BLK) for k in range(group)])
            return carry
        lax.fori_loop(0, width // BLK // group, body, 0)

    def arrived(kind, u):
        taken = (stage == 1) & (kind == BWD) & (u < DIRECT)

        @pl.when(jnp.logical_not(taken))
        def _():
            wait_bytes(flow.at[kind, u], flow_sem.at[kind, u])

        @pl.when(taken)
        def _():
            wait_bytes(flow.at[kind, u, other], flow_sem.at[kind, u])

    def both_arrived(kind, u, v):
        arrived(kind, u)

        @pl.when(v != u)
        def _():
            arrived(kind, v)

    def pair(ref, kind, u, v):
        width = ref.shape[-1]
        return jnp.concatenate([ref[kind, u].reshape(tok, width), ref[kind, v].reshape(tok, width)], axis=0)

    def kept(u, v, fn):
        fn(u)

        @pl.when(v != u)
        def _():
            fn(v)

    def up_product(u, v, last):
        both_arrived(FWD, u, v)

        def fn(slices):
            lhs = pair(flow, FWD, u, v)
            for sl in slices:
                z = jnp.dot(lhs, wa[:, sl], preferred_element_type=F32)
                value, grad = gelu_pair(z)
                value = value.astype(BF16)
                if last:
                    act[BWD, u, :, sl] = (slope[u, :, sl] * grad[:tok]).astype(BF16)
                    act[BWD, v, :, sl] = (slope[v, :, sl] * grad[tok:]).astype(BF16)
                else:
                    slope[u, :, sl] = grad[:tok]
                    slope[v, :, sl] = grad[tok:]
                act[FWD, u, :, sl] = value[:tok]
                act[FWD, v, :, sl] = value[tok:]
        blocks(d_ff, UP_GROUP, fn)

        def out(w):
            keep(flow.at[FWD, w], h_out, w, 0)
            keep(act.at[FWD, w], a_out, w, 2)
            if last:
                keep(act.at[BWD, w], d_out, w, 3)
        kept(u, v, out)

    def across(lhs, ref, sl):
        cut = ref.shape[1] * TURN // 8
        total = lax.dot_general(lhs[:, :cut], ref[sl, :cut], NT, preferred_element_type=F32)
        for k in range(cut, ref.shape[1], TILE):
            turned = [ref[pl.ds(sl.start + q, TILE), k:k + TILE].T for q in range(0, BLK, TILE)]
            total += jnp.dot(lhs[:, k:k + TILE], jnp.concatenate(turned, axis=1), preferred_element_type=F32)
        return total

    def back_product(u, v, swapped):
        both_arrived(BWD, u, v)

        def fn(slices):
            lhs = pair(flow, BWD, u, v)
            for sl in slices:
                if swapped:
                    e = jnp.dot(lhs, wa[:, sl], preferred_element_type=F32)
                else:
                    e = across(lhs, wb, sl)
                act[BWD, u, :, sl] = (e[:tok] * slope[u, :, sl]).astype(BF16)
                act[BWD, v, :, sl] = (e[tok:] * slope[v, :, sl]).astype(BF16)
        blocks(d_ff, UP_GROUP if swapped else TURN_GROUP, fn)

        def out(w):
            keep(flow.at[BWD, w], g_out, w, 1)
            keep(act.at[BWD, w], d_out, w, 3)
        kept(u, v, out)

    def part_copy(kind, u, j):
        slot = lax.rem(u, SLOTS)
        return pltpu.make_async_remote_copy(part.at[kind, slot, j, other], recv.at[kind, u, j], part_send.at[kind, slot],
                                            recv_sem.at[kind, u, j], device_id=peer(stage, other), device_id_type=MESH)

    def direct_copy(u, j, half):
        slot = lax.rem(u, SLOTS)
        if half is side:
            return pltpu.make_async_remote_copy(part.at[BWD, slot, j, side], direct.at[u, j], direct_send.at[slot],
                                                direct_sem.at[0, u, j], device_id=peer(stage - 1, side), device_id_type=MESH)
        return pltpu.make_async_remote_copy(part.at[BWD, slot, j, other], recv.at[FWD, u, j], part_send.at[BWD, slot],
                                            direct_sem.at[1, u, j], device_id=peer(stage - 1, other), device_id_type=MESH)

    def take_direct(first, count):
        def body(i, carry):
            u = first + i
            for j in range(n_blk):
                sl = pl.ds(j * BLK, BLK)
                wait_bytes(direct.at[u, j], direct_sem.at[0, u, j])
                wait_bytes(recv.at[FWD, u, j], direct_sem.at[1, u, j])
                flow[BWD, u, side, :, sl] = (direct[u, j] + recv[FWD, u, j]).astype(BF16)
                pltpu.make_async_remote_copy(flow.at[BWD, u, side, :, sl], flow.at[BWD, u, side, :, sl], cross_send.at[0],
                                             flow_sem.at[BWD, u], device_id=peer(stage, other), device_id_type=MESH).start()
            return carry
        lax.fori_loop(0, count, body, 0)

    def down_product(kind, u, v, straight):
        def free(w):
            @pl.when(w >= SLOTS)
            def _():
                wait_bytes(recv.at[kind, w - SLOTS], part_send.at[kind, lax.rem(w, SLOTS)])

            if not straight:
                @pl.when((w >= SLOTS) & (w < SLOTS + DIRECT))
                def _():
                    wait_bytes(direct.at[w - SLOTS], direct_send.at[lax.rem(w, SLOTS)])
        kept(u, v, free)

        def body(t, carry):
            lhs = pair(act, kind, u, v)
            for k in range(DOWN_GROUP):
                j = t * DOWN_GROUP + k
                sl = pl.ds(pl.multiple_of(j * BLK, BLK), BLK)
                if straight:
                    p = jnp.dot(lhs, wb[:, sl], preferred_element_type=F32)
                else:
                    p = across(lhs, wa, sl)
                p = p.reshape(2, INNER, rows, BLK)
                part[kind, lax.rem(u, SLOTS), j] = p[0]
                part[kind, lax.rem(v, SLOTS), j] = p[1]

            def go(w):
                if straight:
                    for k in range(DOWN_GROUP):
                        part_copy(kind, w, t * DOWN_GROUP + k).start()
                    return

                @pl.when(w >= DIRECT)
                def _():
                    for k in range(DOWN_GROUP):
                        part_copy(kind, w, t * DOWN_GROUP + k).start()

                @pl.when(w < DIRECT)
                def _():
                    for k in range(DOWN_GROUP):
                        j = t * DOWN_GROUP + k
                        sl = pl.ds(pl.multiple_of(j * BLK, BLK), BLK)
                        part[BWD, lax.rem(w, SLOTS), j, side] += flow[BWD, w, side, :, sl].astype(F32)
                    for k in range(DOWN_GROUP):
                        for half in (side, other):
                            direct_copy(w, t * DOWN_GROUP + k, half).start()
            kept(u, v, go)
            return carry
        lax.fori_loop(0, n_blk // DOWN_GROUP, body, 0)

    def hand_on(kind, first, count):
        target = stage + 1 if kind == FWD else stage - 1
        inside = stage < STAGES - 1 if kind == FWD else stage > 0
        out = STAGES - 1 if kind == FWD else 0

        def body(i, carry):
            u = first + i
            slot = lax.rem(u, SLOTS)
            for j in range(n_blk):
                sl = pl.ds(j * BLK, BLK)
                wait_bytes(recv.at[kind, u, j], recv_sem.at[kind, u, j])
                total = flow[kind, u, side, :, sl].astype(F32) + (part[kind, slot, j, side] + recv[kind, u, j])
                send[kind, u, :, sl] = total.astype(BF16)

                @pl.when(inside)
                def _():
                    for half in (other, side):
                        pltpu.make_async_remote_copy(send.at[kind, u, :, sl], flow.at[kind, u, side, :, sl], flow_send.at[kind],
                                                     flow_sem.at[kind, u], device_id=peer(target, half), device_id_type=MESH).start()

            @pl.when(jnp.logical_and(jnp.logical_not(inside), home_of(u) != out))
            def _():
                pltpu.make_async_remote_copy(send.at[kind, u], home.at[kind, slot_of(u)], home_send.at[kind],
                                             home_sem.at[kind, slot_of(u)], device_id=peer(home_of(u), side), device_id_type=MESH).start()
            return carry
        lax.fori_loop(0, count, body, 0)

    def swap_weights():
        n_i = d_model // TILE

        def body(t, carry):
            i = pl.multiple_of(lax.rem(t, n_i) * TILE, TILE)
            j = pl.multiple_of(lax.div(t, n_i) * TILE, TILE)
            up = wa[pl.ds(i, TILE), pl.ds(j, TILE)]
            down = wb[pl.ds(j, TILE), pl.ds(i, TILE)]
            wa[pl.ds(i, TILE), pl.ds(j, TILE)] = down.T
            wb[pl.ds(j, TILE), pl.ds(i, TILE)] = up.T
            return carry
        lax.fori_loop(0, n_i * (d_ff // TILE), body, 0)

    def prepare_last():
        half = UNITS // 2

        def quarter(q, carry):
            for i in range(half):
                arrived(BWD, q * half + i)
                keep(flow.at[BWD, q * half + i], g_out, q * half + i, 1)
            units = pl.ds(q * half, half)

            def fn(slices):
                lhs = flow[BWD, units].reshape(half * tok, d_model)
                for sl in slices:
                    e = lax.dot_general(lhs, wb[sl, :], NT, preferred_element_type=F32)
                    slope[units, :, sl] = e.reshape(half, tok, BLK)
            blocks(d_ff, 1, fn)
            return carry
        lax.fori_loop(0, 2, quarter, 0)
        load_a.wait()
        n_i = d_model // TILE

        def body(t, carry):
            i = pl.multiple_of(lax.rem(t, n_i) * TILE, TILE)
            j = pl.multiple_of(lax.div(t, n_i) * TILE, TILE)
            wb[pl.ds(j, TILE), pl.ds(i, TILE)] = wa[pl.ds(i, TILE), pl.ds(j, TILE)].T
            return carry
        lax.fori_loop(0, n_i * (d_ff // TILE), body, 0)

    def step(t, carry):
        group, place = lax.div(t, 3), lax.rem(t, 3)
        word = words[0]
        for i, w in enumerate(words[1:], 1):
            word = jnp.where(group == i, w, word)
        code = lax.rem(lax.div(word, jnp.where(place == 0, 1, jnp.where(place == 1, PACK, PACK * PACK))), PACK)
        op = lax.rem(code, 32)
        u = lax.rem(lax.div(code, 32), UNITS)
        count = lax.div(code, 256) + 1

        def on(want):
            return pl.when(op == want)

        v = jnp.minimum(u + count - 1, UNITS - 1)

        @pl.when(op <= T1)
        def _():
            @on(F1)
            def _():
                up_product(u, v, False)

            @on(M1)
            def _():
                up_product(u, v, True)

            @on(B1)
            def _():
                back_product(u, v, True)

            @on(T1)
            def _():
                back_product(u, v, False)

        @pl.when((op > T1) & (op <= T2))
        def _():
            @pl.when(op < T2)
            def _():
                down_product(jnp.where(op == F2, FWD, BWD), u, v, True)

            @on(T2)
            def _():
                down_product(BWD, u, v, False)

        @pl.when((op > T2) & (op <= HB))
        def _():
            @on(FR)
            def _():
                hand_on(FWD, u, count)

            @on(BR)
            def _():
                hand_on(BWD, u, count)

            @on(HB)
            def _():
                take_direct(u, count)

        @pl.when(op > HB)
        def _():
            @on(SW)
            def _():
                swap_weights()

            @on(PR)
            def _():
                prepare_last()

            @on(YL)
            def _():
                load_b.start()
                load_b.wait()

            @on(WA)
            def _():
                load_a.wait()

            @on(WB)
            def _():
                load_b.wait()

            @on(XS)
            def _():
                @pl.when(stage == STAGES - 1)
                def _():
                    for k in range(2):
                        relay(k).start()

                @pl.when(stage < 2)
                def _():
                    hand_in(FWD, 0, 1, 1)
                stagings[BWD].wait()
                for k in range(2):
                    for lane in range(2):
                        hand_in(BWD, STAGES - 1, k, lane)

            @on(XR)
            def _():
                for k in range(2):
                    wait_bytes(home.at[FWD, k], relay_sem.at[k])
                    relayed(k).start()

            @on(XW)
            def _():
                for kind, target in ((FWD, 0), (BWD, STAGES - 1)):
                    @pl.when(stage != target)
                    def _():
                        wait_bytes(send.at[BWD, pl.ds(UNITS - 4, 4)], in_send.at[kind])

                    @pl.when(stage == target)
                    def _():
                        wait_bytes(staged[kind], in_send.at[kind])

                @pl.when(stage > 1)
                def _():
                    for k in range(2):
                        relayed(k).wait_send()
        return carry
    lengths = [len(row) for row in PLAN]
    lax.fori_loop(0, jnp.where(stage == 0, lengths[0], jnp.where(stage == 1, lengths[1], jnp.where(stage == 2, lengths[2], lengths[3]))), step, 0)

    for kind, here, out in ((FWD, STAGES - 1, y_out), (BWD, 0, dx_out)):
        for k in range(2):
            @pl.when(stage == here)
            def _():
                pltpu.make_async_copy(send.at[kind, unit_of(k)], out.at[k], out_sem.at[4 + kind]).start()

            @pl.when(stage != here)
            def _():
                wait_bytes(home.at[kind, k], home_sem.at[kind, k])
                pltpu.make_async_copy(home.at[kind, k], out.at[k], out_sem.at[4 + kind]).start()

    for kind in (FWD, BWD):
        for u in range(UNITS - SLOTS, UNITS):
            wait_bytes(recv.at[kind, u], part_send.at[kind, u % SLOTS])
    for kind, last in ((FWD, STAGES - 1), (BWD, 0)):
        @pl.when((stage != last) & jnp.logical_not((stage == 2) & (kind == BWD)))
        def _():
            wait_bytes(flow.at[kind], flow_send.at[kind])

        @pl.when(stage == last)
        def _():
            wait_bytes(send.at[kind, pl.ds(0, UNITS - 2)], home_send.at[kind])

    @pl.when(stage == 2)
    def _():
        wait_bytes(flow.at[BWD, pl.ds(0, UNITS - DIRECT)], flow_send.at[BWD])

    @pl.when(stage == 1)
    def _():
        wait_bytes(flow.at[BWD, pl.ds(0, DIRECT), 0], cross_send.at[0])
    for lane, (ref, out) in enumerate(((flow.at[FWD], h_out), (flow.at[BWD], g_out), (act.at[FWD], a_out), (act.at[BWD], d_out),
                                       (home.at[FWD], y_out), (home.at[BWD], dx_out))):
        pltpu.make_async_copy(ref, out, out_sem.at[lane]).wait()


def run_pipeline(x_loc, g_loc, w_one, w_two):
    rows, d_model = x_loc.shape[1:]
    d_ff = w_one.shape[1]
    n_blk = d_model // BLK
    tok = INNER * rows
    hbm = pl.BlockSpec(memory_space=pl.ANY)
    out = lambda *shape: jax.ShapeDtypeStruct(shape, BF16)
    dma = lambda *shape: pltpu.SemaphoreType.DMA(shape)
    return pl.pallas_call(
        pipeline_kernel,
        name='pipeline',
        out_shape=(out(*x_loc.shape), out(*x_loc.shape), out(UNITS, INNER, rows, d_model), out(UNITS, INNER, rows, d_model),
                   out(UNITS, tok, d_ff), out(UNITS, tok, d_ff)),
        in_specs=[hbm] * 4,
        out_specs=(hbm,) * 6,
        scratch_shapes=[
            pltpu.VMEM((d_model, d_ff), BF16),
            pltpu.VMEM((d_ff, d_model), BF16),
            pltpu.VMEM((2, UNITS, INNER, rows, d_model), BF16),
            pltpu.VMEM((2, UNITS, tok, d_ff), BF16),
            pltpu.VMEM((UNITS, tok, d_ff), F32),
            pltpu.VMEM((2, SLOTS, n_blk, INNER, rows, BLK), F32),
            pltpu.VMEM((2, UNITS, n_blk, rows, BLK), F32),
            pltpu.VMEM((2, UNITS, rows, d_model), BF16),
            pltpu.VMEM((2, 2, rows, d_model), BF16),
            pltpu.VMEM((DIRECT, n_blk, rows, BLK), F32),
            dma(2, UNITS), dma(2, UNITS, n_blk), dma(2, SLOTS), dma(2), dma(2), dma(2, 2), dma(2), dma(2), dma(2),
            dma(2, DIRECT, n_blk), dma(SLOTS), dma(1), dma(2), dma(2), dma(6),
        ],
        compiler_params=pltpu.CompilerParams(collective_id=0, has_side_effects=True, vmem_limit_bytes=67043328),
    )(x_loc, g_loc, w_one, w_two)


GRAD_ROWS, GRAD_COLS, GRAD_PART, GRAD_SLOTS = 1024, 2048, 256, 4


def weight_grad_kernel(h_ref, d_ref, a_ref, g_ref, y_ref, x_ref, up_ref, down_ref, y_out, x_out,
                       h, d, a, g, home, left, right, stage, in_sem, home_sem, out_sem):
    d_model, d_ff = h.shape[1], d.shape[1]
    n_down, n_up, n_col = d_ff // GRAD_ROWS, d_model // GRAD_ROWS, d_ff // GRAD_COLS

    pieces = [a.at[:, pl.ds(t * GRAD_ROWS, GRAD_ROWS)] for t in range(n_down)]
    loads = [(g_ref, g)] + [(a_ref.at[:, pl.ds(t * GRAD_ROWS, GRAD_ROWS)], piece) for t, piece in enumerate(pieces)] + [(h_ref, h), (d_ref, d)]
    loads = [pltpu.make_async_copy(src, dst, in_sem.at[t]) for t, (src, dst) in enumerate(loads)]
    homes = [pltpu.make_async_copy(src, home.at[t], home_sem.at[t]) for t, src in enumerate((y_ref, x_ref))]
    backs = [pltpu.make_async_copy(home.at[t], dst, home_sem.at[t]) for t, dst in enumerate((y_out, x_out))]
    for copy in loads + homes:
        copy.start()

    rows_of = lambda t: pl.ds(t * GRAD_ROWS, GRAD_ROWS)
    blocks = [(a, t, g, 0, down_ref) for t in range(n_down)] + [(h, t, d, c, up_ref) for t in range(n_up) for c in range(n_col)]
    turned = (left, right)
    loads[0].wait()
    loads[1].wait()
    arrived = 2
    turn = -1
    for t, (src, row, other, col, out) in enumerate(blocks):
        slot = t % GRAD_SLOTS
        cols = pl.ds(col * GRAD_COLS, GRAD_COLS)
        after = blocks[t + 1] if t + 1 < len(blocks) else None
        need = (1 + n_down if after is None or after[0] is h else t + 2) + (1 if src is h or (after is not None and after[0] is h) else 0)
        need = min(need, len(loads) - 1) + (1 if src is h else 0)
        while arrived < min(need + 1, len(loads)):
            loads[arrived].wait()
            arrived += 1
        if t >= GRAD_SLOTS:
            pltpu.make_async_copy(stage.at[slot], stage.at[slot], out_sem.at[slot]).wait()
        size = GRAD_PART if after is None or t == 0 else GRAD_ROWS
        for p in range(0, GRAD_ROWS, size):
            if t == 0:
                stage[slot, p:p + size] = lax.dot_general(src[:, p:p + size], other[:, cols], (((0,), (0,)), ((), ())), preferred_element_type=F32)
            else:
                stage[slot, p:p + size] = jnp.dot(turned[turn % 2][p:p + size], other[:, cols], preferred_element_type=F32)
            if p + size == GRAD_ROWS and after is not None and (after[0] is not src or after[1] != row):
                turn += 1
                turned[turn % 2][...] = after[0][:, rows_of(after[1])].T
            for q in range(p, p + size, GRAD_PART):
                pltpu.make_async_copy(stage.at[slot, pl.ds(q, GRAD_PART)], out.at[pl.ds(row * GRAD_ROWS + q, GRAD_PART), cols], out_sem.at[slot]).start()
        if t == 1:
            for copy, back in zip(homes, backs):
                copy.wait()
                back.start()
    for slot in range(GRAD_SLOTS):
        pltpu.make_async_copy(stage.at[slot], stage.at[slot], out_sem.at[slot]).wait()
    for copy in backs:
        copy.wait()


def weight_grads(h, d, a, g, y, dx):
    tokens, d_model = h.shape
    d_ff = d.shape[1]
    n_in = 3 + d_ff // GRAD_ROWS
    hbm = pl.BlockSpec(memory_space=pl.ANY)
    dma = lambda *shape: pltpu.SemaphoreType.DMA(shape)
    like = lambda v: pltpu.VMEM(v.shape, v.dtype)
    return pl.pallas_call(
        weight_grad_kernel,
        name='weight_grads',
        out_shape=(jax.ShapeDtypeStruct((d_model, d_ff), F32), jax.ShapeDtypeStruct((d_ff, d_model), F32),
                   jax.ShapeDtypeStruct(y.shape, BF16), jax.ShapeDtypeStruct(y.shape, BF16)),
        in_specs=[hbm] * 6,
        out_specs=(hbm,) * 4,
        scratch_shapes=[like(h), like(d), like(a), like(g), pltpu.VMEM((2,) + y.shape, BF16), pltpu.VMEM((GRAD_ROWS, tokens), BF16), pltpu.VMEM((GRAD_ROWS, tokens), BF16),
                        pltpu.VMEM((GRAD_SLOTS, GRAD_ROWS, GRAD_COLS), F32),
                        dma(n_in), dma(2), dma(GRAD_SLOTS)],
        compiler_params=pltpu.CompilerParams(vmem_limit_bytes=60 * 1024 * 1024),
    )(h, d, a, g, y, dx)


def solution(mesh):
    tok_spec = P(('data', 'stage', 'inner'))
    up_spec = P(None, ('data', 'stage'), None, 'inner')
    down_spec = P(None, ('data', 'stage'), 'inner', None)

    def device_step(x_loc, g_loc, w_up, w_down):
        y, dx, h, g, a, d = run_pipeline(x_loc, g_loc, w_up[0, 0], w_down[0, 0])
        flat = lambda v: v.reshape(-1, v.shape[-1])
        dw_up, dw_down, y, dx = weight_grads(flat(h), flat(d), flat(a), flat(g), y, dx)
        return y, dx, dw_up[None, None], dw_down[None, None]

    return jax.shard_map(device_step, mesh=mesh, in_specs=(tok_spec, tok_spec, up_spec, down_spec), out_specs=(tok_spec, tok_spec, up_spec, down_spec), check_vma=False)
```

```python
import functools

import jax
import jax.numpy as jnp
from jax import lax
from jax.experimental import pallas as pl
from jax.experimental.pallas import tpu as pltpu
from jax.sharding import PartitionSpec as P

F32 = jnp.float32
BF16 = jnp.bfloat16
MESH = pl.DeviceIdType.MESH

STAGES = 4
INNER = 2
UNITS = 8
SLOTS = 3
DIRECT = 3
BLK = 512
TILE = 256
FWD, BWD = 0, 1
NT = (((1,), (1,)), ((), ()))

F1, M1, B1, T1, F2, B2, T2, FR, BR, HB, SW, PR, YL, WA, WB, XS, XW, XR = range(1, 19)
PLAN = (
    ((WA, 0, 1), (F1, 0, 2), (WB, 0, 1), (XS, 0, 1), (F2, 0, 2), (F1, 2, 2), (FR, 0, 2), (F2, 2, 2),
     (FR, 2, 1), (F1, 4, 2), (FR, 3, 1), (F2, 4, 2), (FR, 4, 2), (F1, 6, 2), (F2, 6, 1), (F2, 7, 1),
     (FR, 6, 2), (XW, 0, 1), (SW, 0, 1), (B1, 0, 2), (B2, 0, 1), (B2, 1, 1), (B1, 2, 1), (B2, 2, 1),
     (B1, 3, 1), (BR, 0, 2), (B2, 3, 1), (BR, 2, 1), (B1, 4, 2), (B2, 4, 2), (BR, 3, 1), (B1, 6, 2),
     (B2, 6, 1), (BR, 4, 1), (B2, 7, 1), (BR, 5, 3)),
    ((WA, 0, 1), (WB, 0, 1), (XS, 0, 1), (F1, 0, 2), (F2, 0, 1), (F2, 1, 1), (FR, 0, 2), (F1, 2, 2),
     (F2, 2, 1), (F2, 3, 1), (FR, 2, 1), (F1, 4, 2), (FR, 3, 1), (F2, 4, 1), (F2, 5, 1), (FR, 4, 2),
     (F1, 6, 2), (F2, 6, 2), (FR, 6, 2), (XW, 0, 1), (SW, 0, 1), (HB, 0, 2), (B1, 0, 2), (B2, 0, 1),
     (HB, 2, 1), (B2, 1, 1), (BR, 0, 1), (B1, 2, 2), (BR, 1, 1), (B2, 2, 2), (BR, 2, 2), (B1, 4, 1),
     (B1, 5, 1), (B2, 4, 2), (B1, 6, 1), (B2, 6, 1), (BR, 4, 1), (B1, 7, 1), (BR, 5, 1), (B2, 7, 1),
     (BR, 6, 2)),
    ((XR, 0, 1), (WA, 0, 1), (WB, 0, 1), (XS, 0, 1), (XW, 0, 1), (F1, 0, 1), (F2, 0, 1), (F1, 1, 1),
     (FR, 0, 1), (F2, 1, 1), (FR, 1, 1), (F1, 2, 1), (F2, 2, 1), (F1, 3, 1), (F2, 3, 1), (FR, 2, 1),
     (F1, 4, 1), (F1, 5, 1), (FR, 3, 1), (F2, 4, 2), (T1, 0, 2), (F1, 6, 2), (T2, 0, 2), (FR, 4, 1),
     (F2, 6, 2), (FR, 5, 1), (T1, 2, 2), (FR, 6, 2), (T2, 2, 2), (BR, 3, 1), (T1, 4, 2), (T2, 4, 2),
     (T1, 6, 2), (BR, 4, 1), (T2, 6, 2), (BR, 5, 3)),
    ((WB, 0, 1), (XS, 0, 1), (XR, 0, 1), (PR, 0, 1), (XW, 0, 1), (M1, 0, 1), (B2, 0, 1), (BR, 0, 1),
     (M1, 1, 1), (B2, 1, 1), (BR, 1, 1), (M1, 2, 2), (B2, 2, 1), (B2, 3, 1), (BR, 2, 2), (M1, 4, 1),
     (B2, 4, 1), (M1, 5, 1), (B2, 5, 1), (BR, 4, 1), (M1, 6, 2), (BR, 5, 1), (B2, 6, 2), (BR, 6, 2),
     (YL, 0, 1), (F2, 0, 2), (FR, 0, 2), (F2, 2, 1), (F2, 3, 2), (FR, 2, 1), (F2, 5, 1), (FR, 3, 2),
     (F2, 6, 1), (FR, 5, 1), (F2, 7, 1), (FR, 6, 2)),
)


PACK = 1024
UP_GROUP = 8
TURN = 5
TURN_GROUP = 4
DOWN_GROUP = 2


def plan_words():
    rows = [[op + 32 * unit + 256 * (count - 1) for op, unit, count in row] for row in PLAN]
    steps = -(-max(len(row) for row in rows) // 3) * 3
    rows = [row + [0] * (steps - len(row)) for row in rows]
    return [[row[t] + PACK * row[t + 1] + PACK * PACK * row[t + 2] for t in range(0, steps, 3)] for row in rows]


def gelu_pair(pre_act):
    root = pre_act * 0.7071067811865476
    normal_cdf = 0.5 * (1.0 + lax.erf(root))
    normal_pdf = jnp.exp2(root * root * -1.4426950408889634) * 0.3989422804014327
    return pre_act * normal_cdf, normal_cdf + pre_act * normal_pdf


def wait_bytes(ref, sem):
    pltpu.make_async_copy(ref, ref, sem).wait()


def pipeline_kernel(x_ref, g_ref, w1_ref, w2_ref,
                    y_out, dx_out, h_out, g_out, a_out, d_out,
                    wa, wb, flow, act, slope, part, recv, send, home, direct,
                    flow_sem, recv_sem, part_send, flow_send, home_send, home_sem, in_send, relay_sem, relay_send,
                    direct_sem, direct_send, cross_send, stage_sem, w_sem, out_sem):
    stage = lax.axis_index('stage')
    side = lax.axis_index('inner')
    other = 1 - side
    rows, d_model = flow.shape[3:]
    tok, d_ff = act.shape[2:]
    n_blk = d_model // BLK

    def peer(s, i):
        return {'stage': s, 'inner': i}

    load_a = pltpu.make_async_copy(w1_ref, wa, w_sem.at[0])
    load_b = pltpu.make_async_copy(w2_ref, wb, w_sem.at[1])

    def unit_of(k):
        return jnp.where(stage < 2, stage + (7 - 2 * stage) * k, 2 * stage - 2 + k)

    staged = (send.at[BWD, pl.ds(UNITS - 2, 2)], send.at[BWD, pl.ds(UNITS - 4, 2)])
    stagings = [pltpu.make_async_copy(src, dst, stage_sem.at[kind]) for kind, (src, dst) in enumerate(zip((x_ref, g_ref), staged))]
    for kind, target in ((FWD, 0), (BWD, STAGES - 1)):
        stagings[kind].start()

        @pl.when(stage == target)
        def _():
            for k in range(2):
                pltpu.make_async_copy((x_ref, g_ref)[kind].at[k], flow.at[kind, unit_of(k), side], flow_sem.at[kind, unit_of(k)]).start()

    @pl.when(stage < STAGES - 1)
    def _():
        load_a.start()
    load_b.start()

    @pl.when(stage == STAGES - 1)
    def _():
        load_a.start()

    barrier = pltpu.get_barrier_semaphore()
    for s in range(STAGES):
        for i in range(INNER):
            @pl.when(jnp.logical_or(stage != s, side != i))
            def _():
                pl.semaphore_signal(barrier, inc=1, device_id=peer(s, i), device_id_type=MESH)
    pl.semaphore_wait(barrier, STAGES * INNER - 1)

    def home_of(u):
        return jnp.where(u < 2, u, jnp.where(u > 5, 7 - u, (u + 2) // 2))

    def slot_of(u):
        return jnp.where(u < 2, 0, jnp.where(u > 5, 1, lax.rem(u, 2)))

    def hand_in(kind, target, k, lane):
        u = unit_of(k)
        src = staged[kind]
        if lane == 0:
            @pl.when(stage != target)
            def _():
                pltpu.make_async_remote_copy(src.at[k], flow.at[kind, u, side], in_send.at[kind], flow_sem.at[kind, u],
                                             device_id=peer(target, side), device_id_type=MESH).start()
        else:
            pltpu.make_async_remote_copy(src.at[k], flow.at[kind, u, side], in_send.at[kind], flow_sem.at[kind, u],
                                         device_id=peer(target, other), device_id_type=MESH).start()

    def relay(k):
        return pltpu.make_async_remote_copy(staged[FWD].at[k], home.at[FWD, k], in_send.at[FWD], relay_sem.at[k],
                                            device_id=peer(stage, other), device_id_type=MESH)

    def relayed(k):
        u = unit_of(k)
        return pltpu.make_async_remote_copy(home.at[FWD, k], flow.at[FWD, u, other], relay_send.at[k], flow_sem.at[FWD, u],
                                            device_id=peer(0, side), device_id_type=MESH)

    stagings[FWD].wait()
    for k in range(2):
        hand_in(FWD, 0, k, 0)

        if k == 0:
            @pl.when(stage < 2)
            def _():
                hand_in(FWD, 0, k, 1)

        @pl.when(stage == 2)
        def _():
            relay(k).start()
    plan = plan_words()
    words = [jnp.where(stage == 0, a, jnp.where(stage == 1, b, jnp.where(stage == 2, c, d))) for a, b, c, d in zip(*plan)]

    def keep(ref, out, u, lane):
        pltpu.make_async_copy(ref, out.at[u], out_sem.at[lane]).start()

    def blocks(width, group, fn):
        def body(t, carry):
            fn([pl.ds(pl.multiple_of((t * group + k) * BLK, BLK), BLK) for k in range(group)])
            return carry
        lax.fori_loop(0, width // BLK // group, body, 0)

    def arrived(kind, u):
        taken = (stage == 1) & (kind == BWD) & (u < DIRECT)

        @pl.when(jnp.logical_not(taken))
        def _():
            wait_bytes(flow.at[kind, u], flow_sem.at[kind, u])

        @pl.when(taken)
        def _():
            wait_bytes(flow.at[kind, u, other], flow_sem.at[kind, u])

    def both_arrived(kind, u, v):
        arrived(kind, u)

        @pl.when(v != u)
        def _():
            arrived(kind, v)

    def pair(ref, kind, u, v):
        width = ref.shape[-1]
        return jnp.concatenate([ref[kind, u].reshape(tok, width), ref[kind, v].reshape(tok, width)], axis=0)

    def kept(u, v, fn):
        fn(u)

        @pl.when(v != u)
        def _():
            fn(v)

    def up_product(u, v, last):
        both_arrived(FWD, u, v)

        def fn(slices):
            lhs = pair(flow, FWD, u, v)
            for sl in slices:
                z = jnp.dot(lhs, wa[:, sl], preferred_element_type=F32)
                value, grad = gelu_pair(z)
                value = value.astype(BF16)
                if last:
                    act[BWD, u, :, sl] = (slope[u, :, sl] * grad[:tok]).astype(BF16)
                    act[BWD, v, :, sl] = (slope[v, :, sl] * grad[tok:]).astype(BF16)
                else:
                    slope[u, :, sl] = grad[:tok]
                    slope[v, :, sl] = grad[tok:]
                act[FWD, u, :, sl] = value[:tok]
                act[FWD, v, :, sl] = value[tok:]
        blocks(d_ff, UP_GROUP, fn)

        def out(w):
            keep(flow.at[FWD, w], h_out, w, 0)
            keep(act.at[FWD, w], a_out, w, 2)
            if last:
                keep(act.at[BWD, w], d_out, w, 3)
        kept(u, v, out)

    def across(lhs, ref, sl):
        cut = ref.shape[1] * TURN // 8
        total = lax.dot_general(lhs[:, :cut], ref[sl, :cut], NT, preferred_element_type=F32)
        for k in range(cut, ref.shape[1], TILE):
            turned = [ref[pl.ds(sl.start + q, TILE), k:k + TILE].T for q in range(0, BLK, TILE)]
            total += jnp.dot(lhs[:, k:k + TILE], jnp.concatenate(turned, axis=1), preferred_element_type=F32)
        return total

    def back_product(u, v, swapped):
        both_arrived(BWD, u, v)

        def fn(slices):
            lhs = pair(flow, BWD, u, v)
            for sl in slices:
                if swapped:
                    e = jnp.dot(lhs, wa[:, sl], preferred_element_type=F32)
                else:
                    e = across(lhs, wb, sl)
                act[BWD, u, :, sl] = (e[:tok] * slope[u, :, sl]).astype(BF16)
                act[BWD, v, :, sl] = (e[tok:] * slope[v, :, sl]).astype(BF16)
        blocks(d_ff, UP_GROUP if swapped else TURN_GROUP, fn)

        def out(w):
            keep(flow.at[BWD, w], g_out, w, 1)
            keep(act.at[BWD, w], d_out, w, 3)
        kept(u, v, out)

    def part_copy(kind, u, j):
        slot = lax.rem(u, SLOTS)
        return pltpu.make_async_remote_copy(part.at[kind, slot, j, other], recv.at[kind, u, j], part_send.at[kind, slot],
                                            recv_sem.at[kind, u, j], device_id=peer(stage, other), device_id_type=MESH)

    def direct_copy(u, j, half):
        slot = lax.rem(u, SLOTS)
        if half is side:
            return pltpu.make_async_remote_copy(part.at[BWD, slot, j, side], direct.at[u, j], direct_send.at[slot],
                                                direct_sem.at[0, u, j], device_id=peer(stage - 1, side), device_id_type=MESH)
        return pltpu.make_async_remote_copy(part.at[BWD, slot, j, other], recv.at[FWD, u, j], part_send.at[BWD, slot],
                                            direct_sem.at[1, u, j], device_id=peer(stage - 1, other), device_id_type=MESH)

    def take_direct(first, count):
        def body(i, carry):
            u = first + i
            for j in range(n_blk):
                sl = pl.ds(j * BLK, BLK)
                wait_bytes(direct.at[u, j], direct_sem.at[0, u, j])
                wait_bytes(recv.at[FWD, u, j], direct_sem.at[1, u, j])
                flow[BWD, u, side, :, sl] = (direct[u, j] + recv[FWD, u, j]).astype(BF16)
                pltpu.make_async_remote_copy(flow.at[BWD, u, side, :, sl], flow.at[BWD, u, side, :, sl], cross_send.at[0],
                                             flow_sem.at[BWD, u], device_id=peer(stage, other), device_id_type=MESH).start()
            return carry
        lax.fori_loop(0, count, body, 0)

    def down_product(kind, u, v, straight):
        def free(w):
            @pl.when(w >= SLOTS)
            def _():
                wait_bytes(recv.at[kind, w - SLOTS], part_send.at[kind, lax.rem(w, SLOTS)])

            if not straight:
                @pl.when((w >= SLOTS) & (w < SLOTS + DIRECT))
                def _():
                    wait_bytes(direct.at[w - SLOTS], direct_send.at[lax.rem(w, SLOTS)])
        kept(u, v, free)

        def body(t, carry):
            lhs = pair(act, kind, u, v)
            for k in range(DOWN_GROUP):
                j = t * DOWN_GROUP + k
                sl = pl.ds(pl.multiple_of(j * BLK, BLK), BLK)
                if straight:
                    p = jnp.dot(lhs, wb[:, sl], preferred_element_type=F32)
                else:
                    p = across(lhs, wa, sl)
                p = p.reshape(2, INNER, rows, BLK)
                part[kind, lax.rem(u, SLOTS), j] = p[0]
                part[kind, lax.rem(v, SLOTS), j] = p[1]

            def go(w):
                if straight:
                    for k in range(DOWN_GROUP):
                        part_copy(kind, w, t * DOWN_GROUP + k).start()
                    return

                @pl.when(w >= DIRECT)
                def _():
                    for k in range(DOWN_GROUP):
                        part_copy(kind, w, t * DOWN_GROUP + k).start()

                @pl.when(w < DIRECT)
                def _():
                    for k in range(DOWN_GROUP):
                        j = t * DOWN_GROUP + k
                        sl = pl.ds(pl.multiple_of(j * BLK, BLK), BLK)
                        part[BWD, lax.rem(w, SLOTS), j, side] += flow[BWD, w, side, :, sl].astype(F32)
                    for k in range(DOWN_GROUP):
                        for half in (other, side):
                            direct_copy(w, t * DOWN_GROUP + k, half).start()
            kept(u, v, go)
            return carry
        lax.fori_loop(0, n_blk // DOWN_GROUP, body, 0)

    def hand_on(kind, first, count):
        target = stage + 1 if kind == FWD else stage - 1
        inside = stage < STAGES - 1 if kind == FWD else stage > 0
        out = STAGES - 1 if kind == FWD else 0

        def body(i, carry):
            u = first + i
            slot = lax.rem(u, SLOTS)
            for j in range(n_blk):
                sl = pl.ds(j * BLK, BLK)
                wait_bytes(recv.at[kind, u, j], recv_sem.at[kind, u, j])
                total = flow[kind, u, side, :, sl].astype(F32) + (part[kind, slot, j, side] + recv[kind, u, j])
                send[kind, u, :, sl] = total.astype(BF16)

                @pl.when(inside)
                def _():
                    for half in (other, side):
                        pltpu.make_async_remote_copy(send.at[kind, u, :, sl], flow.at[kind, u, side, :, sl], flow_send.at[kind],
                                                     flow_sem.at[kind, u], device_id=peer(target, half), device_id_type=MESH).start()

            @pl.when(jnp.logical_and(jnp.logical_not(inside), home_of(u) != out))
            def _():
                pltpu.make_async_remote_copy(send.at[kind, u], home.at[kind, slot_of(u)], home_send.at[kind],
                                             home_sem.at[kind, slot_of(u)], device_id=peer(home_of(u), side), device_id_type=MESH).start()
            return carry
        lax.fori_loop(0, count, body, 0)

    def swap_weights():
        n_i = d_model // TILE

        def body(t, carry):
            i = pl.multiple_of(lax.rem(t, n_i) * TILE, TILE)
            j = pl.multiple_of(lax.div(t, n_i) * TILE, TILE)
            up = wa[pl.ds(i, TILE), pl.ds(j, TILE)]
            down = wb[pl.ds(j, TILE), pl.ds(i, TILE)]
            wa[pl.ds(i, TILE), pl.ds(j, TILE)] = down.T
            wb[pl.ds(j, TILE), pl.ds(i, TILE)] = up.T
            return carry
        lax.fori_loop(0, n_i * (d_ff // TILE), body, 0)

    def prepare_last():
        half = UNITS // 2

        def quarter(q, carry):
            for i in range(half):
                arrived(BWD, q * half + i)
                keep(flow.at[BWD, q * half + i], g_out, q * half + i, 1)
            units = pl.ds(q * half, half)

            def fn(slices):
                lhs = flow[BWD, units].reshape(half * tok, d_model)
                for sl in slices:
                    e = lax.dot_general(lhs, wb[sl, :], NT, preferred_element_type=F32)
                    slope[units, :, sl] = e.reshape(half, tok, BLK)
            blocks(d_ff, 1, fn)
            return carry
        lax.fori_loop(0, 2, quarter, 0)
        load_a.wait()
        n_i = d_model // TILE

        def body(t, carry):
            i = pl.multiple_of(lax.rem(t, n_i) * TILE, TILE)
            j = pl.multiple_of(lax.div(t, n_i) * TILE, TILE)
            wb[pl.ds(j, TILE), pl.ds(i, TILE)] = wa[pl.ds(i, TILE), pl.ds(j, TILE)].T
            return carry
        lax.fori_loop(0, n_i * (d_ff // TILE), body, 0)

    def step(t, carry):
        group, place = lax.div(t, 3), lax.rem(t, 3)
        word = words[0]
        for i, w in enumerate(words[1:], 1):
            word = jnp.where(group == i, w, word)
        code = lax.rem(lax.div(word, jnp.where(place == 0, 1, jnp.where(place == 1, PACK, PACK * PACK))), PACK)
        op = lax.rem(code, 32)
        u = lax.rem(lax.div(code, 32), UNITS)
        count = lax.div(code, 256) + 1

        def on(want):
            return pl.when(op == want)

        v = jnp.minimum(u + count - 1, UNITS - 1)

        @pl.when(op <= T1)
        def _():
            @on(F1)
            def _():
                up_product(u, v, False)

            @on(M1)
            def _():
                up_product(u, v, True)

            @on(B1)
            def _():
                back_product(u, v, True)

            @on(T1)
            def _():
                back_product(u, v, False)

        @pl.when((op > T1) & (op <= T2))
        def _():
            @pl.when(op < T2)
            def _():
                down_product(jnp.where(op == F2, FWD, BWD), u, v, True)

            @on(T2)
            def _():
                down_product(BWD, u, v, False)

        @pl.when((op > T2) & (op <= HB))
        def _():
            @on(FR)
            def _():
                hand_on(FWD, u, count)

            @on(BR)
            def _():
                hand_on(BWD, u, count)

            @on(HB)
            def _():
                take_direct(u, count)

        @pl.when(op > HB)
        def _():
            @on(SW)
            def _():
                swap_weights()

            @on(PR)
            def _():
                prepare_last()

            @on(YL)
            def _():
                load_b.start()
                load_b.wait()

            @on(WA)
            def _():
                load_a.wait()

            @on(WB)
            def _():
                load_b.wait()

            @on(XS)
            def _():
                @pl.when(stage == STAGES - 1)
                def _():
                    for k in range(2):
                        relay(k).start()

                @pl.when(stage < 2)
                def _():
                    hand_in(FWD, 0, 1, 1)
                stagings[BWD].wait()
                for k in range(2):
                    for lane in range(2):
                        hand_in(BWD, STAGES - 1, k, lane)

            @on(XR)
            def _():
                for k in range(2):
                    wait_bytes(home.at[FWD, k], relay_sem.at[k])
                    relayed(k).start()

            @on(XW)
            def _():
                for kind, target in ((FWD, 0), (BWD, STAGES - 1)):
                    @pl.when(stage != target)
                    def _():
                        wait_bytes(send.at[BWD, pl.ds(UNITS - 4, 4)], in_send.at[kind])

                    @pl.when(stage == target)
                    def _():
                        wait_bytes(staged[kind], in_send.at[kind])

                @pl.when(stage > 1)
                def _():
                    for k in range(2):
                        relayed(k).wait_send()
        return carry
    lengths = [len(row) for row in PLAN]
    lax.fori_loop(0, jnp.where(stage == 0, lengths[0], jnp.where(stage == 1, lengths[1], jnp.where(stage == 2, lengths[2], lengths[3]))), step, 0)

    for kind, here, out in ((FWD, STAGES - 1, y_out), (BWD, 0, dx_out)):
        for k in range(2):
            @pl.when(stage == here)
            def _():
                pltpu.make_async_copy(send.at[kind, unit_of(k)], out.at[k], out_sem.at[4 + kind]).start()

            @pl.when(stage != here)
            def _():
                wait_bytes(home.at[kind, k], home_sem.at[kind, k])
                pltpu.make_async_copy(home.at[kind, k], out.at[k], out_sem.at[4 + kind]).start()

    for kind in (FWD, BWD):
        for u in range(UNITS - SLOTS, UNITS):
            wait_bytes(recv.at[kind, u], part_send.at[kind, u % SLOTS])
    for kind, last in ((FWD, STAGES - 1), (BWD, 0)):
        @pl.when((stage != last) & jnp.logical_not((stage == 2) & (kind == BWD)))
        def _():
            wait_bytes(flow.at[kind], flow_send.at[kind])

        @pl.when(stage == last)
        def _():
            wait_bytes(send.at[kind, pl.ds(0, UNITS - 2)], home_send.at[kind])

    @pl.when(stage == 2)
    def _():
        wait_bytes(flow.at[BWD, pl.ds(0, UNITS - DIRECT)], flow_send.at[BWD])

    @pl.when(stage == 1)
    def _():
        wait_bytes(flow.at[BWD, pl.ds(0, DIRECT), 0], cross_send.at[0])
    for lane, (ref, out) in enumerate(((flow.at[FWD], h_out), (flow.at[BWD], g_out), (act.at[FWD], a_out), (act.at[BWD], d_out),
                                       (home.at[FWD], y_out), (home.at[BWD], dx_out))):
        pltpu.make_async_copy(ref, out, out_sem.at[lane]).wait()


def run_pipeline(x_loc, g_loc, w_one, w_two):
    rows, d_model = x_loc.shape[1:]
    d_ff = w_one.shape[1]
    n_blk = d_model // BLK
    tok = INNER * rows
    hbm = pl.BlockSpec(memory_space=pl.ANY)
    out = lambda *shape: jax.ShapeDtypeStruct(shape, BF16)
    dma = lambda *shape: pltpu.SemaphoreType.DMA(shape)
    return pl.pallas_call(
        pipeline_kernel,
        name='pipeline',
        out_shape=(out(*x_loc.shape), out(*x_loc.shape), out(UNITS, INNER, rows, d_model), out(UNITS, INNER, rows, d_model),
                   out(UNITS, tok, d_ff), out(UNITS, tok, d_ff)),
        in_specs=[hbm] * 4,
        out_specs=(hbm,) * 6,
        scratch_shapes=[
            pltpu.VMEM((d_model, d_ff), BF16),
            pltpu.VMEM((d_ff, d_model), BF16),
            pltpu.VMEM((2, UNITS, INNER, rows, d_model), BF16),
            pltpu.VMEM((2, UNITS, tok, d_ff), BF16),
            pltpu.VMEM((UNITS, tok, d_ff), F32),
            pltpu.VMEM((2, SLOTS, n_blk, INNER, rows, BLK), F32),
            pltpu.VMEM((2, UNITS, n_blk, rows, BLK), F32),
            pltpu.VMEM((2, UNITS, rows, d_model), BF16),
            pltpu.VMEM((2, 2, rows, d_model), BF16),
            pltpu.VMEM((DIRECT, n_blk, rows, BLK), F32),
            dma(2, UNITS), dma(2, UNITS, n_blk), dma(2, SLOTS), dma(2), dma(2), dma(2, 2), dma(2), dma(2), dma(2),
            dma(2, DIRECT, n_blk), dma(SLOTS), dma(1), dma(2), dma(2), dma(6),
        ],
        compiler_params=pltpu.CompilerParams(collective_id=0, has_side_effects=True, vmem_limit_bytes=67043328),
    )(x_loc, g_loc, w_one, w_two)


GRAD_ROWS, GRAD_COLS, GRAD_PART, GRAD_SLOTS = 1024, 2048, 256, 4


def weight_grad_kernel(h_ref, d_ref, a_ref, g_ref, y_ref, x_ref, up_ref, down_ref, y_out, x_out,
                       h, d, a, g, home, left, right, stage, in_sem, home_sem, out_sem):
    d_model, d_ff = h.shape[1], d.shape[1]
    n_down, n_up, n_col = d_ff // GRAD_ROWS, d_model // GRAD_ROWS, d_ff // GRAD_COLS

    pieces = [a.at[:, pl.ds(t * GRAD_ROWS, GRAD_ROWS)] for t in range(n_down)]
    loads = [(g_ref, g)] + [(a_ref.at[:, pl.ds(t * GRAD_ROWS, GRAD_ROWS)], piece) for t, piece in enumerate(pieces)] + [(h_ref, h), (d_ref, d)]
    loads = [pltpu.make_async_copy(src, dst, in_sem.at[t]) for t, (src, dst) in enumerate(loads)]
    homes = [pltpu.make_async_copy(src, home.at[t], home_sem.at[t]) for t, src in enumerate((y_ref, x_ref))]
    backs = [pltpu.make_async_copy(home.at[t], dst, home_sem.at[t]) for t, dst in enumerate((y_out, x_out))]
    for copy in loads + homes:
        copy.start()

    rows_of = lambda t: pl.ds(t * GRAD_ROWS, GRAD_ROWS)
    blocks = [(a, t, g, 0, down_ref) for t in range(n_down)] + [(h, t, d, c, up_ref) for t in range(n_up) for c in range(n_col)]
    turned = (left, right)
    loads[0].wait()
    loads[1].wait()
    arrived = 2
    turn = -1
    for t, (src, row, other, col, out) in enumerate(blocks):
        slot = t % GRAD_SLOTS
        cols = pl.ds(col * GRAD_COLS, GRAD_COLS)
        after = blocks[t + 1] if t + 1 < len(blocks) else None
        need = (1 + n_down if after is None or after[0] is h else t + 2) + (1 if src is h or (after is not None and after[0] is h) else 0)
        need = min(need, len(loads) - 1) + (1 if src is h else 0)
        while arrived < min(need + 1, len(loads)):
            loads[arrived].wait()
            arrived += 1
        if t >= GRAD_SLOTS:
            pltpu.make_async_copy(stage.at[slot], stage.at[slot], out_sem.at[slot]).wait()
        size = GRAD_PART if after is None or t == 0 else GRAD_ROWS
        for p in range(0, GRAD_ROWS, size):
            if t == 0:
                stage[slot, p:p + size] = lax.dot_general(src[:, p:p + size], other[:, cols], (((0,), (0,)), ((), ())), preferred_element_type=F32)
            else:
                stage[slot, p:p + size] = jnp.dot(turned[turn % 2][p:p + size], other[:, cols], preferred_element_type=F32)
            if p + size == GRAD_ROWS and after is not None and (after[0] is not src or after[1] != row):
                turn += 1
                turned[turn % 2][...] = after[0][:, rows_of(after[1])].T
            for q in range(p, p + size, GRAD_PART):
                pltpu.make_async_copy(stage.at[slot, pl.ds(q, GRAD_PART)], out.at[pl.ds(row * GRAD_ROWS + q, GRAD_PART), cols], out_sem.at[slot]).start()
        if t == 1:
            for copy, back in zip(homes, backs):
                copy.wait()
                back.start()
    for slot in range(GRAD_SLOTS):
        pltpu.make_async_copy(stage.at[slot], stage.at[slot], out_sem.at[slot]).wait()
    for copy in backs:
        copy.wait()


def weight_grads(h, d, a, g, y, dx):
    tokens, d_model = h.shape
    d_ff = d.shape[1]
    n_in = 3 + d_ff // GRAD_ROWS
    hbm = pl.BlockSpec(memory_space=pl.ANY)
    dma = lambda *shape: pltpu.SemaphoreType.DMA(shape)
    like = lambda v: pltpu.VMEM(v.shape, v.dtype)
    return pl.pallas_call(
        weight_grad_kernel,
        name='weight_grads',
        out_shape=(jax.ShapeDtypeStruct((d_model, d_ff), F32), jax.ShapeDtypeStruct((d_ff, d_model), F32),
                   jax.ShapeDtypeStruct(y.shape, BF16), jax.ShapeDtypeStruct(y.shape, BF16)),
        in_specs=[hbm] * 6,
        out_specs=(hbm,) * 4,
        scratch_shapes=[like(h), like(d), like(a), like(g), pltpu.VMEM((2,) + y.shape, BF16), pltpu.VMEM((GRAD_ROWS, tokens), BF16), pltpu.VMEM((GRAD_ROWS, tokens), BF16),
                        pltpu.VMEM((GRAD_SLOTS, GRAD_ROWS, GRAD_COLS), F32),
                        dma(n_in), dma(2), dma(GRAD_SLOTS)],
        compiler_params=pltpu.CompilerParams(vmem_limit_bytes=60 * 1024 * 1024),
    )(h, d, a, g, y, dx)


def solution(mesh):
    tok_spec = P(('data', 'stage', 'inner'))
    up_spec = P(None, ('data', 'stage'), None, 'inner')
    down_spec = P(None, ('data', 'stage'), 'inner', None)

    def device_step(x_loc, g_loc, w_up, w_down):
        y, dx, h, g, a, d = run_pipeline(x_loc, g_loc, w_up[0, 0], w_down[0, 0])
        flat = lambda v: v.reshape(-1, v.shape[-1])
        dw_up, dw_down, y, dx = weight_grads(flat(h), flat(d), flat(a), flat(g), y, dx)
        return y, dx, dw_up[None, None], dw_down[None, None]

    return jax.shard_map(device_step, mesh=mesh, in_specs=(tok_spec, tok_spec, up_spec, down_spec), out_specs=(tok_spec, tok_spec, up_spec, down_spec), check_vma=False)
```

```python
import functools

import jax
import jax.numpy as jnp
from jax import lax
from jax.experimental import pallas as pl
from jax.experimental.pallas import tpu as pltpu
from jax.sharding import PartitionSpec as P

F32 = jnp.float32
BF16 = jnp.bfloat16
MESH = pl.DeviceIdType.MESH

STAGES = 4
INNER = 2
UNITS = 8
SLOTS = 3
DIRECT = 3
BLK = 512
TILE = 256
FWD, BWD = 0, 1
NT = (((1,), (1,)), ((), ()))

F1, M1, B1, T1, F2, B2, T2, FR, BR, HB, SW, PR, YL, WA, WB, XS, XW, XR = range(1, 19)
PLAN = (
    ((WA, 0, 1), (F1, 0, 2), (WB, 0, 1), (XS, 0, 1), (F2, 0, 2), (F1, 2, 2), (FR, 0, 2), (F2, 2, 2),
     (FR, 2, 1), (F1, 4, 2), (FR, 3, 1), (F2, 4, 2), (FR, 4, 2), (F1, 6, 2), (F2, 6, 1), (F2, 7, 1),
     (FR, 6, 2), (XW, 0, 1), (SW, 0, 1), (B1, 0, 2), (B2, 0, 1), (B2, 1, 1), (B1, 2, 1), (B2, 2, 1),
     (B1, 3, 1), (BR, 0, 2), (B2, 3, 1), (BR, 2, 1), (B1, 4, 2), (B2, 4, 2), (BR, 3, 1), (B1, 6, 2),
     (B2, 6, 1), (BR, 4, 1), (B2, 7, 1), (BR, 5, 3)),
    ((WA, 0, 1), (WB, 0, 1), (XS, 0, 1), (F1, 0, 2), (F2, 0, 1), (F2, 1, 1), (FR, 0, 2), (F1, 2, 2),
     (F2, 2, 1), (F2, 3, 1), (FR, 2, 1), (F1, 4, 2), (FR, 3, 1), (F2, 4, 1), (F2, 5, 1), (FR, 4, 2),
     (F1, 6, 2), (F2, 6, 2), (FR, 6, 2), (XW, 0, 1), (SW, 0, 1), (HB, 0, 2), (B1, 0, 2), (B2, 0, 1),
     (HB, 2, 1), (B2, 1, 1), (BR, 0, 1), (B1, 2, 2), (BR, 1, 1), (B2, 2, 2), (BR, 2, 2), (B1, 4, 1),
     (B1, 5, 1), (B2, 4, 2), (B1, 6, 1), (B2, 6, 1), (BR, 4, 1), (B1, 7, 1), (BR, 5, 1), (B2, 7, 1),
     (BR, 6, 2)),
    ((XR, 0, 1), (WA, 0, 1), (WB, 0, 1), (XS, 0, 1), (XW, 0, 1), (F1, 0, 1), (F2, 0, 1), (F1, 1, 1),
     (FR, 0, 1), (F2, 1, 1), (FR, 1, 1), (F1, 2, 1), (F2, 2, 1), (F1, 3, 1), (F2, 3, 1), (FR, 2, 1),
     (F1, 4, 1), (F1, 5, 1), (FR, 3, 1), (F2, 4, 2), (T1, 0, 2), (F1, 6, 2), (T2, 0, 2), (FR, 4, 1),
     (F2, 6, 2), (FR, 5, 1), (T1, 2, 2), (FR, 6, 2), (T2, 2, 2), (BR, 3, 1), (T1, 4, 2), (T2, 4, 2),
     (T1, 6, 2), (BR, 4, 1), (T2, 6, 2), (BR, 5, 3)),
    ((WB, 0, 1), (XS, 0, 1), (XR, 0, 1), (PR, 0, 1), (XW, 0, 1), (M1, 0, 1), (B2, 0, 1), (BR, 0, 1),
     (M1, 1, 1), (B2, 1, 1), (BR, 1, 1), (M1, 2, 2), (B2, 2, 1), (B2, 3, 1), (BR, 2, 2), (M1, 4, 1),
     (B2, 4, 1), (M1, 5, 1), (B2, 5, 1), (BR, 4, 1), (M1, 6, 2), (BR, 5, 1), (B2, 6, 2), (BR, 6, 2),
     (YL, 0, 1), (F2, 0, 2), (FR, 0, 2), (F2, 2, 1), (F2, 3, 2), (FR, 2, 1), (F2, 5, 1), (FR, 3, 2),
     (F2, 6, 1), (FR, 5, 1), (F2, 7, 1), (FR, 6, 2)),
)


PACK = 1024
UP_GROUP = 8
TURN = 5
TURN_GROUP = 4
DOWN_GROUP = 1


def plan_words():
    rows = [[op + 32 * unit + 256 * (count - 1) for op, unit, count in row] for row in PLAN]
    steps = -(-max(len(row) for row in rows) // 3) * 3
    rows = [row + [0] * (steps - len(row)) for row in rows]
    return [[row[t] + PACK * row[t + 1] + PACK * PACK * row[t + 2] for t in range(0, steps, 3)] for row in rows]


def gelu_pair(pre_act):
    root = pre_act * 0.7071067811865476
    normal_cdf = 0.5 * (1.0 + lax.erf(root))
    normal_pdf = jnp.exp2(root * root * -1.4426950408889634) * 0.3989422804014327
    return pre_act * normal_cdf, normal_cdf + pre_act * normal_pdf


def wait_bytes(ref, sem):
    pltpu.make_async_copy(ref, ref, sem).wait()


def pipeline_kernel(x_ref, g_ref, w1_ref, w2_ref,
                    y_out, dx_out, h_out, g_out, a_out, d_out,
                    wa, wb, flow, act, slope, part, recv, send, home, direct,
                    flow_sem, recv_sem, part_send, flow_send, home_send, home_sem, in_send, relay_sem, relay_send,
                    direct_sem, direct_send, cross_send, stage_sem, w_sem, out_sem):
    stage = lax.axis_index('stage')
    side = lax.axis_index('inner')
    other = 1 - side
    rows, d_model = flow.shape[3:]
    tok, d_ff = act.shape[2:]
    n_blk = d_model // BLK

    def peer(s, i):
        return {'stage': s, 'inner': i}

    load_a = pltpu.make_async_copy(w1_ref, wa, w_sem.at[0])
    load_b = pltpu.make_async_copy(w2_ref, wb, w_sem.at[1])

    def unit_of(k):
        return jnp.where(stage < 2, stage + (7 - 2 * stage) * k, 2 * stage - 2 + k)

    staged = (send.at[BWD, pl.ds(UNITS - 2, 2)], send.at[BWD, pl.ds(UNITS - 4, 2)])
    stagings = [pltpu.make_async_copy(src, dst, stage_sem.at[kind]) for kind, (src, dst) in enumerate(zip((x_ref, g_ref), staged))]
    for kind, target in ((FWD, 0), (BWD, STAGES - 1)):
        stagings[kind].start()

        @pl.when(stage == target)
        def _():
            for k in range(2):
                pltpu.make_async_copy((x_ref, g_ref)[kind].at[k], flow.at[kind, unit_of(k), side], flow_sem.at[kind, unit_of(k)]).start()

    @pl.when(stage < STAGES - 1)
    def _():
        load_a.start()
    load_b.start()

    @pl.when(stage == STAGES - 1)
    def _():
        load_a.start()

    barrier = pltpu.get_barrier_semaphore()
    for s in range(STAGES):
        for i in range(INNER):
            @pl.when(jnp.logical_or(stage != s, side != i))
            def _():
                pl.semaphore_signal(barrier, inc=1, device_id=peer(s, i), device_id_type=MESH)
    pl.semaphore_wait(barrier, STAGES * INNER - 1)

    def home_of(u):
        return jnp.where(u < 2, u, jnp.where(u > 5, 7 - u, (u + 2) // 2))

    def slot_of(u):
        return jnp.where(u < 2, 0, jnp.where(u > 5, 1, lax.rem(u, 2)))

    def hand_in(kind, target, k, lane):
        u = unit_of(k)
        src = staged[kind]
        if lane == 0:
            @pl.when(stage != target)
            def _():
                pltpu.make_async_remote_copy(src.at[k], flow.at[kind, u, side], in_send.at[kind], flow_sem.at[kind, u],
                                             device_id=peer(target, side), device_id_type=MESH).start()
        else:
            pltpu.make_async_remote_copy(src.at[k], flow.at[kind, u, side], in_send.at[kind], flow_sem.at[kind, u],
                                         device_id=peer(target, other), device_id_type=MESH).start()

    def relay(k):
        return pltpu.make_async_remote_copy(staged[FWD].at[k], home.at[FWD, k], in_send.at[FWD], relay_sem.at[k],
                                            device_id=peer(stage, other), device_id_type=MESH)

    def relayed(k):
        u = unit_of(k)
        return pltpu.make_async_remote_copy(home.at[FWD, k], flow.at[FWD, u, other], relay_send.at[k], flow_sem.at[FWD, u],
                                            device_id=peer(0, side), device_id_type=MESH)

    stagings[FWD].wait()
    for k in range(2):
        hand_in(FWD, 0, k, 0)

        if k == 0:
            @pl.when(stage < 2)
            def _():
                hand_in(FWD, 0, k, 1)

        @pl.when(stage == 2)
        def _():
            relay(k).start()
    plan = plan_words()
    words = [jnp.where(stage == 0, a, jnp.where(stage == 1, b, jnp.where(stage == 2, c, d))) for a, b, c, d in zip(*plan)]

    def keep(ref, out, u, lane):
        pltpu.make_async_copy(ref, out.at[u], out_sem.at[lane]).start()

    def blocks(width, group, fn):
        def body(t, carry):
            fn([pl.ds(pl.multiple_of((t * group + k) * BLK, BLK), BLK) for k in range(group)])
            return carry
        lax.fori_loop(0, width // BLK // group, body, 0)

    def arrived(kind, u):
        taken = (stage == 1) & (kind == BWD) & (u < DIRECT)

        @pl.when(jnp.logical_not(taken))
        def _():
            wait_bytes(flow.at[kind, u], flow_sem.at[kind, u])

        @pl.when(taken)
        def _():
            wait_bytes(flow.at[kind, u, other], flow_sem.at[kind, u])

    def both_arrived(kind, u, v):
        arrived(kind, u)

        @pl.when(v != u)
        def _():
            arrived(kind, v)

    def pair(ref, kind, u, v):
        width = ref.shape[-1]
        return jnp.concatenate([ref[kind, u].reshape(tok, width), ref[kind, v].reshape(tok, width)], axis=0)

    def kept(u, v, fn):
        fn(u)

        @pl.when(v != u)
        def _():
            fn(v)

    def up_product(u, v, last):
        both_arrived(FWD, u, v)

        def fn(slices):
            lhs = pair(flow, FWD, u, v)
            for sl in slices:
                z = jnp.dot(lhs, wa[:, sl], preferred_element_type=F32)
                value, grad = gelu_pair(z)
                value = value.astype(BF16)
                if last:
                    act[BWD, u, :, sl] = (slope[u, :, sl] * grad[:tok]).astype(BF16)
                    act[BWD, v, :, sl] = (slope[v, :, sl] * grad[tok:]).astype(BF16)
                else:
                    slope[u, :, sl] = grad[:tok]
                    slope[v, :, sl] = grad[tok:]
                act[FWD, u, :, sl] = value[:tok]
                act[FWD, v, :, sl] = value[tok:]
        blocks(d_ff, UP_GROUP, fn)

        def out(w):
            keep(flow.at[FWD, w], h_out, w, 0)
            keep(act.at[FWD, w], a_out, w, 2)
            if last:
                keep(act.at[BWD, w], d_out, w, 3)
        kept(u, v, out)

    def across(lhs, ref, sl):
        cut = ref.shape[1] * TURN // 8
        total = lax.dot_general(lhs[:, :cut], ref[sl, :cut], NT, preferred_element_type=F32)
        for k in range(cut, ref.shape[1], TILE):
            turned = [ref[pl.ds(sl.start + q, TILE), k:k + TILE].T for q in range(0, BLK, TILE)]
            total += jnp.dot(lhs[:, k:k + TILE], jnp.concatenate(turned, axis=1), preferred_element_type=F32)
        return total

    def back_product(u, v, swapped):
        both_arrived(BWD, u, v)

        def fn(slices):
            lhs = pair(flow, BWD, u, v)
            for sl in slices:
                if swapped:
                    e = jnp.dot(lhs, wa[:, sl], preferred_element_type=F32)
                else:
                    e = across(lhs, wb, sl)
                act[BWD, u, :, sl] = (e[:tok] * slope[u, :, sl]).astype(BF16)
                act[BWD, v, :, sl] = (e[tok:] * slope[v, :, sl]).astype(BF16)
        blocks(d_ff, UP_GROUP if swapped else TURN_GROUP, fn)

        def out(w):
            keep(flow.at[BWD, w], g_out, w, 1)
            keep(act.at[BWD, w], d_out, w, 3)
        kept(u, v, out)

    def part_copy(kind, u, j):
        slot = lax.rem(u, SLOTS)
        return pltpu.make_async_remote_copy(part.at[kind, slot, j, other], recv.at[kind, u, j], part_send.at[kind, slot],
                                            recv_sem.at[kind, u, j], device_id=peer(stage, other), device_id_type=MESH)

    def direct_copy(u, j, half):
        slot = lax.rem(u, SLOTS)
        if half is side:
            return pltpu.make_async_remote_copy(part.at[BWD, slot, j, side], direct.at[u, j], direct_send.at[slot],
                                                direct_sem.at[0, u, j], device_id=peer(stage - 1, side), device_id_type=MESH)
        return pltpu.make_async_remote_copy(part.at[BWD, slot, j, other], recv.at[FWD, u, j], part_send.at[BWD, slot],
                                            direct_sem.at[1, u, j], device_id=peer(stage - 1, other), device_id_type=MESH)

    def take_direct(first, count):
        def body(i, carry):
            u = first + i
            for j in range(n_blk):
                sl = pl.ds(j * BLK, BLK)
                wait_bytes(direct.at[u, j], direct_sem.at[0, u, j])
                wait_bytes(recv.at[FWD, u, j], direct_sem.at[1, u, j])
                flow[BWD, u, side, :, sl] = (direct[u, j] + recv[FWD, u, j]).astype(BF16)
                pltpu.make_async_remote_copy(flow.at[BWD, u, side, :, sl], flow.at[BWD, u, side, :, sl], cross_send.at[0],
                                             flow_sem.at[BWD, u], device_id=peer(stage, other), device_id_type=MESH).start()
            return carry
        lax.fori_loop(0, count, body, 0)

    def down_product(kind, u, v, straight):
        def free(w):
            @pl.when(w >= SLOTS)
            def _():
                wait_bytes(recv.at[kind, w - SLOTS], part_send.at[kind, lax.rem(w, SLOTS)])

            if not straight:
                @pl.when((w >= SLOTS) & (w < SLOTS + DIRECT))
                def _():
                    wait_bytes(direct.at[w - SLOTS], direct_send.at[lax.rem(w, SLOTS)])
        kept(u, v, free)

        def body(t, carry):
            lhs = pair(act, kind, u, v)
            for k in range(DOWN_GROUP):
                j = t * DOWN_GROUP + k
                sl = pl.ds(pl.multiple_of(j * BLK, BLK), BLK)
                if straight:
                    p = jnp.dot(lhs, wb[:, sl], preferred_element_type=F32)
                else:
                    p = across(lhs, wa, sl)
                p = p.reshape(2, INNER, rows, BLK)
                part[kind, lax.rem(u, SLOTS), j] = p[0]
                part[kind, lax.rem(v, SLOTS), j] = p[1]

            def go(w):
                if straight:
                    for k in range(DOWN_GROUP):
                        part_copy(kind, w, t * DOWN_GROUP + k).start()
                    return

                @pl.when(w >= DIRECT)
                def _():
                    for k in range(DOWN_GROUP):
                        part_copy(kind, w, t * DOWN_GROUP + k).start()

                @pl.when(w < DIRECT)
                def _():
                    for k in range(DOWN_GROUP):
                        j = t * DOWN_GROUP + k
                        sl = pl.ds(pl.multiple_of(j * BLK, BLK), BLK)
                        part[BWD, lax.rem(w, SLOTS), j, side] += flow[BWD, w, side, :, sl].astype(F32)
                    for k in range(DOWN_GROUP):
                        for half in (other, side):
                            direct_copy(w, t * DOWN_GROUP + k, half).start()
            kept(u, v, go)
            return carry
        lax.fori_loop(0, n_blk // DOWN_GROUP, body, 0)

    def hand_on(kind, first, count):
        target = stage + 1 if kind == FWD else stage - 1
        inside = stage < STAGES - 1 if kind == FWD else stage > 0
        out = STAGES - 1 if kind == FWD else 0

        def body(i, carry):
            u = first + i
            slot = lax.rem(u, SLOTS)
            for j in range(n_blk):
                sl = pl.ds(j * BLK, BLK)
                wait_bytes(recv.at[kind, u, j], recv_sem.at[kind, u, j])
                total = flow[kind, u, side, :, sl].astype(F32) + (part[kind, slot, j, side] + recv[kind, u, j])
                send[kind, u, :, sl] = total.astype(BF16)

                @pl.when(inside)
                def _():
                    for half in (other, side):
                        pltpu.make_async_remote_copy(send.at[kind, u, :, sl], flow.at[kind, u, side, :, sl], flow_send.at[kind],
                                                     flow_sem.at[kind, u], device_id=peer(target, half), device_id_type=MESH).start()

            @pl.when(jnp.logical_and(jnp.logical_not(inside), home_of(u) != out))
            def _():
                pltpu.make_async_remote_copy(send.at[kind, u], home.at[kind, slot_of(u)], home_send.at[kind],
                                             home_sem.at[kind, slot_of(u)], device_id=peer(home_of(u), side), device_id_type=MESH).start()
            return carry
        lax.fori_loop(0, count, body, 0)

    def swap_weights():
        n_i = d_model // TILE

        def body(t, carry):
            i = pl.multiple_of(lax.rem(t, n_i) * TILE, TILE)
            j = pl.multiple_of(lax.div(t, n_i) * TILE, TILE)
            up = wa[pl.ds(i, TILE), pl.ds(j, TILE)]
            down = wb[pl.ds(j, TILE), pl.ds(i, TILE)]
            wa[pl.ds(i, TILE), pl.ds(j, TILE)] = down.T
            wb[pl.ds(j, TILE), pl.ds(i, TILE)] = up.T
            return carry
        lax.fori_loop(0, n_i * (d_ff // TILE), body, 0)

    def prepare_last():
        half = UNITS // 2

        def quarter(q, carry):
            for i in range(half):
                arrived(BWD, q * half + i)
                keep(flow.at[BWD, q * half + i], g_out, q * half + i, 1)
            units = pl.ds(q * half, half)

            def fn(slices):
                lhs = flow[BWD, units].reshape(half * tok, d_model)
                for sl in slices:
                    e = lax.dot_general(lhs, wb[sl, :], NT, preferred_element_type=F32)
                    slope[units, :, sl] = e.reshape(half, tok, BLK)
            blocks(d_ff, 1, fn)
            return carry
        lax.fori_loop(0, 2, quarter, 0)
        load_a.wait()
        n_i = d_model // TILE

        def body(t, carry):
            i = pl.multiple_of(lax.rem(t, n_i) * TILE, TILE)
            j = pl.multiple_of(lax.div(t, n_i) * TILE, TILE)
            wb[pl.ds(j, TILE), pl.ds(i, TILE)] = wa[pl.ds(i, TILE), pl.ds(j, TILE)].T
            return carry
        lax.fori_loop(0, n_i * (d_ff // TILE), body, 0)

    def step(t, carry):
        group, place = lax.div(t, 3), lax.rem(t, 3)
        word = words[0]
        for i, w in enumerate(words[1:], 1):
            word = jnp.where(group == i, w, word)
        code = lax.rem(lax.div(word, jnp.where(place == 0, 1, jnp.where(place == 1, PACK, PACK * PACK))), PACK)
        op = lax.rem(code, 32)
        u = lax.rem(lax.div(code, 32), UNITS)
        count = lax.div(code, 256) + 1

        def on(want):
            return pl.when(op == want)

        v = jnp.minimum(u + count - 1, UNITS - 1)

        @pl.when(op <= T1)
        def _():
            @on(F1)
            def _():
                up_product(u, v, False)

            @on(M1)
            def _():
                up_product(u, v, True)

            @on(B1)
            def _():
                back_product(u, v, True)

            @on(T1)
            def _():
                back_product(u, v, False)

        @pl.when((op > T1) & (op <= T2))
        def _():
            @pl.when(op < T2)
            def _():
                down_product(jnp.where(op == F2, FWD, BWD), u, v, True)

            @on(T2)
            def _():
                down_product(BWD, u, v, False)

        @pl.when((op > T2) & (op <= HB))
        def _():
            @on(FR)
            def _():
                hand_on(FWD, u, count)

            @on(BR)
            def _():
                hand_on(BWD, u, count)

            @on(HB)
            def _():
                take_direct(u, count)

        @pl.when(op > HB)
        def _():
            @on(SW)
            def _():
                swap_weights()

            @on(PR)
            def _():
                prepare_last()

            @on(YL)
            def _():
                load_b.start()
                load_b.wait()

            @on(WA)
            def _():
                load_a.wait()

            @on(WB)
            def _():
                load_b.wait()

            @on(XS)
            def _():
                @pl.when(stage == STAGES - 1)
                def _():
                    for k in range(2):
                        relay(k).start()

                @pl.when(stage < 2)
                def _():
                    hand_in(FWD, 0, 1, 1)
                stagings[BWD].wait()
                for k in range(2):
                    for lane in range(2):
                        hand_in(BWD, STAGES - 1, k, lane)

            @on(XR)
            def _():
                for k in range(2):
                    wait_bytes(home.at[FWD, k], relay_sem.at[k])
                    relayed(k).start()

            @on(XW)
            def _():
                for kind, target in ((FWD, 0), (BWD, STAGES - 1)):
                    @pl.when(stage != target)
                    def _():
                        wait_bytes(send.at[BWD, pl.ds(UNITS - 4, 4)], in_send.at[kind])

                    @pl.when(stage == target)
                    def _():
                        wait_bytes(staged[kind], in_send.at[kind])

                @pl.when(stage > 1)
                def _():
                    for k in range(2):
                        relayed(k).wait_send()
        return carry
    lengths = [len(row) for row in PLAN]
    lax.fori_loop(0, jnp.where(stage == 0, lengths[0], jnp.where(stage == 1, lengths[1], jnp.where(stage == 2, lengths[2], lengths[3]))), step, 0)

    for kind, here, out in ((FWD, STAGES - 1, y_out), (BWD, 0, dx_out)):
        for k in range(2):
            @pl.when(stage == here)
            def _():
                pltpu.make_async_copy(send.at[kind, unit_of(k)], out.at[k], out_sem.at[4 + kind]).start()

            @pl.when(stage != here)
            def _():
                wait_bytes(home.at[kind, k], home_sem.at[kind, k])
                pltpu.make_async_copy(home.at[kind, k], out.at[k], out_sem.at[4 + kind]).start()

    for kind in (FWD, BWD):
        for u in range(UNITS - SLOTS, UNITS):
            wait_bytes(recv.at[kind, u], part_send.at[kind, u % SLOTS])
    for kind, last in ((FWD, STAGES - 1), (BWD, 0)):
        @pl.when((stage != last) & jnp.logical_not((stage == 2) & (kind == BWD)))
        def _():
            wait_bytes(flow.at[kind], flow_send.at[kind])

        @pl.when(stage == last)
        def _():
            wait_bytes(send.at[kind, pl.ds(0, UNITS - 2)], home_send.at[kind])

    @pl.when(stage == 2)
    def _():
        wait_bytes(flow.at[BWD, pl.ds(0, UNITS - DIRECT)], flow_send.at[BWD])

    @pl.when(stage == 1)
    def _():
        wait_bytes(flow.at[BWD, pl.ds(0, DIRECT), 0], cross_send.at[0])
    for lane, (ref, out) in enumerate(((flow.at[FWD], h_out), (flow.at[BWD], g_out), (act.at[FWD], a_out), (act.at[BWD], d_out),
                                       (home.at[FWD], y_out), (home.at[BWD], dx_out))):
        pltpu.make_async_copy(ref, out, out_sem.at[lane]).wait()


def run_pipeline(x_loc, g_loc, w_one, w_two):
    rows, d_model = x_loc.shape[1:]
    d_ff = w_one.shape[1]
    n_blk = d_model // BLK
    tok = INNER * rows
    hbm = pl.BlockSpec(memory_space=pl.ANY)
    out = lambda *shape: jax.ShapeDtypeStruct(shape, BF16)
    dma = lambda *shape: pltpu.SemaphoreType.DMA(shape)
    return pl.pallas_call(
        pipeline_kernel,
        name='pipeline',
        out_shape=(out(*x_loc.shape), out(*x_loc.shape), out(UNITS, INNER, rows, d_model), out(UNITS, INNER, rows, d_model),
                   out(UNITS, tok, d_ff), out(UNITS, tok, d_ff)),
        in_specs=[hbm] * 4,
        out_specs=(hbm,) * 6,
        scratch_shapes=[
            pltpu.VMEM((d_model, d_ff), BF16),
            pltpu.VMEM((d_ff, d_model), BF16),
            pltpu.VMEM((2, UNITS, INNER, rows, d_model), BF16),
            pltpu.VMEM((2, UNITS, tok, d_ff), BF16),
            pltpu.VMEM((UNITS, tok, d_ff), F32),
            pltpu.VMEM((2, SLOTS, n_blk, INNER, rows, BLK), F32),
            pltpu.VMEM((2, UNITS, n_blk, rows, BLK), F32),
            pltpu.VMEM((2, UNITS, rows, d_model), BF16),
            pltpu.VMEM((2, 2, rows, d_model), BF16),
            pltpu.VMEM((DIRECT, n_blk, rows, BLK), F32),
            dma(2, UNITS), dma(2, UNITS, n_blk), dma(2, SLOTS), dma(2), dma(2), dma(2, 2), dma(2), dma(2), dma(2),
            dma(2, DIRECT, n_blk), dma(SLOTS), dma(1), dma(2), dma(2), dma(6),
        ],
        compiler_params=pltpu.CompilerParams(collective_id=0, has_side_effects=True, vmem_limit_bytes=67043328),
    )(x_loc, g_loc, w_one, w_two)


GRAD_ROWS, GRAD_COLS, GRAD_PART, GRAD_SLOTS = 1024, 2048, 256, 4


def weight_grad_kernel(h_ref, d_ref, a_ref, g_ref, y_ref, x_ref, up_ref, down_ref, y_out, x_out,
                       h, d, a, g, home, left, right, stage, in_sem, home_sem, out_sem):
    d_model, d_ff = h.shape[1], d.shape[1]
    n_down, n_up, n_col = d_ff // GRAD_ROWS, d_model // GRAD_ROWS, d_ff // GRAD_COLS

    pieces = [a.at[:, pl.ds(t * GRAD_ROWS, GRAD_ROWS)] for t in range(n_down)]
    loads = [(g_ref, g)] + [(a_ref.at[:, pl.ds(t * GRAD_ROWS, GRAD_ROWS)], piece) for t, piece in enumerate(pieces)] + [(h_ref, h), (d_ref, d)]
    loads = [pltpu.make_async_copy(src, dst, in_sem.at[t]) for t, (src, dst) in enumerate(loads)]
    homes = [pltpu.make_async_copy(src, home.at[t], home_sem.at[t]) for t, src in enumerate((y_ref, x_ref))]
    backs = [pltpu.make_async_copy(home.at[t], dst, home_sem.at[t]) for t, dst in enumerate((y_out, x_out))]
    for copy in loads + homes:
        copy.start()

    rows_of = lambda t: pl.ds(t * GRAD_ROWS, GRAD_ROWS)
    blocks = [(a, t, g, 0, down_ref) for t in range(n_down)] + [(h, t, d, c, up_ref) for t in range(n_up) for c in range(n_col)]
    turned = (left, right)
    loads[0].wait()
    loads[1].wait()
    arrived = 2
    turn = -1
    for t, (src, row, other, col, out) in enumerate(blocks):
        slot = t % GRAD_SLOTS
        cols = pl.ds(col * GRAD_COLS, GRAD_COLS)
        after = blocks[t + 1] if t + 1 < len(blocks) else None
        need = (1 + n_down if after is None or after[0] is h else t + 2) + (1 if src is h or (after is not None and after[0] is h) else 0)
        need = min(need, len(loads) - 1) + (1 if src is h else 0)
        while arrived < min(need + 1, len(loads)):
            loads[arrived].wait()
            arrived += 1
        if t >= GRAD_SLOTS:
            pltpu.make_async_copy(stage.at[slot], stage.at[slot], out_sem.at[slot]).wait()
        size = GRAD_PART if after is None or t == 0 else GRAD_ROWS
        for p in range(0, GRAD_ROWS, size):
            if t == 0:
                stage[slot, p:p + size] = lax.dot_general(src[:, p:p + size], other[:, cols], (((0,), (0,)), ((), ())), preferred_element_type=F32)
            else:
                stage[slot, p:p + size] = jnp.dot(turned[turn % 2][p:p + size], other[:, cols], preferred_element_type=F32)
            if p + size == GRAD_ROWS and after is not None and (after[0] is not src or after[1] != row):
                turn += 1
                turned[turn % 2][...] = after[0][:, rows_of(after[1])].T
            for q in range(p, p + size, GRAD_PART):
                pltpu.make_async_copy(stage.at[slot, pl.ds(q, GRAD_PART)], out.at[pl.ds(row * GRAD_ROWS + q, GRAD_PART), cols], out_sem.at[slot]).start()
        if t == 1:
            for copy, back in zip(homes, backs):
                copy.wait()
                back.start()
    for slot in range(GRAD_SLOTS):
        pltpu.make_async_copy(stage.at[slot], stage.at[slot], out_sem.at[slot]).wait()
    for copy in backs:
        copy.wait()


def weight_grads(h, d, a, g, y, dx):
    tokens, d_model = h.shape
    d_ff = d.shape[1]
    n_in = 3 + d_ff // GRAD_ROWS
    hbm = pl.BlockSpec(memory_space=pl.ANY)
    dma = lambda *shape: pltpu.SemaphoreType.DMA(shape)
    like = lambda v: pltpu.VMEM(v.shape, v.dtype)
    return pl.pallas_call(
        weight_grad_kernel,
        name='weight_grads',
        out_shape=(jax.ShapeDtypeStruct((d_model, d_ff), F32), jax.ShapeDtypeStruct((d_ff, d_model), F32),
                   jax.ShapeDtypeStruct(y.shape, BF16), jax.ShapeDtypeStruct(y.shape, BF16)),
        in_specs=[hbm] * 6,
        out_specs=(hbm,) * 4,
        scratch_shapes=[like(h), like(d), like(a), like(g), pltpu.VMEM((2,) + y.shape, BF16), pltpu.VMEM((GRAD_ROWS, tokens), BF16), pltpu.VMEM((GRAD_ROWS, tokens), BF16),
                        pltpu.VMEM((GRAD_SLOTS, GRAD_ROWS, GRAD_COLS), F32),
                        dma(n_in), dma(2), dma(GRAD_SLOTS)],
        compiler_params=pltpu.CompilerParams(vmem_limit_bytes=60 * 1024 * 1024),
    )(h, d, a, g, y, dx)


def solution(mesh):
    tok_spec = P(('data', 'stage', 'inner'))
    up_spec = P(None, ('data', 'stage'), None, 'inner')
    down_spec = P(None, ('data', 'stage'), 'inner', None)

    def device_step(x_loc, g_loc, w_up, w_down):
        y, dx, h, g, a, d = run_pipeline(x_loc, g_loc, w_up[0, 0], w_down[0, 0])
        flat = lambda v: v.reshape(-1, v.shape[-1])
        dw_up, dw_down, y, dx = weight_grads(flat(h), flat(d), flat(a), flat(g), y, dx)
        return y, dx, dw_up[None, None], dw_down[None, None]

    return jax.shard_map(device_step, mesh=mesh, in_specs=(tok_spec, tok_spec, up_spec, down_spec), out_specs=(tok_spec, tok_spec, up_spec, down_spec), check_vma=False)
```
